32 devices in a mesh: pb: 4 (over y, x), neg: 8 (over z, core).
Axes of the slice: x: 2, y: 2, z: 4, core: 2. Of those that a mesh axis runs over, the one named last changes fastest.
Arguments:
- hidden: bfloat16 [4, 32, 128, 1024], P('pb', 'neg'), may hold values from -6 to 6
- lengths: int32 [4, 32], P('pb', 'neg'), may hold values from 32 to 128
- teacher: float32 [4, 32], P('pb', 'neg'), may hold values from -8 to 8
- norm_gain: float32 [1024], replicated, may hold values from 0.1 to 1.9
- final_gain: float32 [1024], replicated, may hold values from 0.1 to 1.9
- score_vector: float32 [1024], replicated, may hold values from -0.1875 to 0.1875
- query_weight: bfloat16 [1024, 1024], P(('pb', 'neg')), may hold values from -0.1875 to 0.1875
- key_matrix: bfloat16 [1024, 512], P(('pb', 'neg')), may hold values from -0.1875 to 0.1875
- value_matrix: bfloat16 [1024, 512], P(('pb', 'neg')), may hold values from -0.1875 to 0.1875
- out_weight: bfloat16 [1024, 1024], P(None, ('pb', 'neg')), may hold values from -0.1875 to 0.1875
Outputs:
- scores: float32 [4, 32], P('pb', 'neg')
- loss: float32 [], replicated
- grad_hidden: bfloat16 [4, 32, 128, 1024], P('pb', 'neg')
- grad_query: float32 [1024, 1024], P(('pb', 'neg'))
- grad_key: float32 [1024, 512], P(('pb', 'neg'))
- grad_value: float32 [1024, 512], P(('pb', 'neg'))
- grad_out: float32 [1024, 1024], P(None, ('pb', 'neg'))
The draws below stay inside these ranges and needn't reach their ends.
Inputs may be any that keep to these rules, and one draw needn't show every extreme that they name: `lengths`: the number of real tokens of the pair; its other positions out of 128 are padding.
All inputs are finite; a program needn't handle non-finite values.
Results may differ from the reference program's by a relative error of at most 0.013.
Values may be sent and summed in bfloat16 or wider, within the bound.
A program may use at most 64 MiB of HBM per device.

```python
import jax
import jax.numpy as jnp
from jax import lax

HIDDEN_WIDTH = 1024
HQ = 8
KEY_VALUE_HEADS = 4
HEAD_WIDTH = 128
SEQ = 128
PAIR_DEV = 4
QUERIES = 4
LIST = 32


def place_ends(array, key, smallest, largest):
    shape = array.shape
    index_at = [jax.random.randint(jax.random.fold_in(key, axis), (), 0, shape[axis]) for axis in range(len(shape))]
    array = array.at[tuple(index_at)].set(smallest)
    longest = shape.index(max(shape))
    index_at[longest] = (index_at[longest] + 1) % shape[longest]
    return array.at[tuple(index_at)].set(largest)


def levels(own_key, extent, cuts, least, high):
    loudness = 1.0
    for position, shards_of in cuts:
        heights = jax.random.uniform(jax.random.fold_in(jax.random.fold_in(own_key, 6), position), (shards_of,), jnp.float32, least / len(cuts), high / len(cuts))
        loudness = loudness * jnp.repeat(jnp.exp(heights), extent[position] // shards_of).reshape((-1,) + (1,) * (len(extent) - 1 - position))
    return loudness


def bell_draw(rng, dims, scale, bound, split=(), kind=jnp.bfloat16):
    array = jax.random.normal(rng, dims, jnp.float32) * scale
    if len(split) > 0:
        array = levels(rng, dims, split, -0.22, 0.18) * array
    return jnp.clip(array, min=-bound, max=bound).astype(kind)


def setup_inputs(seed: int = 0) -> dict:
    keys = jax.random.split(jax.random.key(seed), 11)
    hidden = bell_draw(keys[0], (QUERIES, LIST, SEQ, HIDDEN_WIDTH), 1.0, 6.0, ((0, 4), (1, 8)))
    lengths = place_ends(jax.random.randint(keys[1], (QUERIES, LIST), SEQ // 4, SEQ + 1), jax.random.fold_in(keys[1], 1), SEQ // 4, SEQ).astype(jnp.int32)
    teacher = bell_draw(keys[2], (QUERIES, LIST), 2.0, 8.0, ((0, 4), (1, 8)), jnp.float32)
    norm_gain = jnp.clip(1.0 + 0.18 * jax.random.normal(keys[3], (HIDDEN_WIDTH,), jnp.float32), 0.1, 1.9)
    final_gain = jnp.clip(1.0 + 0.18 * jax.random.normal(keys[4], (HIDDEN_WIDTH,), jnp.float32), 0.1, 1.9)
    score_vector = bell_draw(keys[5], (HIDDEN_WIDTH,), HIDDEN_WIDTH ** -0.5, 0.1875, (), jnp.float32)
    query_weight = bell_draw(keys[6], (HIDDEN_WIDTH, HQ * HEAD_WIDTH), HIDDEN_WIDTH ** -0.5, 0.1875, ((0, 32),))
    key_matrix = bell_draw(keys[7], (HIDDEN_WIDTH, KEY_VALUE_HEADS * HEAD_WIDTH), HIDDEN_WIDTH ** -0.5, 0.1875, ((0, 32),))
    value_matrix = bell_draw(keys[8], (HIDDEN_WIDTH, KEY_VALUE_HEADS * HEAD_WIDTH), HIDDEN_WIDTH ** -0.5, 0.1875, ((0, 32),))
    out_weight = bell_draw(keys[9], (HQ * HEAD_WIDTH, HIDDEN_WIDTH), (HQ * HEAD_WIDTH) ** -0.5, 0.1875, ((1, 32),))
    return dict(hidden=hidden, lengths=lengths, teacher=teacher, norm_gain=norm_gain, final_gain=final_gain, score_vector=score_vector, query_weight=query_weight, key_matrix=key_matrix, value_matrix=value_matrix, out_weight=out_weight)


EPSILON = 1e-06
ROPE_BASE = 1000000.0
TEACHER_TEMP = 2.0
GRAD_SCALE = 512.0

def rope_tables(seq_len, head_size):
    half = head_size // 2
    freqs = ROPE_BASE ** (-(jnp.arange(half, dtype=jnp.float32) * 2.0) / head_size)
    angles = jnp.arange(seq_len, dtype=jnp.float32)[:, None] * freqs[None, :]
    angles = jnp.concatenate([angles, angles], axis=1)
    return (jnp.cos(angles), jnp.sin(angles))

def rotate_half(vector):
    half = vector.shape[-1] // 2
    return jnp.concatenate([-vector[..., half:], vector[..., :half]], axis=-1)

def unrotate_half(vector):
    half = vector.shape[-1] // 2
    return jnp.concatenate([vector[..., half:], -vector[..., :half]], axis=-1)

def forward_pairs(tokens_in, lengths_here, norm_gain, final_gain, score_vector, query_weight, key_matrix, value_matrix, out_weight):
    pair_count, seq_len, model_width = tokens_in.shape
    head_count = query_weight.shape[1] // HEAD_WIDTH
    group_count = key_matrix.shape[1] // HEAD_WIDTH
    group_size = head_count // group_count
    inputs_wide = tokens_in.astype(jnp.float32)
    inv_rms = lax.rsqrt(lax.optimization_barrier(jnp.mean(inputs_wide * inputs_wide, axis=-1, keepdims=True)) + EPSILON)
    normed = (inputs_wide * inv_rms * norm_gain).astype(jnp.bfloat16)
    flat_rows = normed.reshape(pair_count * seq_len, model_width)
    key_proj = jnp.dot(flat_rows, key_matrix, preferred_element_type=jnp.float32).reshape(pair_count, seq_len, group_count, HEAD_WIDTH)
    value_proj = jnp.dot(flat_rows, value_matrix, preferred_element_type=jnp.float32).reshape(pair_count, seq_len, group_count, HEAD_WIDTH)
    positions = jnp.arange(seq_len, dtype=jnp.int32)
    last_index = (lengths_here - 1).astype(jnp.int32)
    onehot = (positions[None, :] == last_index[:, None]).astype(jnp.float32)
    normed_last = jnp.take_along_axis(normed, last_index[:, None, None], axis=1)[:, 0]
    query_proj = jnp.dot(normed_last, query_weight, preferred_element_type=jnp.float32).reshape(pair_count, head_count, HEAD_WIDTH)
    query_scale = lax.rsqrt(lax.optimization_barrier(jnp.mean(query_proj * query_proj, axis=-1, keepdims=True)) + EPSILON)
    query_unit = query_proj * query_scale
    key_scale = lax.rsqrt(lax.optimization_barrier(jnp.mean(key_proj * key_proj, axis=-1, keepdims=True)) + EPSILON)
    key_unit = key_proj * key_scale
    cos_table, sin_table = rope_tables(seq_len, HEAD_WIDTH)
    cos_query = jnp.dot(onehot, cos_table, precision=lax.Precision.HIGHEST)
    sin_query = jnp.dot(onehot, sin_table, precision=lax.Precision.HIGHEST)
    query_rot = (query_unit * cos_query[:, None, :] + rotate_half(query_unit) * sin_query[:, None, :]).astype(jnp.bfloat16)
    key_rot = (key_unit * cos_table[None, :, None, :] + rotate_half(key_unit) * sin_table[None, :, None, :]).astype(jnp.bfloat16)
    value_cast = value_proj.astype(jnp.bfloat16)
    grouped = query_rot.reshape(pair_count, group_count, group_size, HEAD_WIDTH)
    logits = jnp.einsum('pkgd,pskd->pkgs', grouped.astype(jnp.float32), key_rot.astype(jnp.float32)) * HEAD_WIDTH ** (-0.5)
    visible = (positions[None, :] <= last_index[:, None])[:, None, None, :]
    expos = jnp.where(visible, jnp.exp(logits), 0.0)
    attention_weights = expos / lax.optimization_barrier(jnp.sum(expos, axis=-1, keepdims=True))
    probs_cast = attention_weights.astype(jnp.bfloat16)
    context = jnp.einsum('pkgs,pskd->pkgd', probs_cast.astype(jnp.float32), value_cast.astype(jnp.float32))
    context = context.astype(jnp.bfloat16).reshape(pair_count, head_count * HEAD_WIDTH)
    attended = jnp.dot(context, out_weight, preferred_element_type=jnp.float32)
    residual = jnp.take_along_axis(inputs_wide, last_index[:, None, None], axis=1)[:, 0] + attended
    out_scale = lax.rsqrt(lax.optimization_barrier(jnp.mean(residual * residual, axis=-1, keepdims=True)) + EPSILON)
    out_unit = residual * out_scale
    scores_here = lax.optimization_barrier(jnp.sum(out_unit * final_gain * score_vector, axis=-1))
    stored = (tokens_in, onehot, inv_rms, normed, normed_last, query_unit, query_scale, key_unit, key_scale, cos_query, sin_query, cos_table, sin_table, query_rot, key_rot, value_cast, attention_weights, probs_cast, context, out_unit, out_scale)
    return (scores_here, stored)

def backward_pairs(stored, grad_score, norm_gain, final_gain, score_vector, query_weight, key_matrix, value_matrix, out_weight):
    tokens_in, onehot, inv_rms, normed, normed_last, query_unit, query_scale, key_unit, key_scale, cos_query, sin_query, cos_table, sin_table, query_rot, key_rot, value_cast, attention_weights, probs_cast, context, out_unit, out_scale = stored
    pair_count, seq_len, model_width = tokens_in.shape
    head_count = query_weight.shape[1] // HEAD_WIDTH
    group_count = key_matrix.shape[1] // HEAD_WIDTH
    group_size = head_count // group_count
    grad_unit = grad_score[:, None] * score_vector * final_gain
    grad_resid = out_scale * (grad_unit - out_unit * lax.optimization_barrier(jnp.mean(grad_unit * out_unit, axis=-1, keepdims=True)))
    grad_resid_cast = grad_resid.astype(jnp.bfloat16)
    grad_out = jnp.dot(context.T, grad_resid_cast, preferred_element_type=jnp.float32)
    grad_context = jnp.dot(grad_resid_cast, out_weight.T, preferred_element_type=jnp.float32).astype(jnp.bfloat16)
    grad_context = grad_context.reshape(pair_count, group_count, group_size, HEAD_WIDTH).astype(jnp.float32)
    grad_probs = jnp.einsum('pkgd,pskd->pkgs', grad_context, value_cast.astype(jnp.float32))
    grad_vals = jnp.einsum('pkgs,pkgd->pskd', probs_cast.astype(jnp.float32), grad_context)
    spread = lax.optimization_barrier(jnp.sum(attention_weights * grad_probs, axis=-1, keepdims=True))
    logit_gradient = (attention_weights * (grad_probs - spread)).astype(jnp.bfloat16).astype(jnp.float32)
    grouped = query_rot.reshape(pair_count, group_count, group_size, HEAD_WIDTH).astype(jnp.float32)
    rotated_query_gradient = jnp.einsum('pkgs,pskd->pkgd', logit_gradient, key_rot.astype(jnp.float32)) * HEAD_WIDTH ** (-0.5)
    rotated_query_gradient = rotated_query_gradient.reshape(pair_count, head_count, HEAD_WIDTH)
    grad_krot = jnp.einsum('pkgs,pkgd->pskd', logit_gradient, grouped) * HEAD_WIDTH ** (-0.5)
    grad_qunit = rotated_query_gradient * cos_query[:, None, :] + unrotate_half(rotated_query_gradient * sin_query[:, None, :])
    grad_kunit = grad_krot * cos_table[None, :, None, :] + unrotate_half(grad_krot * sin_table[None, :, None, :])
    grad_qproj = query_scale * (grad_qunit - query_unit * lax.optimization_barrier(jnp.mean(grad_qunit * query_unit, axis=-1, keepdims=True)))
    grad_kproj = key_scale * (grad_kunit - key_unit * lax.optimization_barrier(jnp.mean(grad_kunit * key_unit, axis=-1, keepdims=True)))
    grad_q_cast = grad_qproj.reshape(pair_count, head_count * HEAD_WIDTH).astype(jnp.bfloat16)
    grad_k_cast = grad_kproj.reshape(pair_count * seq_len, group_count * HEAD_WIDTH).astype(jnp.bfloat16)
    grad_v_cast = grad_vals.reshape(pair_count * seq_len, group_count * HEAD_WIDTH).astype(jnp.bfloat16)
    flat_rows = normed.reshape(pair_count * seq_len, model_width)
    grad_query = jnp.dot(normed_last.T, grad_q_cast, preferred_element_type=jnp.float32)
    grad_key = jnp.dot(flat_rows.T, grad_k_cast, preferred_element_type=jnp.float32)
    grad_value = jnp.dot(flat_rows.T, grad_v_cast, preferred_element_type=jnp.float32)
    grad_normed = jnp.dot(grad_k_cast, key_matrix.T, preferred_element_type=jnp.float32)
    grad_normed = grad_normed + jnp.dot(grad_v_cast, value_matrix.T, preferred_element_type=jnp.float32)
    grad_normed = grad_normed.reshape(pair_count, seq_len, model_width)
    grad_last = jnp.dot(grad_q_cast, query_weight.T, preferred_element_type=jnp.float32)
    grad_normed = grad_normed + onehot[:, :, None] * grad_last[:, None, :]
    inputs_wide = tokens_in.astype(jnp.float32)
    grad_scaled = grad_normed * norm_gain
    grad_input = inv_rms * grad_scaled - inputs_wide * inv_rms * inv_rms * inv_rms * lax.optimization_barrier(jnp.mean(grad_scaled * inputs_wide, axis=-1, keepdims=True))
    grad_input = grad_input + onehot[:, :, None] * grad_resid[:, None, :]
    return (grad_input.astype(jnp.bfloat16), (grad_query, grad_key, grad_value, grad_out))

def reference(hidden, lengths, teacher, norm_gain, final_gain, score_vector, query_weight, key_matrix, value_matrix, out_weight):
    query_count, list_len, seq_len, model_width = hidden.shape
    block_count = list_len // PAIR_DEV
    weights = (query_weight, key_matrix, value_matrix, out_weight)

    def score_block(carry, item):
        block_tokens, block_lengths = item
        block_scores, stored = forward_pairs(block_tokens, block_lengths, norm_gain, final_gain, score_vector, weights[0], weights[1], weights[2], weights[3])
        return (carry, block_scores)
    score_rows = []
    for query_pos in range(query_count):
        blocks_in = hidden[query_pos].reshape(block_count, PAIR_DEV, seq_len, model_width)
        blocks_len = lengths[query_pos].reshape(block_count, PAIR_DEV)
        carry_out, block_scores = lax.scan(score_block, jnp.zeros((), jnp.float32), (blocks_in, blocks_len))
        score_rows.append(block_scores.reshape(list_len))
    scores = jnp.stack(score_rows, axis=0)
    scaled = teacher / TEACHER_TEMP
    expo_s = jnp.exp(scores)
    expo_t = jnp.exp(scaled)
    total_s = lax.optimization_barrier(jnp.sum(expo_s, axis=-1, keepdims=True))
    total_t = lax.optimization_barrier(jnp.sum(expo_t, axis=-1, keepdims=True))
    prob_s = expo_s / total_s
    prob_t = expo_t / total_t
    loss = jnp.sum(prob_t * (scaled - jnp.log(total_t) - (scores - jnp.log(total_s))))
    grad_score = GRAD_SCALE * (prob_s - prob_t)

    def grad_block(carry, item):
        block_tokens, block_lengths, block_grad = item
        block_scores, stored = forward_pairs(block_tokens, block_lengths, norm_gain, final_gain, score_vector, weights[0], weights[1], weights[2], weights[3])
        grad_input, grads = backward_pairs(stored, block_grad, norm_gain, final_gain, score_vector, weights[0], weights[1], weights[2], weights[3])
        summed = (carry[0] + grads[0], carry[1] + grads[1], carry[2] + grads[2], carry[3] + grads[3])
        return (summed, grad_input)
    total_blocks = query_count * block_count
    start = (jnp.zeros(query_weight.shape, jnp.float32), jnp.zeros(key_matrix.shape, jnp.float32), jnp.zeros(value_matrix.shape, jnp.float32), jnp.zeros(out_weight.shape, jnp.float32))
    items = (hidden.reshape(total_blocks, PAIR_DEV, seq_len, model_width), lengths.reshape(total_blocks, PAIR_DEV), grad_score.reshape(total_blocks, PAIR_DEV))
    grads, grad_blocks = lax.scan(grad_block, start, items)
    grad_hidden = grad_blocks.reshape(query_count, list_len, seq_len, model_width)
    return (scores, loss, grad_hidden, grads[0], grads[1], grads[2], grads[3])
```

```python
import functools

import jax
import jax.numpy as jnp
import numpy as np
from jax import lax
from jax.experimental import pallas as pl
from jax.experimental.pallas import tpu as pltpu
from jax.sharding import PartitionSpec as P

HEAD_WIDTH = 128
MESH_ID = pl.DeviceIdType.MESH

EPSILON = 1e-06
ROPE_BASE = 1000000.0
TEACHER_TEMP = 2.0
GRAD_SCALE = 512.0


def rope_tables(seq_len, head_size):
    half = head_size // 2
    freqs = ROPE_BASE ** (-(jnp.arange(half, dtype=jnp.float32) * 2.0) / head_size)
    angles = jnp.arange(seq_len, dtype=jnp.float32)[:, None] * freqs[None, :]
    angles = jnp.concatenate([angles, angles], axis=1)
    return (jnp.cos(angles), jnp.sin(angles))


def signed_tables(seq_len, head_size):
    half = head_size // 2
    freqs = ROPE_BASE ** (-(np.arange(half) * 2.0) / head_size)
    angles = np.arange(seq_len)[:, None] * freqs[None, :]
    cos = np.concatenate([np.cos(angles)] * 2, axis=1)
    sin = np.concatenate([-np.sin(angles), np.sin(angles)], axis=1)
    return (jnp.asarray(cos, jnp.float32), jnp.asarray(sin, jnp.float32))


def rotate_half(vector):
    half = vector.shape[-1] // 2
    return jnp.concatenate([-vector[..., half:], vector[..., :half]], axis=-1)


def unrotate_half(vector):
    half = vector.shape[-1] // 2
    return jnp.concatenate([vector[..., half:], -vector[..., :half]], axis=-1)


def forward_pairs(
    tokens_in,
    lengths_here,
    norm_gain,
    final_gain,
    score_vector,
    query_weight,
    key_matrix,
    value_matrix,
    out_weight,
):
    pair_count, seq_len, model_width = tokens_in.shape
    head_count = query_weight.shape[1] // HEAD_WIDTH
    group_count = key_matrix.shape[1] // HEAD_WIDTH
    group_size = head_count // group_count
    inputs_wide = tokens_in.astype(jnp.float32)
    inv_rms = lax.rsqrt(jnp.mean(inputs_wide * inputs_wide, axis=-1, keepdims=True) + EPSILON)
    normed = (inputs_wide * inv_rms * norm_gain).astype(jnp.bfloat16)
    flat_rows = normed.reshape(pair_count * seq_len, model_width)
    key_proj = jnp.dot(flat_rows, key_matrix, preferred_element_type=jnp.float32).reshape(
        pair_count, seq_len, group_count, HEAD_WIDTH
    )
    value_proj = jnp.dot(flat_rows, value_matrix, preferred_element_type=jnp.float32).reshape(
        pair_count, seq_len, group_count, HEAD_WIDTH
    )
    positions = jnp.arange(seq_len, dtype=jnp.int32)
    last_index = lengths_here - 1
    onehot = (positions[None, :] == last_index[:, None]).astype(jnp.float32)
    normed_last = jnp.take_along_axis(normed, last_index[:, None, None], axis=1)[:, 0]
    query_proj = jnp.dot(normed_last, query_weight, preferred_element_type=jnp.float32).reshape(
        pair_count, head_count, HEAD_WIDTH
    )
    query_scale = lax.rsqrt(jnp.mean(query_proj * query_proj, axis=-1, keepdims=True) + EPSILON)
    query_unit = query_proj * query_scale
    key_scale = lax.rsqrt(jnp.mean(key_proj * key_proj, axis=-1, keepdims=True) + EPSILON)
    key_unit = key_proj * key_scale
    cos_table, sin_table = rope_tables(seq_len, HEAD_WIDTH)
    cos_query = jnp.dot(onehot, cos_table, precision=lax.Precision.HIGHEST)
    sin_query = jnp.dot(onehot, sin_table, precision=lax.Precision.HIGHEST)
    query_rot = (
        query_unit * cos_query[:, None, :] + rotate_half(query_unit) * sin_query[:, None, :]
    ).astype(jnp.bfloat16)
    key_rot = (
        key_unit * cos_table[None, :, None, :] + rotate_half(key_unit) * sin_table[None, :, None, :]
    ).astype(jnp.bfloat16)
    value_cast = value_proj.astype(jnp.bfloat16)
    grouped = query_rot.reshape(pair_count, group_count, group_size, HEAD_WIDTH)
    logits = jnp.einsum(
        "pkgd,pskd->pkgs", grouped, key_rot, preferred_element_type=jnp.float32
    ) * HEAD_WIDTH ** (-0.5)
    visible = (positions[None, :] <= last_index[:, None])[:, None, None, :]
    expos = jnp.where(visible, jnp.exp(logits), 0.0)
    attention_weights = expos / jnp.sum(expos, axis=-1, keepdims=True)
    probs_cast = attention_weights.astype(jnp.bfloat16)
    context = jnp.einsum(
        "pkgs,pskd->pkgd", probs_cast, value_cast, preferred_element_type=jnp.float32
    )
    context = context.astype(jnp.bfloat16).reshape(pair_count, head_count * HEAD_WIDTH)
    attended = jnp.dot(context, out_weight, preferred_element_type=jnp.float32)
    residual = jnp.take_along_axis(inputs_wide, last_index[:, None, None], axis=1)[:, 0] + attended
    out_scale = lax.rsqrt(jnp.mean(residual * residual, axis=-1, keepdims=True) + EPSILON)
    out_unit = residual * out_scale
    scores_here = jnp.sum(out_unit * final_gain * score_vector, axis=-1)
    stored = (
        tokens_in,
        onehot,
        inv_rms,
        normed,
        normed_last,
        query_unit,
        query_scale,
        key_unit,
        key_scale,
        cos_query,
        sin_query,
        cos_table,
        sin_table,
        query_rot,
        key_rot,
        value_cast,
        attention_weights,
        probs_cast,
        context,
        out_unit,
        out_scale,
    )
    return (scores_here, stored)


def backward_pairs(
    stored,
    grad_score,
    norm_gain,
    final_gain,
    score_vector,
    query_weight,
    key_matrix,
    value_matrix,
    out_weight,
):
    (
        tokens_in,
        onehot,
        inv_rms,
        normed,
        normed_last,
        query_unit,
        query_scale,
        key_unit,
        key_scale,
        cos_query,
        sin_query,
        cos_table,
        sin_table,
        query_rot,
        key_rot,
        value_cast,
        attention_weights,
        probs_cast,
        context,
        out_unit,
        out_scale,
    ) = stored
    pair_count, seq_len, model_width = tokens_in.shape
    head_count = query_weight.shape[1] // HEAD_WIDTH
    group_count = key_matrix.shape[1] // HEAD_WIDTH
    group_size = head_count // group_count
    grad_unit = grad_score[:, None] * score_vector * final_gain
    grad_resid = out_scale * (
        grad_unit - out_unit * jnp.mean(grad_unit * out_unit, axis=-1, keepdims=True)
    )
    grad_resid_cast = grad_resid.astype(jnp.bfloat16)
    grad_context = jnp.dot(
        grad_resid_cast, out_weight.T, preferred_element_type=jnp.float32
    ).astype(jnp.bfloat16)
    grad_context = grad_context.reshape(pair_count, group_count, group_size, HEAD_WIDTH)
    grad_probs = jnp.einsum(
        "pkgd,pskd->pkgs", grad_context, value_cast, preferred_element_type=jnp.float32
    )
    grad_vals = jnp.einsum(
        "pkgs,pkgd->pskd", probs_cast, grad_context, preferred_element_type=jnp.float32
    )
    spread = jnp.sum(attention_weights * grad_probs, axis=-1, keepdims=True)
    logit_gradient = (attention_weights * (grad_probs - spread)).astype(jnp.bfloat16)
    grouped = query_rot.reshape(pair_count, group_count, group_size, HEAD_WIDTH)
    rotated_query_gradient = jnp.einsum(
        "pkgs,pskd->pkgd", logit_gradient, key_rot, preferred_element_type=jnp.float32
    ) * HEAD_WIDTH ** (-0.5)
    rotated_query_gradient = rotated_query_gradient.reshape(pair_count, head_count, HEAD_WIDTH)
    grad_krot = jnp.einsum(
        "pkgs,pkgd->pskd", logit_gradient, grouped, preferred_element_type=jnp.float32
    ) * HEAD_WIDTH ** (-0.5)
    grad_qunit = rotated_query_gradient * cos_query[:, None, :] + unrotate_half(
        rotated_query_gradient * sin_query[:, None, :]
    )
    grad_kunit = grad_krot * cos_table[None, :, None, :] + unrotate_half(
        grad_krot * sin_table[None, :, None, :]
    )
    grad_qproj = query_scale * (
        grad_qunit - query_unit * jnp.mean(grad_qunit * query_unit, axis=-1, keepdims=True)
    )
    grad_kproj = key_scale * (
        grad_kunit - key_unit * jnp.mean(grad_kunit * key_unit, axis=-1, keepdims=True)
    )
    grad_q_cast = grad_qproj.reshape(pair_count, head_count * HEAD_WIDTH).astype(jnp.bfloat16)
    grad_k_cast = grad_kproj.reshape(pair_count * seq_len, group_count * HEAD_WIDTH).astype(
        jnp.bfloat16
    )
    grad_v_cast = grad_vals.reshape(pair_count * seq_len, group_count * HEAD_WIDTH).astype(
        jnp.bfloat16
    )
    flat_rows = normed.reshape(pair_count * seq_len, model_width)
    last_rows = jnp.concatenate([normed_last, grad_resid_cast, grad_q_cast, context], axis=1)
    grad_kv = jnp.dot(
        flat_rows.T,
        jnp.concatenate([grad_k_cast, grad_v_cast], axis=1),
        preferred_element_type=jnp.float32,
    )
    grad_normed = jnp.dot(grad_k_cast, key_matrix.T, preferred_element_type=jnp.float32)
    grad_normed = grad_normed + jnp.dot(
        grad_v_cast, value_matrix.T, preferred_element_type=jnp.float32
    )
    grad_normed = grad_normed.reshape(pair_count, seq_len, model_width)
    grad_last = jnp.dot(grad_q_cast, query_weight.T, preferred_element_type=jnp.float32)
    grad_normed = grad_normed + onehot[:, :, None] * grad_last[:, None, :]
    inputs_wide = tokens_in.astype(jnp.float32)
    grad_scaled = grad_normed * norm_gain
    grad_input = inv_rms * grad_scaled - inputs_wide * inv_rms * inv_rms * inv_rms * jnp.mean(
        grad_scaled * inputs_wide, axis=-1, keepdims=True
    )
    grad_input = grad_input + onehot[:, :, None] * grad_resid[:, None, :]
    return (grad_input.astype(jnp.bfloat16), last_rows, grad_kv)


class Place:
    def __init__(self):
        self.pb_count = lax.axis_size("pb")
        self.neg_count = lax.axis_size("neg")
        self.line_count = self.neg_count // 2
        self.pb = lax.axis_index("pb")
        neg = lax.axis_index("neg")
        self.line = neg // 2
        self.core = neg % 2
        self.partner = 1 - self.core

    def slot(self, pb, line, core):
        return pb * self.neg_count + line * 2 + core

    def line_peer(self, step):
        return lax.rem(self.line + step, self.line_count)

    def pb_peer(self, step):
        return lax.rem(self.pb + step, self.pb_count)

    def to_line(self, line):
        return (self.pb, line * 2 + self.core)

    def to_pb(self, pb):
        return (pb, self.line * 2 + self.core)

    def to_partner(self):
        return (self.pb, self.line * 2 + self.partner)

    def greet(self):
        barrier = pltpu.get_barrier_semaphore()
        targets = [self.to_line(self.line_peer(k)) for k in range(1, self.line_count)]
        targets += [self.to_pb(self.pb_peer(k)) for k in range(1, self.pb_count)]
        targets += [self.to_partner()]
        for target in targets:
            pl.semaphore_signal(barrier, inc=1, device_id=target, device_id_type=MESH_ID)
        pl.semaphore_wait(barrier, len(targets))


def remote(src, dst, send_sem, recv_sem, target):
    return pltpu.make_async_remote_copy(
        src_ref=src,
        dst_ref=dst,
        send_sem=send_sem,
        recv_sem=recv_sem,
        device_id=target,
        device_id_type=MESH_ID,
    )


def gather_sems(pb_count, neg_count):
    line_count = neg_count // 2
    return [
        pltpu.SemaphoreType.DMA((line_count,)),
        pltpu.SemaphoreType.DMA((line_count,)),
        pltpu.SemaphoreType.DMA((2, line_count)),
        pltpu.SemaphoreType.DMA((2, line_count)),
        pltpu.SemaphoreType.DMA((2, line_count)),
        pltpu.SemaphoreType.DMA((2, line_count)),
        pltpu.SemaphoreType.DMA((pb_count, line_count)),
        pltpu.SemaphoreType.DMA((pb_count, line_count)),
        pltpu.SemaphoreType.DMA,
    ]


class Gather:
    def __init__(self, place, own, full, sems):
        self.place, self.own, self.full = place, own, full
        self.line_send, self.line_recv, self.pb_send, self.pb_recv = sems[:4]
        self.half_send, self.half_recv = sems[4:6]
        self.core_send, self.core_recv, self.local_sem = sems[6:]
        self.sent = []
        across = place.pb + 1 - 2 * (place.pb % 2)
        along = place.pb + 2 - 4 * (place.pb // 2)
        self.near = (across, along)
        self.corner = 3 - place.pb

    def rows(self, pb, line, core):
        size = self.own.shape[0]
        start = self.place.slot(pb, line, core) * size
        return self.full.at[pl.ds(pl.multiple_of(start, size), size)]

    def send(self, src, dst, send_sem, recv_sem, target):
        copy = remote(src, dst, send_sem, recv_sem, target)
        copy.start()
        self.sent.append(copy)

    def spread(self, src, line):
        at = self.place
        dst = self.rows(at.pb, line, at.core)
        for side in range(2):
            self.send(
                src, dst, self.pb_send.at[side, line], self.pb_recv.at[side, line], at.to_pb(self.near[side])
            )
        self.pass_on(src, at.pb, line)

    def pass_on(self, src, pb, line):
        at = self.place
        dst = self.rows(pb, line, at.core)
        self.send(src, dst, self.core_send.at[pb, line], self.core_recv.at[pb, line], at.to_partner())

    def arrive(self, block, recv_sem):
        remote(block, block, self.local_sem, recv_sem, self.place.to_partner()).wait_recv()

    def start(self):
        at = self.place
        mine = self.rows(at.pb, at.line, at.core)
        self.local = pltpu.make_async_copy(self.own, mine, self.local_sem)
        self.local.start()
        for k in range(1, at.line_count):
            line = at.line_peer(k)
            self.send(
                self.own, mine, self.line_send.at[k], self.line_recv.at[at.line], at.to_line(line)
            )
        self.spread(self.own, at.line)

    def middle(self):
        at = self.place
        for k in range(1, at.line_count):
            line = at.line_peer(k)
            block = self.rows(at.pb, line, at.core)
            self.arrive(block, self.line_recv.at[line])
            self.spread(block, line)

    def half(self, block, side):
        size = block.shape[0] // 2
        return block.at[pl.ds(side * size, size)]

    def relay(self):
        at = self.place
        for step in range(at.line_count):
            line = at.line_peer(step)
            for side in range(2):
                block = self.rows(self.near[side], line, at.core)
                self.arrive(block, self.pb_recv.at[side, line])
                part = self.half(block, side)
                self.send(
                    part,
                    part,
                    self.half_send.at[side, line],
                    self.half_recv.at[side, line],
                    at.to_pb(self.near[1 - side]),
                )
                self.pass_on(block, self.near[side], line)

    def finish(self):
        at = self.place
        for step in range(at.line_count):
            line = at.line_peer(step)
            block = self.rows(self.corner, line, at.core)
            for side in range(2):
                self.arrive(self.half(block, side), self.half_recv.at[side, line])
            self.pass_on(block, self.corner, line)
        for pb in range(at.pb_count):
            for line in range(at.line_count):
                self.arrive(self.rows(pb, line, at.partner), self.core_recv.at[pb, line])
        self.local.wait()

    def drain(self):
        for copy in self.sent:
            copy.wait_send()


VMEM_SPEC = pl.BlockSpec(memory_space=pltpu.VMEM)


def mm(left, right, left_dim=1, right_dim=0, precision=None):
    return lax.dot_general(
        left,
        right,
        (((left_dim,), (right_dim,)), ((), ())),
        preferred_element_type=jnp.float32,
        precision=precision,
    )


def lane_mean(array):
    return jnp.mean(array, axis=-1, keepdims=True)


def tile(array, index):
    return array[:, index * HEAD_WIDTH : (index + 1) * HEAD_WIDTH]


class Exchange:
    def __init__(self, at, src, dst, send_sem, recv_sem):
        self.at, self.src, self.dst = at, src, dst
        self.send_sem, self.recv_sem = send_sem, recv_sem

    def start(self):
        at = self.at

        def one(step, carry):
            peer = lax.rem(at.me + step, at.count)
            target = (peer // at.neg_count, lax.rem(peer, at.neg_count))
            remote(
                self.src.at[peer], self.dst.at[at.me], self.send_sem, self.recv_sem, target
            ).start()
            return carry

        lax.fori_loop(1, at.count, one, 0)
        self.dst[at.me] = self.src[at.me]

    def wait(self, sem_of):
        block = self.dst.at[pl.ds(0, self.at.count - 1)]
        copy = remote(block, block, self.send_sem, self.recv_sem, self.at.to_partner())
        getattr(copy, sem_of)()


def step_kernel(
    sizes,
    x,
    lengths,
    teacher,
    norm_gain,
    final_gain,
    score_vector,
    cos_table,
    sin_table,
    own_q,
    own_k,
    own_v,
    own_out,
    scores_out,
    loss_out,
    grad_hidden,
    grad_query,
    grad_key,
    grad_value,
    grad_out,
    own_o,
    full_q,
    full_k,
    full_v,
    full_o,
    normed,
    inv_wide,
    key_unit,
    key_scale,
    key_rot,
    value_cast,
    grad_k,
    grad_v,
    logit_grad,
    probs_ref,
    query_blocks,
    context_blocks,
    last_grad,
    resid_grad,
    context_own,
    context_full,
    late_own,
    late_full,
    early_src,
    early_dst,
    resid_src,
    resid_dst,
    list_src,
    list_dst,
    partial,
    from_core,
    paired,
    from_pb,
    summed,
    from_line,
    early_sems,
    resid_sems,
    list_sems,
    core_send,
    core_recv,
    pb_send,
    pb_recv,
    line_send,
    line_recv,
    any_sem,
    *gather_sem_refs,
):
    pairs, seq, groups, share = sizes
    bf16, f32 = jnp.bfloat16, jnp.float32
    at = Place()
    at.count = at.pb_count * at.neg_count
    at.me = at.slot(at.pb, at.line, at.core)
    model = x.shape[1]
    rows_all = pairs * seq
    per_group = own_q.shape[1] // own_k.shape[1]
    slots = per_group * pairs
    stacked = groups * slots
    kv_width = groups * HEAD_WIDTH

    barrier = pltpu.get_barrier_semaphore()

    def greet(step, carry):
        peer = lax.rem(at.me + step, at.count)
        target = (peer // at.neg_count, lax.rem(peer, at.neg_count))
        pl.semaphore_signal(barrier, inc=1, device_id=target, device_id_type=MESH_ID)
        return carry

    lax.fori_loop(1, at.count, greet, 0)

    each = len(gather_sem_refs) // 6
    gathers = []
    for place_of, (own, full) in enumerate(
        (
            (own_k, full_k),
            (own_v, full_v),
            (own_q, full_q),
            (own_o, full_o),
            (context_own, context_full),
            (late_own, late_full),
        )
    ):
        sems = gather_sem_refs[place_of * each : (place_of + 1) * each]
        gathers.append(Gather(at, own, full, sems))
    gather_k, gather_v, gather_q, gather_o, gather_context, gather_late = gathers

    diagonal = lax.broadcasted_iota(jnp.int32, (share, share), 0) == lax.broadcasted_iota(
        jnp.int32, (share, share), 1
    )
    own_o[...] = mm(diagonal.astype(f32).astype(bf16), own_out[...], 1, 1).astype(bf16)

    pl.semaphore_wait(barrier, at.count - 1)
    gather_k.start()
    gather_v.start()
    gather_q.start()
    gather_o.start()

    def norm_pair(pair, carry):
        rows = pl.ds(pl.multiple_of(pair * seq, seq), seq)
        wide = x[rows, :].astype(f32)
        inv = lax.rsqrt(lane_mean(wide * wide) + EPSILON)
        inv_wide[rows, :] = jnp.broadcast_to(inv, (seq, HEAD_WIDTH))
        normed[rows, :] = (wide * inv * norm_gain[...]).astype(bf16)
        return carry

    lax.fori_loop(0, pairs, norm_pair, 0)

    row8 = lax.broadcasted_iota(jnp.int32, (slots, 1), 0)
    pair8 = lax.rem(row8, pairs)
    upper8 = row8 < pairs
    last8 = jnp.zeros((slots, 1), jnp.int32)
    teacher8 = jnp.zeros((slots, 1), f32)
    for pair in range(pairs):
        last8 = jnp.where(pair8 == pair, lengths[0, pair] - 1, last8)
        teacher8 = jnp.where(pair8 == pair, teacher[0, pair], teacher8)
    place8 = pair8 * seq + last8
    column8 = lax.broadcasted_iota(jnp.int32, (slots, rows_all), 1)
    onehot8 = (column8 == place8).astype(f32).astype(bf16)
    visible8 = (column8 >= pair8 * seq) & (column8 <= place8)
    visible = jnp.concatenate([visible8.astype(f32)] * groups, axis=0) > 0.5
    position8 = (lax.broadcasted_iota(jnp.int32, (slots, seq), 1) == last8).astype(f32)

    gather_k.middle()
    gather_v.middle()
    gather_k.relay()

    x_last = mm(onehot8, x[...])
    normed_last = mm(onehot8, normed[...]).astype(bf16)
    cos8 = mm(position8, cos_table[...], precision=lax.Precision.HIGHEST)
    sin8 = mm(position8, sin_table[...], precision=lax.Precision.HIGHEST)
    cos_rows = jnp.concatenate([cos8] * groups, axis=0)
    sin_rows = jnp.concatenate([sin8] * groups, axis=0)

    gather_q.middle()
    gather_v.relay()
    gather_k.finish()

    def key_pair(pair, carry):
        rows = pl.ds(pl.multiple_of(pair * seq, seq), seq)
        proj = mm(normed[rows, :], full_k[...])
        for group in range(groups):
            lanes = slice(group * HEAD_WIDTH, (group + 1) * HEAD_WIDTH)
            part = proj[:, lanes]
            scale = lax.rsqrt(lane_mean(part * part) + EPSILON)
            unit = part * scale
            key_unit[rows, lanes] = unit
            key_scale[rows, lanes] = jnp.broadcast_to(scale, (seq, HEAD_WIDTH))
            turned = unit * cos_table[...] + pltpu.roll(unit, HEAD_WIDTH // 2, 1) * sin_table[...]
            key_rot[rows, lanes] = turned.astype(bf16)
        return carry

    lax.fori_loop(0, pairs, key_pair, 0)

    gather_o.middle()
    gather_q.relay()
    gather_v.finish()

    def value_pair(pair, carry):
        rows = pl.ds(pl.multiple_of(pair * seq, seq), seq)
        value_cast[rows, :] = mm(normed[rows, :], full_v[...]).astype(bf16)
        return carry

    lax.fori_loop(0, pairs, value_pair, 0)

    gather_o.relay()
    gather_q.finish()

    def stack_heads(wide):
        return jnp.concatenate(
            [
                jnp.where(upper8, tile(wide, per_group * group), tile(wide, per_group * group + 1))
                for group in range(groups)
            ],
            axis=0,
        )

    def spread_heads(stack):
        parts = []
        for group in range(groups):
            part = stack[group * slots : (group + 1) * slots]
            parts += [jnp.where(upper8, part, 0.0), jnp.where(upper8, 0.0, part)]
        return jnp.concatenate(parts, axis=1).astype(bf16)

    def diagonal_of(wide):
        return jnp.concatenate(
            [
                wide[group * slots : (group + 1) * slots, group * HEAD_WIDTH : (group + 1) * HEAD_WIDTH]
                for group in range(groups)
            ],
            axis=0,
        )

    def blocks_of(stack):
        rows = []
        for group in range(groups):
            part = stack[group * slots : (group + 1) * slots]
            rows.append(
                jnp.concatenate(
                    [part if other == group else jnp.zeros_like(part) for other in range(groups)],
                    axis=1,
                )
            )
        return jnp.concatenate(rows, axis=0).astype(bf16)

    query_proj = stack_heads(mm(normed_last, full_q[...]))
    query_scale = lax.rsqrt(lane_mean(query_proj * query_proj) + EPSILON)
    query_unit = query_proj * query_scale
    query_rot = query_unit * cos_rows + pltpu.roll(query_unit, HEAD_WIDTH // 2, 1) * sin_rows
    query_wide = blocks_of(query_rot)
    query_blocks[...] = query_wide
    logits = mm(query_wide, key_rot[...], 1, 1) * HEAD_WIDTH ** (-0.5)
    expos = jnp.where(visible, jnp.exp(logits), 0.0)
    attention_weights = expos / jnp.sum(expos, axis=-1, keepdims=True)
    probs = attention_weights.astype(bf16)
    probs_ref[...] = probs
    context = diagonal_of(mm(probs, value_cast[...]))
    context_own[...] = context.astype(bf16)
    context_wide = spread_heads(context)

    lane_block = lax.rem(
        lax.broadcasted_iota(jnp.int32, (slots, model), 1) // share, HEAD_WIDTH // share
    )

    def pack(parts, turn):
        total = jnp.zeros((slots, model), f32)
        for block, part in enumerate(parts):
            shift = ((block - turn) * share) % model
            moved = part if shift == 0 else pltpu.roll(part, shift, 1)
            total = jnp.where(lane_block == block, moved, total)
        return total

    def by_head(wide):
        return [jnp.where(upper8, wide, 0.0), jnp.where(upper8, 0.0, wide)]

    turns = HEAD_WIDTH // share
    pulled = mm(probs, normed[...])
    pulled_parts = [pulled[group * slots : (group + 1) * slots] for group in range(groups)]
    last_parts = by_head(normed_last.astype(f32))
    for turn in range(turns):
        both = jnp.concatenate([pack(pulled_parts, turn), pack(last_parts, turn)], axis=0)
        both = both.astype(bf16)
        for index in range(model // HEAD_WIDTH):
            early_src[index * turns + turn] = tile(both, index)

    gather_o.finish()
    attended = mm(context_wide, full_o[...], 1, 1)
    attended = attended + pltpu.roll(attended, pairs, 0)
    residual = x_last + attended
    out_scale = lax.rsqrt(lane_mean(residual * residual) + EPSILON)
    out_unit = residual * out_scale
    gain = final_gain[...] * score_vector[...]
    score8 = jnp.sum(out_unit * gain, axis=-1, keepdims=True)

    lane8 = lax.broadcasted_iota(jnp.int32, (slots, HEAD_WIDTH), 1)
    listing = jnp.where(lane8 == 0, score8, jnp.where(lane8 == 1, teacher8, 0.0))
    list_src[...] = listing
    me_tile = list_dst.at[at.me]
    list_here, list_there, list_sent = list_sems.at[0], list_sems.at[1], list_sems.at[2]
    neg = lax.axis_index("neg")

    def list_near(step, carry):
        peer = lax.rem(neg + step, at.neg_count)
        remote(list_src, me_tile, list_sent, list_here, (at.pb, peer)).start()
        return carry

    def list_far(step, carry):
        peer = lax.rem(neg + step, at.neg_count)
        for k in range(1, at.pb_count):
            remote(list_src, me_tile, list_sent, list_there, (at.pb_peer(k), peer)).start()
        return carry

    lax.fori_loop(1, at.neg_count, list_near, 0)
    lax.fori_loop(0, at.neg_count, list_far, 0)
    list_dst[at.me] = listing
    early = Exchange(at, early_src, early_dst, early_sems.at[0], early_sems.at[1])
    gather_context.start()
    early.start()

    row_lane = lax.broadcasted_iota(jnp.int32, (slots, HEAD_WIDTH), 0)
    score_row = jnp.sum(jnp.where(row_lane == lane8, score8, 0.0), axis=0, keepdims=True)
    scores_out[...] = score_row[:, :pairs]

    near_block = list_dst.at[pl.ds(0, at.neg_count - 1)]
    remote(near_block, near_block, list_sent, list_here, at.to_partner()).wait_recv()

    real3 = lax.broadcasted_iota(jnp.int32, (at.neg_count, slots, 1), 1) < pairs
    lane3 = lax.broadcasted_iota(jnp.int32, (at.neg_count, slots, HEAD_WIDTH), 2)

    def query_terms(block):
        score = jnp.sum(jnp.where(lane3 == 0, block, 0.0), axis=-1, keepdims=True)
        scaled = jnp.sum(jnp.where(lane3 == 1, block, 0.0), axis=-1, keepdims=True) / TEACHER_TEMP
        total = lambda array: jnp.sum(
            jnp.sum(jnp.where(real3, array, 0.0), axis=0), axis=0, keepdims=True
        )
        expo_t = jnp.exp(scaled)
        return score, scaled, expo_t, total(jnp.exp(score)), total(expo_t), total

    here = list_dst[pl.ds(pl.multiple_of(at.pb * at.neg_count, at.neg_count), at.neg_count)]
    _, _, _, total_s, total_t, _ = query_terms(here)
    grad_score = GRAD_SCALE * (
        jnp.exp(score8) / total_s - jnp.exp(teacher8 / TEACHER_TEMP) / total_t
    )
    grad_unit = grad_score * gain
    grad_resid = out_scale * (grad_unit - out_unit * lane_mean(grad_unit * out_unit))
    resid_grad[...] = grad_resid
    resid_cast = grad_resid.astype(bf16)
    grad_context = stack_heads(mm(resid_cast, full_o[...])).astype(bf16)
    context_blocks[...] = blocks_of(grad_context.astype(f32))
    late_own[0:stacked, :] = grad_context

    resid_parts = by_head(resid_cast.astype(f32))
    for turn in range(turns):
        packed = pack(resid_parts, turn).astype(bf16)
        for index in range(model // HEAD_WIDTH):
            resid_src[index * turns + turn] = tile(packed, index)
    resid = Exchange(at, resid_src, resid_dst, resid_sems.at[0], resid_sems.at[1])
    resid.start()

    grad_probs = mm(context_blocks[...], value_cast[...], 1, 1)
    spread = jnp.sum(attention_weights * grad_probs, axis=-1, keepdims=True)
    logit_gradient = (attention_weights * (grad_probs - spread)).astype(bf16)
    logit_grad[...] = logit_gradient

    def key_back(pair, carry):
        start = pl.multiple_of(pair * seq, seq)
        rows = pl.ds(start, seq)
        turned = mm(logit_grad[:, rows], query_blocks[...], 0, 0) * HEAD_WIDTH ** (-0.5)
        for group in range(groups):
            lanes = slice(group * HEAD_WIDTH, (group + 1) * HEAD_WIDTH)
            part = turned[:, lanes]
            unit = key_unit[rows, lanes]
            back = part * cos_table[...] - pltpu.roll(part, HEAD_WIDTH // 2, 1) * sin_table[...]
            back = key_scale[rows, lanes] * (back - unit * lane_mean(back * unit))
            grad_k[rows, lanes] = back.astype(bf16)
        return carry

    lax.fori_loop(0, pairs, key_back, 0)

    block_rows = model // at.pb_count
    copies = []

    def send(src, dst, send_sem, recv_sem, target):
        copy = remote(src, dst, send_sem, recv_sem, target)
        copy.start()
        copies.append(copy)

    def arrive(block, recv_sem):
        remote(block, block, any_sem, recv_sem, at.to_partner()).wait_recv()

    for k in range(1, at.pb_count + 1):
        pb = at.pb_peer(k % at.pb_count)
        lanes = pl.ds(pl.multiple_of(pb * block_rows, block_rows), block_rows)
        product = mm(normed[:, lanes], grad_k[...], 0, 0)
        partial[pb] = product.astype(bf16).reshape(at.line_count, 2, share, kv_width)
        send(
            partial.at[pb, :, at.partner],
            from_core.at[pb],
            core_send.at[pb],
            core_recv.at[pb],
            at.to_partner(),
        )

    turned_q = diagonal_of(mm(logit_gradient, key_rot[...])) * HEAD_WIDTH ** (-0.5)
    back_q = turned_q * cos_rows - pltpu.roll(turned_q, HEAD_WIDTH // 2, 1) * sin_rows
    back_q = query_scale * (back_q - query_unit * lane_mean(back_q * query_unit))
    grad_q_cast = back_q.astype(bf16)
    late_own[stacked : 2 * stacked, :] = grad_q_cast

    for k in range(1, at.pb_count + 1):
        pb = at.pb_peer(k % at.pb_count)
        arrive(from_core.at[pb], core_recv.at[pb])
        both = partial[pb, :, at.core].astype(f32) + from_core[pb].astype(f32)
        paired[pb] = both.astype(bf16)
        if k < at.pb_count:
            send(paired.at[pb], from_pb.at[at.pb], pb_send.at[k], pb_recv.at[at.pb], at.to_pb(pb))
    gather_late.start()
    gather_context.middle()
    gather_context.relay()

    back_last = mm(spread_heads(grad_q_cast.astype(f32)), full_q[...], 1, 1)
    last_grad[...] = back_last + pltpu.roll(back_last, pairs, 0)

    def value_back(pair, carry):
        start = pl.multiple_of(pair * seq, seq)
        rows = pl.ds(start, seq)
        grad_v[rows, :] = mm(probs_ref[:, rows], context_blocks[...], 0, 0).astype(bf16)
        return carry

    lax.fori_loop(0, pairs, value_back, 0)

    seq_row = lax.broadcasted_iota(jnp.int32, (seq, 1), 0)

    def hidden_back(pair, carry):
        rows = pl.ds(pl.multiple_of(pair * seq, seq), seq)
        total = mm(grad_k[rows, :], full_k[...], 1, 1) + mm(grad_v[rows, :], full_v[...], 1, 1)
        hit = seq_row == lengths[0, pair] - 1
        total = total + jnp.where(hit, last_grad[pl.ds(pair, 1), :], 0.0)
        scaled = total * norm_gain[...]
        wide = x[rows, :].astype(f32)
        inv = inv_wide[rows, 0:1]
        mean = lane_mean(scaled * wide)
        result = inv * scaled - wide * (inv * inv * inv * mean)
        result = result + jnp.where(hit, resid_grad[pl.ds(pair, 1), :], 0.0)
        grad_hidden[rows, :] = result.astype(bf16)
        return carry

    lax.fori_loop(0, pairs // 2, hidden_back, 0)

    for k in range(1, at.pb_count):
        pb = at.pb_peer(k)
        arrive(from_pb.at[pb], pb_recv.at[pb])
    for step in range(1, at.line_count + 1):
        line = at.line_peer(step % at.line_count)
        total = paired[at.pb, line].astype(f32)
        for k in range(1, at.pb_count):
            total = total + from_pb[at.pb_peer(k), line].astype(f32)
        if step < at.line_count:
            summed[line] = total.astype(bf16)
            send(
                summed.at[line],
                from_line.at[at.line],
                line_send.at[line],
                line_recv.at[at.line],
                at.to_line(line),
            )
    gather_late.middle()
    gather_late.relay()
    gather_context.finish()

    lax.fori_loop(pairs // 2, pairs, hidden_back, 0)

    far_block = list_dst.at[pl.ds(0, at.count - at.neg_count)]
    remote(far_block, far_block, list_sent, list_there, at.to_partner()).wait_recv()
    loss = jnp.zeros((1, 1), f32)
    for pb in range(at.pb_count):
        block = list_dst[pb * at.neg_count : (pb + 1) * at.neg_count]
        score, scaled, expo_t, sum_s, sum_t, total = query_terms(block)
        loss = loss + total(expo_t / sum_t * (scaled - jnp.log(sum_t) - (score - jnp.log(sum_s))))
    loss_out[...] = loss

    gather_late.finish()
    early.wait("wait_recv")
    resid.wait("wait_recv")

    def rows_of(full, start, group):
        wide = full[...].astype(f32).reshape(at.count, -1, slots, HEAD_WIDTH)
        return wide[:, start + group].reshape(at.count * slots, HEAD_WIDTH).astype(bf16)

    pulled_rows = rows_of(early_dst, 0, 0)
    last_rows = rows_of(early_dst, 1, 0)
    resid_rows = rows_of(resid_dst, 0, 0)
    for group in range(groups):
        found = mm(pulled_rows, rows_of(late_full, 0, group), 0, 0)
        lanes = slice(group * HEAD_WIDTH, (group + 1) * HEAD_WIDTH)
        grad_value[:, lanes] = found[group * share : (group + 1) * share]
        found = mm(last_rows, rows_of(late_full, groups, group), 0, 0)
        for part in range(per_group):
            head = per_group * group + part
            grad_query[:, head * HEAD_WIDTH : (head + 1) * HEAD_WIDTH] = found[
                part * share : (part + 1) * share
            ]
        found = mm(rows_of(context_full, 0, group), resid_rows, 0, 0)
        for part in range(per_group):
            head = per_group * group + part
            moved = found if part == 0 else pltpu.roll(found, HEAD_WIDTH - part * share, 1)
            grad_out[head * HEAD_WIDTH : (head + 1) * HEAD_WIDTH, :] = moved[:, :share]

    for step in range(1, at.line_count):
        line = at.line_peer(step)
        arrive(from_line.at[line], line_recv.at[line])
    final = paired[at.pb, at.line].astype(f32)
    for k in range(1, at.pb_count):
        final = final + from_pb[at.pb_peer(k), at.line].astype(f32)
    for step in range(1, at.line_count):
        final = final + from_line[at.line_peer(step)].astype(f32)
    grad_key[...] = final

    for gather in gathers:
        gather.drain()
    for copy in copies:
        copy.wait_send()
    early.wait("wait_send")
    resid.wait("wait_send")
    sent_block = list_dst.at[pl.ds(0, at.count - 1)]
    remote(sent_block, sent_block, list_sent, list_here, at.to_partner()).wait_send()


def run_step(operands, sizes, pb_count, neg_count):
    pairs, seq, groups, share = sizes
    x, own_q, own_k = operands[0], operands[8], operands[9]
    model, width, kv_width = x.shape[1], own_q.shape[1], own_k.shape[1]
    rows = pairs * seq
    count = pb_count * neg_count
    line_count = neg_count // 2
    slots = width // kv_width * pairs
    stacked = groups * slots
    bf16, f32 = jnp.bfloat16, jnp.float32
    block = (pb_count, line_count, share, kv_width)
    dma = pltpu.SemaphoreType.DMA
    vmem = pltpu.VMEM
    smem_spec = pl.BlockSpec(memory_space=pltpu.SMEM)
    return pl.pallas_call(
        functools.partial(step_kernel, sizes),
        out_shape=(
            jax.ShapeDtypeStruct((1, pairs), f32),
            jax.ShapeDtypeStruct((1, 1), f32),
            jax.ShapeDtypeStruct((rows, model), bf16),
            jax.ShapeDtypeStruct((share, width), f32),
            jax.ShapeDtypeStruct((share, kv_width), f32),
            jax.ShapeDtypeStruct((share, kv_width), f32),
            jax.ShapeDtypeStruct((width, share), f32),
        ),
        in_specs=[VMEM_SPEC, smem_spec, smem_spec] + [VMEM_SPEC] * 9,
        out_specs=(VMEM_SPEC,) * 7,
        scratch_shapes=[
            vmem((share, width), bf16),
            vmem((model, width), bf16),
            vmem((model, kv_width), bf16),
            vmem((model, kv_width), bf16),
            vmem((model, width), bf16),
            vmem((rows, model), bf16),
            vmem((rows, HEAD_WIDTH), f32),
            vmem((rows, kv_width), f32),
            vmem((rows, kv_width), f32),
            vmem((rows, kv_width), bf16),
            vmem((rows, kv_width), bf16),
            vmem((rows, kv_width), bf16),
            vmem((rows, kv_width), bf16),
            vmem((stacked, rows), bf16),
            vmem((stacked, rows), bf16),
            vmem((stacked, kv_width), bf16),
            vmem((stacked, kv_width), bf16),
            vmem((slots, model), f32),
            vmem((slots, model), f32),
            vmem((stacked, HEAD_WIDTH), bf16),
            vmem((stacked * count, HEAD_WIDTH), bf16),
            vmem((2 * stacked, HEAD_WIDTH), bf16),
            vmem((2 * stacked * count, HEAD_WIDTH), bf16),
            vmem((count, 2 * slots, HEAD_WIDTH), bf16),
            vmem((count, 2 * slots, HEAD_WIDTH), bf16),
            vmem((count, slots, HEAD_WIDTH), bf16),
            vmem((count, slots, HEAD_WIDTH), bf16),
            vmem((slots, HEAD_WIDTH), f32),
            vmem((count, slots, HEAD_WIDTH), f32),
            vmem((pb_count, line_count, 2, share, kv_width), bf16),
            vmem(block, bf16),
            vmem(block, bf16),
            vmem(block, bf16),
            vmem(block[1:], bf16),
            vmem(block[1:], bf16),
            dma((2,)),
            dma((2,)),
            dma((3,)),
            dma((pb_count,)),
            dma((pb_count,)),
            dma((pb_count,)),
            dma((pb_count,)),
            dma((line_count,)),
            dma((line_count,)),
            dma,
        ]
        + gather_sems(pb_count, neg_count) * 6,
        compiler_params=pltpu.CompilerParams(
            collective_id=0, has_side_effects=True, vmem_limit_bytes=60 * 2**20
        ),
    )(*operands)


def shards(
    hidden,
    lengths,
    teacher,
    norm_gain,
    final_gain,
    score_vector,
    query_weight,
    key_matrix,
    value_matrix,
    out_weight,
):
    both = ("pb", "neg")
    width = query_weight.shape[1]
    kv_width = key_matrix.shape[1]
    share, out_share = query_weight.shape[0], out_weight.shape[1]
    pb_count, neg_count = lax.axis_size("pb"), lax.axis_size("neg")
    pair_count, seq_len, model_width = hidden.shape[1:]
    group_count = kv_width // HEAD_WIDTH
    own_kernels = (
        pb_count == 4
        and neg_count % 2 == 0
        and share == out_share
        and share % 32 == 0
        and model_width == share * pb_count * neg_count
        and width == 2 * kv_width
        and pair_count * 2 == 8
        and seq_len == HEAD_WIDTH
        and share * group_count == HEAD_WIDTH
    )
    if own_kernels:
        cos_table, sin_table = signed_tables(seq_len, HEAD_WIDTH)
        scores, loss, grad_rows, grad_query, grad_key, grad_value, grad_out = run_step(
            (
                hidden.reshape(pair_count * seq_len, model_width),
                lengths,
                teacher,
                norm_gain[None],
                final_gain[None],
                score_vector[None],
                cos_table,
                sin_table,
                query_weight,
                key_matrix,
                value_matrix,
                out_weight,
            ),
            (pair_count, seq_len, group_count, share),
            pb_count,
            neg_count,
        )
        return (
            scores,
            loss.reshape(()),
            grad_rows.reshape(hidden.shape),
            grad_query,
            grad_key,
            grad_value,
            grad_out,
        )
    packed = jnp.concatenate([query_weight, key_matrix, value_matrix, out_weight.T], axis=1)
    everything = lax.all_gather(packed, both, axis=0, tiled=True)
    full_query = everything[:, :width]
    full_key = everything[:, width : width + kv_width]
    full_value = everything[:, width + kv_width : width + 2 * kv_width]
    full_out_t = everything[:, width + 2 * kv_width :]
    weights = (full_query, full_key, full_value, full_out_t.T)
    scores_here, stored = forward_pairs(
        hidden[0], lengths[0], norm_gain, final_gain, score_vector, *weights
    )
    listing = jnp.concatenate([scores_here, teacher[0]])[None]
    listed = lax.all_gather(listing, "neg", axis=0, tiled=True)
    all_scores = listed[:, :pair_count]
    all_scaled = listed[:, pair_count:] / TEACHER_TEMP
    my_total_s = jnp.sum(jnp.exp(all_scores))
    expo_t = jnp.exp(all_scaled)
    my_total_t = jnp.sum(expo_t)
    loss_here = jnp.sum(
        expo_t
        / my_total_t
        * (all_scaled - jnp.log(my_total_t) - (all_scores - jnp.log(my_total_s)))
    )
    prob_s = jnp.exp(scores_here) / my_total_s
    prob_t = jnp.exp(teacher[0] / TEACHER_TEMP) / my_total_t
    grad_score = GRAD_SCALE * (prob_s - prob_t)
    grad_input, last_rows, grad_kv = backward_pairs(
        stored, grad_score, norm_gain, final_gain, score_vector, *weights
    )
    grad_kv = grad_kv.astype(jnp.bfloat16)
    reduced = lax.psum_scatter(grad_kv, both, scatter_dimension=0, tiled=True)
    reduced = reduced.astype(jnp.float32)
    rows = lax.all_gather(last_rows, both, axis=0, tiled=True)
    loss_value = lax.psum(loss_here, "pb")
    index = lax.axis_index("pb") * neg_count + lax.axis_index("neg")
    normed_cols = lax.dynamic_slice_in_dim(rows, index * share, share, axis=1)
    resid_cols = lax.dynamic_slice_in_dim(rows, model_width + index * out_share, out_share, axis=1)
    rest = 2 * model_width
    all_q = rows[:, rest : rest + width]
    all_context = rows[:, rest + width :]
    grad_query = jnp.dot(normed_cols.T, all_q, preferred_element_type=jnp.float32)
    grad_out = jnp.dot(all_context.T, resid_cols, preferred_element_type=jnp.float32)
    return (
        scores_here[None],
        loss_value,
        grad_input[None],
        grad_query,
        reduced[:, :kv_width],
        reduced[:, kv_width:],
        grad_out,
    )


def solution(mesh):
    placed = (
        P("pb", "neg", None, None),
        P("pb", "neg"),
        P("pb", "neg"),
        P(),
        P(),
        P(),
        P(("pb", "neg"), None),
        P(("pb", "neg"), None),
        P(("pb", "neg"), None),
        P(None, ("pb", "neg")),
    )
    return jax.shard_map(
        shards,
        mesh=mesh,
        in_specs=placed,
        out_specs=(
            P("pb", "neg"),
            P(),
            P("pb", "neg", None, None),
            P(("pb", "neg"), None),
            P(("pb", "neg"), None),
            P(("pb", "neg"), None),
            P(None, ("pb", "neg")),
        ),
        check_vma=False,
    )
```

```python
import functools

import jax
import jax.numpy as jnp
import numpy as np
from jax import lax
from jax.experimental import pallas as pl
from jax.experimental.pallas import tpu as pltpu
from jax.sharding import PartitionSpec as P

HEAD_WIDTH = 128
MESH_ID = pl.DeviceIdType.MESH

EPSILON = 1e-06
ROPE_BASE = 1000000.0
TEACHER_TEMP = 2.0
GRAD_SCALE = 512.0


def rope_tables(seq_len, head_size):
    half = head_size // 2
    freqs = ROPE_BASE ** (-(jnp.arange(half, dtype=jnp.float32) * 2.0) / head_size)
    angles = jnp.arange(seq_len, dtype=jnp.float32)[:, None] * freqs[None, :]
    angles = jnp.concatenate([angles, angles], axis=1)
    return (jnp.cos(angles), jnp.sin(angles))


def signed_tables(seq_len, head_size):
    half = head_size // 2
    freqs = ROPE_BASE ** (-(np.arange(half) * 2.0) / head_size)
    angles = np.arange(seq_len)[:, None] * freqs[None, :]
    cos = np.concatenate([np.cos(angles)] * 2, axis=1)
    sin = np.concatenate([-np.sin(angles), np.sin(angles)], axis=1)
    return (jnp.asarray(cos, jnp.float32), jnp.asarray(sin, jnp.float32))


def rotate_half(vector):
    half = vector.shape[-1] // 2
    return jnp.concatenate([-vector[..., half:], vector[..., :half]], axis=-1)


def unrotate_half(vector):
    half = vector.shape[-1] // 2
    return jnp.concatenate([vector[..., half:], -vector[..., :half]], axis=-1)


def forward_pairs(
    tokens_in,
    lengths_here,
    norm_gain,
    final_gain,
    score_vector,
    query_weight,
    key_matrix,
    value_matrix,
    out_weight,
):
    pair_count, seq_len, model_width = tokens_in.shape
    head_count = query_weight.shape[1] // HEAD_WIDTH
    group_count = key_matrix.shape[1] // HEAD_WIDTH
    group_size = head_count // group_count
    inputs_wide = tokens_in.astype(jnp.float32)
    inv_rms = lax.rsqrt(jnp.mean(inputs_wide * inputs_wide, axis=-1, keepdims=True) + EPSILON)
    normed = (inputs_wide * inv_rms * norm_gain).astype(jnp.bfloat16)
    flat_rows = normed.reshape(pair_count * seq_len, model_width)
    key_proj = jnp.dot(flat_rows, key_matrix, preferred_element_type=jnp.float32).reshape(
        pair_count, seq_len, group_count, HEAD_WIDTH
    )
    value_proj = jnp.dot(flat_rows, value_matrix, preferred_element_type=jnp.float32).reshape(
        pair_count, seq_len, group_count, HEAD_WIDTH
    )
    positions = jnp.arange(seq_len, dtype=jnp.int32)
    last_index = lengths_here - 1
    onehot = (positions[None, :] == last_index[:, None]).astype(jnp.float32)
    normed_last = jnp.take_along_axis(normed, last_index[:, None, None], axis=1)[:, 0]
    query_proj = jnp.dot(normed_last, query_weight, preferred_element_type=jnp.float32).reshape(
        pair_count, head_count, HEAD_WIDTH
    )
    query_scale = lax.rsqrt(jnp.mean(query_proj * query_proj, axis=-1, keepdims=True) + EPSILON)
    query_unit = query_proj * query_scale
    key_scale = lax.rsqrt(jnp.mean(key_proj * key_proj, axis=-1, keepdims=True) + EPSILON)
    key_unit = key_proj * key_scale
    cos_table, sin_table = rope_tables(seq_len, HEAD_WIDTH)
    cos_query = jnp.dot(onehot, cos_table, precision=lax.Precision.HIGHEST)
    sin_query = jnp.dot(onehot, sin_table, precision=lax.Precision.HIGHEST)
    query_rot = (
        query_unit * cos_query[:, None, :] + rotate_half(query_unit) * sin_query[:, None, :]
    ).astype(jnp.bfloat16)
    key_rot = (
        key_unit * cos_table[None, :, None, :] + rotate_half(key_unit) * sin_table[None, :, None, :]
    ).astype(jnp.bfloat16)
    value_cast = value_proj.astype(jnp.bfloat16)
    grouped = query_rot.reshape(pair_count, group_count, group_size, HEAD_WIDTH)
    logits = jnp.einsum(
        "pkgd,pskd->pkgs", grouped, key_rot, preferred_element_type=jnp.float32
    ) * HEAD_WIDTH ** (-0.5)
    visible = (positions[None, :] <= last_index[:, None])[:, None, None, :]
    expos = jnp.where(visible, jnp.exp(logits), 0.0)
    attention_weights = expos / jnp.sum(expos, axis=-1, keepdims=True)
    probs_cast = attention_weights.astype(jnp.bfloat16)
    context = jnp.einsum(
        "pkgs,pskd->pkgd", probs_cast, value_cast, preferred_element_type=jnp.float32
    )
    context = context.astype(jnp.bfloat16).reshape(pair_count, head_count * HEAD_WIDTH)
    attended = jnp.dot(context, out_weight, preferred_element_type=jnp.float32)
    residual = jnp.take_along_axis(inputs_wide, last_index[:, None, None], axis=1)[:, 0] + attended
    out_scale = lax.rsqrt(jnp.mean(residual * residual, axis=-1, keepdims=True) + EPSILON)
    out_unit = residual * out_scale
    scores_here = jnp.sum(out_unit * final_gain * score_vector, axis=-1)
    stored = (
        tokens_in,
        onehot,
        inv_rms,
        normed,
        normed_last,
        query_unit,
        query_scale,
        key_unit,
        key_scale,
        cos_query,
        sin_query,
        cos_table,
        sin_table,
        query_rot,
        key_rot,
        value_cast,
        attention_weights,
        probs_cast,
        context,
        out_unit,
        out_scale,
    )
    return (scores_here, stored)


def backward_pairs(
    stored,
    grad_score,
    norm_gain,
    final_gain,
    score_vector,
    query_weight,
    key_matrix,
    value_matrix,
    out_weight,
):
    (
        tokens_in,
        onehot,
        inv_rms,
        normed,
        normed_last,
        query_unit,
        query_scale,
        key_unit,
        key_scale,
        cos_query,
        sin_query,
        cos_table,
        sin_table,
        query_rot,
        key_rot,
        value_cast,
        attention_weights,
        probs_cast,
        context,
        out_unit,
        out_scale,
    ) = stored
    pair_count, seq_len, model_width = tokens_in.shape
    head_count = query_weight.shape[1] // HEAD_WIDTH
    group_count = key_matrix.shape[1] // HEAD_WIDTH
    group_size = head_count // group_count
    grad_unit = grad_score[:, None] * score_vector * final_gain
    grad_resid = out_scale * (
        grad_unit - out_unit * jnp.mean(grad_unit * out_unit, axis=-1, keepdims=True)
    )
    grad_resid_cast = grad_resid.astype(jnp.bfloat16)
    grad_context = jnp.dot(
        grad_resid_cast, out_weight.T, preferred_element_type=jnp.float32
    ).astype(jnp.bfloat16)
    grad_context = grad_context.reshape(pair_count, group_count, group_size, HEAD_WIDTH)
    grad_probs = jnp.einsum(
        "pkgd,pskd->pkgs", grad_context, value_cast, preferred_element_type=jnp.float32
    )
    grad_vals = jnp.einsum(
        "pkgs,pkgd->pskd", probs_cast, grad_context, preferred_element_type=jnp.float32
    )
    spread = jnp.sum(attention_weights * grad_probs, axis=-1, keepdims=True)
    logit_gradient = (attention_weights * (grad_probs - spread)).astype(jnp.bfloat16)
    grouped = query_rot.reshape(pair_count, group_count, group_size, HEAD_WIDTH)
    rotated_query_gradient = jnp.einsum(
        "pkgs,pskd->pkgd", logit_gradient, key_rot, preferred_element_type=jnp.float32
    ) * HEAD_WIDTH ** (-0.5)
    rotated_query_gradient = rotated_query_gradient.reshape(pair_count, head_count, HEAD_WIDTH)
    grad_krot = jnp.einsum(
        "pkgs,pkgd->pskd", logit_gradient, grouped, preferred_element_type=jnp.float32
    ) * HEAD_WIDTH ** (-0.5)
    grad_qunit = rotated_query_gradient * cos_query[:, None, :] + unrotate_half(
        rotated_query_gradient * sin_query[:, None, :]
    )
    grad_kunit = grad_krot * cos_table[None, :, None, :] + unrotate_half(
        grad_krot * sin_table[None, :, None, :]
    )
    grad_qproj = query_scale * (
        grad_qunit - query_unit * jnp.mean(grad_qunit * query_unit, axis=-1, keepdims=True)
    )
    grad_kproj = key_scale * (
        grad_kunit - key_unit * jnp.mean(grad_kunit * key_unit, axis=-1, keepdims=True)
    )
    grad_q_cast = grad_qproj.reshape(pair_count, head_count * HEAD_WIDTH).astype(jnp.bfloat16)
    grad_k_cast = grad_kproj.reshape(pair_count * seq_len, group_count * HEAD_WIDTH).astype(
        jnp.bfloat16
    )
    grad_v_cast = grad_vals.reshape(pair_count * seq_len, group_count * HEAD_WIDTH).astype(
        jnp.bfloat16
    )
    flat_rows = normed.reshape(pair_count * seq_len, model_width)
    last_rows = jnp.concatenate([normed_last, grad_resid_cast, grad_q_cast, context], axis=1)
    grad_kv = jnp.dot(
        flat_rows.T,
        jnp.concatenate([grad_k_cast, grad_v_cast], axis=1),
        preferred_element_type=jnp.float32,
    )
    grad_normed = jnp.dot(grad_k_cast, key_matrix.T, preferred_element_type=jnp.float32)
    grad_normed = grad_normed + jnp.dot(
        grad_v_cast, value_matrix.T, preferred_element_type=jnp.float32
    )
    grad_normed = grad_normed.reshape(pair_count, seq_len, model_width)
    grad_last = jnp.dot(grad_q_cast, query_weight.T, preferred_element_type=jnp.float32)
    grad_normed = grad_normed + onehot[:, :, None] * grad_last[:, None, :]
    inputs_wide = tokens_in.astype(jnp.float32)
    grad_scaled = grad_normed * norm_gain
    grad_input = inv_rms * grad_scaled - inputs_wide * inv_rms * inv_rms * inv_rms * jnp.mean(
        grad_scaled * inputs_wide, axis=-1, keepdims=True
    )
    grad_input = grad_input + onehot[:, :, None] * grad_resid[:, None, :]
    return (grad_input.astype(jnp.bfloat16), last_rows, grad_kv)


class Place:
    def __init__(self):
        self.pb_count = lax.axis_size("pb")
        self.neg_count = lax.axis_size("neg")
        self.line_count = self.neg_count // 2
        self.pb = lax.axis_index("pb")
        neg = lax.axis_index("neg")
        self.line = neg // 2
        self.core = neg % 2
        self.partner = 1 - self.core

    def slot(self, pb, line, core):
        return pb * self.neg_count + line * 2 + core

    def line_peer(self, step):
        return lax.rem(self.line + step, self.line_count)

    def pb_peer(self, step):
        return lax.rem(self.pb + step, self.pb_count)

    def to_line(self, line):
        return (self.pb, line * 2 + self.core)

    def to_pb(self, pb):
        return (pb, self.line * 2 + self.core)

    def to_partner(self):
        return (self.pb, self.line * 2 + self.partner)

    def greet(self):
        barrier = pltpu.get_barrier_semaphore()
        targets = [self.to_line(self.line_peer(k)) for k in range(1, self.line_count)]
        targets += [self.to_pb(self.pb_peer(k)) for k in range(1, self.pb_count)]
        targets += [self.to_partner()]
        for target in targets:
            pl.semaphore_signal(barrier, inc=1, device_id=target, device_id_type=MESH_ID)
        pl.semaphore_wait(barrier, len(targets))


def remote(src, dst, send_sem, recv_sem, target):
    return pltpu.make_async_remote_copy(
        src_ref=src,
        dst_ref=dst,
        send_sem=send_sem,
        recv_sem=recv_sem,
        device_id=target,
        device_id_type=MESH_ID,
    )


def gather_sems(pb_count, neg_count):
    line_count = neg_count // 2
    return [
        pltpu.SemaphoreType.DMA((line_count,)),
        pltpu.SemaphoreType.DMA((line_count,)),
        pltpu.SemaphoreType.DMA((2, line_count)),
        pltpu.SemaphoreType.DMA((2, line_count)),
        pltpu.SemaphoreType.DMA((2, line_count)),
        pltpu.SemaphoreType.DMA((2, line_count)),
        pltpu.SemaphoreType.DMA((pb_count, line_count)),
        pltpu.SemaphoreType.DMA((pb_count, line_count)),
        pltpu.SemaphoreType.DMA,
    ]


class Gather:
    def __init__(self, place, own, full, sems):
        self.place, self.own, self.full = place, own, full
        self.line_send, self.line_recv, self.pb_send, self.pb_recv = sems[:4]
        self.half_send, self.half_recv = sems[4:6]
        self.core_send, self.core_recv, self.local_sem = sems[6:]
        self.sent = []
        across = place.pb + 1 - 2 * (place.pb % 2)
        along = place.pb + 2 - 4 * (place.pb // 2)
        self.near = (across, along)
        self.corner = 3 - place.pb

    def rows(self, pb, line, core):
        size = self.own.shape[0]
        start = self.place.slot(pb, line, core) * size
        return self.full.at[pl.ds(pl.multiple_of(start, size), size)]

    def send(self, src, dst, send_sem, recv_sem, target):
        copy = remote(src, dst, send_sem, recv_sem, target)
        copy.start()
        self.sent.append(copy)

    def spread(self, src, line):
        at = self.place
        dst = self.rows(at.pb, line, at.core)
        for side in range(2):
            self.send(
                src, dst, self.pb_send.at[side, line], self.pb_recv.at[side, line], at.to_pb(self.near[side])
            )
        self.pass_on(src, at.pb, line)

    def pass_on(self, src, pb, line):
        at = self.place
        dst = self.rows(pb, line, at.core)
        self.send(src, dst, self.core_send.at[pb, line], self.core_recv.at[pb, line], at.to_partner())

    def arrive(self, block, recv_sem):
        remote(block, block, self.local_sem, recv_sem, self.place.to_partner()).wait_recv()

    def start(self):
        at = self.place
        mine = self.rows(at.pb, at.line, at.core)
        self.local = pltpu.make_async_copy(self.own, mine, self.local_sem)
        self.local.start()
        for k in range(1, at.line_count):
            line = at.line_peer(k)
            self.send(
                self.own, mine, self.line_send.at[k], self.line_recv.at[at.line], at.to_line(line)
            )
        self.spread(self.own, at.line)

    def middle(self):
        at = self.place
        for k in range(1, at.line_count):
            line = at.line_peer(k)
            block = self.rows(at.pb, line, at.core)
            self.arrive(block, self.line_recv.at[line])
            self.spread(block, line)

    def half(self, block, side):
        size = block.shape[0] // 2
        return block.at[pl.ds(side * size, size)]

    def relay(self):
        at = self.place
        for step in range(at.line_count):
            line = at.line_peer(step)
            for side in range(2):
                block = self.rows(self.near[side], line, at.core)
                self.arrive(block, self.pb_recv.at[side, line])
                part = self.half(block, side)
                self.send(
                    part,
                    part,
                    self.half_send.at[side, line],
                    self.half_recv.at[side, line],
                    at.to_pb(self.near[1 - side]),
                )
                self.pass_on(block, self.near[side], line)

    def finish(self):
        at = self.place
        for step in range(at.line_count):
            line = at.line_peer(step)
            block = self.rows(self.corner, line, at.core)
            for side in range(2):
                self.arrive(self.half(block, side), self.half_recv.at[side, line])
            self.pass_on(block, self.corner, line)
        for pb in range(at.pb_count):
            for line in range(at.line_count):
                self.arrive(self.rows(pb, line, at.partner), self.core_recv.at[pb, line])
        self.local.wait()

    def drain(self):
        for copy in self.sent:
            copy.wait_send()


VMEM_SPEC = pl.BlockSpec(memory_space=pltpu.VMEM)


def mm(left, right, left_dim=1, right_dim=0, precision=None):
    return lax.dot_general(
        left,
        right,
        (((left_dim,), (right_dim,)), ((), ())),
        preferred_element_type=jnp.float32,
        precision=precision,
    )


def lane_mean(array):
    return jnp.mean(array, axis=-1, keepdims=True)


def tile(array, index):
    return array[:, index * HEAD_WIDTH : (index + 1) * HEAD_WIDTH]


class Exchange:
    def __init__(self, at, src, dst, send_sem, recv_sem):
        self.at, self.src, self.dst = at, src, dst
        self.send_sem, self.recv_sem = send_sem, recv_sem

    def start(self):
        at = self.at
        for pb, neg in at.others:
            peer = pb * at.neg_count + neg
            remote(
                self.src.at[peer], self.dst.at[at.me], self.send_sem, self.recv_sem, (pb, neg)
            ).start()
        self.dst[at.me] = self.src[at.me]

    def wait(self, sem_of):
        block = self.dst.at[pl.ds(0, self.at.count - 1)]
        copy = remote(block, block, self.send_sem, self.recv_sem, self.at.to_partner())
        getattr(copy, sem_of)()


def step_kernel(
    sizes,
    hidden,
    lengths,
    teacher,
    norm_gain_in,
    final_gain_in,
    score_vector_in,
    cos_table_in,
    sin_table_in,
    own_q_in,
    own_k_in,
    own_v_in,
    own_o_in,
    scores_out,
    loss_out,
    grad_hidden,
    grad_query,
    grad_key,
    grad_value,
    grad_out,
    x,
    norm_gain,
    final_gain,
    score_vector,
    cos_table,
    sin_table,
    own_q,
    own_k,
    own_v,
    own_o,
    full_q,
    full_k,
    full_v,
    full_o,
    normed,
    inv_wide,
    key_unit,
    key_scale,
    key_rot,
    value_cast,
    grad_k,
    grad_v,
    logit_grad,
    probs_ref,
    query_blocks,
    context_blocks,
    last_grad,
    resid_grad,
    context_own,
    context_full,
    late_own,
    late_full,
    early_src,
    early_dst,
    resid_src,
    resid_dst,
    list_src,
    list_dst,
    partial,
    from_core,
    paired,
    from_pb,
    summed,
    from_line,
    early_sems,
    resid_sems,
    list_sems,
    core_send,
    core_recv,
    pb_send,
    pb_recv,
    line_send,
    line_recv,
    any_sem,
    load_sems,
    *gather_sem_refs,
):
    pairs, seq, groups, share = sizes
    bf16, f32 = jnp.bfloat16, jnp.float32
    at = Place()
    at.count = at.pb_count * at.neg_count
    at.me = at.slot(at.pb, at.line, at.core)
    neg = lax.axis_index("neg")
    pb_all = [at.pb] + [at.pb_peer(k) for k in range(1, at.pb_count)]
    neg_all = [neg] + [lax.rem(neg + k, at.neg_count) for k in range(1, at.neg_count)]
    at.others = [
        (pb, peer)
        for i, pb in enumerate(pb_all)
        for j, peer in enumerate(neg_all)
        if i + j > 0
    ]
    model = x.shape[1]
    rows_all = pairs * seq
    per_group = own_q.shape[1] // own_k.shape[1]
    slots = per_group * pairs
    stacked = groups * slots
    kv_width = groups * HEAD_WIDTH

    barrier = pltpu.get_barrier_semaphore()

    for target in at.others:
        pl.semaphore_signal(barrier, inc=1, device_id=target, device_id_type=MESH_ID)
    loads = []
    moves = (
        (own_k_in, own_k),
        (own_v_in, own_v),
        (own_q_in, own_q),
        (own_o_in, own_o),
        (norm_gain_in, norm_gain),
        (final_gain_in, final_gain),
        (score_vector_in, score_vector),
        (cos_table_in, cos_table),
        (sin_table_in, sin_table),
    )
    small_loads = []
    for place_of, (source, target) in enumerate(moves):
        load = pltpu.make_async_copy(source, target, load_sems.at[pairs + place_of])
        load.start()
        small_loads.append(load)
    for pair in range(pairs):
        rows = pl.ds(pair * seq, seq)
        load = pltpu.make_async_copy(hidden.at[rows], x.at[rows], load_sems.at[pair])
        load.start()
        loads.append(load)

    each = len(gather_sem_refs) // 6
    gathers = []
    for place_of, (own, full) in enumerate(
        (
            (own_k, full_k),
            (own_v, full_v),
            (own_q, full_q),
            (own_o, full_o),
            (context_own, context_full),
            (late_own, late_full),
        )
    ):
        sems = gather_sem_refs[place_of * each : (place_of + 1) * each]
        gathers.append(Gather(at, own, full, sems))
    gather_k, gather_v, gather_q, gather_o, gather_context, gather_late = gathers

    def norm_pair(pair, carry):
        rows = pl.ds(pl.multiple_of(pair * seq, seq), seq)
        wide = x[rows, :].astype(f32)
        inv = lax.rsqrt(lane_mean(wide * wide) + EPSILON)
        inv_wide[rows, :] = jnp.broadcast_to(inv, (seq, HEAD_WIDTH))
        normed[rows, :] = (wide * inv * norm_gain[...]).astype(bf16)
        return carry

    for load in small_loads:
        load.wait()
    for pair in range(pairs):
        loads[pair].wait()
        norm_pair(pair, 0)

    row8 = lax.broadcasted_iota(jnp.int32, (slots, 1), 0)
    pair8 = lax.rem(row8, pairs)
    upper8 = row8 < pairs
    last8 = jnp.zeros((slots, 1), jnp.int32)
    teacher8 = jnp.zeros((slots, 1), f32)
    for pair in range(pairs):
        last8 = jnp.where(pair8 == pair, lengths[0, pair] - 1, last8)
        teacher8 = jnp.where(pair8 == pair, teacher[0, pair], teacher8)
    place8 = pair8 * seq + last8
    column8 = lax.broadcasted_iota(jnp.int32, (slots, rows_all), 1)
    onehot8 = (column8 == place8).astype(f32).astype(bf16)
    visible8 = (column8 >= pair8 * seq) & (column8 <= place8)
    visible = jnp.concatenate([visible8.astype(f32)] * groups, axis=0) > 0.5
    position8 = (lax.broadcasted_iota(jnp.int32, (slots, seq), 1) == last8).astype(f32)

    x_last = mm(onehot8, x[...])
    normed_last = mm(onehot8, normed[...]).astype(bf16)
    cos8 = mm(position8, cos_table[...], precision=lax.Precision.HIGHEST)
    sin8 = mm(position8, sin_table[...], precision=lax.Precision.HIGHEST)
    cos_rows = jnp.concatenate([cos8] * groups, axis=0)
    sin_rows = jnp.concatenate([sin8] * groups, axis=0)

    pl.semaphore_wait(barrier, at.count - 1)
    gather_k.start()
    gather_v.start()
    gather_q.start()
    gather_o.start()
    gather_k.middle()
    gather_v.middle()
    gather_k.relay()
    gather_q.middle()
    gather_v.relay()
    gather_k.finish()

    def key_pair(pair, carry):
        rows = pl.ds(pl.multiple_of(pair * seq, seq), seq)
        proj = mm(normed[rows, :], full_k[...])
        for group in range(groups):
            lanes = slice(group * HEAD_WIDTH, (group + 1) * HEAD_WIDTH)
            part = proj[:, lanes]
            scale = lax.rsqrt(lane_mean(part * part) + EPSILON)
            unit = part * scale
            key_unit[rows, lanes] = unit
            key_scale[rows, lanes] = jnp.broadcast_to(scale, (seq, HEAD_WIDTH))
            turned = unit * cos_table[...] + pltpu.roll(unit, HEAD_WIDTH // 2, 1) * sin_table[...]
            key_rot[rows, lanes] = turned.astype(bf16)
        return carry

    lax.fori_loop(0, pairs, key_pair, 0)

    gather_o.middle()
    gather_q.relay()
    gather_v.finish()

    def value_pair(pair, carry):
        rows = pl.ds(pl.multiple_of(pair * seq, seq), seq)
        value_cast[rows, :] = mm(normed[rows, :], full_v[...]).astype(bf16)
        return carry

    lax.fori_loop(0, pairs, value_pair, 0)

    gather_o.relay()
    gather_q.finish()

    def stack_heads(wide):
        return jnp.concatenate(
            [
                jnp.where(upper8, tile(wide, per_group * group), tile(wide, per_group * group + 1))
                for group in range(groups)
            ],
            axis=0,
        )

    def spread_heads(stack):
        parts = []
        for group in range(groups):
            part = stack[group * slots : (group + 1) * slots]
            parts += [jnp.where(upper8, part, 0.0), jnp.where(upper8, 0.0, part)]
        return jnp.concatenate(parts, axis=1).astype(bf16)

    def diagonal_of(wide):
        return jnp.concatenate(
            [
                wide[group * slots : (group + 1) * slots, group * HEAD_WIDTH : (group + 1) * HEAD_WIDTH]
                for group in range(groups)
            ],
            axis=0,
        )

    def blocks_of(stack):
        rows = []
        for group in range(groups):
            part = stack[group * slots : (group + 1) * slots]
            rows.append(
                jnp.concatenate(
                    [part if other == group else jnp.zeros_like(part) for other in range(groups)],
                    axis=1,
                )
            )
        return jnp.concatenate(rows, axis=0).astype(bf16)

    query_proj = stack_heads(mm(normed_last, full_q[...]))
    query_scale = lax.rsqrt(lane_mean(query_proj * query_proj) + EPSILON)
    query_unit = query_proj * query_scale
    query_rot = query_unit * cos_rows + pltpu.roll(query_unit, HEAD_WIDTH // 2, 1) * sin_rows
    query_wide = blocks_of(query_rot)
    query_blocks[...] = query_wide
    logits = mm(query_wide, key_rot[...], 1, 1) * HEAD_WIDTH ** (-0.5)
    expos = jnp.where(visible, jnp.exp(logits), 0.0)
    attention_weights = expos / jnp.sum(expos, axis=-1, keepdims=True)
    probs = attention_weights.astype(bf16)
    probs_ref[...] = probs
    context = diagonal_of(mm(probs, value_cast[...]))
    context_own[...] = context.astype(bf16)
    context_wide = spread_heads(context)
    gather_context.start()

    lane_block = lax.rem(
        lax.broadcasted_iota(jnp.int32, (slots, model), 1) // share, HEAD_WIDTH // share
    )

    def pack(parts, turn):
        total = jnp.zeros((slots, model), f32)
        for block, part in enumerate(parts):
            shift = ((block - turn) * share) % model
            moved = part if shift == 0 else pltpu.roll(part, shift, 1)
            total = jnp.where(lane_block == block, moved, total)
        return total

    def by_head(wide):
        return [jnp.where(upper8, wide, 0.0), jnp.where(upper8, 0.0, wide)]

    turns = HEAD_WIDTH // share
    pulled = mm(probs, normed[...])
    pulled_parts = [pulled[group * slots : (group + 1) * slots] for group in range(groups)]
    last_parts = by_head(normed_last.astype(f32))
    for turn in range(turns):
        both = jnp.concatenate([pack(pulled_parts, turn), pack(last_parts, turn)], axis=0)
        both = both.astype(bf16)
        for index in range(model // HEAD_WIDTH):
            early_src[index * turns + turn] = tile(both, index)

    early = Exchange(at, early_src, early_dst, early_sems.at[0], early_sems.at[1])
    early.start()

    gather_o.finish()
    attended = mm(context_wide, full_o[...], 1, 1)
    attended = attended + pltpu.roll(attended, pairs, 0)
    residual = x_last + attended
    out_scale = lax.rsqrt(lane_mean(residual * residual) + EPSILON)
    out_unit = residual * out_scale
    gain = final_gain[...] * score_vector[...]
    score8 = jnp.sum(out_unit * gain, axis=-1, keepdims=True)

    lane8 = lax.broadcasted_iota(jnp.int32, (slots, HEAD_WIDTH), 1)
    row_lane = lax.broadcasted_iota(jnp.int32, (slots, HEAD_WIDTH), 0)

    def as_row(column):
        return jnp.sum(jnp.where(row_lane == lane8, column, 0.0), axis=0, keepdims=True)

    score_row = as_row(score8)
    lane1 = lax.broadcasted_iota(jnp.int32, (1, HEAD_WIDTH), 1)
    listing = jnp.where(lane1 < pairs, score_row, as_row(teacher8))
    list_src[...] = listing
    me_row = list_dst.at[at.me]
    list_here, list_there, list_sent = list_sems.at[0], list_sems.at[1], list_sems.at[2]
    for place_of, target in enumerate(at.others):
        arrived = list_here if place_of < at.neg_count - 1 else list_there
        remote(list_src, me_row, list_sent, arrived, target).start()
    list_dst[at.me] = listing
    scores_out[...] = score_row[:, :pairs]
    gather_context.middle()
    gather_context.relay()

    near_block = list_dst.at[pl.ds(0, at.neg_count - 1)]
    remote(near_block, near_block, list_sent, list_here, at.to_partner()).wait_recv()

    def total(array):
        return jnp.sum(jnp.sum(array, axis=1, keepdims=True), axis=0, keepdims=True)

    def query_terms(first):
        block = list_dst[pl.ds(first, at.neg_count)].reshape(at.neg_count, HEAD_WIDTH)
        real = lax.broadcasted_iota(jnp.int32, block.shape, 1) < pairs
        score = jnp.where(real, block, 0.0)
        scaled = pltpu.roll(block, HEAD_WIDTH - pairs, 1)
        scaled = jnp.where(real, scaled, 0.0) / TEACHER_TEMP
        expo_t = jnp.where(real, jnp.exp(scaled), 0.0)
        total_s = total(jnp.where(real, jnp.exp(score), 0.0))
        return score, scaled, expo_t, total_s, total(expo_t)

    _, _, _, total_s, total_t = query_terms(pl.multiple_of(at.pb * at.neg_count, at.neg_count))
    grad_score = GRAD_SCALE * (
        jnp.exp(score8) / total_s - jnp.exp(teacher8 / TEACHER_TEMP) / total_t
    )
    grad_unit = grad_score * gain
    grad_resid = out_scale * (grad_unit - out_unit * lane_mean(grad_unit * out_unit))
    resid_grad[...] = grad_resid
    resid_cast = grad_resid.astype(bf16)
    grad_context = stack_heads(mm(resid_cast, full_o[...])).astype(bf16)
    context_blocks[...] = blocks_of(grad_context.astype(f32))
    late_own[0:stacked, :] = grad_context

    grad_probs = mm(context_blocks[...], value_cast[...], 1, 1)
    spread = jnp.sum(attention_weights * grad_probs, axis=-1, keepdims=True)
    logit_gradient = (attention_weights * (grad_probs - spread)).astype(bf16)
    logit_grad[...] = logit_gradient

    turned_q = diagonal_of(mm(logit_gradient, key_rot[...])) * HEAD_WIDTH ** (-0.5)
    back_q = turned_q * cos_rows - pltpu.roll(turned_q, HEAD_WIDTH // 2, 1) * sin_rows
    back_q = query_scale * (back_q - query_unit * lane_mean(back_q * query_unit))
    grad_q_cast = back_q.astype(bf16)
    late_own[stacked : 2 * stacked, :] = grad_q_cast
    gather_late.start()

    def key_back(pair, carry):
        start = pl.multiple_of(pair * seq, seq)
        rows = pl.ds(start, seq)
        turned = mm(logit_grad[:, rows], query_blocks[...], 0, 0) * HEAD_WIDTH ** (-0.5)
        for group in range(groups):
            lanes = slice(group * HEAD_WIDTH, (group + 1) * HEAD_WIDTH)
            part = turned[:, lanes]
            unit = key_unit[rows, lanes]
            back = part * cos_table[...] - pltpu.roll(part, HEAD_WIDTH // 2, 1) * sin_table[...]
            back = key_scale[rows, lanes] * (back - unit * lane_mean(back * unit))
            grad_k[rows, lanes] = back.astype(bf16)
        return carry

    lax.fori_loop(0, pairs, key_back, 0)

    block_rows = model // at.pb_count
    copies = []

    def send(src, dst, send_sem, recv_sem, target):
        copy = remote(src, dst, send_sem, recv_sem, target)
        copy.start()
        copies.append(copy)

    def arrive(block, recv_sem):
        remote(block, block, any_sem, recv_sem, at.to_partner()).wait_recv()

    for k in range(1, at.pb_count + 1):
        pb = at.pb_peer(k % at.pb_count)
        lanes = pl.ds(pl.multiple_of(pb * block_rows, block_rows), block_rows)
        product = mm(normed[:, lanes], grad_k[...], 0, 0)
        partial[pb] = product.astype(bf16).reshape(at.line_count, 2, share, kv_width)
        send(
            partial.at[pb, :, at.partner],
            from_core.at[pb],
            core_send.at[pb],
            core_recv.at[pb],
            at.to_partner(),
        )

    for k in range(1, at.pb_count + 1):
        pb = at.pb_peer(k % at.pb_count)
        arrive(from_core.at[pb], core_recv.at[pb])
        both = partial[pb, :, at.core].astype(f32) + from_core[pb].astype(f32)
        paired[pb] = both.astype(bf16)
    for step in range(1, at.line_count + 1):
        line = at.line_peer(step % at.line_count)
        for k in range(1, at.pb_count):
            pb = at.pb_peer(k)
            send(
                paired.at[pb, line],
                from_pb.at[at.pb, line],
                pb_send.at[k, line],
                pb_recv.at[at.pb, line],
                at.to_pb(pb),
            )

    resid_parts = by_head(resid_cast.astype(f32))
    for turn in range(turns):
        packed = pack(resid_parts, turn).astype(bf16)
        for index in range(model // HEAD_WIDTH):
            resid_src[index * turns + turn] = tile(packed, index)
    resid = Exchange(at, resid_src, resid_dst, resid_sems.at[0], resid_sems.at[1])
    resid.start()

    gather_late.middle()
    gather_late.relay()
    gather_context.finish()

    back_last = mm(spread_heads(grad_q_cast.astype(f32)), full_q[...], 1, 1)
    last_grad[...] = back_last + pltpu.roll(back_last, pairs, 0)

    def value_back(pair, carry):
        start = pl.multiple_of(pair * seq, seq)
        rows = pl.ds(start, seq)
        grad_v[rows, :] = mm(probs_ref[:, rows], context_blocks[...], 0, 0).astype(bf16)
        return carry

    lax.fori_loop(0, pairs, value_back, 0)

    seq_row = lax.broadcasted_iota(jnp.int32, (seq, 1), 0)

    def hidden_back(pair, carry):
        rows = pl.ds(pl.multiple_of(pair * seq, seq), seq)
        total = mm(grad_k[rows, :], full_k[...], 1, 1) + mm(grad_v[rows, :], full_v[...], 1, 1)
        hit = seq_row == lengths[0, pair] - 1
        total = total + jnp.where(hit, last_grad[pl.ds(pair, 1), :], 0.0)
        scaled = total * norm_gain[...]
        wide = x[rows, :].astype(f32)
        inv = inv_wide[rows, 0:1]
        mean = lane_mean(scaled * wide)
        result = inv * scaled - wide * (inv * inv * inv * mean)
        result = result + jnp.where(hit, resid_grad[pl.ds(pair, 1), :], 0.0)
        grad_hidden[rows, :] = result.astype(bf16)
        return carry

    def add_line(step):
        line = at.line_peer(step % at.line_count)
        total = paired[at.pb, line].astype(f32)
        for k in range(1, at.pb_count):
            pb = at.pb_peer(k)
            arrive(from_pb.at[pb, line], pb_recv.at[pb, line])
            total = total + from_pb[pb, line].astype(f32)
        if step < at.line_count:
            summed[line] = total.astype(bf16)
            send(
                summed.at[line],
                from_line.at[at.line],
                line_send.at[line],
                line_recv.at[at.line],
                at.to_line(line),
            )
        return total

    hidden_back(0, 0)
    add_line(1)
    hidden_back(1, 0)
    add_line(2)
    hidden_back(2, 0)
    for step in range(3, at.line_count + 1):
        own_sum = add_line(step)
    for pair in range(3, pairs):
        hidden_back(pair, 0)

    far_block = list_dst.at[pl.ds(0, at.count - at.neg_count)]
    remote(far_block, far_block, list_sent, list_there, at.to_partner()).wait_recv()
    loss = jnp.zeros((1, 1), f32)
    for pb in range(at.pb_count):
        score, scaled, expo_t, sum_s, sum_t = query_terms(pb * at.neg_count)
        loss = loss + total(expo_t / sum_t * (scaled - jnp.log(sum_t) - (score - jnp.log(sum_s))))
    loss_out[...] = loss

    gather_late.finish()
    early.wait("wait_recv")
    resid.wait("wait_recv")

    def rows_of(full, start, group):
        wide = full[...].astype(f32).reshape(at.count, -1, slots, HEAD_WIDTH)
        return wide[:, start + group].reshape(at.count * slots, HEAD_WIDTH).astype(bf16)

    pulled_rows = rows_of(early_dst, 0, 0)
    last_rows = rows_of(early_dst, 1, 0)
    resid_rows = rows_of(resid_dst, 0, 0)
    for group in range(groups):
        found = mm(pulled_rows, rows_of(late_full, 0, group), 0, 0)
        lanes = slice(group * HEAD_WIDTH, (group + 1) * HEAD_WIDTH)
        grad_value[:, lanes] = found[group * share : (group + 1) * share]
        found = mm(last_rows, rows_of(late_full, groups, group), 0, 0)
        for part in range(per_group):
            head = per_group * group + part
            grad_query[:, head * HEAD_WIDTH : (head + 1) * HEAD_WIDTH] = found[
                part * share : (part + 1) * share
            ]
        found = mm(resid_rows, rows_of(context_full, 0, group), 0, 0)
        for part in range(per_group):
            head = per_group * group + part
            grad_out[:, head * HEAD_WIDTH : (head + 1) * HEAD_WIDTH] = found[
                part * share : (part + 1) * share
            ]

    final = own_sum
    for step in range(1, at.line_count):
        line = at.line_peer(step)
        arrive(from_line.at[line], line_recv.at[line])
        final = final + from_line[line].astype(f32)
    grad_key[...] = final

    for gather in gathers:
        gather.drain()
    for copy in copies:
        copy.wait_send()
    early.wait("wait_send")
    resid.wait("wait_send")
    sent_block = list_dst.at[pl.ds(0, at.count - 1)]
    remote(sent_block, sent_block, list_sent, list_here, at.to_partner()).wait_send()


def write_kernel(count, *refs):
    sources, targets, sems = refs[:count], refs[count : 2 * count], refs[2 * count]
    copies = [
        pltpu.make_async_copy(sources[i], targets[i], sems.at[i]) for i in range(2, count)
    ]
    for copy in copies:
        copy.start()
    for i in range(2):
        targets[i][...] = sources[i][...]
    for copy in copies:
        copy.wait()


def write_outputs(arrays):
    count = len(arrays)
    return pl.pallas_call(
        functools.partial(write_kernel, count),
        out_shape=tuple(jax.ShapeDtypeStruct(a.shape, a.dtype) for a in arrays),
        in_specs=[VMEM_SPEC] * count,
        out_specs=(VMEM_SPEC,) * 2 + (pl.BlockSpec(memory_space=pl.ANY),) * (count - 2),
        scratch_shapes=[pltpu.SemaphoreType.DMA((count,))],
        compiler_params=pltpu.CompilerParams(vmem_limit_bytes=4 * 2**20),
    )(*arrays)


def run_step(operands, sizes, pb_count, neg_count):
    pairs, seq, groups, share = sizes
    x, own_q, own_k = operands[0], operands[8], operands[9]
    model, width, kv_width = x.shape[1], own_q.shape[1], own_k.shape[1]
    rows = pairs * seq
    count = pb_count * neg_count
    line_count = neg_count // 2
    slots = width // kv_width * pairs
    stacked = groups * slots
    bf16, f32 = jnp.bfloat16, jnp.float32
    block = (pb_count, line_count, share, kv_width)
    dma = pltpu.SemaphoreType.DMA
    vmem = pltpu.VMEM
    smem_spec = pl.BlockSpec(memory_space=pltpu.SMEM)
    hbm_spec = pl.BlockSpec(memory_space=pltpu.HBM)
    return pl.pallas_call(
        functools.partial(step_kernel, sizes),
        out_shape=(
            vmem((1, pairs), f32),
            vmem((1, 1), f32),
            vmem((rows, model), bf16),
            vmem((share, width), f32),
            vmem((share, kv_width), f32),
            vmem((share, kv_width), f32),
            vmem((share, width), f32),
        ),
        in_specs=[hbm_spec, smem_spec, smem_spec] + [hbm_spec] * 9,
        out_specs=(VMEM_SPEC,) * 7,
        scratch_shapes=[
            vmem((rows, model), bf16),
        ]
        + [vmem(a.shape, a.dtype) for a in operands[3:]]
        + [
            vmem((model, width), bf16),
            vmem((model, kv_width), bf16),
            vmem((model, kv_width), bf16),
            vmem((model, width), bf16),
            vmem((rows, model), bf16),
            vmem((rows, HEAD_WIDTH), f32),
            vmem((rows, kv_width), f32),
            vmem((rows, kv_width), f32),
            vmem((rows, kv_width), bf16),
            vmem((rows, kv_width), bf16),
            vmem((rows, kv_width), bf16),
            vmem((rows, kv_width), bf16),
            vmem((stacked, rows), bf16),
            vmem((stacked, rows), bf16),
            vmem((stacked, kv_width), bf16),
            vmem((stacked, kv_width), bf16),
            vmem((slots, model), f32),
            vmem((slots, model), f32),
            vmem((stacked, HEAD_WIDTH), bf16),
            vmem((stacked * count, HEAD_WIDTH), bf16),
            vmem((2 * stacked, HEAD_WIDTH), bf16),
            vmem((2 * stacked * count, HEAD_WIDTH), bf16),
            vmem((count, 2 * slots, HEAD_WIDTH), bf16),
            vmem((count, 2 * slots, HEAD_WIDTH), bf16),
            vmem((count, slots, HEAD_WIDTH), bf16),
            vmem((count, slots, HEAD_WIDTH), bf16),
            vmem((1, HEAD_WIDTH), f32),
            vmem((count, 1, HEAD_WIDTH), f32),
            vmem((pb_count, line_count, 2, share, kv_width), bf16),
            vmem(block, bf16),
            vmem(block, bf16),
            vmem(block, bf16),
            vmem(block[1:], bf16),
            vmem(block[1:], bf16),
            dma((2,)),
            dma((2,)),
            dma((3,)),
            dma((pb_count,)),
            dma((pb_count,)),
            dma((pb_count, line_count)),
            dma((pb_count, line_count)),
            dma((line_count,)),
            dma((line_count,)),
            dma,
            dma((pairs + 9,)),
        ]
        + gather_sems(pb_count, neg_count) * 6,
        compiler_params=pltpu.CompilerParams(
            collective_id=0, has_side_effects=True, vmem_limit_bytes=62 * 2**20
        ),
    )(*operands)


def shards(
    hidden,
    lengths,
    teacher,
    norm_gain,
    final_gain,
    score_vector,
    query_weight,
    key_matrix,
    value_matrix,
    out_weight,
):
    both = ("pb", "neg")
    width = query_weight.shape[1]
    kv_width = key_matrix.shape[1]
    share, out_share = query_weight.shape[0], out_weight.shape[1]
    pb_count, neg_count = lax.axis_size("pb"), lax.axis_size("neg")
    pair_count, seq_len, model_width = hidden.shape[1:]
    group_count = kv_width // HEAD_WIDTH
    own_kernels = (
        pb_count == 4
        and neg_count % 2 == 0
        and share == out_share
        and share % 32 == 0
        and model_width == share * pb_count * neg_count
        and width == 2 * kv_width
        and pair_count * 2 == 8
        and seq_len == HEAD_WIDTH
        and share * group_count == HEAD_WIDTH
    )
    if own_kernels:
        cos_table, sin_table = signed_tables(seq_len, HEAD_WIDTH)
        results = run_step(
            (
                hidden.reshape(pair_count * seq_len, model_width),
                lengths,
                teacher,
                norm_gain[None],
                final_gain[None],
                score_vector[None],
                cos_table,
                sin_table,
                query_weight,
                key_matrix,
                value_matrix,
                out_weight.T,
            ),
            (pair_count, seq_len, group_count, share),
            pb_count,
            neg_count,
        )
        scores, loss, grad_rows, grad_query, grad_key, grad_value, grad_out = write_outputs(results)
        return (
            scores,
            loss.reshape(()),
            grad_rows.reshape(hidden.shape),
            grad_query,
            grad_key,
            grad_value,
            grad_out.T,
        )
    packed = jnp.concatenate([query_weight, key_matrix, value_matrix, out_weight.T], axis=1)
    everything = lax.all_gather(packed, both, axis=0, tiled=True)
    full_query = everything[:, :width]
    full_key = everything[:, width : width + kv_width]
    full_value = everything[:, width + kv_width : width + 2 * kv_width]
    full_out_t = everything[:, width + 2 * kv_width :]
    weights = (full_query, full_key, full_value, full_out_t.T)
    scores_here, stored = forward_pairs(
        hidden[0], lengths[0], norm_gain, final_gain, score_vector, *weights
    )
    listing = jnp.concatenate([scores_here, teacher[0]])[None]
    listed = lax.all_gather(listing, "neg", axis=0, tiled=True)
    all_scores = listed[:, :pair_count]
    all_scaled = listed[:, pair_count:] / TEACHER_TEMP
    my_total_s = jnp.sum(jnp.exp(all_scores))
    expo_t = jnp.exp(all_scaled)
    my_total_t = jnp.sum(expo_t)
    loss_here = jnp.sum(
        expo_t
        / my_total_t
        * (all_scaled - jnp.log(my_total_t) - (all_scores - jnp.log(my_total_s)))
    )
    prob_s = jnp.exp(scores_here) / my_total_s
    prob_t = jnp.exp(teacher[0] / TEACHER_TEMP) / my_total_t
    grad_score = GRAD_SCALE * (prob_s - prob_t)
    grad_input, last_rows, grad_kv = backward_pairs(
        stored, grad_score, norm_gain, final_gain, score_vector, *weights
    )
    grad_kv = grad_kv.astype(jnp.bfloat16)
    reduced = lax.psum_scatter(grad_kv, both, scatter_dimension=0, tiled=True)
    reduced = reduced.astype(jnp.float32)
    rows = lax.all_gather(last_rows, both, axis=0, tiled=True)
    loss_value = lax.psum(loss_here, "pb")
    index = lax.axis_index("pb") * neg_count + lax.axis_index("neg")
    normed_cols = lax.dynamic_slice_in_dim(rows, index * share, share, axis=1)
    resid_cols = lax.dynamic_slice_in_dim(rows, model_width + index * out_share, out_share, axis=1)
    rest = 2 * model_width
    all_q = rows[:, rest : rest + width]
    all_context = rows[:, rest + width :]
    grad_query = jnp.dot(normed_cols.T, all_q, preferred_element_type=jnp.float32)
    grad_out = jnp.dot(all_context.T, resid_cols, preferred_element_type=jnp.float32)
    return (
        scores_here[None],
        loss_value,
        grad_input[None],
        grad_query,
        reduced[:, :kv_width],
        reduced[:, kv_width:],
        grad_out,
    )


def solution(mesh):
    placed = (
        P("pb", "neg", None, None),
        P("pb", "neg"),
        P("pb", "neg"),
        P(),
        P(),
        P(),
        P(("pb", "neg"), None),
        P(("pb", "neg"), None),
        P(("pb", "neg"), None),
        P(None, ("pb", "neg")),
    )
    return jax.shard_map(
        shards,
        mesh=mesh,
        in_specs=placed,
        out_specs=(
            P("pb", "neg"),
            P(),
            P("pb", "neg", None, None),
            P(("pb", "neg"), None),
            P(("pb", "neg"), None),
            P(("pb", "neg"), None),
            P(None, ("pb", "neg")),
        ),
        check_vma=False,
    )
```

```python
import functools

import jax
import jax.numpy as jnp
import numpy as np
from jax import lax
from jax.experimental import pallas as pl
from jax.experimental.pallas import tpu as pltpu
from jax.sharding import PartitionSpec as P

HEAD_WIDTH = 128
MESH_ID = pl.DeviceIdType.MESH

EPSILON = 1e-06
ROPE_BASE = 1000000.0
TEACHER_TEMP = 2.0
GRAD_SCALE = 512.0


def rope_tables(seq_len, head_size):
    half = head_size // 2
    freqs = ROPE_BASE ** (-(jnp.arange(half, dtype=jnp.float32) * 2.0) / head_size)
    angles = jnp.arange(seq_len, dtype=jnp.float32)[:, None] * freqs[None, :]
    angles = jnp.concatenate([angles, angles], axis=1)
    return (jnp.cos(angles), jnp.sin(angles))


def signed_tables(seq_len, head_size):
    half = head_size // 2
    freqs = ROPE_BASE ** (-(np.arange(half) * 2.0) / head_size)
    angles = np.arange(seq_len)[:, None] * freqs[None, :]
    cos = np.concatenate([np.cos(angles)] * 2, axis=1)
    sin = np.concatenate([-np.sin(angles), np.sin(angles)], axis=1)
    return (jnp.asarray(cos, jnp.float32), jnp.asarray(sin, jnp.float32))


def rotate_half(vector):
    half = vector.shape[-1] // 2
    return jnp.concatenate([-vector[..., half:], vector[..., :half]], axis=-1)


def unrotate_half(vector):
    half = vector.shape[-1] // 2
    return jnp.concatenate([vector[..., half:], -vector[..., :half]], axis=-1)


def forward_pairs(
    tokens_in,
    lengths_here,
    norm_gain,
    final_gain,
    score_vector,
    query_weight,
    key_matrix,
    value_matrix,
    out_weight,
):
    pair_count, seq_len, model_width = tokens_in.shape
    head_count = query_weight.shape[1] // HEAD_WIDTH
    group_count = key_matrix.shape[1] // HEAD_WIDTH
    group_size = head_count // group_count
    inputs_wide = tokens_in.astype(jnp.float32)
    inv_rms = lax.rsqrt(jnp.mean(inputs_wide * inputs_wide, axis=-1, keepdims=True) + EPSILON)
    normed = (inputs_wide * inv_rms * norm_gain).astype(jnp.bfloat16)
    flat_rows = normed.reshape(pair_count * seq_len, model_width)
    key_proj = jnp.dot(flat_rows, key_matrix, preferred_element_type=jnp.float32).reshape(
        pair_count, seq_len, group_count, HEAD_WIDTH
    )
    value_proj = jnp.dot(flat_rows, value_matrix, preferred_element_type=jnp.float32).reshape(
        pair_count, seq_len, group_count, HEAD_WIDTH
    )
    positions = jnp.arange(seq_len, dtype=jnp.int32)
    last_index = lengths_here - 1
    onehot = (positions[None, :] == last_index[:, None]).astype(jnp.float32)
    normed_last = jnp.take_along_axis(normed, last_index[:, None, None], axis=1)[:, 0]
    query_proj = jnp.dot(normed_last, query_weight, preferred_element_type=jnp.float32).reshape(
        pair_count, head_count, HEAD_WIDTH
    )
    query_scale = lax.rsqrt(jnp.mean(query_proj * query_proj, axis=-1, keepdims=True) + EPSILON)
    query_unit = query_proj * query_scale
    key_scale = lax.rsqrt(jnp.mean(key_proj * key_proj, axis=-1, keepdims=True) + EPSILON)
    key_unit = key_proj * key_scale
    cos_table, sin_table = rope_tables(seq_len, HEAD_WIDTH)
    cos_query = jnp.dot(onehot, cos_table, precision=lax.Precision.HIGHEST)
    sin_query = jnp.dot(onehot, sin_table, precision=lax.Precision.HIGHEST)
    query_rot = (
        query_unit * cos_query[:, None, :] + rotate_half(query_unit) * sin_query[:, None, :]
    ).astype(jnp.bfloat16)
    key_rot = (
        key_unit * cos_table[None, :, None, :] + rotate_half(key_unit) * sin_table[None, :, None, :]
    ).astype(jnp.bfloat16)
    value_cast = value_proj.astype(jnp.bfloat16)
    grouped = query_rot.reshape(pair_count, group_count, group_size, HEAD_WIDTH)
    logits = jnp.einsum(
        "pkgd,pskd->pkgs", grouped, key_rot, preferred_element_type=jnp.float32
    ) * HEAD_WIDTH ** (-0.5)
    visible = (positions[None, :] <= last_index[:, None])[:, None, None, :]
    expos = jnp.where(visible, jnp.exp(logits), 0.0)
    attention_weights = expos / jnp.sum(expos, axis=-1, keepdims=True)
    probs_cast = attention_weights.astype(jnp.bfloat16)
    context = jnp.einsum(
        "pkgs,pskd->pkgd", probs_cast, value_cast, preferred_element_type=jnp.float32
    )
    context = context.astype(jnp.bfloat16).reshape(pair_count, head_count * HEAD_WIDTH)
    attended = jnp.dot(context, out_weight, preferred_element_type=jnp.float32)
    residual = jnp.take_along_axis(inputs_wide, last_index[:, None, None], axis=1)[:, 0] + attended
    out_scale = lax.rsqrt(jnp.mean(residual * residual, axis=-1, keepdims=True) + EPSILON)
    out_unit = residual * out_scale
    scores_here = jnp.sum(out_unit * final_gain * score_vector, axis=-1)
    stored = (
        tokens_in,
        onehot,
        inv_rms,
        normed,
        normed_last,
        query_unit,
        query_scale,
        key_unit,
        key_scale,
        cos_query,
        sin_query,
        cos_table,
        sin_table,
        query_rot,
        key_rot,
        value_cast,
        attention_weights,
        probs_cast,
        context,
        out_unit,
        out_scale,
    )
    return (scores_here, stored)


def backward_pairs(
    stored,
    grad_score,
    norm_gain,
    final_gain,
    score_vector,
    query_weight,
    key_matrix,
    value_matrix,
    out_weight,
):
    (
        tokens_in,
        onehot,
        inv_rms,
        normed,
        normed_last,
        query_unit,
        query_scale,
        key_unit,
        key_scale,
        cos_query,
        sin_query,
        cos_table,
        sin_table,
        query_rot,
        key_rot,
        value_cast,
        attention_weights,
        probs_cast,
        context,
        out_unit,
        out_scale,
    ) = stored
    pair_count, seq_len, model_width = tokens_in.shape
    head_count = query_weight.shape[1] // HEAD_WIDTH
    group_count = key_matrix.shape[1] // HEAD_WIDTH
    group_size = head_count // group_count
    grad_unit = grad_score[:, None] * score_vector * final_gain
    grad_resid = out_scale * (
        grad_unit - out_unit * jnp.mean(grad_unit * out_unit, axis=-1, keepdims=True)
    )
    grad_resid_cast = grad_resid.astype(jnp.bfloat16)
    grad_context = jnp.dot(
        grad_resid_cast, out_weight.T, preferred_element_type=jnp.float32
    ).astype(jnp.bfloat16)
    grad_context = grad_context.reshape(pair_count, group_count, group_size, HEAD_WIDTH)
    grad_probs = jnp.einsum(
        "pkgd,pskd->pkgs", grad_context, value_cast, preferred_element_type=jnp.float32
    )
    grad_vals = jnp.einsum(
        "pkgs,pkgd->pskd", probs_cast, grad_context, preferred_element_type=jnp.float32
    )
    spread = jnp.sum(attention_weights * grad_probs, axis=-1, keepdims=True)
    logit_gradient = (attention_weights * (grad_probs - spread)).astype(jnp.bfloat16)
    grouped = query_rot.reshape(pair_count, group_count, group_size, HEAD_WIDTH)
    rotated_query_gradient = jnp.einsum(
        "pkgs,pskd->pkgd", logit_gradient, key_rot, preferred_element_type=jnp.float32
    ) * HEAD_WIDTH ** (-0.5)
    rotated_query_gradient = rotated_query_gradient.reshape(pair_count, head_count, HEAD_WIDTH)
    grad_krot = jnp.einsum(
        "pkgs,pkgd->pskd", logit_gradient, grouped, preferred_element_type=jnp.float32
    ) * HEAD_WIDTH ** (-0.5)
    grad_qunit = rotated_query_gradient * cos_query[:, None, :] + unrotate_half(
        rotated_query_gradient * sin_query[:, None, :]
    )
    grad_kunit = grad_krot * cos_table[None, :, None, :] + unrotate_half(
        grad_krot * sin_table[None, :, None, :]
    )
    grad_qproj = query_scale * (
        grad_qunit - query_unit * jnp.mean(grad_qunit * query_unit, axis=-1, keepdims=True)
    )
    grad_kproj = key_scale * (
        grad_kunit - key_unit * jnp.mean(grad_kunit * key_unit, axis=-1, keepdims=True)
    )
    grad_q_cast = grad_qproj.reshape(pair_count, head_count * HEAD_WIDTH).astype(jnp.bfloat16)
    grad_k_cast = grad_kproj.reshape(pair_count * seq_len, group_count * HEAD_WIDTH).astype(
        jnp.bfloat16
    )
    grad_v_cast = grad_vals.reshape(pair_count * seq_len, group_count * HEAD_WIDTH).astype(
        jnp.bfloat16
    )
    flat_rows = normed.reshape(pair_count * seq_len, model_width)
    last_rows = jnp.concatenate([normed_last, grad_resid_cast, grad_q_cast, context], axis=1)
    grad_kv = jnp.dot(
        flat_rows.T,
        jnp.concatenate([grad_k_cast, grad_v_cast], axis=1),
        preferred_element_type=jnp.float32,
    )
    grad_normed = jnp.dot(grad_k_cast, key_matrix.T, preferred_element_type=jnp.float32)
    grad_normed = grad_normed + jnp.dot(
        grad_v_cast, value_matrix.T, preferred_element_type=jnp.float32
    )
    grad_normed = grad_normed.reshape(pair_count, seq_len, model_width)
    grad_last = jnp.dot(grad_q_cast, query_weight.T, preferred_element_type=jnp.float32)
    grad_normed = grad_normed + onehot[:, :, None] * grad_last[:, None, :]
    inputs_wide = tokens_in.astype(jnp.float32)
    grad_scaled = grad_normed * norm_gain
    grad_input = inv_rms * grad_scaled - inputs_wide * inv_rms * inv_rms * inv_rms * jnp.mean(
        grad_scaled * inputs_wide, axis=-1, keepdims=True
    )
    grad_input = grad_input + onehot[:, :, None] * grad_resid[:, None, :]
    return (grad_input.astype(jnp.bfloat16), last_rows, grad_kv)


class Place:
    def __init__(self):
        self.pb_count = lax.axis_size("pb")
        self.neg_count = lax.axis_size("neg")
        self.line_count = self.neg_count // 2
        self.pb = lax.axis_index("pb")
        neg = lax.axis_index("neg")
        self.line = neg // 2
        self.core = neg % 2
        self.partner = 1 - self.core

    def slot(self, pb, line, core):
        return pb * self.neg_count + line * 2 + core

    def line_peer(self, step):
        return lax.rem(self.line + step, self.line_count)

    def pb_peer(self, step):
        return lax.rem(self.pb + step, self.pb_count)

    def to_line(self, line):
        return (self.pb, line * 2 + self.core)

    def to_pb(self, pb):
        return (pb, self.line * 2 + self.core)

    def to_partner(self):
        return (self.pb, self.line * 2 + self.partner)

    def greet(self):
        barrier = pltpu.get_barrier_semaphore()
        targets = [self.to_line(self.line_peer(k)) for k in range(1, self.line_count)]
        targets += [self.to_pb(self.pb_peer(k)) for k in range(1, self.pb_count)]
        targets += [self.to_partner()]
        for target in targets:
            pl.semaphore_signal(barrier, inc=1, device_id=target, device_id_type=MESH_ID)
        pl.semaphore_wait(barrier, len(targets))


def remote(src, dst, send_sem, recv_sem, target):
    return pltpu.make_async_remote_copy(
        src_ref=src,
        dst_ref=dst,
        send_sem=send_sem,
        recv_sem=recv_sem,
        device_id=target,
        device_id_type=MESH_ID,
    )


def gather_sems(pb_count, neg_count):
    line_count = neg_count // 2
    dma = pltpu.SemaphoreType.DMA
    return [dma((line_count,)), dma((2, line_count)), dma((line_count,)), dma((2,))]


class Gather:
    def __init__(self, place, own, full, sems, halve_corner):
        self.place, self.own, self.full = place, own, full
        self.line_recv, self.pb_recv, self.corner_recv, ends = sems
        self.send_sem, self.core_recv = ends.at[0], ends.at[1]
        self.halve_corner = halve_corner
        across = place.pb + 1 - 2 * (place.pb % 2)
        along = place.pb + 2 - 4 * (place.pb // 2)
        self.near = (across, along)
        self.corner = 3 - place.pb
        half = place.line // 2
        self.is_inner = (place.line == 1) | (place.line == 2)
        self.mate = place.line + 1 - 2 * (place.line % 2)
        self.far_inner = 2 - half
        self.far_outer = 3 - 3 * half
        self.size = own.shape[0]
        if halve_corner:
            self.own_lines = (place.line, lax.rem(place.line + 2, 4))
            self.mate_lines = (self.mate, lax.rem(self.mate + 2, 4))
        else:
            self.own_lines = (place.line, self.mate, self.far_inner, self.far_outer)
            self.mate_lines = ()

    def rows(self, pb, line, core):
        start = self.place.slot(pb, line, core) * self.size
        return self.full.at[pl.ds(pl.multiple_of(start, self.size), self.size)]

    def blocks(self, count):
        return self.full.at[pl.ds(0, count * self.size)]

    def send(self, src, dst, recv_sem, target):
        remote(src, dst, self.send_sem, recv_sem, target).start()

    def spread(self, src, line):
        at = self.place
        dst = self.rows(at.pb, line, at.core)
        for side in range(2):
            self.send(src, dst, self.pb_recv.at[side, line], at.to_pb(self.near[side]))
        self.pass_on(src, at.pb, line)

    def pass_on(self, src, pb, line):
        at = self.place
        self.send(src, self.rows(pb, line, at.core), self.core_recv, at.to_partner())

    def arrive(self, block, recv_sem):
        remote(block, block, self.send_sem, recv_sem, self.place.to_partner()).wait_recv()

    def start(self):
        at = self.place
        mine = self.rows(at.pb, at.line, at.core)
        for line in (self.mate, self.far_inner):
            self.send(self.own, mine, self.line_recv.at[at.line], at.to_line(line))
        self.spread(self.own, at.line)
        mine[...] = self.own[...]

    def middle(self):
        at = self.place
        for line in (self.mate, self.far_inner, self.far_outer):
            block = self.rows(at.pb, line, at.core)
            self.arrive(block, self.line_recv.at[line])
            if line is not self.mate:

                @pl.when(self.is_inner)
                def _():
                    self.send(block, block, self.line_recv.at[line], at.to_line(self.mate))

            self.spread(block, line)

    def half(self, block, side):
        size = block.shape[0] // 2
        return block.at[pl.ds(side * size, size)]

    def relay(self):
        at = self.place
        for line in self.own_lines + self.mate_lines:
            for side in range(2):
                block = self.rows(self.near[side], line, at.core)
                self.arrive(block, self.pb_recv.at[side, line])
                if not any(line is other for other in self.mate_lines):
                    part = self.half(block, side)
                    self.send(part, part, self.corner_recv.at[line], at.to_pb(self.near[1 - side]))
                self.pass_on(block, self.near[side], line)

    def corner_in(self, lines, hand_over):
        at = self.place
        for line in lines:
            block = self.rows(self.corner, line, at.core)
            self.arrive(block, self.corner_recv.at[line])
            if hand_over:
                self.send(block, block, self.corner_recv.at[line], at.to_line(self.mate))
            self.pass_on(block, self.corner, line)

    def hand(self):
        if self.halve_corner:
            self.corner_in(self.own_lines, True)

    def finish(self):
        at = self.place
        self.corner_in(self.mate_lines if self.halve_corner else self.own_lines, False)
        self.arrive(self.blocks(at.count // 2), self.core_recv)

    def drain(self):
        at = self.place
        block = self.blocks(at.count - 2)
        remote(block, block, self.send_sem, self.core_recv, at.to_partner()).wait_send()

        @pl.when(self.is_inner)
        def _():
            block = self.blocks(2)
            remote(block, block, self.send_sem, self.core_recv, at.to_partner()).wait_send()


VMEM_SPEC = pl.BlockSpec(memory_space=pltpu.VMEM)


def mm(left, right, left_dim=1, right_dim=0, precision=None):
    return lax.dot_general(
        left,
        right,
        (((left_dim,), (right_dim,)), ((), ())),
        preferred_element_type=jnp.float32,
        precision=precision,
    )


def lane_mean(array):
    return jnp.mean(array, axis=-1, keepdims=True)


def tile(array, index):
    return array[:, index * HEAD_WIDTH : (index + 1) * HEAD_WIDTH]


class Exchange:
    def __init__(self, at, src, dst, send_sem, recv_sem):
        self.at, self.src, self.dst = at, src, dst
        self.send_sem, self.recv_sem = send_sem, recv_sem

    def start(self):
        at = self.at
        for pb, neg in at.others:
            peer = pb * at.neg_count + neg
            remote(
                self.src.at[peer], self.dst.at[at.me], self.send_sem, self.recv_sem, (pb, neg)
            ).start()
        self.dst[at.me] = self.src[at.me]

    def wait(self, sem_of):
        block = self.dst.at[pl.ds(0, self.at.count - 1)]
        copy = remote(block, block, self.send_sem, self.recv_sem, self.at.to_partner())
        getattr(copy, sem_of)()


def step_kernel(
    sizes,
    hidden,
    lengths,
    teacher,
    norm_gain_in,
    final_gain_in,
    score_vector_in,
    cos_table_in,
    sin_table_in,
    own_q_in,
    own_k_in,
    own_v_in,
    own_o_in,
    scores_out,
    loss_out,
    grad_hidden,
    grad_query,
    grad_key,
    grad_value,
    grad_out,
    x,
    norm_gain,
    final_gain,
    score_vector,
    cos_table,
    sin_table,
    own_q,
    own_k,
    own_v,
    own_o,
    full_q,
    full_k,
    full_v,
    full_o,
    normed,
    inv_wide,
    key_unit,
    key_scale,
    key_rot,
    value_cast,
    grad_k,
    grad_v,
    logit_grad,
    probs_ref,
    query_blocks,
    context_blocks,
    last_grad,
    resid_grad,
    context_own,
    context_full,
    late_own,
    late_full,
    early_src,
    early_dst,
    resid_src,
    resid_dst,
    list_src,
    list_dst,
    partial,
    from_core,
    paired,
    from_pb,
    summed,
    from_line,
    early_sems,
    resid_sems,
    list_sems,
    core_send,
    core_recv,
    pb_send,
    pb_recv,
    line_send,
    line_recv,
    any_sem,
    load_sems,
    *gather_sem_refs,
):
    pairs, seq, groups, share = sizes
    bf16, f32 = jnp.bfloat16, jnp.float32
    at = Place()
    at.count = at.pb_count * at.neg_count
    at.me = at.slot(at.pb, at.line, at.core)
    neg = lax.axis_index("neg")
    pb_all = [at.pb] + [at.pb_peer(k) for k in range(1, at.pb_count)]
    neg_all = [neg] + [lax.rem(neg + k, at.neg_count) for k in range(1, at.neg_count)]
    at.others = [
        (pb, peer)
        for i, pb in enumerate(pb_all)
        for j, peer in enumerate(neg_all)
        if i + j > 0
    ]
    model = x.shape[1]
    rows_all = pairs * seq
    per_group = own_q.shape[1] // own_k.shape[1]
    slots = per_group * pairs
    stacked = groups * slots
    kv_width = groups * HEAD_WIDTH

    barrier = pltpu.get_barrier_semaphore()

    for target in at.others:
        pl.semaphore_signal(barrier, inc=1, device_id=target, device_id_type=MESH_ID)
    loads = []
    moves = (
        (own_k_in, own_k),
        (own_v_in, own_v),
        (own_q_in, own_q),
        (own_o_in, own_o),
        (norm_gain_in, norm_gain),
        (final_gain_in, final_gain),
        (score_vector_in, score_vector),
        (cos_table_in, cos_table),
        (sin_table_in, sin_table),
    )
    small_loads = []
    for place_of, (source, target) in enumerate(moves):
        load = pltpu.make_async_copy(source, target, load_sems.at[pairs + place_of])
        load.start()
        small_loads.append(load)
    for pair in range(pairs):
        rows = pl.ds(pair * seq, seq)
        load = pltpu.make_async_copy(hidden.at[rows], x.at[rows], load_sems.at[pair])
        load.start()
        loads.append(load)

    half_width = own_q.shape[1] // 2
    low, high = pl.ds(0, half_width), pl.ds(half_width, half_width)
    parts = (
        (own_k, full_k, True),
        (own_v, full_v, True),
        (own_q.at[:, low], full_q.at[:, low], True),
        (own_q.at[:, high], full_q.at[:, high], True),
        (own_o.at[:, low], full_o.at[:, low], True),
        (own_o.at[:, high], full_o.at[:, high], False),
        (context_own, context_full, False),
        (late_own, late_full, False),
    )
    each = len(gather_sem_refs) // len(parts)
    gathers = [
        Gather(at, own, full, gather_sem_refs[i * each : (i + 1) * each], halve)
        for i, (own, full, halve) in enumerate(parts)
    ]
    gather_k, gather_v, gather_q0, gather_q1, gather_o0, gather_o1 = gathers[:6]
    gather_context, gather_late = gathers[6:]

    def norm_pair(pair, carry):
        rows = pl.ds(pl.multiple_of(pair * seq, seq), seq)
        wide = x[rows, :].astype(f32)
        inv = lax.rsqrt(lane_mean(wide * wide) + EPSILON)
        inv_wide[rows, :] = jnp.broadcast_to(inv, (seq, HEAD_WIDTH))
        normed[rows, :] = (wide * inv * norm_gain[...]).astype(bf16)
        return carry

    for load in small_loads:
        load.wait()
    for pair in range(pairs):
        loads[pair].wait()
        norm_pair(pair, 0)

    row8 = lax.broadcasted_iota(jnp.int32, (slots, 1), 0)
    pair8 = lax.rem(row8, pairs)
    upper8 = row8 < pairs
    last8 = jnp.zeros((slots, 1), jnp.int32)
    teacher8 = jnp.zeros((slots, 1), f32)
    for pair in range(pairs):
        last8 = jnp.where(pair8 == pair, lengths[0, pair] - 1, last8)
        teacher8 = jnp.where(pair8 == pair, teacher[0, pair], teacher8)
    place8 = pair8 * seq + last8
    column8 = lax.broadcasted_iota(jnp.int32, (slots, rows_all), 1)
    onehot8 = (column8 == place8).astype(f32).astype(bf16)
    visible8 = (column8 >= pair8 * seq) & (column8 <= place8)
    visible = jnp.concatenate([visible8.astype(f32)] * groups, axis=0) > 0.5
    position8 = (lax.broadcasted_iota(jnp.int32, (slots, seq), 1) == last8).astype(f32)

    x_last = mm(onehot8, x[...])
    normed_last = mm(onehot8, normed[...]).astype(bf16)
    cos8 = mm(position8, cos_table[...], precision=lax.Precision.HIGHEST)
    sin8 = mm(position8, sin_table[...], precision=lax.Precision.HIGHEST)
    cos_rows = jnp.concatenate([cos8] * groups, axis=0)
    sin_rows = jnp.concatenate([sin8] * groups, axis=0)

    pl.semaphore_wait(barrier, at.count - 1)
    for gather in gathers[:6]:
        gather.start()
    gather_k.middle()
    gather_v.middle()
    gather_k.relay()
    gather_q0.middle()
    gather_v.relay()
    gather_k.hand()
    gather_q1.middle()
    gather_q0.relay()
    gather_v.hand()
    gather_k.finish()

    def key_pair(pair, carry):
        rows = pl.ds(pl.multiple_of(pair * seq, seq), seq)
        proj = mm(normed[rows, :], full_k[...])
        for group in range(groups):
            lanes = slice(group * HEAD_WIDTH, (group + 1) * HEAD_WIDTH)
            part = proj[:, lanes]
            scale = lax.rsqrt(lane_mean(part * part) + EPSILON)
            unit = part * scale
            key_unit[rows, lanes] = unit
            key_scale[rows, lanes] = jnp.broadcast_to(scale, (seq, HEAD_WIDTH))
            turned = unit * cos_table[...] + pltpu.roll(unit, HEAD_WIDTH // 2, 1) * sin_table[...]
            key_rot[rows, lanes] = turned.astype(bf16)
        return carry

    def value_pair(pair, carry):
        rows = pl.ds(pl.multiple_of(pair * seq, seq), seq)
        value_cast[rows, :] = mm(normed[rows, :], full_v[...]).astype(bf16)
        return carry

    key_pair(0, 0)
    gather_o0.middle()
    key_pair(1, 0)
    gather_q1.relay()
    gather_q0.hand()
    key_pair(2, 0)
    gather_v.finish()
    key_pair(3, 0)
    gather_o1.middle()
    gather_o0.relay()
    gather_q1.hand()
    value_pair(0, 0)
    value_pair(1, 0)
    gather_q0.finish()
    gather_o1.relay()
    gather_o0.hand()
    value_pair(2, 0)
    value_pair(3, 0)
    gather_q1.finish()

    def stack_heads(wide):
        return jnp.concatenate(
            [
                jnp.where(upper8, tile(wide, per_group * group), tile(wide, per_group * group + 1))
                for group in range(groups)
            ],
            axis=0,
        )

    def spread_heads(stack):
        parts = []
        for group in range(groups):
            part = stack[group * slots : (group + 1) * slots]
            parts += [jnp.where(upper8, part, 0.0), jnp.where(upper8, 0.0, part)]
        return jnp.concatenate(parts, axis=1).astype(bf16)

    def diagonal_of(wide):
        return jnp.concatenate(
            [
                wide[group * slots : (group + 1) * slots, group * HEAD_WIDTH : (group + 1) * HEAD_WIDTH]
                for group in range(groups)
            ],
            axis=0,
        )

    def blocks_of(stack):
        rows = []
        for group in range(groups):
            part = stack[group * slots : (group + 1) * slots]
            rows.append(
                jnp.concatenate(
                    [part if other == group else jnp.zeros_like(part) for other in range(groups)],
                    axis=1,
                )
            )
        return jnp.concatenate(rows, axis=0).astype(bf16)

    query_proj = stack_heads(mm(normed_last, full_q[...]))
    query_scale = lax.rsqrt(lane_mean(query_proj * query_proj) + EPSILON)
    query_unit = query_proj * query_scale
    query_rot = query_unit * cos_rows + pltpu.roll(query_unit, HEAD_WIDTH // 2, 1) * sin_rows
    query_wide = blocks_of(query_rot)
    query_blocks[...] = query_wide
    logits = mm(query_wide, key_rot[...], 1, 1) * HEAD_WIDTH ** (-0.5)
    expos = jnp.where(visible, jnp.exp(logits), 0.0)
    attention_weights = expos / jnp.sum(expos, axis=-1, keepdims=True)
    probs = attention_weights.astype(bf16)
    probs_ref[...] = probs
    context = diagonal_of(mm(probs, value_cast[...]))
    context_own[...] = context.astype(bf16)
    context_wide = spread_heads(context)
    gather_context.start()

    lane_block = lax.rem(
        lax.broadcasted_iota(jnp.int32, (slots, model), 1) // share, HEAD_WIDTH // share
    )

    def pack(parts, turn):
        total = jnp.zeros((slots, model), f32)
        for block, part in enumerate(parts):
            shift = ((block - turn) * share) % model
            moved = part if shift == 0 else pltpu.roll(part, shift, 1)
            total = jnp.where(lane_block == block, moved, total)
        return total

    def by_head(wide):
        return [jnp.where(upper8, wide, 0.0), jnp.where(upper8, 0.0, wide)]

    turns = HEAD_WIDTH // share
    pulled = mm(probs, normed[...])
    pulled_parts = [pulled[group * slots : (group + 1) * slots] for group in range(groups)]
    last_parts = by_head(normed_last.astype(f32))
    for turn in range(turns):
        both = jnp.concatenate([pack(pulled_parts, turn), pack(last_parts, turn)], axis=0)
        both = both.astype(bf16)
        for index in range(model // HEAD_WIDTH):
            early_src[index * turns + turn] = tile(both, index)

    early = Exchange(at, early_src, early_dst, early_sems.at[0], early_sems.at[1])
    early.start()

    gather_o0.finish()
    gather_o1.finish()
    attended = mm(context_wide, full_o[...], 1, 1)
    attended = attended + pltpu.roll(attended, pairs, 0)
    residual = x_last + attended
    out_scale = lax.rsqrt(lane_mean(residual * residual) + EPSILON)
    out_unit = residual * out_scale
    gain = final_gain[...] * score_vector[...]
    score8 = jnp.sum(out_unit * gain, axis=-1, keepdims=True)

    lane8 = lax.broadcasted_iota(jnp.int32, (slots, HEAD_WIDTH), 1)
    row_lane = lax.broadcasted_iota(jnp.int32, (slots, HEAD_WIDTH), 0)

    def as_row(column):
        return jnp.sum(jnp.where(row_lane == lane8, column, 0.0), axis=0, keepdims=True)

    score_row = as_row(score8)
    lane1 = lax.broadcasted_iota(jnp.int32, (1, HEAD_WIDTH), 1)
    listing = jnp.where(lane1 < pairs, score_row, as_row(teacher8))
    list_src[...] = listing
    me_row = list_dst.at[at.me]
    list_here, list_there, list_sent = list_sems.at[0], list_sems.at[1], list_sems.at[2]
    for place_of, target in enumerate(at.others):
        arrived = list_here if place_of < at.neg_count - 1 else list_there
        remote(list_src, me_row, list_sent, arrived, target).start()
    list_dst[at.me] = listing
    scores_out[...] = score_row[:, :pairs]
    gather_context.middle()
    gather_context.relay()

    near_block = list_dst.at[pl.ds(0, at.neg_count - 1)]
    remote(near_block, near_block, list_sent, list_here, at.to_partner()).wait_recv()

    def total(array):
        return jnp.sum(jnp.sum(array, axis=1, keepdims=True), axis=0, keepdims=True)

    def query_terms(first):
        block = list_dst[pl.ds(first, at.neg_count)].reshape(at.neg_count, HEAD_WIDTH)
        real = lax.broadcasted_iota(jnp.int32, block.shape, 1) < pairs
        score = jnp.where(real, block, 0.0)
        scaled = pltpu.roll(block, HEAD_WIDTH - pairs, 1)
        scaled = jnp.where(real, scaled, 0.0) / TEACHER_TEMP
        expo_t = jnp.where(real, jnp.exp(scaled), 0.0)
        total_s = total(jnp.where(real, jnp.exp(score), 0.0))
        return score, scaled, expo_t, total_s, total(expo_t)

    _, _, _, total_s, total_t = query_terms(pl.multiple_of(at.pb * at.neg_count, at.neg_count))
    grad_score = GRAD_SCALE * (
        jnp.exp(score8) / total_s - jnp.exp(teacher8 / TEACHER_TEMP) / total_t
    )
    grad_unit = grad_score * gain
    grad_resid = out_scale * (grad_unit - out_unit * lane_mean(grad_unit * out_unit))
    resid_grad[...] = grad_resid
    resid_cast = grad_resid.astype(bf16)
    grad_context = stack_heads(mm(resid_cast, full_o[...])).astype(bf16)
    context_blocks[...] = blocks_of(grad_context.astype(f32))
    late_own[0:stacked, :] = grad_context

    grad_probs = mm(context_blocks[...], value_cast[...], 1, 1)
    spread = jnp.sum(attention_weights * grad_probs, axis=-1, keepdims=True)
    logit_gradient = (attention_weights * (grad_probs - spread)).astype(bf16)
    logit_grad[...] = logit_gradient

    turned_q = diagonal_of(mm(logit_gradient, key_rot[...])) * HEAD_WIDTH ** (-0.5)
    back_q = turned_q * cos_rows - pltpu.roll(turned_q, HEAD_WIDTH // 2, 1) * sin_rows
    back_q = query_scale * (back_q - query_unit * lane_mean(back_q * query_unit))
    grad_q_cast = back_q.astype(bf16)
    late_own[stacked : 2 * stacked, :] = grad_q_cast
    gather_late.start()

    def key_back(pair, carry):
        start = pl.multiple_of(pair * seq, seq)
        rows = pl.ds(start, seq)
        turned = mm(logit_grad[:, rows], query_blocks[...], 0, 0) * HEAD_WIDTH ** (-0.5)
        for group in range(groups):
            lanes = slice(group * HEAD_WIDTH, (group + 1) * HEAD_WIDTH)
            part = turned[:, lanes]
            unit = key_unit[rows, lanes]
            back = part * cos_table[...] - pltpu.roll(part, HEAD_WIDTH // 2, 1) * sin_table[...]
            back = key_scale[rows, lanes] * (back - unit * lane_mean(back * unit))
            grad_k[rows, lanes] = back.astype(bf16)
        return carry

    lax.fori_loop(0, pairs, key_back, 0)

    block_rows = model // at.pb_count
    copies = []

    def send(src, dst, send_sem, recv_sem, target):
        copy = remote(src, dst, send_sem, recv_sem, target)
        copy.start()
        copies.append(copy)

    def arrive(block, recv_sem):
        remote(block, block, any_sem, recv_sem, at.to_partner()).wait_recv()

    for k in range(1, at.pb_count + 1):
        pb = at.pb_peer(k % at.pb_count)
        lanes = pl.ds(pl.multiple_of(pb * block_rows, block_rows), block_rows)
        product = mm(normed[:, lanes], grad_k[...], 0, 0)
        partial[pb] = product.astype(bf16).reshape(at.line_count, 2, share, kv_width)
        send(
            partial.at[pb, :, at.partner],
            from_core.at[pb],
            core_send.at[pb],
            core_recv.at[pb],
            at.to_partner(),
        )

    for k in range(1, at.pb_count + 1):
        pb = at.pb_peer(k % at.pb_count)
        arrive(from_core.at[pb], core_recv.at[pb])
        both = partial[pb, :, at.core].astype(f32) + from_core[pb].astype(f32)
        paired[pb] = both.astype(bf16)
    gather_late.middle()
    for step in range(1, at.line_count + 1):
        line = at.line_peer(step % at.line_count)
        for k in range(1, at.pb_count):
            pb = at.pb_peer(k)
            send(
                paired.at[pb, line],
                from_pb.at[at.pb, line],
                pb_send.at[k, line],
                pb_recv.at[at.pb, line],
                at.to_pb(pb),
            )

    resid_parts = by_head(resid_cast.astype(f32))
    for turn in range(turns):
        packed = pack(resid_parts, turn).astype(bf16)
        for index in range(model // HEAD_WIDTH):
            resid_src[index * turns + turn] = tile(packed, index)
    resid = Exchange(at, resid_src, resid_dst, resid_sems.at[0], resid_sems.at[1])
    resid.start()

    back_last = mm(spread_heads(grad_q_cast.astype(f32)), full_q[...], 1, 1)
    last_grad[...] = back_last + pltpu.roll(back_last, pairs, 0)

    def value_back(pair, carry):
        start = pl.multiple_of(pair * seq, seq)
        rows = pl.ds(start, seq)
        grad_v[rows, :] = mm(probs_ref[:, rows], context_blocks[...], 0, 0).astype(bf16)
        return carry

    lax.fori_loop(0, pairs, value_back, 0)

    seq_row = lax.broadcasted_iota(jnp.int32, (seq, 1), 0)

    def hidden_back(pair, carry):
        rows = pl.ds(pl.multiple_of(pair * seq, seq), seq)
        total = mm(grad_k[rows, :], full_k[...], 1, 1) + mm(grad_v[rows, :], full_v[...], 1, 1)
        hit = seq_row == lengths[0, pair] - 1
        total = total + jnp.where(hit, last_grad[pl.ds(pair, 1), :], 0.0)
        scaled = total * norm_gain[...]
        wide = x[rows, :].astype(f32)
        inv = inv_wide[rows, 0:1]
        mean = lane_mean(scaled * wide)
        result = inv * scaled - wide * (inv * inv * inv * mean)
        result = result + jnp.where(hit, resid_grad[pl.ds(pair, 1), :], 0.0)
        grad_hidden[rows, :] = result.astype(bf16)
        return carry

    def add_line(step):
        line = at.line_peer(step % at.line_count)
        total = paired[at.pb, line].astype(f32)
        for k in range(1, at.pb_count):
            pb = at.pb_peer(k)
            arrive(from_pb.at[pb, line], pb_recv.at[pb, line])
            total = total + from_pb[pb, line].astype(f32)
        if step < at.line_count:
            summed[line] = total.astype(bf16)
            send(
                summed.at[line],
                from_line.at[at.line],
                line_send.at[line],
                line_recv.at[at.line],
                at.to_line(line),
            )
        return total

    hidden_back(0, 0)
    add_line(1)
    hidden_back(1, 0)
    add_line(2)
    hidden_back(2, 0)
    for step in range(3, at.line_count + 1):
        own_sum = add_line(step)
    gather_late.relay()
    gather_context.finish()
    for pair in range(3, pairs):
        hidden_back(pair, 0)

    far_block = list_dst.at[pl.ds(0, at.count - at.neg_count)]
    remote(far_block, far_block, list_sent, list_there, at.to_partner()).wait_recv()
    loss = jnp.zeros((1, 1), f32)
    for pb in range(at.pb_count):
        score, scaled, expo_t, sum_s, sum_t = query_terms(pb * at.neg_count)
        loss = loss + total(expo_t / sum_t * (scaled - jnp.log(sum_t) - (score - jnp.log(sum_s))))
    loss_out[...] = loss

    gather_late.finish()
    early.wait("wait_recv")
    resid.wait("wait_recv")

    def rows_of(full, start, group):
        wide = full[...].astype(f32).reshape(at.count, -1, slots, HEAD_WIDTH)
        return wide[:, start + group].reshape(at.count * slots, HEAD_WIDTH).astype(bf16)

    pulled_rows = rows_of(early_dst, 0, 0)
    last_rows = rows_of(early_dst, 1, 0)
    resid_rows = rows_of(resid_dst, 0, 0)
    for group in range(groups):
        found = mm(pulled_rows, rows_of(late_full, 0, group), 0, 0)
        lanes = slice(group * HEAD_WIDTH, (group + 1) * HEAD_WIDTH)
        grad_value[:, lanes] = found[group * share : (group + 1) * share]
        found = mm(last_rows, rows_of(late_full, groups, group), 0, 0)
        for part in range(per_group):
            head = per_group * group + part
            grad_query[:, head * HEAD_WIDTH : (head + 1) * HEAD_WIDTH] = found[
                part * share : (part + 1) * share
            ]
        found = mm(resid_rows, rows_of(context_full, 0, group), 0, 0)
        for part in range(per_group):
            head = per_group * group + part
            grad_out[:, head * HEAD_WIDTH : (head + 1) * HEAD_WIDTH] = found[
                part * share : (part + 1) * share
            ]

    final = own_sum
    for step in range(1, at.line_count):
        line = at.line_peer(step)
        arrive(from_line.at[line], line_recv.at[line])
        final = final + from_line[line].astype(f32)
    grad_key[...] = final

    for gather in gathers:
        gather.drain()
    for copy in copies:
        copy.wait_send()
    early.wait("wait_send")
    resid.wait("wait_send")
    sent_block = list_dst.at[pl.ds(0, at.count - 1)]
    remote(sent_block, sent_block, list_sent, list_here, at.to_partner()).wait_send()


def write_kernel(count, *refs):
    sources, targets, sems = refs[:count], refs[count : 2 * count], refs[2 * count]
    copies = [
        pltpu.make_async_copy(sources[i], targets[i], sems.at[i]) for i in range(2, count)
    ]
    for copy in copies:
        copy.start()
    for i in range(2):
        targets[i][...] = sources[i][...]
    for copy in copies:
        copy.wait()


def write_outputs(arrays):
    count = len(arrays)
    return pl.pallas_call(
        functools.partial(write_kernel, count),
        out_shape=tuple(jax.ShapeDtypeStruct(a.shape, a.dtype) for a in arrays),
        in_specs=[VMEM_SPEC] * count,
        out_specs=(VMEM_SPEC,) * 2 + (pl.BlockSpec(memory_space=pl.ANY),) * (count - 2),
        scratch_shapes=[pltpu.SemaphoreType.DMA((count,))],
        compiler_params=pltpu.CompilerParams(vmem_limit_bytes=4 * 2**20),
    )(*arrays)


def run_step(operands, sizes, pb_count, neg_count):
    pairs, seq, groups, share = sizes
    x, own_q, own_k = operands[0], operands[8], operands[9]
    model, width, kv_width = x.shape[1], own_q.shape[1], own_k.shape[1]
    rows = pairs * seq
    count = pb_count * neg_count
    line_count = neg_count // 2
    slots = width // kv_width * pairs
    stacked = groups * slots
    bf16, f32 = jnp.bfloat16, jnp.float32
    block = (pb_count, line_count, share, kv_width)
    dma = pltpu.SemaphoreType.DMA
    vmem = pltpu.VMEM
    smem_spec = pl.BlockSpec(memory_space=pltpu.SMEM)
    hbm_spec = pl.BlockSpec(memory_space=pltpu.HBM)
    return pl.pallas_call(
        functools.partial(step_kernel, sizes),
        out_shape=(
            vmem((1, pairs), f32),
            vmem((1, 1), f32),
            vmem((rows, model), bf16),
            vmem((share, width), f32),
            vmem((share, kv_width), f32),
            vmem((share, kv_width), f32),
            vmem((share, width), f32),
        ),
        in_specs=[hbm_spec, smem_spec, smem_spec] + [hbm_spec] * 9,
        out_specs=(VMEM_SPEC,) * 7,
        scratch_shapes=[
            vmem((rows, model), bf16),
        ]
        + [vmem(a.shape, a.dtype) for a in operands[3:]]
        + [
            vmem((model, width), bf16),
            vmem((model, kv_width), bf16),
            vmem((model, kv_width), bf16),
            vmem((model, width), bf16),
            vmem((rows, model), bf16),
            vmem((rows, HEAD_WIDTH), f32),
            vmem((rows, kv_width), f32),
            vmem((rows, kv_width), f32),
            vmem((rows, kv_width), bf16),
            vmem((rows, kv_width), bf16),
            vmem((rows, kv_width), bf16),
            vmem((rows, kv_width), bf16),
            vmem((stacked, rows), bf16),
            vmem((stacked, rows), bf16),
            vmem((stacked, kv_width), bf16),
            vmem((stacked, kv_width), bf16),
            vmem((slots, model), f32),
            vmem((slots, model), f32),
            vmem((stacked, HEAD_WIDTH), bf16),
            vmem((stacked * count, HEAD_WIDTH), bf16),
            vmem((2 * stacked, HEAD_WIDTH), bf16),
            vmem((2 * stacked * count, HEAD_WIDTH), bf16),
            vmem((count, 2 * slots, HEAD_WIDTH), bf16),
            vmem((count, 2 * slots, HEAD_WIDTH), bf16),
            vmem((count, slots, HEAD_WIDTH), bf16),
            vmem((count, slots, HEAD_WIDTH), bf16),
            vmem((1, HEAD_WIDTH), f32),
            vmem((count, 1, HEAD_WIDTH), f32),
            vmem((pb_count, line_count, 2, share, kv_width), bf16),
            vmem(block, bf16),
            vmem(block, bf16),
            vmem(block, bf16),
            vmem(block[1:], bf16),
            vmem(block[1:], bf16),
            dma((2,)),
            dma((2,)),
            dma((3,)),
            dma((pb_count,)),
            dma((pb_count,)),
            dma((pb_count, line_count)),
            dma((pb_count, line_count)),
            dma((line_count,)),
            dma((line_count,)),
            dma,
            dma((pairs + 9,)),
        ]
        + gather_sems(pb_count, neg_count) * 8,
        compiler_params=pltpu.CompilerParams(
            collective_id=0, has_side_effects=True, vmem_limit_bytes=62 * 2**20
        ),
    )(*operands)


def shards(
    hidden,
    lengths,
    teacher,
    norm_gain,
    final_gain,
    score_vector,
    query_weight,
    key_matrix,
    value_matrix,
    out_weight,
):
    both = ("pb", "neg")
    width = query_weight.shape[1]
    kv_width = key_matrix.shape[1]
    share, out_share = query_weight.shape[0], out_weight.shape[1]
    pb_count, neg_count = lax.axis_size("pb"), lax.axis_size("neg")
    pair_count, seq_len, model_width = hidden.shape[1:]
    group_count = kv_width // HEAD_WIDTH
    own_kernels = (
        pb_count == 4
        and neg_count == 8
        and share == out_share
        and share % 32 == 0
        and model_width == share * pb_count * neg_count
        and width == 2 * kv_width
        and pair_count * 2 == 8
        and seq_len == HEAD_WIDTH
        and share * group_count == HEAD_WIDTH
    )
    if own_kernels:
        cos_table, sin_table = signed_tables(seq_len, HEAD_WIDTH)
        results = run_step(
            (
                hidden.reshape(pair_count * seq_len, model_width),
                lengths,
                teacher,
                norm_gain[None],
                final_gain[None],
                score_vector[None],
                cos_table,
                sin_table,
                query_weight,
                key_matrix,
                value_matrix,
                out_weight.T,
            ),
            (pair_count, seq_len, group_count, share),
            pb_count,
            neg_count,
        )
        scores, loss, grad_rows, grad_query, grad_key, grad_value, grad_out = write_outputs(results)
        return (
            scores,
            loss.reshape(()),
            grad_rows.reshape(hidden.shape),
            grad_query,
            grad_key,
            grad_value,
            grad_out.T,
        )
    packed = jnp.concatenate([query_weight, key_matrix, value_matrix, out_weight.T], axis=1)
    everything = lax.all_gather(packed, both, axis=0, tiled=True)
    full_query = everything[:, :width]
    full_key = everything[:, width : width + kv_width]
    full_value = everything[:, width + kv_width : width + 2 * kv_width]
    full_out_t = everything[:, width + 2 * kv_width :]
    weights = (full_query, full_key, full_value, full_out_t.T)
    scores_here, stored = forward_pairs(
        hidden[0], lengths[0], norm_gain, final_gain, score_vector, *weights
    )
    listing = jnp.concatenate([scores_here, teacher[0]])[None]
    listed = lax.all_gather(listing, "neg", axis=0, tiled=True)
    all_scores = listed[:, :pair_count]
    all_scaled = listed[:, pair_count:] / TEACHER_TEMP
    my_total_s = jnp.sum(jnp.exp(all_scores))
    expo_t = jnp.exp(all_scaled)
    my_total_t = jnp.sum(expo_t)
    loss_here = jnp.sum(
        expo_t
        / my_total_t
        * (all_scaled - jnp.log(my_total_t) - (all_scores - jnp.log(my_total_s)))
    )
    prob_s = jnp.exp(scores_here) / my_total_s
    prob_t = jnp.exp(teacher[0] / TEACHER_TEMP) / my_total_t
    grad_score = GRAD_SCALE * (prob_s - prob_t)
    grad_input, last_rows, grad_kv = backward_pairs(
        stored, grad_score, norm_gain, final_gain, score_vector, *weights
    )
    grad_kv = grad_kv.astype(jnp.bfloat16)
    reduced = lax.psum_scatter(grad_kv, both, scatter_dimension=0, tiled=True)
    reduced = reduced.astype(jnp.float32)
    rows = lax.all_gather(last_rows, both, axis=0, tiled=True)
    loss_value = lax.psum(loss_here, "pb")
    index = lax.axis_index("pb") * neg_count + lax.axis_index("neg")
    normed_cols = lax.dynamic_slice_in_dim(rows, index * share, share, axis=1)
    resid_cols = lax.dynamic_slice_in_dim(rows, model_width + index * out_share, out_share, axis=1)
    rest = 2 * model_width
    all_q = rows[:, rest : rest + width]
    all_context = rows[:, rest + width :]
    grad_query = jnp.dot(normed_cols.T, all_q, preferred_element_type=jnp.float32)
    grad_out = jnp.dot(all_context.T, resid_cols, preferred_element_type=jnp.float32)
    return (
        scores_here[None],
        loss_value,
        grad_input[None],
        grad_query,
        reduced[:, :kv_width],
        reduced[:, kv_width:],
        grad_out,
    )


def solution(mesh):
    placed = (
        P("pb", "neg", None, None),
        P("pb", "neg"),
        P("pb", "neg"),
        P(),
        P(),
        P(),
        P(("pb", "neg"), None),
        P(("pb", "neg"), None),
        P(("pb", "neg"), None),
        P(None, ("pb", "neg")),
    )
    return jax.shard_map(
        shards,
        mesh=mesh,
        in_specs=placed,
        out_specs=(
            P("pb", "neg"),
            P(),
            P("pb", "neg", None, None),
            P(("pb", "neg"), None),
            P(("pb", "neg"), None),
            P(("pb", "neg"), None),
            P(None, ("pb", "neg")),
        ),
        check_vma=False,
    )
```

```python
import functools

import jax
import jax.numpy as jnp
import numpy as np
from jax import lax
from jax.experimental import pallas as pl
from jax.experimental.pallas import tpu as pltpu
from jax.sharding import PartitionSpec as P

HEAD_WIDTH = 128
MESH_ID = pl.DeviceIdType.MESH

EPSILON = 1e-06
ROPE_BASE = 1000000.0
TEACHER_TEMP = 2.0
GRAD_SCALE = 512.0


def rope_tables(seq_len, head_size):
    half = head_size // 2
    freqs = ROPE_BASE ** (-(jnp.arange(half, dtype=jnp.float32) * 2.0) / head_size)
    angles = jnp.arange(seq_len, dtype=jnp.float32)[:, None] * freqs[None, :]
    angles = jnp.concatenate([angles, angles], axis=1)
    return (jnp.cos(angles), jnp.sin(angles))


def signed_tables(seq_len, head_size):
    half = head_size // 2
    freqs = ROPE_BASE ** (-(np.arange(half) * 2.0) / head_size)
    angles = np.arange(seq_len)[:, None] * freqs[None, :]
    cos = np.concatenate([np.cos(angles)] * 2, axis=1)
    sin = np.concatenate([-np.sin(angles), np.sin(angles)], axis=1)
    return (jnp.asarray(cos, jnp.float32), jnp.asarray(sin, jnp.float32))


def rotate_half(vector):
    half = vector.shape[-1] // 2
    return jnp.concatenate([-vector[..., half:], vector[..., :half]], axis=-1)


def unrotate_half(vector):
    half = vector.shape[-1] // 2
    return jnp.concatenate([vector[..., half:], -vector[..., :half]], axis=-1)


def forward_pairs(
    tokens_in,
    lengths_here,
    norm_gain,
    final_gain,
    score_vector,
    query_weight,
    key_matrix,
    value_matrix,
    out_weight,
):
    pair_count, seq_len, model_width = tokens_in.shape
    head_count = query_weight.shape[1] // HEAD_WIDTH
    group_count = key_matrix.shape[1] // HEAD_WIDTH
    group_size = head_count // group_count
    inputs_wide = tokens_in.astype(jnp.float32)
    inv_rms = lax.rsqrt(jnp.mean(inputs_wide * inputs_wide, axis=-1, keepdims=True) + EPSILON)
    normed = (inputs_wide * inv_rms * norm_gain).astype(jnp.bfloat16)
    flat_rows = normed.reshape(pair_count * seq_len, model_width)
    key_proj = jnp.dot(flat_rows, key_matrix, preferred_element_type=jnp.float32).reshape(
        pair_count, seq_len, group_count, HEAD_WIDTH
    )
    value_proj = jnp.dot(flat_rows, value_matrix, preferred_element_type=jnp.float32).reshape(
        pair_count, seq_len, group_count, HEAD_WIDTH
    )
    positions = jnp.arange(seq_len, dtype=jnp.int32)
    last_index = lengths_here - 1
    onehot = (positions[None, :] == last_index[:, None]).astype(jnp.float32)
    normed_last = jnp.take_along_axis(normed, last_index[:, None, None], axis=1)[:, 0]
    query_proj = jnp.dot(normed_last, query_weight, preferred_element_type=jnp.float32).reshape(
        pair_count, head_count, HEAD_WIDTH
    )
    query_scale = lax.rsqrt(jnp.mean(query_proj * query_proj, axis=-1, keepdims=True) + EPSILON)
    query_unit = query_proj * query_scale
    key_scale = lax.rsqrt(jnp.mean(key_proj * key_proj, axis=-1, keepdims=True) + EPSILON)
    key_unit = key_proj * key_scale
    cos_table, sin_table = rope_tables(seq_len, HEAD_WIDTH)
    cos_query = jnp.dot(onehot, cos_table, precision=lax.Precision.HIGHEST)
    sin_query = jnp.dot(onehot, sin_table, precision=lax.Precision.HIGHEST)
    query_rot = (
        query_unit * cos_query[:, None, :] + rotate_half(query_unit) * sin_query[:, None, :]
    ).astype(jnp.bfloat16)
    key_rot = (
        key_unit * cos_table[None, :, None, :] + rotate_half(key_unit) * sin_table[None, :, None, :]
    ).astype(jnp.bfloat16)
    value_cast = value_proj.astype(jnp.bfloat16)
    grouped = query_rot.reshape(pair_count, group_count, group_size, HEAD_WIDTH)
    logits = jnp.einsum(
        "pkgd,pskd->pkgs", grouped, key_rot, preferred_element_type=jnp.float32
    ) * HEAD_WIDTH ** (-0.5)
    visible = (positions[None, :] <= last_index[:, None])[:, None, None, :]
    expos = jnp.where(visible, jnp.exp(logits), 0.0)
    attention_weights = expos / jnp.sum(expos, axis=-1, keepdims=True)
    probs_cast = attention_weights.astype(jnp.bfloat16)
    context = jnp.einsum(
        "pkgs,pskd->pkgd", probs_cast, value_cast, preferred_element_type=jnp.float32
    )
    context = context.astype(jnp.bfloat16).reshape(pair_count, head_count * HEAD_WIDTH)
    attended = jnp.dot(context, out_weight, preferred_element_type=jnp.float32)
    residual = jnp.take_along_axis(inputs_wide, last_index[:, None, None], axis=1)[:, 0] + attended
    out_scale = lax.rsqrt(jnp.mean(residual * residual, axis=-1, keepdims=True) + EPSILON)
    out_unit = residual * out_scale
    scores_here = jnp.sum(out_unit * final_gain * score_vector, axis=-1)
    stored = (
        tokens_in,
        onehot,
        inv_rms,
        normed,
        normed_last,
        query_unit,
        query_scale,
        key_unit,
        key_scale,
        cos_query,
        sin_query,
        cos_table,
        sin_table,
        query_rot,
        key_rot,
        value_cast,
        attention_weights,
        probs_cast,
        context,
        out_unit,
        out_scale,
    )
    return (scores_here, stored)


def backward_pairs(
    stored,
    grad_score,
    norm_gain,
    final_gain,
    score_vector,
    query_weight,
    key_matrix,
    value_matrix,
    out_weight,
):
    (
        tokens_in,
        onehot,
        inv_rms,
        normed,
        normed_last,
        query_unit,
        query_scale,
        key_unit,
        key_scale,
        cos_query,
        sin_query,
        cos_table,
        sin_table,
        query_rot,
        key_rot,
        value_cast,
        attention_weights,
        probs_cast,
        context,
        out_unit,
        out_scale,
    ) = stored
    pair_count, seq_len, model_width = tokens_in.shape
    head_count = query_weight.shape[1] // HEAD_WIDTH
    group_count = key_matrix.shape[1] // HEAD_WIDTH
    group_size = head_count // group_count
    grad_unit = grad_score[:, None] * score_vector * final_gain
    grad_resid = out_scale * (
        grad_unit - out_unit * jnp.mean(grad_unit * out_unit, axis=-1, keepdims=True)
    )
    grad_resid_cast = grad_resid.astype(jnp.bfloat16)
    grad_context = jnp.dot(
        grad_resid_cast, out_weight.T, preferred_element_type=jnp.float32
    ).astype(jnp.bfloat16)
    grad_context = grad_context.reshape(pair_count, group_count, group_size, HEAD_WIDTH)
    grad_probs = jnp.einsum(
        "pkgd,pskd->pkgs", grad_context, value_cast, preferred_element_type=jnp.float32
    )
    grad_vals = jnp.einsum(
        "pkgs,pkgd->pskd", probs_cast, grad_context, preferred_element_type=jnp.float32
    )
    spread = jnp.sum(attention_weights * grad_probs, axis=-1, keepdims=True)
    logit_gradient = (attention_weights * (grad_probs - spread)).astype(jnp.bfloat16)
    grouped = query_rot.reshape(pair_count, group_count, group_size, HEAD_WIDTH)
    rotated_query_gradient = jnp.einsum(
        "pkgs,pskd->pkgd", logit_gradient, key_rot, preferred_element_type=jnp.float32
    ) * HEAD_WIDTH ** (-0.5)
    rotated_query_gradient = rotated_query_gradient.reshape(pair_count, head_count, HEAD_WIDTH)
    grad_krot = jnp.einsum(
        "pkgs,pkgd->pskd", logit_gradient, grouped, preferred_element_type=jnp.float32
    ) * HEAD_WIDTH ** (-0.5)
    grad_qunit = rotated_query_gradient * cos_query[:, None, :] + unrotate_half(
        rotated_query_gradient * sin_query[:, None, :]
    )
    grad_kunit = grad_krot * cos_table[None, :, None, :] + unrotate_half(
        grad_krot * sin_table[None, :, None, :]
    )
    grad_qproj = query_scale * (
        grad_qunit - query_unit * jnp.mean(grad_qunit * query_unit, axis=-1, keepdims=True)
    )
    grad_kproj = key_scale * (
        grad_kunit - key_unit * jnp.mean(grad_kunit * key_unit, axis=-1, keepdims=True)
    )
    grad_q_cast = grad_qproj.reshape(pair_count, head_count * HEAD_WIDTH).astype(jnp.bfloat16)
    grad_k_cast = grad_kproj.reshape(pair_count * seq_len, group_count * HEAD_WIDTH).astype(
        jnp.bfloat16
    )
    grad_v_cast = grad_vals.reshape(pair_count * seq_len, group_count * HEAD_WIDTH).astype(
        jnp.bfloat16
    )
    flat_rows = normed.reshape(pair_count * seq_len, model_width)
    last_rows = jnp.concatenate([normed_last, grad_resid_cast, grad_q_cast, context], axis=1)
    grad_kv = jnp.dot(
        flat_rows.T,
        jnp.concatenate([grad_k_cast, grad_v_cast], axis=1),
        preferred_element_type=jnp.float32,
    )
    grad_normed = jnp.dot(grad_k_cast, key_matrix.T, preferred_element_type=jnp.float32)
    grad_normed = grad_normed + jnp.dot(
        grad_v_cast, value_matrix.T, preferred_element_type=jnp.float32
    )
    grad_normed = grad_normed.reshape(pair_count, seq_len, model_width)
    grad_last = jnp.dot(grad_q_cast, query_weight.T, preferred_element_type=jnp.float32)
    grad_normed = grad_normed + onehot[:, :, None] * grad_last[:, None, :]
    inputs_wide = tokens_in.astype(jnp.float32)
    grad_scaled = grad_normed * norm_gain
    grad_input = inv_rms * grad_scaled - inputs_wide * inv_rms * inv_rms * inv_rms * jnp.mean(
        grad_scaled * inputs_wide, axis=-1, keepdims=True
    )
    grad_input = grad_input + onehot[:, :, None] * grad_resid[:, None, :]
    return (grad_input.astype(jnp.bfloat16), last_rows, grad_kv)


class Place:
    def __init__(self):
        self.pb_count = lax.axis_size("pb")
        self.neg_count = lax.axis_size("neg")
        self.line_count = self.neg_count // 2
        self.pb = lax.axis_index("pb")
        neg = lax.axis_index("neg")
        self.line = neg // 2
        self.core = neg % 2
        self.partner = 1 - self.core

    def slot(self, pb, line, core):
        return pb * self.neg_count + line * 2 + core

    def line_peer(self, step):
        return lax.rem(self.line + step, self.line_count)

    def pb_peer(self, step):
        return lax.rem(self.pb + step, self.pb_count)

    def to_line(self, line):
        return (self.pb, line * 2 + self.core)

    def to_pb(self, pb):
        return (pb, self.line * 2 + self.core)

    def to_partner(self):
        return (self.pb, self.line * 2 + self.partner)

    def greet(self):
        barrier = pltpu.get_barrier_semaphore()
        targets = [self.to_line(self.line_peer(k)) for k in range(1, self.line_count)]
        targets += [self.to_pb(self.pb_peer(k)) for k in range(1, self.pb_count)]
        targets += [self.to_partner()]
        for target in targets:
            pl.semaphore_signal(barrier, inc=1, device_id=target, device_id_type=MESH_ID)
        pl.semaphore_wait(barrier, len(targets))


def remote(src, dst, send_sem, recv_sem, target):
    return pltpu.make_async_remote_copy(
        src_ref=src,
        dst_ref=dst,
        send_sem=send_sem,
        recv_sem=recv_sem,
        device_id=target,
        device_id_type=MESH_ID,
    )


def gather_sems(neg_count, large):
    line_count = neg_count // 2
    dma = pltpu.SemaphoreType.DMA
    if large:
        return [dma((line_count,)), dma((line_count,)), dma((line_count,)), dma((2,))]
    return [dma((1,)), dma((1,)), dma((1,)), dma((2,))]


class Gather:
    def __init__(self, place, own, full, sems, halve_corner, direct):
        self.place, self.own, self.full = place, own, full
        self.line_recv, self.pb_recv, self.corner_recv, ends = sems
        self.send_sem, self.core_recv = ends.at[0], ends.at[1]
        self.halve_corner, self.direct = halve_corner, direct
        across = place.pb + 1 - 2 * (place.pb % 2)
        along = place.pb + 2 - 4 * (place.pb // 2)
        self.near = (across, along)
        self.corner = 3 - place.pb
        half = place.line // 2
        self.is_inner = (place.line == 1) | (place.line == 2)
        self.mate = place.line + 1 - 2 * (place.line % 2)
        self.far_inner = 2 - half
        self.far_outer = 3 - 3 * half
        self.size = own.shape[0]
        if halve_corner:
            self.own_lines = (place.line, lax.rem(place.line + 2, 4))
            self.mate_lines = (self.mate, lax.rem(self.mate + 2, 4))
        else:
            self.own_lines = (place.line, self.mate, self.far_inner, self.far_outer)
            self.mate_lines = ()

    def rows(self, pb, line, core):
        start = self.place.slot(pb, line, core) * self.size
        return self.full.at[pl.ds(pl.multiple_of(start, self.size), self.size)]

    def blocks(self, count):
        return self.full.at[pl.ds(0, count * self.size)]

    def send(self, src, dst, recv_sem, target):
        remote(src, dst, self.send_sem, recv_sem, target).start()

    def of(self, sems, line):
        return sems.at[0] if self.direct else sems.at[line]

    def spread(self, src, line):
        at = self.place
        dst = self.rows(at.pb, line, at.core)
        for side in range(2):
            self.send(src, dst, self.of(self.pb_recv, line), at.to_pb(self.near[side]))
        self.pass_on(src, at.pb, line)

    def pass_on(self, src, pb, line):
        at = self.place
        self.send(src, self.rows(pb, line, at.core), self.core_recv, at.to_partner())

    def arrive(self, block, recv_sem):
        remote(block, block, self.send_sem, recv_sem, self.place.to_partner()).wait_recv()

    def start(self):
        at = self.place
        mine = self.rows(at.pb, at.line, at.core)
        peers = (self.mate, self.far_inner) + ((self.far_outer,) if self.direct else ())
        for line in peers:
            self.send(self.own, mine, self.of(self.line_recv, at.line), at.to_line(line))
        self.spread(self.own, at.line)
        mine[...] = self.own[...]

    def middle(self):
        at = self.place
        if self.direct:
            self.arrive(self.blocks(at.line_count - 1), self.line_recv.at[0])
        for line in (self.mate, self.far_inner, self.far_outer):
            block = self.rows(at.pb, line, at.core)
            if not self.direct:
                self.arrive(block, self.line_recv.at[line])
                if line is not self.mate:

                    @pl.when(self.is_inner)
                    def _():
                        self.send(block, block, self.line_recv.at[line], at.to_line(self.mate))

            self.spread(block, line)

    def half(self, block, side):
        size = block.shape[0] // 2
        return block.at[pl.ds(side * size, size)]

    def relay(self):
        at = self.place
        if self.direct:
            self.arrive(self.blocks(2 * at.line_count), self.pb_recv.at[0])
        for line in self.own_lines + self.mate_lines:
            if not self.direct:
                self.arrive(self.blocks(2), self.pb_recv.at[line])
            for side in range(2):
                block = self.rows(self.near[side], line, at.core)
                if not any(line is other for other in self.mate_lines):
                    part = self.half(block, side)
                    target = at.to_pb(self.near[1 - side])
                    self.send(part, part, self.of(self.corner_recv, line), target)
                self.pass_on(block, self.near[side], line)

    def corner_in(self, lines, hand_over):
        at = self.place
        if self.direct:
            self.arrive(self.blocks(at.line_count), self.corner_recv.at[0])
        for line in lines:
            block = self.rows(self.corner, line, at.core)
            if not self.direct:
                self.arrive(block, self.corner_recv.at[line])
            if hand_over:
                self.send(block, block, self.corner_recv.at[line], at.to_line(self.mate))
            self.pass_on(block, self.corner, line)

    def hand(self):
        if self.halve_corner:
            self.corner_in(self.own_lines, True)

    def finish(self):
        at = self.place
        self.corner_in(self.mate_lines if self.halve_corner else self.own_lines, False)
        self.arrive(self.blocks(at.count // 2), self.core_recv)

    def drain(self):
        at = self.place
        block = self.blocks(at.count - (1 if self.direct else 2))
        remote(block, block, self.send_sem, self.core_recv, at.to_partner()).wait_send()
        if not self.direct:

            @pl.when(self.is_inner)
            def _():
                block = self.blocks(2)
                remote(block, block, self.send_sem, self.core_recv, at.to_partner()).wait_send()


VMEM_SPEC = pl.BlockSpec(memory_space=pltpu.VMEM)


def mm(left, right, left_dim=1, right_dim=0, precision=None):
    return lax.dot_general(
        left,
        right,
        (((left_dim,), (right_dim,)), ((), ())),
        preferred_element_type=jnp.float32,
        precision=precision,
    )


def lane_mean(array):
    return jnp.mean(array, axis=-1, keepdims=True)


def tile(array, index):
    return array[:, index * HEAD_WIDTH : (index + 1) * HEAD_WIDTH]


class Exchange:
    def __init__(self, at, src, dst, send_sem, recv_sem):
        self.at, self.src, self.dst = at, src, dst
        self.send_sem, self.recv_sem = send_sem, recv_sem

    def start(self):
        at = self.at
        for pb, neg in at.others:
            peer = pb * at.neg_count + neg
            remote(
                self.src.at[peer], self.dst.at[at.me], self.send_sem, self.recv_sem, (pb, neg)
            ).start()
        self.dst[at.me] = self.src[at.me]

    def wait(self, sem_of):
        block = self.dst.at[pl.ds(0, self.at.count - 1)]
        copy = remote(block, block, self.send_sem, self.recv_sem, self.at.to_partner())
        getattr(copy, sem_of)()


def step_kernel(
    sizes,
    hidden,
    lengths,
    teacher,
    norm_gain_in,
    final_gain_in,
    score_vector_in,
    cos_table_in,
    sin_table_in,
    own_q_in,
    own_k_in,
    own_v_in,
    own_o_in,
    scores_out,
    loss_out,
    grad_hidden,
    grad_query,
    grad_key,
    grad_value,
    grad_out,
    x,
    norm_gain,
    final_gain,
    score_vector,
    cos_table,
    sin_table,
    own_q,
    own_k,
    own_v,
    own_o,
    full_q,
    full_k,
    full_v,
    full_o,
    normed,
    normed_t,
    inv_wide,
    key_unit,
    key_scale,
    key_rot,
    value_cast,
    grad_k,
    grad_v,
    logit_grad,
    probs_ref,
    query_blocks,
    context_blocks,
    last_grad,
    resid_grad,
    context_own,
    context_full,
    late_own,
    late_full,
    early_src,
    early_dst,
    resid_src,
    resid_dst,
    list_src,
    list_dst,
    partial,
    from_core,
    paired,
    from_pb,
    summed,
    from_line,
    early_sems,
    resid_sems,
    list_sems,
    core_send,
    core_recv,
    pb_send,
    pb_recv,
    line_send,
    line_recv,
    any_sem,
    load_sems,
    *gather_sem_refs,
):
    pairs, seq, groups, share = sizes
    bf16, f32 = jnp.bfloat16, jnp.float32
    at = Place()
    at.count = at.pb_count * at.neg_count
    at.me = at.slot(at.pb, at.line, at.core)
    neg = lax.axis_index("neg")
    pb_all = [at.pb] + [at.pb_peer(k) for k in range(1, at.pb_count)]
    neg_all = [neg] + [lax.rem(neg + k, at.neg_count) for k in range(1, at.neg_count)]
    at.others = [
        (pb, peer)
        for i, pb in enumerate(pb_all)
        for j, peer in enumerate(neg_all)
        if i + j > 0
    ]
    model = x.shape[1]
    rows_all = pairs * seq
    per_group = own_q.shape[1] // own_k.shape[1]
    slots = per_group * pairs
    stacked = groups * slots
    kv_width = groups * HEAD_WIDTH

    barrier = pltpu.get_barrier_semaphore()

    for target in at.others:
        pl.semaphore_signal(barrier, inc=1, device_id=target, device_id_type=MESH_ID)
    loads = []
    moves = (
        (own_k_in, own_k),
        (own_v_in, own_v),
        (own_q_in, own_q),
        (own_o_in, own_o),
        (norm_gain_in, norm_gain),
        (final_gain_in, final_gain),
        (score_vector_in, score_vector),
        (cos_table_in, cos_table),
        (sin_table_in, sin_table),
    )
    small_loads = []
    for place_of, (source, target) in enumerate(moves):
        load = pltpu.make_async_copy(source, target, load_sems.at[pairs + place_of])
        load.start()
        small_loads.append(load)
    for pair in range(pairs):
        rows = pl.ds(pair * seq, seq)
        load = pltpu.make_async_copy(hidden.at[rows], x.at[rows], load_sems.at[pair])
        load.start()
        loads.append(load)

    half_width = own_q.shape[1] // 2
    low, high = pl.ds(0, half_width), pl.ds(half_width, half_width)
    parts = (
        (own_k, full_k, True),
        (own_v, full_v, True),
        (own_q.at[:, low], full_q.at[:, low], True),
        (own_q.at[:, high], full_q.at[:, high], True),
        (own_o.at[:, low], full_o.at[:, low], True),
        (own_o.at[:, high], full_o.at[:, high], False),
        (context_own, context_full, False),
        (late_own, late_full, False),
    )
    each = len(gather_sem_refs) // len(parts)
    gathers = [
        Gather(at, own, full, gather_sem_refs[i * each : (i + 1) * each], halve, i >= 6)
        for i, (own, full, halve) in enumerate(parts)
    ]
    gather_k, gather_v, gather_q0, gather_q1, gather_o0, gather_o1 = gathers[:6]
    gather_context, gather_late = gathers[6:]

    for load in small_loads:
        load.wait()
    pl.semaphore_wait(barrier, at.count - 1)
    for gather in gathers[:4]:
        gather.start()

    def norm_pair(pair, carry):
        rows = pl.ds(pl.multiple_of(pair * seq, seq), seq)
        wide = x[rows, :].astype(f32)
        inv = lax.rsqrt(lane_mean(wide * wide) + EPSILON)
        inv_wide[rows, :] = jnp.broadcast_to(inv, (seq, HEAD_WIDTH))
        scaled = wide * inv * norm_gain[...]
        normed[rows, :] = scaled.astype(bf16)
        normed_t[:, rows] = scaled.T.astype(bf16)
        return carry

    for pair in range(pairs):
        loads[pair].wait()
        norm_pair(pair, 0)

    row8 = lax.broadcasted_iota(jnp.int32, (slots, 1), 0)
    pair8 = lax.rem(row8, pairs)
    upper8 = row8 < pairs
    last8 = jnp.zeros((slots, 1), jnp.int32)
    teacher8 = jnp.zeros((slots, 1), f32)
    for pair in range(pairs):
        last8 = jnp.where(pair8 == pair, lengths[0, pair] - 1, last8)
        teacher8 = jnp.where(pair8 == pair, teacher[0, pair], teacher8)
    place8 = pair8 * seq + last8
    column8 = lax.broadcasted_iota(jnp.int32, (slots, rows_all), 1)
    onehot8 = (column8 == place8).astype(f32).astype(bf16)
    visible8 = (column8 >= pair8 * seq) & (column8 <= place8)
    visible = jnp.concatenate([visible8.astype(f32)] * groups, axis=0) > 0.5
    position8 = (lax.broadcasted_iota(jnp.int32, (slots, seq), 1) == last8).astype(f32)

    x_last = mm(onehot8, x[...])
    normed_last = mm(onehot8, normed[...]).astype(bf16)
    cos8 = mm(position8, cos_table[...], precision=lax.Precision.HIGHEST)
    sin8 = mm(position8, sin_table[...], precision=lax.Precision.HIGHEST)
    cos_rows = jnp.concatenate([cos8] * groups, axis=0)
    sin_rows = jnp.concatenate([sin8] * groups, axis=0)

    def key_pair(pair, carry):
        rows = pl.ds(pl.multiple_of(pair * seq, seq), seq)
        proj = mm(normed[rows, :], full_k[...])
        for group in range(groups):
            lanes = slice(group * HEAD_WIDTH, (group + 1) * HEAD_WIDTH)
            part = proj[:, lanes]
            scale = lax.rsqrt(lane_mean(part * part) + EPSILON)
            unit = part * scale
            key_unit[rows, lanes] = unit
            key_scale[rows, lanes] = jnp.broadcast_to(scale, (seq, HEAD_WIDTH))
            turned = unit * cos_table[...] + pltpu.roll(unit, HEAD_WIDTH // 2, 1) * sin_table[...]
            key_rot[rows, lanes] = turned.astype(bf16)
        return carry

    def value_pair(pair, carry):
        rows = pl.ds(pl.multiple_of(pair * seq, seq), seq)
        value_cast[rows, :] = mm(normed[rows, :], full_v[...]).astype(bf16)
        return carry

    gather_k.middle()
    gather_o0.start()
    gather_o1.start()
    gather_v.middle()
    gather_q0.middle()
    gather_k.relay()
    gather_q1.middle()
    gather_v.relay()
    gather_k.hand()
    gather_o0.middle()
    gather_o1.middle()
    gather_q0.relay()
    gather_v.hand()
    gather_q1.relay()
    gather_q0.hand()
    gather_k.finish()
    key_pair(0, 0)
    key_pair(1, 0)
    gather_o0.relay()
    gather_q1.hand()
    gather_v.finish()
    key_pair(2, 0)
    key_pair(3, 0)
    gather_o1.relay()
    gather_o0.hand()
    for pair in range(pairs):
        value_pair(pair, 0)
    gather_q0.finish()
    gather_q1.finish()

    def stack_heads(wide):
        return jnp.concatenate(
            [
                jnp.where(upper8, tile(wide, per_group * group), tile(wide, per_group * group + 1))
                for group in range(groups)
            ],
            axis=0,
        )

    def spread_heads(stack):
        parts = []
        for group in range(groups):
            part = stack[group * slots : (group + 1) * slots]
            parts += [jnp.where(upper8, part, 0.0), jnp.where(upper8, 0.0, part)]
        return jnp.concatenate(parts, axis=1).astype(bf16)

    def diagonal_of(wide):
        return jnp.concatenate(
            [
                wide[group * slots : (group + 1) * slots, group * HEAD_WIDTH : (group + 1) * HEAD_WIDTH]
                for group in range(groups)
            ],
            axis=0,
        )

    def blocks_of(stack):
        rows = []
        for group in range(groups):
            part = stack[group * slots : (group + 1) * slots]
            rows.append(
                jnp.concatenate(
                    [part if other == group else jnp.zeros_like(part) for other in range(groups)],
                    axis=1,
                )
            )
        return jnp.concatenate(rows, axis=0).astype(bf16)

    query_proj = stack_heads(mm(normed_last, full_q[...]))
    query_scale = lax.rsqrt(lane_mean(query_proj * query_proj) + EPSILON)
    query_unit = query_proj * query_scale
    query_rot = query_unit * cos_rows + pltpu.roll(query_unit, HEAD_WIDTH // 2, 1) * sin_rows
    query_wide = blocks_of(query_rot)
    query_blocks[...] = query_wide
    logits = mm(query_wide, key_rot[...], 1, 1) * HEAD_WIDTH ** (-0.5)
    expos = jnp.where(visible, jnp.exp(logits), 0.0)
    attention_weights = expos / jnp.sum(expos, axis=-1, keepdims=True)
    probs = attention_weights.astype(bf16)
    probs_ref[...] = probs
    context = diagonal_of(mm(probs, value_cast[...]))
    context_own[...] = context.astype(bf16)
    context_wide = spread_heads(context)
    gather_context.start()

    lane_block = lax.rem(
        lax.broadcasted_iota(jnp.int32, (slots, model), 1) // share, HEAD_WIDTH // share
    )

    def pack(parts, turn):
        total = jnp.zeros((slots, model), f32)
        for block, part in enumerate(parts):
            shift = ((block - turn) * share) % model
            moved = part if shift == 0 else pltpu.roll(part, shift, 1)
            total = jnp.where(lane_block == block, moved, total)
        return total

    def by_head(wide):
        return [jnp.where(upper8, wide, 0.0), jnp.where(upper8, 0.0, wide)]

    turns = HEAD_WIDTH // share
    pulled = mm(probs, normed[...])
    pulled_parts = [pulled[group * slots : (group + 1) * slots] for group in range(groups)]
    last_parts = by_head(normed_last.astype(f32))
    for turn in range(turns):
        both = jnp.concatenate([pack(pulled_parts, turn), pack(last_parts, turn)], axis=0)
        both = both.astype(bf16)
        for index in range(model // HEAD_WIDTH):
            early_src[index * turns + turn] = tile(both, index)

    early = Exchange(at, early_src, early_dst, early_sems.at[0], early_sems.at[1])
    early.start()

    gather_o0.finish()
    gather_o1.finish()
    attended = mm(context_wide, full_o[...], 1, 1)
    attended = attended + pltpu.roll(attended, pairs, 0)
    residual = x_last + attended
    out_scale = lax.rsqrt(lane_mean(residual * residual) + EPSILON)
    out_unit = residual * out_scale
    gain = final_gain[...] * score_vector[...]
    score8 = jnp.sum(out_unit * gain, axis=-1, keepdims=True)

    lane8 = lax.broadcasted_iota(jnp.int32, (slots, HEAD_WIDTH), 1)
    row_lane = lax.broadcasted_iota(jnp.int32, (slots, HEAD_WIDTH), 0)

    def as_row(column):
        return jnp.sum(jnp.where(row_lane == lane8, column, 0.0), axis=0, keepdims=True)

    score_row = as_row(score8)
    lane1 = lax.broadcasted_iota(jnp.int32, (1, HEAD_WIDTH), 1)
    listing = jnp.where(lane1 < pairs, score_row, as_row(teacher8))
    list_src[...] = listing
    me_row = list_dst.at[at.me]
    list_here, list_there, list_sent = list_sems.at[0], list_sems.at[1], list_sems.at[2]
    for place_of, target in enumerate(at.others):
        arrived = list_here if place_of < at.neg_count - 1 else list_there
        remote(list_src, me_row, list_sent, arrived, target).start()
    list_dst[at.me] = listing
    scores_out[...] = score_row[:, :pairs]
    gather_context.middle()

    near_block = list_dst.at[pl.ds(0, at.neg_count - 1)]
    remote(near_block, near_block, list_sent, list_here, at.to_partner()).wait_recv()

    def total(array):
        return jnp.sum(jnp.sum(array, axis=1, keepdims=True), axis=0, keepdims=True)

    def query_terms(first):
        block = list_dst[pl.ds(first, at.neg_count)].reshape(at.neg_count, HEAD_WIDTH)
        real = lax.broadcasted_iota(jnp.int32, block.shape, 1) < pairs
        score = jnp.where(real, block, 0.0)
        scaled = pltpu.roll(block, HEAD_WIDTH - pairs, 1)
        scaled = jnp.where(real, scaled, 0.0) / TEACHER_TEMP
        expo_t = jnp.where(real, jnp.exp(scaled), 0.0)
        total_s = total(jnp.where(real, jnp.exp(score), 0.0))
        return score, scaled, expo_t, total_s, total(expo_t)

    _, _, _, total_s, total_t = query_terms(pl.multiple_of(at.pb * at.neg_count, at.neg_count))
    grad_score = GRAD_SCALE * (
        jnp.exp(score8) / total_s - jnp.exp(teacher8 / TEACHER_TEMP) / total_t
    )
    grad_unit = grad_score * gain
    grad_resid = out_scale * (grad_unit - out_unit * lane_mean(grad_unit * out_unit))
    resid_grad[...] = grad_resid
    resid_cast = grad_resid.astype(bf16)
    grad_context = stack_heads(mm(resid_cast, full_o[...])).astype(bf16)
    context_blocks[...] = blocks_of(grad_context.astype(f32))
    late_own[0:stacked, :] = grad_context

    grad_probs = mm(context_blocks[...], value_cast[...], 1, 1)
    spread = jnp.sum(attention_weights * grad_probs, axis=-1, keepdims=True)
    logit_gradient = (attention_weights * (grad_probs - spread)).astype(bf16)
    logit_grad[...] = logit_gradient

    turned_q = diagonal_of(mm(logit_gradient, key_rot[...])) * HEAD_WIDTH ** (-0.5)
    back_q = turned_q * cos_rows - pltpu.roll(turned_q, HEAD_WIDTH // 2, 1) * sin_rows
    back_q = query_scale * (back_q - query_unit * lane_mean(back_q * query_unit))
    grad_q_cast = back_q.astype(bf16)
    late_own[stacked : 2 * stacked, :] = grad_q_cast
    gather_late.start()
    gather_context.relay()

    def key_back(pair, carry):
        start = pl.multiple_of(pair * seq, seq)
        rows = pl.ds(start, seq)
        turned = mm(logit_grad[:, rows], query_blocks[...], 0, 0) * HEAD_WIDTH ** (-0.5)
        for group in range(groups):
            lanes = slice(group * HEAD_WIDTH, (group + 1) * HEAD_WIDTH)
            part = turned[:, lanes]
            unit = key_unit[rows, lanes]
            back = part * cos_table[...] - pltpu.roll(part, HEAD_WIDTH // 2, 1) * sin_table[...]
            back = key_scale[rows, lanes] * (back - unit * lane_mean(back * unit))
            grad_k[rows, lanes] = back.astype(bf16)
        return carry

    for pair in range(pairs):
        key_back(pair, 0)

    block_rows = model // at.pb_count

    def send(src, dst, send_sem, recv_sem, target):
        remote(src, dst, send_sem, recv_sem, target).start()

    def arrive(block, recv_sem):
        remote(block, block, any_sem, recv_sem, at.to_partner()).wait_recv()

    for k in range(1, at.pb_count + 1):
        pb = at.pb_peer(k % at.pb_count)
        chosen = pl.ds(pl.multiple_of(pb * block_rows, block_rows), block_rows)
        product = mm(normed_t[chosen, :], grad_k[...])
        partial[pb] = product.astype(bf16).reshape(at.line_count, 2, share, kv_width)
        send(
            partial.at[pb, :, at.partner],
            from_core.at[pb],
            core_send,
            core_recv.at[pb],
            at.to_partner(),
        )

    for k in range(1, at.pb_count + 1):
        pb = at.pb_peer(k % at.pb_count)
        arrive(from_core.at[pb], core_recv.at[pb])
        both = partial[pb, :, at.core].astype(f32) + from_core[pb].astype(f32)
        paired[pb] = both.astype(bf16)
    gather_late.middle()
    for step in range(1, at.line_count + 1):
        line = at.line_peer(step % at.line_count)
        for k in range(1, at.pb_count):
            pb = at.pb_peer(k)
            send(
                paired.at[pb, line],
                from_pb.at[at.pb, line],
                pb_send,
                pb_recv.at[line],
                at.to_pb(pb),
            )

    resid_parts = by_head(resid_cast.astype(f32))
    for turn in range(turns):
        packed = pack(resid_parts, turn).astype(bf16)
        for index in range(model // HEAD_WIDTH):
            resid_src[index * turns + turn] = tile(packed, index)
    resid = Exchange(at, resid_src, resid_dst, resid_sems.at[0], resid_sems.at[1])
    resid.start()

    back_last = mm(spread_heads(grad_q_cast.astype(f32)), full_q[...], 1, 1)
    last_grad[...] = back_last + pltpu.roll(back_last, pairs, 0)

    def value_back(pair, carry):
        start = pl.multiple_of(pair * seq, seq)
        rows = pl.ds(start, seq)
        grad_v[rows, :] = mm(probs_ref[:, rows], context_blocks[...], 0, 0).astype(bf16)
        return carry

    lax.fori_loop(0, pairs, value_back, 0)

    seq_row = lax.broadcasted_iota(jnp.int32, (seq, 1), 0)

    def hidden_back(pair, carry):
        rows = pl.ds(pl.multiple_of(pair * seq, seq), seq)
        total = mm(grad_k[rows, :], full_k[...], 1, 1) + mm(grad_v[rows, :], full_v[...], 1, 1)
        hit = seq_row == lengths[0, pair] - 1
        total = total + jnp.where(hit, last_grad[pl.ds(pair, 1), :], 0.0)
        scaled = total * norm_gain[...]
        wide = x[rows, :].astype(f32)
        inv = inv_wide[rows, 0:1]
        mean = lane_mean(scaled * wide)
        result = inv * scaled - wide * (inv * inv * inv * mean)
        result = result + jnp.where(hit, resid_grad[pl.ds(pair, 1), :], 0.0)
        grad_hidden[rows, :] = result.astype(bf16)
        return carry

    def add_line(step):
        line = at.line_peer(step % at.line_count)
        total = paired[at.pb, line].astype(f32)
        arrive(from_pb.at[pl.ds(0, at.pb_count - 1), line], pb_recv.at[line])
        for k in range(1, at.pb_count):
            pb = at.pb_peer(k)
            total = total + from_pb[pb, line].astype(f32)
        if step < at.line_count:
            summed[line] = total.astype(bf16)
            send(
                summed.at[line],
                from_line.at[at.line],
                line_send,
                line_recv,
                at.to_line(line),
            )
        return total

    hidden_back(0, 0)
    add_line(1)
    gather_late.relay()
    hidden_back(1, 0)
    add_line(2)
    gather_context.finish()
    hidden_back(2, 0)
    for step in range(3, at.line_count + 1):
        own_sum = add_line(step)
    for pair in range(3, pairs):
        hidden_back(pair, 0)

    far_block = list_dst.at[pl.ds(0, at.count - at.neg_count)]
    remote(far_block, far_block, list_sent, list_there, at.to_partner()).wait_recv()
    loss = jnp.zeros((1, 1), f32)
    for pb in range(at.pb_count):
        score, scaled, expo_t, sum_s, sum_t = query_terms(pb * at.neg_count)
        loss = loss + total(expo_t / sum_t * (scaled - jnp.log(sum_t) - (score - jnp.log(sum_s))))
    loss_out[...] = loss

    gather_late.finish()
    early.wait("wait_recv")
    resid.wait("wait_recv")

    def rows_of(full, start, group):
        wide = full[...].astype(f32).reshape(at.count, -1, slots, HEAD_WIDTH)
        return wide[:, start + group].reshape(at.count * slots, HEAD_WIDTH).astype(bf16)

    pulled_rows = rows_of(early_dst, 0, 0)
    last_rows = rows_of(early_dst, 1, 0)
    resid_rows = rows_of(resid_dst, 0, 0)
    for group in range(groups):
        found = mm(pulled_rows, rows_of(late_full, 0, group), 0, 0)
        lanes = slice(group * HEAD_WIDTH, (group + 1) * HEAD_WIDTH)
        grad_value[:, lanes] = found[group * share : (group + 1) * share]
        found = mm(last_rows, rows_of(late_full, groups, group), 0, 0)
        for part in range(per_group):
            head = per_group * group + part
            grad_query[:, head * HEAD_WIDTH : (head + 1) * HEAD_WIDTH] = found[
                part * share : (part + 1) * share
            ]
        found = mm(resid_rows, rows_of(context_full, 0, group), 0, 0)
        for part in range(per_group):
            head = per_group * group + part
            grad_out[:, head * HEAD_WIDTH : (head + 1) * HEAD_WIDTH] = found[
                part * share : (part + 1) * share
            ]

    final = own_sum
    arrive(from_line.at[pl.ds(0, at.line_count - 1)], line_recv)
    for step in range(1, at.line_count):
        line = at.line_peer(step)
        final = final + from_line[line].astype(f32)
    grad_key[...] = final

    for gather in gathers:
        gather.drain()
    pieces = from_line.at[pl.ds(0, at.line_count - 1)]
    for block, sem in (
        (from_core, core_send),
        (from_pb.at[pl.ds(0, at.pb_count - 1)], pb_send),
        (pieces, line_send),
    ):
        remote(block, block, sem, any_sem, at.to_partner()).wait_send()
    early.wait("wait_send")
    resid.wait("wait_send")
    sent_block = list_dst.at[pl.ds(0, at.count - 1)]
    remote(sent_block, sent_block, list_sent, list_here, at.to_partner()).wait_send()


def write_kernel(count, *refs):
    sources, targets, sems = refs[:count], refs[count : 2 * count], refs[2 * count]
    copies = [
        pltpu.make_async_copy(sources[i], targets[i], sems.at[i]) for i in range(2, count)
    ]
    for copy in copies:
        copy.start()
    for i in range(2):
        targets[i][...] = sources[i][...]
    for copy in copies:
        copy.wait()


def write_outputs(arrays):
    count = len(arrays)
    return pl.pallas_call(
        functools.partial(write_kernel, count),
        out_shape=tuple(jax.ShapeDtypeStruct(a.shape, a.dtype) for a in arrays),
        in_specs=[VMEM_SPEC] * count,
        out_specs=(VMEM_SPEC,) * 2 + (pl.BlockSpec(memory_space=pl.ANY),) * (count - 2),
        scratch_shapes=[pltpu.SemaphoreType.DMA((count,))],
        compiler_params=pltpu.CompilerParams(vmem_limit_bytes=4 * 2**20),
    )(*arrays)


def run_step(operands, sizes, pb_count, neg_count):
    pairs, seq, groups, share = sizes
    x, own_q, own_k = operands[0], operands[8], operands[9]
    model, width, kv_width = x.shape[1], own_q.shape[1], own_k.shape[1]
    rows = pairs * seq
    count = pb_count * neg_count
    line_count = neg_count // 2
    slots = width // kv_width * pairs
    stacked = groups * slots
    bf16, f32 = jnp.bfloat16, jnp.float32
    block = (pb_count, line_count, share, kv_width)
    dma = pltpu.SemaphoreType.DMA
    vmem = pltpu.VMEM
    smem_spec = pl.BlockSpec(memory_space=pltpu.SMEM)
    hbm_spec = pl.BlockSpec(memory_space=pltpu.HBM)
    return pl.pallas_call(
        functools.partial(step_kernel, sizes),
        out_shape=(
            vmem((1, pairs), f32),
            vmem((1, 1), f32),
            vmem((rows, model), bf16),
            vmem((share, width), f32),
            vmem((share, kv_width), f32),
            vmem((share, kv_width), f32),
            vmem((share, width), f32),
        ),
        in_specs=[hbm_spec, smem_spec, smem_spec] + [hbm_spec] * 9,
        out_specs=(VMEM_SPEC,) * 7,
        scratch_shapes=[
            vmem((rows, model), bf16),
        ]
        + [vmem(a.shape, a.dtype) for a in operands[3:]]
        + [
            vmem((model, width), bf16),
            vmem((model, kv_width), bf16),
            vmem((model, kv_width), bf16),
            vmem((model, width), bf16),
            vmem((rows, model), bf16),
            vmem((model, rows), bf16),
            vmem((rows, HEAD_WIDTH), f32),
            vmem((rows, kv_width), f32),
            vmem((rows, kv_width), f32),
            vmem((rows, kv_width), bf16),
            vmem((rows, kv_width), bf16),
            vmem((rows, kv_width), bf16),
            vmem((rows, kv_width), bf16),
            vmem((stacked, rows), bf16),
            vmem((stacked, rows), bf16),
            vmem((stacked, kv_width), bf16),
            vmem((stacked, kv_width), bf16),
            vmem((slots, model), f32),
            vmem((slots, model), f32),
            vmem((stacked, HEAD_WIDTH), bf16),
            vmem((stacked * count, HEAD_WIDTH), bf16),
            vmem((2 * stacked, HEAD_WIDTH), bf16),
            vmem((2 * stacked * count, HEAD_WIDTH), bf16),
            vmem((count, 2 * slots, HEAD_WIDTH), bf16),
            vmem((count, 2 * slots, HEAD_WIDTH), bf16),
            vmem((count, slots, HEAD_WIDTH), bf16),
            vmem((count, slots, HEAD_WIDTH), bf16),
            vmem((1, HEAD_WIDTH), f32),
            vmem((count, 1, HEAD_WIDTH), f32),
            vmem((pb_count, line_count, 2, share, kv_width), bf16),
            vmem(block, bf16),
            vmem(block, bf16),
            vmem(block, bf16),
            vmem(block[1:], bf16),
            vmem(block[1:], bf16),
            dma((2,)),
            dma((2,)),
            dma((3,)),
            dma,
            dma((pb_count,)),
            dma,
            dma((line_count,)),
            dma,
            dma,
            dma,
            dma((pairs + 9,)),
        ]
        + gather_sems(neg_count, True) * 6
        + gather_sems(neg_count, False) * 2,
        compiler_params=pltpu.CompilerParams(
            collective_id=0, has_side_effects=True, vmem_limit_bytes=62 * 2**20
        ),
    )(*operands)


def shards(
    hidden,
    lengths,
    teacher,
    norm_gain,
    final_gain,
    score_vector,
    query_weight,
    key_matrix,
    value_matrix,
    out_weight,
):
    both = ("pb", "neg")
    width = query_weight.shape[1]
    kv_width = key_matrix.shape[1]
    share, out_share = query_weight.shape[0], out_weight.shape[1]
    pb_count, neg_count = lax.axis_size("pb"), lax.axis_size("neg")
    pair_count, seq_len, model_width = hidden.shape[1:]
    group_count = kv_width // HEAD_WIDTH
    own_kernels = (
        pb_count == 4
        and neg_count == 8
        and share == out_share
        and share % 32 == 0
        and model_width == share * pb_count * neg_count
        and width == 2 * kv_width
        and pair_count * 2 == 8
        and seq_len == HEAD_WIDTH
        and share * group_count == HEAD_WIDTH
    )
    if own_kernels:
        cos_table, sin_table = signed_tables(seq_len, HEAD_WIDTH)
        results = run_step(
            (
                hidden.reshape(pair_count * seq_len, model_width),
                lengths,
                teacher,
                norm_gain[None],
                final_gain[None],
                score_vector[None],
                cos_table,
                sin_table,
                query_weight,
                key_matrix,
                value_matrix,
                out_weight.T,
            ),
            (pair_count, seq_len, group_count, share),
            pb_count,
            neg_count,
        )
        scores, loss, grad_rows, grad_query, grad_key, grad_value, grad_out = write_outputs(results)
        return (
            scores,
            loss.reshape(()),
            grad_rows.reshape(hidden.shape),
            grad_query,
            grad_key,
            grad_value,
            grad_out.T,
        )
    packed = jnp.concatenate([query_weight, key_matrix, value_matrix, out_weight.T], axis=1)
    everything = lax.all_gather(packed, both, axis=0, tiled=True)
    full_query = everything[:, :width]
    full_key = everything[:, width : width + kv_width]
    full_value = everything[:, width + kv_width : width + 2 * kv_width]
    full_out_t = everything[:, width + 2 * kv_width :]
    weights = (full_query, full_key, full_value, full_out_t.T)
    scores_here, stored = forward_pairs(
        hidden[0], lengths[0], norm_gain, final_gain, score_vector, *weights
    )
    listing = jnp.concatenate([scores_here, teacher[0]])[None]
    listed = lax.all_gather(listing, "neg", axis=0, tiled=True)
    all_scores = listed[:, :pair_count]
    all_scaled = listed[:, pair_count:] / TEACHER_TEMP
    my_total_s = jnp.sum(jnp.exp(all_scores))
    expo_t = jnp.exp(all_scaled)
    my_total_t = jnp.sum(expo_t)
    loss_here = jnp.sum(
        expo_t
        / my_total_t
        * (all_scaled - jnp.log(my_total_t) - (all_scores - jnp.log(my_total_s)))
    )
    prob_s = jnp.exp(scores_here) / my_total_s
    prob_t = jnp.exp(teacher[0] / TEACHER_TEMP) / my_total_t
    grad_score = GRAD_SCALE * (prob_s - prob_t)
    grad_input, last_rows, grad_kv = backward_pairs(
        stored, grad_score, norm_gain, final_gain, score_vector, *weights
    )
    grad_kv = grad_kv.astype(jnp.bfloat16)
    reduced = lax.psum_scatter(grad_kv, both, scatter_dimension=0, tiled=True)
    reduced = reduced.astype(jnp.float32)
    rows = lax.all_gather(last_rows, both, axis=0, tiled=True)
    loss_value = lax.psum(loss_here, "pb")
    index = lax.axis_index("pb") * neg_count + lax.axis_index("neg")
    normed_cols = lax.dynamic_slice_in_dim(rows, index * share, share, axis=1)
    resid_cols = lax.dynamic_slice_in_dim(rows, model_width + index * out_share, out_share, axis=1)
    rest = 2 * model_width
    all_q = rows[:, rest : rest + width]
    all_context = rows[:, rest + width :]
    grad_query = jnp.dot(normed_cols.T, all_q, preferred_element_type=jnp.float32)
    grad_out = jnp.dot(all_context.T, resid_cols, preferred_element_type=jnp.float32)
    return (
        scores_here[None],
        loss_value,
        grad_input[None],
        grad_query,
        reduced[:, :kv_width],
        reduced[:, kv_width:],
        grad_out,
    )


def solution(mesh):
    placed = (
        P("pb", "neg", None, None),
        P("pb", "neg"),
        P("pb", "neg"),
        P(),
        P(),
        P(),
        P(("pb", "neg"), None),
        P(("pb", "neg"), None),
        P(("pb", "neg"), None),
        P(None, ("pb", "neg")),
    )
    return jax.shard_map(
        shards,
        mesh=mesh,
        in_specs=placed,
        out_specs=(
            P("pb", "neg"),
            P(),
            P("pb", "neg", None, None),
            P(("pb", "neg"), None),
            P(("pb", "neg"), None),
            P(("pb", "neg"), None),
            P(None, ("pb", "neg")),
        ),
        check_vma=False,
    )
```

```python
import functools

import jax
import jax.numpy as jnp
import numpy as np
from jax import lax
from jax.experimental import pallas as pl
from jax.experimental.pallas import tpu as pltpu
from jax.sharding import PartitionSpec as P

HEAD_WIDTH = 128
MESH_ID = pl.DeviceIdType.MESH

EPSILON = 1e-06
ROPE_BASE = 1000000.0
TEACHER_TEMP = 2.0
GRAD_SCALE = 512.0


def rope_tables(seq_len, head_size):
    half = head_size // 2
    freqs = ROPE_BASE ** (-(jnp.arange(half, dtype=jnp.float32) * 2.0) / head_size)
    angles = jnp.arange(seq_len, dtype=jnp.float32)[:, None] * freqs[None, :]
    angles = jnp.concatenate([angles, angles], axis=1)
    return (jnp.cos(angles), jnp.sin(angles))


def signed_tables(seq_len, head_size):
    half = head_size // 2
    freqs = ROPE_BASE ** (-(np.arange(half) * 2.0) / head_size)
    angles = np.arange(seq_len)[:, None] * freqs[None, :]
    cos = np.concatenate([np.cos(angles)] * 2, axis=1)
    sin = np.concatenate([-np.sin(angles), np.sin(angles)], axis=1)
    return (jnp.asarray(cos, jnp.float32), jnp.asarray(sin, jnp.float32))


def rotate_half(vector):
    half = vector.shape[-1] // 2
    return jnp.concatenate([-vector[..., half:], vector[..., :half]], axis=-1)


def unrotate_half(vector):
    half = vector.shape[-1] // 2
    return jnp.concatenate([vector[..., half:], -vector[..., :half]], axis=-1)


def forward_pairs(
    tokens_in,
    lengths_here,
    norm_gain,
    final_gain,
    score_vector,
    query_weight,
    key_matrix,
    value_matrix,
    out_weight,
):
    pair_count, seq_len, model_width = tokens_in.shape
    head_count = query_weight.shape[1] // HEAD_WIDTH
    group_count = key_matrix.shape[1] // HEAD_WIDTH
    group_size = head_count // group_count
    inputs_wide = tokens_in.astype(jnp.float32)
    inv_rms = lax.rsqrt(jnp.mean(inputs_wide * inputs_wide, axis=-1, keepdims=True) + EPSILON)
    normed = (inputs_wide * inv_rms * norm_gain).astype(jnp.bfloat16)
    flat_rows = normed.reshape(pair_count * seq_len, model_width)
    key_proj = jnp.dot(flat_rows, key_matrix, preferred_element_type=jnp.float32).reshape(
        pair_count, seq_len, group_count, HEAD_WIDTH
    )
    value_proj = jnp.dot(flat_rows, value_matrix, preferred_element_type=jnp.float32).reshape(
        pair_count, seq_len, group_count, HEAD_WIDTH
    )
    positions = jnp.arange(seq_len, dtype=jnp.int32)
    last_index = lengths_here - 1
    onehot = (positions[None, :] == last_index[:, None]).astype(jnp.float32)
    normed_last = jnp.take_along_axis(normed, last_index[:, None, None], axis=1)[:, 0]
    query_proj = jnp.dot(normed_last, query_weight, preferred_element_type=jnp.float32).reshape(
        pair_count, head_count, HEAD_WIDTH
    )
    query_scale = lax.rsqrt(jnp.mean(query_proj * query_proj, axis=-1, keepdims=True) + EPSILON)
    query_unit = query_proj * query_scale
    key_scale = lax.rsqrt(jnp.mean(key_proj * key_proj, axis=-1, keepdims=True) + EPSILON)
    key_unit = key_proj * key_scale
    cos_table, sin_table = rope_tables(seq_len, HEAD_WIDTH)
    cos_query = jnp.dot(onehot, cos_table, precision=lax.Precision.HIGHEST)
    sin_query = jnp.dot(onehot, sin_table, precision=lax.Precision.HIGHEST)
    query_rot = (
        query_unit * cos_query[:, None, :] + rotate_half(query_unit) * sin_query[:, None, :]
    ).astype(jnp.bfloat16)
    key_rot = (
        key_unit * cos_table[None, :, None, :] + rotate_half(key_unit) * sin_table[None, :, None, :]
    ).astype(jnp.bfloat16)
    value_cast = value_proj.astype(jnp.bfloat16)
    grouped = query_rot.reshape(pair_count, group_count, group_size, HEAD_WIDTH)
    logits = jnp.einsum(
        "pkgd,pskd->pkgs", grouped, key_rot, preferred_element_type=jnp.float32
    ) * HEAD_WIDTH ** (-0.5)
    visible = (positions[None, :] <= last_index[:, None])[:, None, None, :]
    expos = jnp.where(visible, jnp.exp(logits), 0.0)
    attention_weights = expos / jnp.sum(expos, axis=-1, keepdims=True)
    probs_cast = attention_weights.astype(jnp.bfloat16)
    context = jnp.einsum(
        "pkgs,pskd->pkgd", probs_cast, value_cast, preferred_element_type=jnp.float32
    )
    context = context.astype(jnp.bfloat16).reshape(pair_count, head_count * HEAD_WIDTH)
    attended = jnp.dot(context, out_weight, preferred_element_type=jnp.float32)
    residual = jnp.take_along_axis(inputs_wide, last_index[:, None, None], axis=1)[:, 0] + attended
    out_scale = lax.rsqrt(jnp.mean(residual * residual, axis=-1, keepdims=True) + EPSILON)
    out_unit = residual * out_scale
    scores_here = jnp.sum(out_unit * final_gain * score_vector, axis=-1)
    stored = (
        tokens_in,
        onehot,
        inv_rms,
        normed,
        normed_last,
        query_unit,
        query_scale,
        key_unit,
        key_scale,
        cos_query,
        sin_query,
        cos_table,
        sin_table,
        query_rot,
        key_rot,
        value_cast,
        attention_weights,
        probs_cast,
        context,
        out_unit,
        out_scale,
    )
    return (scores_here, stored)


def backward_pairs(
    stored,
    grad_score,
    norm_gain,
    final_gain,
    score_vector,
    query_weight,
    key_matrix,
    value_matrix,
    out_weight,
):
    (
        tokens_in,
        onehot,
        inv_rms,
        normed,
        normed_last,
        query_unit,
        query_scale,
        key_unit,
        key_scale,
        cos_query,
        sin_query,
        cos_table,
        sin_table,
        query_rot,
        key_rot,
        value_cast,
        attention_weights,
        probs_cast,
        context,
        out_unit,
        out_scale,
    ) = stored
    pair_count, seq_len, model_width = tokens_in.shape
    head_count = query_weight.shape[1] // HEAD_WIDTH
    group_count = key_matrix.shape[1] // HEAD_WIDTH
    group_size = head_count // group_count
    grad_unit = grad_score[:, None] * score_vector * final_gain
    grad_resid = out_scale * (
        grad_unit - out_unit * jnp.mean(grad_unit * out_unit, axis=-1, keepdims=True)
    )
    grad_resid_cast = grad_resid.astype(jnp.bfloat16)
    grad_context = jnp.dot(
        grad_resid_cast, out_weight.T, preferred_element_type=jnp.float32
    ).astype(jnp.bfloat16)
    grad_context = grad_context.reshape(pair_count, group_count, group_size, HEAD_WIDTH)
    grad_probs = jnp.einsum(
        "pkgd,pskd->pkgs", grad_context, value_cast, preferred_element_type=jnp.float32
    )
    grad_vals = jnp.einsum(
        "pkgs,pkgd->pskd", probs_cast, grad_context, preferred_element_type=jnp.float32
    )
    spread = jnp.sum(attention_weights * grad_probs, axis=-1, keepdims=True)
    logit_gradient = (attention_weights * (grad_probs - spread)).astype(jnp.bfloat16)
    grouped = query_rot.reshape(pair_count, group_count, group_size, HEAD_WIDTH)
    rotated_query_gradient = jnp.einsum(
        "pkgs,pskd->pkgd", logit_gradient, key_rot, preferred_element_type=jnp.float32
    ) * HEAD_WIDTH ** (-0.5)
    rotated_query_gradient = rotated_query_gradient.reshape(pair_count, head_count, HEAD_WIDTH)
    grad_krot = jnp.einsum(
        "pkgs,pkgd->pskd", logit_gradient, grouped, preferred_element_type=jnp.float32
    ) * HEAD_WIDTH ** (-0.5)
    grad_qunit = rotated_query_gradient * cos_query[:, None, :] + unrotate_half(
        rotated_query_gradient * sin_query[:, None, :]
    )
    grad_kunit = grad_krot * cos_table[None, :, None, :] + unrotate_half(
        grad_krot * sin_table[None, :, None, :]
    )
    grad_qproj = query_scale * (
        grad_qunit - query_unit * jnp.mean(grad_qunit * query_unit, axis=-1, keepdims=True)
    )
    grad_kproj = key_scale * (
        grad_kunit - key_unit * jnp.mean(grad_kunit * key_unit, axis=-1, keepdims=True)
    )
    grad_q_cast = grad_qproj.reshape(pair_count, head_count * HEAD_WIDTH).astype(jnp.bfloat16)
    grad_k_cast = grad_kproj.reshape(pair_count * seq_len, group_count * HEAD_WIDTH).astype(
        jnp.bfloat16
    )
    grad_v_cast = grad_vals.reshape(pair_count * seq_len, group_count * HEAD_WIDTH).astype(
        jnp.bfloat16
    )
    flat_rows = normed.reshape(pair_count * seq_len, model_width)
    last_rows = jnp.concatenate([normed_last, grad_resid_cast, grad_q_cast, context], axis=1)
    grad_kv = jnp.dot(
        flat_rows.T,
        jnp.concatenate([grad_k_cast, grad_v_cast], axis=1),
        preferred_element_type=jnp.float32,
    )
    grad_normed = jnp.dot(grad_k_cast, key_matrix.T, preferred_element_type=jnp.float32)
    grad_normed = grad_normed + jnp.dot(
        grad_v_cast, value_matrix.T, preferred_element_type=jnp.float32
    )
    grad_normed = grad_normed.reshape(pair_count, seq_len, model_width)
    grad_last = jnp.dot(grad_q_cast, query_weight.T, preferred_element_type=jnp.float32)
    grad_normed = grad_normed + onehot[:, :, None] * grad_last[:, None, :]
    inputs_wide = tokens_in.astype(jnp.float32)
    grad_scaled = grad_normed * norm_gain
    grad_input = inv_rms * grad_scaled - inputs_wide * inv_rms * inv_rms * inv_rms * jnp.mean(
        grad_scaled * inputs_wide, axis=-1, keepdims=True
    )
    grad_input = grad_input + onehot[:, :, None] * grad_resid[:, None, :]
    return (grad_input.astype(jnp.bfloat16), last_rows, grad_kv)


class Place:
    def __init__(self):
        self.pb_count = lax.axis_size("pb")
        self.neg_count = lax.axis_size("neg")
        self.line_count = self.neg_count // 2
        self.pb = lax.axis_index("pb")
        neg = lax.axis_index("neg")
        self.line = neg // 2
        self.core = neg % 2
        self.partner = 1 - self.core

    def slot(self, pb, line, core):
        return pb * self.neg_count + line * 2 + core

    def line_peer(self, step):
        return lax.rem(self.line + step, self.line_count)

    def pb_peer(self, step):
        return lax.rem(self.pb + step, self.pb_count)

    def to_line(self, line):
        return (self.pb, line * 2 + self.core)

    def to_pb(self, pb):
        return (pb, self.line * 2 + self.core)

    def to_partner(self):
        return (self.pb, self.line * 2 + self.partner)

    def greet(self):
        barrier = pltpu.get_barrier_semaphore()
        targets = [self.to_line(self.line_peer(k)) for k in range(1, self.line_count)]
        targets += [self.to_pb(self.pb_peer(k)) for k in range(1, self.pb_count)]
        targets += [self.to_partner()]
        for target in targets:
            pl.semaphore_signal(barrier, inc=1, device_id=target, device_id_type=MESH_ID)
        pl.semaphore_wait(barrier, len(targets))


def remote(src, dst, send_sem, recv_sem, target):
    return pltpu.make_async_remote_copy(
        src_ref=src,
        dst_ref=dst,
        send_sem=send_sem,
        recv_sem=recv_sem,
        device_id=target,
        device_id_type=MESH_ID,
    )


def gather_sems(neg_count, large):
    line_count = neg_count // 2
    dma = pltpu.SemaphoreType.DMA
    if large:
        return [dma((line_count,)), dma((line_count,)), dma((line_count,)), dma((2,))]
    return [dma((1,)), dma((1,)), dma((1,)), dma((2,))]


class Gather:
    def __init__(self, place, own, full, sems, halve_corner, direct):
        self.place, self.own, self.full = place, own, full
        self.line_recv, self.pb_recv, self.corner_recv, ends = sems
        self.send_sem, self.core_recv = ends.at[0], ends.at[1]
        self.halve_corner, self.direct = halve_corner, direct
        across = place.pb + 1 - 2 * (place.pb % 2)
        along = place.pb + 2 - 4 * (place.pb // 2)
        self.near = (across, along)
        self.corner = 3 - place.pb
        half = place.line // 2
        self.is_inner = (place.line == 1) | (place.line == 2)
        self.mate = place.line + 1 - 2 * (place.line % 2)
        self.far_inner = 2 - half
        self.far_outer = 3 - 3 * half
        self.size = own.shape[0]
        if halve_corner:
            self.own_lines = (place.line, lax.rem(place.line + 2, 4))
            self.mate_lines = (self.mate, lax.rem(self.mate + 2, 4))
        else:
            self.own_lines = (place.line, self.mate, self.far_inner, self.far_outer)
            self.mate_lines = ()

    def rows(self, pb, line, core):
        start = self.place.slot(pb, line, core) * self.size
        return self.full.at[pl.ds(pl.multiple_of(start, self.size), self.size)]

    def blocks(self, count):
        return self.full.at[pl.ds(0, count * self.size)]

    def send(self, src, dst, recv_sem, target):
        remote(src, dst, self.send_sem, recv_sem, target).start()

    def of(self, sems, line):
        return sems.at[0] if self.direct else sems.at[line]

    def spread(self, src, line):
        at = self.place
        dst = self.rows(at.pb, line, at.core)
        for side in range(2):
            self.send(src, dst, self.of(self.pb_recv, line), at.to_pb(self.near[side]))
        self.pass_on(src, at.pb, line)

    def pass_on(self, src, pb, line):
        at = self.place
        self.send(src, self.rows(pb, line, at.core), self.core_recv, at.to_partner())

    def arrive(self, block, recv_sem):
        remote(block, block, self.send_sem, recv_sem, self.place.to_partner()).wait_recv()

    def start(self):
        at = self.place
        mine = self.rows(at.pb, at.line, at.core)
        peers = (self.mate, self.far_inner) + ((self.far_outer,) if self.direct else ())
        for line in peers:
            self.send(self.own, mine, self.of(self.line_recv, at.line), at.to_line(line))
        self.spread(self.own, at.line)
        mine[...] = self.own[...]

    def middle(self):
        at = self.place
        if self.direct:
            self.arrive(self.blocks(at.line_count - 1), self.line_recv.at[0])
        for line in (self.mate, self.far_inner, self.far_outer):
            block = self.rows(at.pb, line, at.core)
            if not self.direct:
                self.arrive(block, self.line_recv.at[line])
                if line is not self.mate:

                    @pl.when(self.is_inner)
                    def _():
                        self.send(block, block, self.line_recv.at[line], at.to_line(self.mate))

            self.spread(block, line)

    def half(self, block, side):
        size = block.shape[0] // 2
        return block.at[pl.ds(side * size, size)]

    def relay(self):
        at = self.place
        if self.direct:
            self.arrive(self.blocks(2 * at.line_count), self.pb_recv.at[0])
        for line in self.own_lines + self.mate_lines:
            if not self.direct:
                self.arrive(self.blocks(2), self.pb_recv.at[line])
            for side in range(2):
                block = self.rows(self.near[side], line, at.core)
                if not any(line is other for other in self.mate_lines):
                    part = self.half(block, side)
                    target = at.to_pb(self.near[1 - side])
                    self.send(part, part, self.of(self.corner_recv, line), target)
                self.pass_on(block, self.near[side], line)

    def corner_in(self, lines, hand_over):
        at = self.place
        if self.direct:
            self.arrive(self.blocks(at.line_count), self.corner_recv.at[0])
        for line in lines:
            block = self.rows(self.corner, line, at.core)
            if not self.direct:
                self.arrive(block, self.corner_recv.at[line])
            if hand_over:
                self.send(block, block, self.corner_recv.at[line], at.to_line(self.mate))
            self.pass_on(block, self.corner, line)

    def hand(self):
        if self.halve_corner:
            self.corner_in(self.own_lines, True)

    def tail(self):
        self.corner_in(self.mate_lines if self.halve_corner else self.own_lines, False)

    def finish(self):
        self.arrive(self.blocks(self.place.count // 2), self.core_recv)

    def drain(self):
        at = self.place
        block = self.blocks(at.count - (1 if self.direct else 2))
        remote(block, block, self.send_sem, self.core_recv, at.to_partner()).wait_send()
        if not self.direct:

            @pl.when(self.is_inner)
            def _():
                block = self.blocks(2)
                remote(block, block, self.send_sem, self.core_recv, at.to_partner()).wait_send()


VMEM_SPEC = pl.BlockSpec(memory_space=pltpu.VMEM)


def mm(left, right, left_dim=1, right_dim=0, precision=None):
    return lax.dot_general(
        left,
        right,
        (((left_dim,), (right_dim,)), ((), ())),
        preferred_element_type=jnp.float32,
        precision=precision,
    )


def lane_mean(array):
    return jnp.mean(array, axis=-1, keepdims=True)


def tile(array, index):
    return array[:, index * HEAD_WIDTH : (index + 1) * HEAD_WIDTH]


class Exchange:
    def __init__(self, at, src, dst, send_sem, recv_sem):
        self.at, self.src, self.dst = at, src, dst
        self.send_sem, self.recv_sem = send_sem, recv_sem

    def start(self):
        at = self.at
        for pb, neg in at.others:
            peer = pb * at.neg_count + neg
            remote(
                self.src.at[peer], self.dst.at[at.me], self.send_sem, self.recv_sem, (pb, neg)
            ).start()
        self.dst[at.me] = self.src[at.me]

    def wait(self, sem_of):
        block = self.dst.at[pl.ds(0, self.at.count - 1)]
        copy = remote(block, block, self.send_sem, self.recv_sem, self.at.to_partner())
        getattr(copy, sem_of)()


def step_kernel(
    sizes,
    hidden,
    lengths,
    teacher,
    norm_gain_in,
    final_gain_in,
    score_vector_in,
    cos_table_in,
    sin_table_in,
    own_q_in,
    own_k_in,
    own_v_in,
    own_o_in,
    scores_out,
    loss_out,
    grad_hidden,
    grad_query,
    grad_key,
    grad_value,
    grad_out,
    x,
    norm_gain,
    final_gain,
    score_vector,
    cos_table,
    sin_table,
    own_q,
    own_k,
    own_v,
    own_o,
    full_q,
    full_k,
    full_v,
    full_o,
    normed,
    normed_t,
    inv_wide,
    key_unit,
    key_scale,
    key_rot,
    value_cast,
    grad_k,
    grad_v,
    logit_grad,
    probs_ref,
    query_blocks,
    context_blocks,
    last_grad,
    resid_grad,
    context_own,
    context_full,
    late_own,
    late_full,
    early_src,
    early_dst,
    resid_src,
    resid_dst,
    list_src,
    list_dst,
    partial,
    from_core,
    paired,
    from_pb,
    summed,
    from_line,
    early_sems,
    resid_sems,
    list_sems,
    core_send,
    core_recv,
    pb_send,
    pb_recv,
    line_send,
    line_recv,
    any_sem,
    load_sems,
    *gather_sem_refs,
):
    pairs, seq, groups, share = sizes
    bf16, f32 = jnp.bfloat16, jnp.float32
    at = Place()
    at.count = at.pb_count * at.neg_count
    at.me = at.slot(at.pb, at.line, at.core)
    neg = lax.axis_index("neg")
    pb_all = [at.pb] + [at.pb_peer(k) for k in range(1, at.pb_count)]
    neg_all = [neg] + [lax.rem(neg + k, at.neg_count) for k in range(1, at.neg_count)]
    at.others = [
        (pb, peer)
        for i, pb in enumerate(pb_all)
        for j, peer in enumerate(neg_all)
        if i + j > 0
    ]
    model = x.shape[1]
    rows_all = pairs * seq
    per_group = own_q.shape[1] // own_k.shape[1]
    slots = per_group * pairs
    stacked = groups * slots
    kv_width = groups * HEAD_WIDTH

    barrier = pltpu.get_barrier_semaphore()

    for target in at.others:
        pl.semaphore_signal(barrier, inc=1, device_id=target, device_id_type=MESH_ID)
    loads = []
    moves = (
        (own_k_in, own_k),
        (own_v_in, own_v),
        (own_q_in, own_q),
        (own_o_in, own_o),
        (norm_gain_in, norm_gain),
        (final_gain_in, final_gain),
        (score_vector_in, score_vector),
        (cos_table_in, cos_table),
        (sin_table_in, sin_table),
    )
    small_loads = []
    for place_of, (source, target) in enumerate(moves):
        load = pltpu.make_async_copy(source, target, load_sems.at[pairs + place_of])
        load.start()
        small_loads.append(load)
    for pair in range(pairs):
        rows = pl.ds(pair * seq, seq)
        load = pltpu.make_async_copy(hidden.at[rows], x.at[rows], load_sems.at[pair])
        load.start()
        loads.append(load)

    half_width = own_q.shape[1] // 2
    low, high = pl.ds(0, half_width), pl.ds(half_width, half_width)
    parts = (
        (own_k, full_k, True),
        (own_v, full_v, True),
        (own_q.at[:, low], full_q.at[:, low], True),
        (own_q.at[:, high], full_q.at[:, high], True),
        (own_o.at[:, low], full_o.at[:, low], True),
        (own_o.at[:, high], full_o.at[:, high], False),
        (context_own, context_full, False),
        (late_own, late_full, False),
    )
    each = len(gather_sem_refs) // len(parts)
    gathers = [
        Gather(at, own, full, gather_sem_refs[i * each : (i + 1) * each], halve, i >= 6)
        for i, (own, full, halve) in enumerate(parts)
    ]
    gather_k, gather_v, gather_q0, gather_q1, gather_o0, gather_o1 = gathers[:6]
    gather_context, gather_late = gathers[6:]

    for load in small_loads:
        load.wait()
    pl.semaphore_wait(barrier, at.count - 1)
    for gather in gathers[:4]:
        gather.start()

    def norm_pair(pair, carry):
        rows = pl.ds(pl.multiple_of(pair * seq, seq), seq)
        wide = x[rows, :].astype(f32)
        inv = lax.rsqrt(lane_mean(wide * wide) + EPSILON)
        inv_wide[rows, :] = jnp.broadcast_to(inv, (seq, HEAD_WIDTH))
        scaled = wide * inv * norm_gain[...]
        normed[rows, :] = scaled.astype(bf16)
        normed_t[:, rows] = scaled.T.astype(bf16)
        return carry

    for pair in range(pairs):
        loads[pair].wait()
        norm_pair(pair, 0)

    row8 = lax.broadcasted_iota(jnp.int32, (slots, 1), 0)
    pair8 = lax.rem(row8, pairs)
    upper8 = row8 < pairs
    last8 = jnp.zeros((slots, 1), jnp.int32)
    teacher8 = jnp.zeros((slots, 1), f32)
    for pair in range(pairs):
        last8 = jnp.where(pair8 == pair, lengths[0, pair] - 1, last8)
        teacher8 = jnp.where(pair8 == pair, teacher[0, pair], teacher8)
    place8 = pair8 * seq + last8
    column8 = lax.broadcasted_iota(jnp.int32, (slots, rows_all), 1)
    onehot8 = (column8 == place8).astype(f32).astype(bf16)
    visible8 = (column8 >= pair8 * seq) & (column8 <= place8)
    visible = jnp.concatenate([visible8.astype(f32)] * groups, axis=0) > 0.5
    position8 = (lax.broadcasted_iota(jnp.int32, (slots, seq), 1) == last8).astype(f32)

    x_last = mm(onehot8, x[...])
    normed_last = mm(onehot8, normed[...]).astype(bf16)
    cos8 = mm(position8, cos_table[...], precision=lax.Precision.HIGHEST)
    sin8 = mm(position8, sin_table[...], precision=lax.Precision.HIGHEST)
    cos_rows = jnp.concatenate([cos8] * groups, axis=0)
    sin_rows = jnp.concatenate([sin8] * groups, axis=0)

    def key_pair(pair, carry):
        rows = pl.ds(pl.multiple_of(pair * seq, seq), seq)
        proj = mm(normed[rows, :], full_k[...])
        for group in range(groups):
            lanes = slice(group * HEAD_WIDTH, (group + 1) * HEAD_WIDTH)
            part = proj[:, lanes]
            scale = lax.rsqrt(lane_mean(part * part) + EPSILON)
            unit = part * scale
            key_unit[rows, lanes] = unit
            key_scale[rows, lanes] = jnp.broadcast_to(scale, (seq, HEAD_WIDTH))
            turned = unit * cos_table[...] + pltpu.roll(unit, HEAD_WIDTH // 2, 1) * sin_table[...]
            key_rot[rows, lanes] = turned.astype(bf16)
        return carry

    def value_pair(pair, carry):
        rows = pl.ds(pl.multiple_of(pair * seq, seq), seq)
        value_cast[rows, :] = mm(normed[rows, :], full_v[...]).astype(bf16)
        return carry

    gather_k.middle()
    gather_o0.start()
    gather_o1.start()
    gather_v.middle()
    gather_q0.middle()
    gather_k.relay()
    gather_q1.middle()
    gather_v.relay()
    gather_k.hand()
    gather_o0.middle()
    gather_o1.middle()
    gather_q0.relay()
    gather_v.hand()
    gather_q1.relay()
    gather_q0.hand()
    gather_k.tail()
    gather_o0.relay()
    gather_q1.hand()
    gather_v.tail()
    gather_k.finish()
    key_pair(0, 0)
    key_pair(1, 0)
    gather_o1.relay()
    gather_o0.hand()
    gather_q0.tail()
    key_pair(2, 0)
    key_pair(3, 0)
    gather_q1.tail()
    gather_v.finish()
    for pair in range(pairs):
        value_pair(pair, 0)
    gather_o0.tail()
    gather_q0.finish()
    gather_q1.finish()

    def stack_heads(wide):
        return jnp.concatenate(
            [
                jnp.where(upper8, tile(wide, per_group * group), tile(wide, per_group * group + 1))
                for group in range(groups)
            ],
            axis=0,
        )

    def spread_heads(stack):
        parts = []
        for group in range(groups):
            part = stack[group * slots : (group + 1) * slots]
            parts += [jnp.where(upper8, part, 0.0), jnp.where(upper8, 0.0, part)]
        return jnp.concatenate(parts, axis=1).astype(bf16)

    def diagonal_of(wide):
        return jnp.concatenate(
            [
                wide[group * slots : (group + 1) * slots, group * HEAD_WIDTH : (group + 1) * HEAD_WIDTH]
                for group in range(groups)
            ],
            axis=0,
        )

    def blocks_of(stack):
        rows = []
        for group in range(groups):
            part = stack[group * slots : (group + 1) * slots]
            rows.append(
                jnp.concatenate(
                    [part if other == group else jnp.zeros_like(part) for other in range(groups)],
                    axis=1,
                )
            )
        return jnp.concatenate(rows, axis=0).astype(bf16)

    query_proj = stack_heads(mm(normed_last, full_q[...]))
    query_scale = lax.rsqrt(lane_mean(query_proj * query_proj) + EPSILON)
    query_unit = query_proj * query_scale
    query_rot = query_unit * cos_rows + pltpu.roll(query_unit, HEAD_WIDTH // 2, 1) * sin_rows
    query_wide = blocks_of(query_rot)
    query_blocks[...] = query_wide
    logits = mm(query_wide, key_rot[...], 1, 1) * HEAD_WIDTH ** (-0.5)
    expos = jnp.where(visible, jnp.exp(logits), 0.0)
    attention_weights = expos / jnp.sum(expos, axis=-1, keepdims=True)
    probs = attention_weights.astype(bf16)
    probs_ref[...] = probs
    context = diagonal_of(mm(probs, value_cast[...]))
    context_own[...] = context.astype(bf16)
    context_wide = spread_heads(context)
    gather_context.start()
    gather_o1.tail()

    lane_block = lax.rem(
        lax.broadcasted_iota(jnp.int32, (slots, model), 1) // share, HEAD_WIDTH // share
    )

    def pack(parts, turn):
        total = jnp.zeros((slots, model), f32)
        for block, part in enumerate(parts):
            shift = ((block - turn) * share) % model
            moved = part if shift == 0 else pltpu.roll(part, shift, 1)
            total = jnp.where(lane_block == block, moved, total)
        return total

    def by_head(wide):
        return [jnp.where(upper8, wide, 0.0), jnp.where(upper8, 0.0, wide)]

    turns = HEAD_WIDTH // share
    pulled = mm(probs, normed[...])
    pulled_parts = [pulled[group * slots : (group + 1) * slots] for group in range(groups)]
    last_parts = by_head(normed_last.astype(f32))
    for turn in range(turns):
        both = jnp.concatenate([pack(pulled_parts, turn), pack(last_parts, turn)], axis=0)
        both = both.astype(bf16)
        for index in range(model // HEAD_WIDTH):
            early_src[index * turns + turn] = tile(both, index)

    early = Exchange(at, early_src, early_dst, early_sems.at[0], early_sems.at[1])
    early.start()

    gather_o0.finish()
    gather_o1.finish()
    attended = mm(context_wide, full_o[...], 1, 1)
    attended = attended + pltpu.roll(attended, pairs, 0)
    residual = x_last + attended
    out_scale = lax.rsqrt(lane_mean(residual * residual) + EPSILON)
    out_unit = residual * out_scale
    gain = final_gain[...] * score_vector[...]
    score8 = jnp.sum(out_unit * gain, axis=-1, keepdims=True)

    lane8 = lax.broadcasted_iota(jnp.int32, (slots, HEAD_WIDTH), 1)
    row_lane = lax.broadcasted_iota(jnp.int32, (slots, HEAD_WIDTH), 0)

    def as_row(column):
        return jnp.sum(jnp.where(row_lane == lane8, column, 0.0), axis=0, keepdims=True)

    score_row = as_row(score8)
    lane1 = lax.broadcasted_iota(jnp.int32, (1, HEAD_WIDTH), 1)
    listing = jnp.where(lane1 < pairs, score_row, as_row(teacher8))
    list_src[...] = listing
    me_row = list_dst.at[at.me]
    list_here, list_there, list_sent = list_sems.at[0], list_sems.at[1], list_sems.at[2]
    for place_of, target in enumerate(at.others):
        arrived = list_here if place_of < at.neg_count - 1 else list_there
        remote(list_src, me_row, list_sent, arrived, target).start()
    list_dst[at.me] = listing
    scores_out[...] = score_row[:, :pairs]
    gather_context.middle()

    near_block = list_dst.at[pl.ds(0, at.neg_count - 1)]
    remote(near_block, near_block, list_sent, list_here, at.to_partner()).wait_recv()

    def total(array):
        return jnp.sum(jnp.sum(array, axis=1, keepdims=True), axis=0, keepdims=True)

    def query_terms(first):
        block = list_dst[pl.ds(first, at.neg_count)].reshape(at.neg_count, HEAD_WIDTH)
        real = lax.broadcasted_iota(jnp.int32, block.shape, 1) < pairs
        score = jnp.where(real, block, 0.0)
        scaled = pltpu.roll(block, HEAD_WIDTH - pairs, 1)
        scaled = jnp.where(real, scaled, 0.0) / TEACHER_TEMP
        expo_t = jnp.where(real, jnp.exp(scaled), 0.0)
        total_s = total(jnp.where(real, jnp.exp(score), 0.0))
        return score, scaled, expo_t, total_s, total(expo_t)

    _, _, _, total_s, total_t = query_terms(pl.multiple_of(at.pb * at.neg_count, at.neg_count))
    grad_score = GRAD_SCALE * (
        jnp.exp(score8) / total_s - jnp.exp(teacher8 / TEACHER_TEMP) / total_t
    )
    grad_unit = grad_score * gain
    grad_resid = out_scale * (grad_unit - out_unit * lane_mean(grad_unit * out_unit))
    resid_grad[...] = grad_resid
    resid_cast = grad_resid.astype(bf16)
    grad_context = stack_heads(mm(resid_cast, full_o[...])).astype(bf16)
    context_blocks[...] = blocks_of(grad_context.astype(f32))
    late_own[0:stacked, :] = grad_context

    grad_probs = mm(context_blocks[...], value_cast[...], 1, 1)
    spread = jnp.sum(attention_weights * grad_probs, axis=-1, keepdims=True)
    logit_gradient = (attention_weights * (grad_probs - spread)).astype(bf16)
    logit_grad[...] = logit_gradient

    turned_q = diagonal_of(mm(logit_gradient, key_rot[...])) * HEAD_WIDTH ** (-0.5)
    back_q = turned_q * cos_rows - pltpu.roll(turned_q, HEAD_WIDTH // 2, 1) * sin_rows
    back_q = query_scale * (back_q - query_unit * lane_mean(back_q * query_unit))
    grad_q_cast = back_q.astype(bf16)
    late_own[stacked : 2 * stacked, :] = grad_q_cast
    gather_late.start()
    gather_context.relay()

    cuts = 2
    cut_width = kv_width // cuts
    block_rows = model // at.pb_count

    def key_back(cut):
        columns = slice(cut * cut_width, (cut + 1) * cut_width)

        def one(pair, carry):
            rows = pl.ds(pl.multiple_of(pair * seq, seq), seq)
            turned = mm(logit_grad[:, rows], query_blocks[:, columns], 0, 0) * HEAD_WIDTH ** (-0.5)
            for group in range(groups // cuts):
                start = cut * cut_width + group * HEAD_WIDTH
                lanes = slice(start, start + HEAD_WIDTH)
                part = tile(turned, group)
                unit = key_unit[rows, lanes]
                back = part * cos_table[...] - pltpu.roll(part, HEAD_WIDTH // 2, 1) * sin_table[...]
                back = key_scale[rows, lanes] * (back - unit * lane_mean(back * unit))
                grad_k[rows, lanes] = back.astype(bf16)
            return carry

        lax.fori_loop(0, pairs, one, 0)

    def send(src, dst, send_sem, recv_sem, target):
        remote(src, dst, send_sem, recv_sem, target).start()

    def arrive(block, recv_sem):
        remote(block, block, any_sem, recv_sem, at.to_partner()).wait_recv()

    def key_products(cut):
        columns = slice(cut * cut_width, (cut + 1) * cut_width)
        for k in range(1, at.pb_count + 1):
            pb = at.pb_peer(k % at.pb_count)
            chosen = pl.ds(pl.multiple_of(pb * block_rows, block_rows), block_rows)
            product = mm(normed_t[chosen, :], grad_k[:, columns])
            partial[cut, pb] = product.astype(bf16).reshape(at.line_count, 2, share, cut_width)
            send(
                partial.at[cut, pb, :, at.partner],
                from_core.at[cut, pb],
                core_send,
                core_recv.at[cut, pb],
                at.to_partner(),
            )

    def key_pairs(cut):
        for k in range(1, at.pb_count + 1):
            pb = at.pb_peer(k % at.pb_count)
            arrive(from_core.at[cut, pb], core_recv.at[cut, pb])
            both = partial[cut, pb, :, at.core].astype(f32) + from_core[cut, pb].astype(f32)
            paired[pb, :, cut] = both.astype(bf16)
        for step in range(1, at.line_count + 1):
            line = at.line_peer(step % at.line_count)
            for k in range(1, at.pb_count):
                pb = at.pb_peer(k)
                send(
                    paired.at[pb, line, cut],
                    from_pb.at[at.pb, line, cut],
                    pb_send,
                    pb_recv.at[line],
                    at.to_pb(pb),
                )

    key_back(0)
    key_products(0)
    key_back(1)
    key_pairs(0)
    key_products(1)
    gather_late.middle()
    key_pairs(1)

    resid_parts = by_head(resid_cast.astype(f32))
    for turn in range(turns):
        packed = pack(resid_parts, turn).astype(bf16)
        for index in range(model // HEAD_WIDTH):
            resid_src[index * turns + turn] = tile(packed, index)
    resid = Exchange(at, resid_src, resid_dst, resid_sems.at[0], resid_sems.at[1])
    resid.start()

    back_last = mm(spread_heads(grad_q_cast.astype(f32)), full_q[...], 1, 1)
    last_grad[...] = back_last + pltpu.roll(back_last, pairs, 0)

    def value_back(pair, carry):
        start = pl.multiple_of(pair * seq, seq)
        rows = pl.ds(start, seq)
        grad_v[rows, :] = mm(probs_ref[:, rows], context_blocks[...], 0, 0).astype(bf16)
        return carry

    lax.fori_loop(0, pairs, value_back, 0)

    seq_row = lax.broadcasted_iota(jnp.int32, (seq, 1), 0)

    def hidden_back(pair, carry):
        rows = pl.ds(pl.multiple_of(pair * seq, seq), seq)
        total = mm(grad_k[rows, :], full_k[...], 1, 1) + mm(grad_v[rows, :], full_v[...], 1, 1)
        hit = seq_row == lengths[0, pair] - 1
        total = total + jnp.where(hit, last_grad[pl.ds(pair, 1), :], 0.0)
        scaled = total * norm_gain[...]
        wide = x[rows, :].astype(f32)
        inv = inv_wide[rows, 0:1]
        mean = lane_mean(scaled * wide)
        result = inv * scaled - wide * (inv * inv * inv * mean)
        result = result + jnp.where(hit, resid_grad[pl.ds(pair, 1), :], 0.0)
        grad_hidden[rows, :] = result.astype(bf16)
        return carry

    def add_line(step):
        line = at.line_peer(step % at.line_count)
        total = paired[at.pb, line].astype(f32)
        arrive(from_pb.at[pl.ds(0, at.pb_count - 1), line], pb_recv.at[line])
        for k in range(1, at.pb_count):
            pb = at.pb_peer(k)
            total = total + from_pb[pb, line].astype(f32)
        if step < at.line_count:
            summed[line] = total.astype(bf16)
            send(
                summed.at[line],
                from_line.at[at.line],
                line_send,
                line_recv,
                at.to_line(line),
            )
        return total

    hidden_back(0, 0)
    add_line(1)
    gather_late.relay()
    hidden_back(1, 0)
    add_line(2)
    gather_context.tail()
    hidden_back(2, 0)
    for step in range(3, at.line_count + 1):
        own_sum = add_line(step)
    gather_late.tail()
    for pair in range(3, pairs):
        hidden_back(pair, 0)

    far_block = list_dst.at[pl.ds(0, at.count - at.neg_count)]
    remote(far_block, far_block, list_sent, list_there, at.to_partner()).wait_recv()
    loss = jnp.zeros((1, 1), f32)
    for pb in range(at.pb_count):
        score, scaled, expo_t, sum_s, sum_t = query_terms(pb * at.neg_count)
        loss = loss + total(expo_t / sum_t * (scaled - jnp.log(sum_t) - (score - jnp.log(sum_s))))
    loss_out[...] = loss

    gather_context.finish()
    gather_late.finish()
    early.wait("wait_recv")
    resid.wait("wait_recv")

    def rows_of(full, start, group):
        wide = full[...].astype(f32).reshape(at.count, -1, slots, HEAD_WIDTH)
        return wide[:, start + group].reshape(at.count * slots, HEAD_WIDTH).astype(bf16)

    pulled_rows = rows_of(early_dst, 0, 0)
    last_rows = rows_of(early_dst, 1, 0)
    resid_rows = rows_of(resid_dst, 0, 0)
    for group in range(groups):
        found = mm(pulled_rows, rows_of(late_full, 0, group), 0, 0)
        lanes = slice(group * HEAD_WIDTH, (group + 1) * HEAD_WIDTH)
        grad_value[:, lanes] = found[group * share : (group + 1) * share]
        found = mm(last_rows, rows_of(late_full, groups, group), 0, 0)
        for part in range(per_group):
            head = per_group * group + part
            grad_query[:, head * HEAD_WIDTH : (head + 1) * HEAD_WIDTH] = found[
                part * share : (part + 1) * share
            ]
        found = mm(resid_rows, rows_of(context_full, 0, group), 0, 0)
        for part in range(per_group):
            head = per_group * group + part
            grad_out[:, head * HEAD_WIDTH : (head + 1) * HEAD_WIDTH] = found[
                part * share : (part + 1) * share
            ]

    final = own_sum
    arrive(from_line.at[pl.ds(0, at.line_count - 1)], line_recv)
    for step in range(1, at.line_count):
        line = at.line_peer(step)
        final = final + from_line[line].astype(f32)
    for cut in range(cuts):
        grad_key[:, cut * cut_width : (cut + 1) * cut_width] = final[cut]

    for gather in gathers:
        gather.drain()
    pieces = from_line.at[pl.ds(0, at.line_count - 1)]
    for block, sem in (
        (from_core, core_send),
        (from_pb.at[pl.ds(0, at.pb_count - 1)], pb_send),
        (pieces, line_send),
    ):
        remote(block, block, sem, any_sem, at.to_partner()).wait_send()
    early.wait("wait_send")
    resid.wait("wait_send")
    sent_block = list_dst.at[pl.ds(0, at.count - 1)]
    remote(sent_block, sent_block, list_sent, list_here, at.to_partner()).wait_send()


def write_kernel(count, *refs):
    sources, targets, sems = refs[:count], refs[count : 2 * count], refs[2 * count]
    copies = [
        pltpu.make_async_copy(sources[i], targets[i], sems.at[i]) for i in range(2, count)
    ]
    for copy in copies:
        copy.start()
    for i in range(2):
        targets[i][...] = sources[i][...]
    for copy in copies:
        copy.wait()


def write_outputs(arrays):
    count = len(arrays)
    return pl.pallas_call(
        functools.partial(write_kernel, count),
        out_shape=tuple(jax.ShapeDtypeStruct(a.shape, a.dtype) for a in arrays),
        in_specs=[VMEM_SPEC] * count,
        out_specs=(VMEM_SPEC,) * 2 + (pl.BlockSpec(memory_space=pl.ANY),) * (count - 2),
        scratch_shapes=[pltpu.SemaphoreType.DMA((count,))],
        compiler_params=pltpu.CompilerParams(vmem_limit_bytes=4 * 2**20),
    )(*arrays)


def run_step(operands, sizes, pb_count, neg_count):
    pairs, seq, groups, share = sizes
    x, own_q, own_k = operands[0], operands[8], operands[9]
    model, width, kv_width = x.shape[1], own_q.shape[1], own_k.shape[1]
    rows = pairs * seq
    count = pb_count * neg_count
    line_count = neg_count // 2
    slots = width // kv_width * pairs
    stacked = groups * slots
    bf16, f32 = jnp.bfloat16, jnp.float32
    block = (pb_count, line_count, 2, share, kv_width // 2)
    dma = pltpu.SemaphoreType.DMA
    vmem = pltpu.VMEM
    smem_spec = pl.BlockSpec(memory_space=pltpu.SMEM)
    hbm_spec = pl.BlockSpec(memory_space=pltpu.HBM)
    return pl.pallas_call(
        functools.partial(step_kernel, sizes),
        out_shape=(
            vmem((1, pairs), f32),
            vmem((1, 1), f32),
            vmem((rows, model), bf16),
            vmem((share, width), f32),
            vmem((share, kv_width), f32),
            vmem((share, kv_width), f32),
            vmem((share, width), f32),
        ),
        in_specs=[hbm_spec, smem_spec, smem_spec] + [hbm_spec] * 9,
        out_specs=(VMEM_SPEC,) * 7,
        scratch_shapes=[
            vmem((rows, model), bf16),
        ]
        + [vmem(a.shape, a.dtype) for a in operands[3:]]
        + [
            vmem((model, width), bf16),
            vmem((model, kv_width), bf16),
            vmem((model, kv_width), bf16),
            vmem((model, width), bf16),
            vmem((rows, model), bf16),
            vmem((model, rows), bf16),
            vmem((rows, HEAD_WIDTH), f32),
            vmem((rows, kv_width), f32),
            vmem((rows, kv_width), f32),
            vmem((rows, kv_width), bf16),
            vmem((rows, kv_width), bf16),
            vmem((rows, kv_width), bf16),
            vmem((rows, kv_width), bf16),
            vmem((stacked, rows), bf16),
            vmem((stacked, rows), bf16),
            vmem((stacked, kv_width), bf16),
            vmem((stacked, kv_width), bf16),
            vmem((slots, model), f32),
            vmem((slots, model), f32),
            vmem((stacked, HEAD_WIDTH), bf16),
            vmem((stacked * count, HEAD_WIDTH), bf16),
            vmem((2 * stacked, HEAD_WIDTH), bf16),
            vmem((2 * stacked * count, HEAD_WIDTH), bf16),
            vmem((count, 2 * slots, HEAD_WIDTH), bf16),
            vmem((count, 2 * slots, HEAD_WIDTH), bf16),
            vmem((count, slots, HEAD_WIDTH), bf16),
            vmem((count, slots, HEAD_WIDTH), bf16),
            vmem((1, HEAD_WIDTH), f32),
            vmem((count, 1, HEAD_WIDTH), f32),
            vmem((2, pb_count, line_count, 2, share, kv_width // 2), bf16),
            vmem((2, pb_count, line_count, share, kv_width // 2), bf16),
            vmem(block, bf16),
            vmem(block, bf16),
            vmem(block[1:], bf16),
            vmem(block[1:], bf16),
            dma((2,)),
            dma((2,)),
            dma((3,)),
            dma,
            dma((2, pb_count)),
            dma,
            dma((line_count,)),
            dma,
            dma,
            dma,
            dma((pairs + 9,)),
        ]
        + gather_sems(neg_count, True) * 6
        + gather_sems(neg_count, False) * 2,
        compiler_params=pltpu.CompilerParams(
            collective_id=0, has_side_effects=True, vmem_limit_bytes=62 * 2**20
        ),
    )(*operands)


def shards(
    hidden,
    lengths,
    teacher,
    norm_gain,
    final_gain,
    score_vector,
    query_weight,
    key_matrix,
    value_matrix,
    out_weight,
):
    both = ("pb", "neg")
    width = query_weight.shape[1]
    kv_width = key_matrix.shape[1]
    share, out_share = query_weight.shape[0], out_weight.shape[1]
    pb_count, neg_count = lax.axis_size("pb"), lax.axis_size("neg")
    pair_count, seq_len, model_width = hidden.shape[1:]
    group_count = kv_width // HEAD_WIDTH
    own_kernels = (
        pb_count == 4
        and neg_count == 8
        and share == out_share
        and share % 32 == 0
        and model_width == share * pb_count * neg_count
        and width == 2 * kv_width
        and pair_count * 2 == 8
        and seq_len == HEAD_WIDTH
        and share * group_count == HEAD_WIDTH
    )
    if own_kernels:
        cos_table, sin_table = signed_tables(seq_len, HEAD_WIDTH)
        results = run_step(
            (
                hidden.reshape(pair_count * seq_len, model_width),
                lengths,
                teacher,
                norm_gain[None],
                final_gain[None],
                score_vector[None],
                cos_table,
                sin_table,
                query_weight,
                key_matrix,
                value_matrix,
                out_weight.T,
            ),
            (pair_count, seq_len, group_count, share),
            pb_count,
            neg_count,
        )
        scores, loss, grad_rows, grad_query, grad_key, grad_value, grad_out = write_outputs(results)
        return (
            scores,
            loss.reshape(()),
            grad_rows.reshape(hidden.shape),
            grad_query,
            grad_key,
            grad_value,
            grad_out.T,
        )
    packed = jnp.concatenate([query_weight, key_matrix, value_matrix, out_weight.T], axis=1)
    everything = lax.all_gather(packed, both, axis=0, tiled=True)
    full_query = everything[:, :width]
    full_key = everything[:, width : width + kv_width]
    full_value = everything[:, width + kv_width : width + 2 * kv_width]
    full_out_t = everything[:, width + 2 * kv_width :]
    weights = (full_query, full_key, full_value, full_out_t.T)
    scores_here, stored = forward_pairs(
        hidden[0], lengths[0], norm_gain, final_gain, score_vector, *weights
    )
    listing = jnp.concatenate([scores_here, teacher[0]])[None]
    listed = lax.all_gather(listing, "neg", axis=0, tiled=True)
    all_scores = listed[:, :pair_count]
    all_scaled = listed[:, pair_count:] / TEACHER_TEMP
    my_total_s = jnp.sum(jnp.exp(all_scores))
    expo_t = jnp.exp(all_scaled)
    my_total_t = jnp.sum(expo_t)
    loss_here = jnp.sum(
        expo_t
        / my_total_t
        * (all_scaled - jnp.log(my_total_t) - (all_scores - jnp.log(my_total_s)))
    )
    prob_s = jnp.exp(scores_here) / my_total_s
    prob_t = jnp.exp(teacher[0] / TEACHER_TEMP) / my_total_t
    grad_score = GRAD_SCALE * (prob_s - prob_t)
    grad_input, last_rows, grad_kv = backward_pairs(
        stored, grad_score, norm_gain, final_gain, score_vector, *weights
    )
    grad_kv = grad_kv.astype(jnp.bfloat16)
    reduced = lax.psum_scatter(grad_kv, both, scatter_dimension=0, tiled=True)
    reduced = reduced.astype(jnp.float32)
    rows = lax.all_gather(last_rows, both, axis=0, tiled=True)
    loss_value = lax.psum(loss_here, "pb")
    index = lax.axis_index("pb") * neg_count + lax.axis_index("neg")
    normed_cols = lax.dynamic_slice_in_dim(rows, index * share, share, axis=1)
    resid_cols = lax.dynamic_slice_in_dim(rows, model_width + index * out_share, out_share, axis=1)
    rest = 2 * model_width
    all_q = rows[:, rest : rest + width]
    all_context = rows[:, rest + width :]
    grad_query = jnp.dot(normed_cols.T, all_q, preferred_element_type=jnp.float32)
    grad_out = jnp.dot(all_context.T, resid_cols, preferred_element_type=jnp.float32)
    return (
        scores_here[None],
        loss_value,
        grad_input[None],
        grad_query,
        reduced[:, :kv_width],
        reduced[:, kv_width:],
        grad_out,
    )


def solution(mesh):
    placed = (
        P("pb", "neg", None, None),
        P("pb", "neg"),
        P("pb", "neg"),
        P(),
        P(),
        P(),
        P(("pb", "neg"), None),
        P(("pb", "neg"), None),
        P(("pb", "neg"), None),
        P(None, ("pb", "neg")),
    )
    return jax.shard_map(
        shards,
        mesh=mesh,
        in_specs=placed,
        out_specs=(
            P("pb", "neg"),
            P(),
            P("pb", "neg", None, None),
            P(("pb", "neg"), None),
            P(("pb", "neg"), None),
            P(("pb", "neg"), None),
            P(None, ("pb", "neg")),
        ),
        check_vma=False,
    )
```

```python
import functools

import jax
import jax.numpy as jnp
import numpy as np
from jax import lax
from jax.experimental import pallas as pl
from jax.experimental.pallas import tpu as pltpu
from jax.sharding import PartitionSpec as P

HEAD_WIDTH = 128
MESH_ID = pl.DeviceIdType.MESH

EPSILON = 1e-06
ROPE_BASE = 1000000.0
TEACHER_TEMP = 2.0
GRAD_SCALE = 512.0


def rope_tables(seq_len, head_size):
    half = head_size // 2
    freqs = ROPE_BASE ** (-(jnp.arange(half, dtype=jnp.float32) * 2.0) / head_size)
    angles = jnp.arange(seq_len, dtype=jnp.float32)[:, None] * freqs[None, :]
    angles = jnp.concatenate([angles, angles], axis=1)
    return (jnp.cos(angles), jnp.sin(angles))


def signed_tables(seq_len, head_size):
    half = head_size // 2
    freqs = ROPE_BASE ** (-(np.arange(half) * 2.0) / head_size)
    angles = np.arange(seq_len)[:, None] * freqs[None, :]
    cos = np.concatenate([np.cos(angles)] * 2, axis=1)
    sin = np.concatenate([-np.sin(angles), np.sin(angles)], axis=1)
    return (jnp.asarray(cos, jnp.float32), jnp.asarray(sin, jnp.float32))


def rotate_half(vector):
    half = vector.shape[-1] // 2
    return jnp.concatenate([-vector[..., half:], vector[..., :half]], axis=-1)


def unrotate_half(vector):
    half = vector.shape[-1] // 2
    return jnp.concatenate([vector[..., half:], -vector[..., :half]], axis=-1)


def forward_pairs(
    tokens_in,
    lengths_here,
    norm_gain,
    final_gain,
    score_vector,
    query_weight,
    key_matrix,
    value_matrix,
    out_weight,
):
    pair_count, seq_len, model_width = tokens_in.shape
    head_count = query_weight.shape[1] // HEAD_WIDTH
    group_count = key_matrix.shape[1] // HEAD_WIDTH
    group_size = head_count // group_count
    inputs_wide = tokens_in.astype(jnp.float32)
    inv_rms = lax.rsqrt(jnp.mean(inputs_wide * inputs_wide, axis=-1, keepdims=True) + EPSILON)
    normed = (inputs_wide * inv_rms * norm_gain).astype(jnp.bfloat16)
    flat_rows = normed.reshape(pair_count * seq_len, model_width)
    key_proj = jnp.dot(flat_rows, key_matrix, preferred_element_type=jnp.float32).reshape(
        pair_count, seq_len, group_count, HEAD_WIDTH
    )
    value_proj = jnp.dot(flat_rows, value_matrix, preferred_element_type=jnp.float32).reshape(
        pair_count, seq_len, group_count, HEAD_WIDTH
    )
    positions = jnp.arange(seq_len, dtype=jnp.int32)
    last_index = lengths_here - 1
    onehot = (positions[None, :] == last_index[:, None]).astype(jnp.float32)
    normed_last = jnp.take_along_axis(normed, last_index[:, None, None], axis=1)[:, 0]
    query_proj = jnp.dot(normed_last, query_weight, preferred_element_type=jnp.float32).reshape(
        pair_count, head_count, HEAD_WIDTH
    )
    query_scale = lax.rsqrt(jnp.mean(query_proj * query_proj, axis=-1, keepdims=True) + EPSILON)
    query_unit = query_proj * query_scale
    key_scale = lax.rsqrt(jnp.mean(key_proj * key_proj, axis=-1, keepdims=True) + EPSILON)
    key_unit = key_proj * key_scale
    cos_table, sin_table = rope_tables(seq_len, HEAD_WIDTH)
    cos_query = jnp.dot(onehot, cos_table, precision=lax.Precision.HIGHEST)
    sin_query = jnp.dot(onehot, sin_table, precision=lax.Precision.HIGHEST)
    query_rot = (
        query_unit * cos_query[:, None, :] + rotate_half(query_unit) * sin_query[:, None, :]
    ).astype(jnp.bfloat16)
    key_rot = (
        key_unit * cos_table[None, :, None, :] + rotate_half(key_unit) * sin_table[None, :, None, :]
    ).astype(jnp.bfloat16)
    value_cast = value_proj.astype(jnp.bfloat16)
    grouped = query_rot.reshape(pair_count, group_count, group_size, HEAD_WIDTH)
    logits = jnp.einsum(
        "pkgd,pskd->pkgs", grouped, key_rot, preferred_element_type=jnp.float32
    ) * HEAD_WIDTH ** (-0.5)
    visible = (positions[None, :] <= last_index[:, None])[:, None, None, :]
    expos = jnp.where(visible, jnp.exp(logits), 0.0)
    attention_weights = expos / jnp.sum(expos, axis=-1, keepdims=True)
    probs_cast = attention_weights.astype(jnp.bfloat16)
    context = jnp.einsum(
        "pkgs,pskd->pkgd", probs_cast, value_cast, preferred_element_type=jnp.float32
    )
    context = context.astype(jnp.bfloat16).reshape(pair_count, head_count * HEAD_WIDTH)
    attended = jnp.dot(context, out_weight, preferred_element_type=jnp.float32)
    residual = jnp.take_along_axis(inputs_wide, last_index[:, None, None], axis=1)[:, 0] + attended
    out_scale = lax.rsqrt(jnp.mean(residual * residual, axis=-1, keepdims=True) + EPSILON)
    out_unit = residual * out_scale
    scores_here = jnp.sum(out_unit * final_gain * score_vector, axis=-1)
    stored = (
        tokens_in,
        onehot,
        inv_rms,
        normed,
        normed_last,
        query_unit,
        query_scale,
        key_unit,
        key_scale,
        cos_query,
        sin_query,
        cos_table,
        sin_table,
        query_rot,
        key_rot,
        value_cast,
        attention_weights,
        probs_cast,
        context,
        out_unit,
        out_scale,
    )
    return (scores_here, stored)


def backward_pairs(
    stored,
    grad_score,
    norm_gain,
    final_gain,
    score_vector,
    query_weight,
    key_matrix,
    value_matrix,
    out_weight,
):
    (
        tokens_in,
        onehot,
        inv_rms,
        normed,
        normed_last,
        query_unit,
        query_scale,
        key_unit,
        key_scale,
        cos_query,
        sin_query,
        cos_table,
        sin_table,
        query_rot,
        key_rot,
        value_cast,
        attention_weights,
        probs_cast,
        context,
        out_unit,
        out_scale,
    ) = stored
    pair_count, seq_len, model_width = tokens_in.shape
    head_count = query_weight.shape[1] // HEAD_WIDTH
    group_count = key_matrix.shape[1] // HEAD_WIDTH
    group_size = head_count // group_count
    grad_unit = grad_score[:, None] * score_vector * final_gain
    grad_resid = out_scale * (
        grad_unit - out_unit * jnp.mean(grad_unit * out_unit, axis=-1, keepdims=True)
    )
    grad_resid_cast = grad_resid.astype(jnp.bfloat16)
    grad_context = jnp.dot(
        grad_resid_cast, out_weight.T, preferred_element_type=jnp.float32
    ).astype(jnp.bfloat16)
    grad_context = grad_context.reshape(pair_count, group_count, group_size, HEAD_WIDTH)
    grad_probs = jnp.einsum(
        "pkgd,pskd->pkgs", grad_context, value_cast, preferred_element_type=jnp.float32
    )
    grad_vals = jnp.einsum(
        "pkgs,pkgd->pskd", probs_cast, grad_context, preferred_element_type=jnp.float32
    )
    spread = jnp.sum(attention_weights * grad_probs, axis=-1, keepdims=True)
    logit_gradient = (attention_weights * (grad_probs - spread)).astype(jnp.bfloat16)
    grouped = query_rot.reshape(pair_count, group_count, group_size, HEAD_WIDTH)
    rotated_query_gradient = jnp.einsum(
        "pkgs,pskd->pkgd", logit_gradient, key_rot, preferred_element_type=jnp.float32
    ) * HEAD_WIDTH ** (-0.5)
    rotated_query_gradient = rotated_query_gradient.reshape(pair_count, head_count, HEAD_WIDTH)
    grad_krot = jnp.einsum(
        "pkgs,pkgd->pskd", logit_gradient, grouped, preferred_element_type=jnp.float32
    ) * HEAD_WIDTH ** (-0.5)
    grad_qunit = rotated_query_gradient * cos_query[:, None, :] + unrotate_half(
        rotated_query_gradient * sin_query[:, None, :]
    )
    grad_kunit = grad_krot * cos_table[None, :, None, :] + unrotate_half(
        grad_krot * sin_table[None, :, None, :]
    )
    grad_qproj = query_scale * (
        grad_qunit - query_unit * jnp.mean(grad_qunit * query_unit, axis=-1, keepdims=True)
    )
    grad_kproj = key_scale * (
        grad_kunit - key_unit * jnp.mean(grad_kunit * key_unit, axis=-1, keepdims=True)
    )
    grad_q_cast = grad_qproj.reshape(pair_count, head_count * HEAD_WIDTH).astype(jnp.bfloat16)
    grad_k_cast = grad_kproj.reshape(pair_count * seq_len, group_count * HEAD_WIDTH).astype(
        jnp.bfloat16
    )
    grad_v_cast = grad_vals.reshape(pair_count * seq_len, group_count * HEAD_WIDTH).astype(
        jnp.bfloat16
    )
    flat_rows = normed.reshape(pair_count * seq_len, model_width)
    last_rows = jnp.concatenate([normed_last, grad_resid_cast, grad_q_cast, context], axis=1)
    grad_kv = jnp.dot(
        flat_rows.T,
        jnp.concatenate([grad_k_cast, grad_v_cast], axis=1),
        preferred_element_type=jnp.float32,
    )
    grad_normed = jnp.dot(grad_k_cast, key_matrix.T, preferred_element_type=jnp.float32)
    grad_normed = grad_normed + jnp.dot(
        grad_v_cast, value_matrix.T, preferred_element_type=jnp.float32
    )
    grad_normed = grad_normed.reshape(pair_count, seq_len, model_width)
    grad_last = jnp.dot(grad_q_cast, query_weight.T, preferred_element_type=jnp.float32)
    grad_normed = grad_normed + onehot[:, :, None] * grad_last[:, None, :]
    inputs_wide = tokens_in.astype(jnp.float32)
    grad_scaled = grad_normed * norm_gain
    grad_input = inv_rms * grad_scaled - inputs_wide * inv_rms * inv_rms * inv_rms * jnp.mean(
        grad_scaled * inputs_wide, axis=-1, keepdims=True
    )
    grad_input = grad_input + onehot[:, :, None] * grad_resid[:, None, :]
    return (grad_input.astype(jnp.bfloat16), last_rows, grad_kv)


class Place:
    def __init__(self):
        self.pb_count = lax.axis_size("pb")
        self.neg_count = lax.axis_size("neg")
        self.line_count = self.neg_count // 2
        self.pb = lax.axis_index("pb")
        neg = lax.axis_index("neg")
        self.line = neg // 2
        self.core = neg % 2
        self.partner = 1 - self.core

    def slot(self, pb, line, core):
        return pb * self.neg_count + line * 2 + core

    def line_peer(self, step):
        return lax.rem(self.line + step, self.line_count)

    def pb_peer(self, step):
        return lax.rem(self.pb + step, self.pb_count)

    def to_line(self, line):
        return (self.pb, line * 2 + self.core)

    def to_pb(self, pb):
        return (pb, self.line * 2 + self.core)

    def to_partner(self):
        return (self.pb, self.line * 2 + self.partner)

    def greet(self):
        barrier = pltpu.get_barrier_semaphore()
        targets = [self.to_line(self.line_peer(k)) for k in range(1, self.line_count)]
        targets += [self.to_pb(self.pb_peer(k)) for k in range(1, self.pb_count)]
        targets += [self.to_partner()]
        for target in targets:
            pl.semaphore_signal(barrier, inc=1, device_id=target, device_id_type=MESH_ID)
        pl.semaphore_wait(barrier, len(targets))


def remote(src, dst, send_sem, recv_sem, target):
    return pltpu.make_async_remote_copy(
        src_ref=src,
        dst_ref=dst,
        send_sem=send_sem,
        recv_sem=recv_sem,
        device_id=target,
        device_id_type=MESH_ID,
    )


def gather_sems(neg_count, large):
    line_count = neg_count // 2
    dma = pltpu.SemaphoreType.DMA
    if large:
        return [dma((line_count,)), dma((line_count,)), dma((line_count,)), dma((2,))]
    return [dma((1,)), dma((1,)), dma((1,)), dma((2,))]


class Gather:
    def __init__(self, place, own, full, sems, halve_corner, direct):
        self.place, self.own, self.full = place, own, full
        self.line_recv, self.pb_recv, self.corner_recv, ends = sems
        self.send_sem, self.core_recv = ends.at[0], ends.at[1]
        self.halve_corner, self.direct = halve_corner, direct
        across = place.pb + 1 - 2 * (place.pb % 2)
        along = place.pb + 2 - 4 * (place.pb // 2)
        self.near = (across, along)
        self.corner = 3 - place.pb
        half = place.line // 2
        self.is_inner = (place.line == 1) | (place.line == 2)
        self.mate = place.line + 1 - 2 * (place.line % 2)
        self.far_inner = 2 - half
        self.far_outer = 3 - 3 * half
        self.size = own.shape[0]
        if halve_corner:
            self.own_lines = (place.line, lax.rem(place.line + 2, 4))
            self.mate_lines = (self.mate, lax.rem(self.mate + 2, 4))
        else:
            self.own_lines = (place.line, self.mate, self.far_inner, self.far_outer)
            self.mate_lines = ()

    def rows(self, pb, line, core):
        start = self.place.slot(pb, line, core) * self.size
        return self.full.at[pl.ds(pl.multiple_of(start, self.size), self.size)]

    def blocks(self, count):
        return self.full.at[pl.ds(0, count * self.size)]

    def send(self, src, dst, recv_sem, target):
        remote(src, dst, self.send_sem, recv_sem, target).start()

    def of(self, sems, line):
        return sems.at[0] if self.direct else sems.at[line]

    def spread(self, src, line):
        at = self.place
        dst = self.rows(at.pb, line, at.core)
        for side in range(2):
            self.send(src, dst, self.of(self.pb_recv, line), at.to_pb(self.near[side]))
        self.pass_on(src, at.pb, line)

    def pass_on(self, src, pb, line):
        at = self.place
        self.send(src, self.rows(pb, line, at.core), self.core_recv, at.to_partner())

    def arrive(self, block, recv_sem):
        remote(block, block, self.send_sem, recv_sem, self.place.to_partner()).wait_recv()

    def start(self):
        at = self.place
        mine = self.rows(at.pb, at.line, at.core)
        peers = (self.mate, self.far_inner) + ((self.far_outer,) if self.direct else ())
        for line in peers:
            self.send(self.own, mine, self.of(self.line_recv, at.line), at.to_line(line))
        self.spread(self.own, at.line)
        mine[...] = self.own[...]

    def middle(self):
        at = self.place
        if self.direct:
            self.arrive(self.blocks(at.line_count - 1), self.line_recv.at[0])
        for line in (self.mate, self.far_inner, self.far_outer):
            block = self.rows(at.pb, line, at.core)
            if not self.direct:
                self.arrive(block, self.line_recv.at[line])
                if line is not self.mate:

                    @pl.when(self.is_inner)
                    def _():
                        self.send(block, block, self.line_recv.at[line], at.to_line(self.mate))

            self.spread(block, line)

    def half(self, block, side):
        size = block.shape[0] // 2
        return block.at[pl.ds(side * size, size)]

    def relay(self):
        at = self.place
        if self.direct:
            self.arrive(self.blocks(2 * at.line_count), self.pb_recv.at[0])
        for line in self.own_lines + self.mate_lines:
            if not self.direct:
                self.arrive(self.blocks(2), self.pb_recv.at[line])
            for side in range(2):
                block = self.rows(self.near[side], line, at.core)
                if not any(line is other for other in self.mate_lines):
                    part = self.half(block, side)
                    target = at.to_pb(self.near[1 - side])
                    self.send(part, part, self.of(self.corner_recv, line), target)
                self.pass_on(block, self.near[side], line)

    def corner_in(self, lines, hand_over):
        at = self.place
        if self.direct:
            self.arrive(self.blocks(at.line_count), self.corner_recv.at[0])
        for line in lines:
            block = self.rows(self.corner, line, at.core)
            if not self.direct:
                self.arrive(block, self.corner_recv.at[line])
            if hand_over:
                self.send(block, block, self.corner_recv.at[line], at.to_line(self.mate))
            self.pass_on(block, self.corner, line)

    def hand(self):
        if self.halve_corner:
            self.corner_in(self.own_lines, True)

    def tail(self):
        self.corner_in(self.mate_lines if self.halve_corner else self.own_lines, False)

    def finish(self):
        self.arrive(self.blocks(self.place.count // 2), self.core_recv)

    def drain(self):
        at = self.place
        block = self.blocks(at.count - (1 if self.direct else 2))
        remote(block, block, self.send_sem, self.core_recv, at.to_partner()).wait_send()
        if not self.direct:

            @pl.when(self.is_inner)
            def _():
                block = self.blocks(2)
                remote(block, block, self.send_sem, self.core_recv, at.to_partner()).wait_send()


VMEM_SPEC = pl.BlockSpec(memory_space=pltpu.VMEM)


def mm(left, right, left_dim=1, right_dim=0, precision=None):
    return lax.dot_general(
        left,
        right,
        (((left_dim,), (right_dim,)), ((), ())),
        preferred_element_type=jnp.float32,
        precision=precision,
    )


def lane_mean(array):
    return jnp.mean(array, axis=-1, keepdims=True)


def tile(array, index):
    return array[:, index * HEAD_WIDTH : (index + 1) * HEAD_WIDTH]


class Exchange:
    def __init__(self, at, src, dst, send_sem, recv_sem):
        self.at, self.src, self.dst = at, src, dst
        self.send_sem, self.recv_sem = send_sem, recv_sem

    def start(self):
        at = self.at
        for pb, neg in at.others:
            peer = pb * at.neg_count + neg
            remote(
                self.src.at[peer], self.dst.at[at.me], self.send_sem, self.recv_sem, (pb, neg)
            ).start()
        self.dst[at.me] = self.src[at.me]

    def wait(self, sem_of):
        block = self.dst.at[pl.ds(0, self.at.count - 1)]
        copy = remote(block, block, self.send_sem, self.recv_sem, self.at.to_partner())
        getattr(copy, sem_of)()


def step_kernel(
    sizes,
    hidden,
    lengths,
    teacher,
    norm_gain_in,
    final_gain_in,
    score_vector_in,
    cos_table_in,
    sin_table_in,
    own_q_in,
    own_k_in,
    own_v_in,
    own_o_in,
    scores_out,
    loss_out,
    grad_hidden,
    grad_query,
    grad_key,
    grad_value,
    grad_out,
    x,
    norm_gain,
    final_gain,
    score_vector,
    cos_table,
    sin_table,
    own_q,
    own_k,
    own_v,
    own_o,
    full_q,
    full_k,
    full_v,
    full_o,
    normed,
    normed_t,
    inv_wide,
    key_unit,
    key_scale,
    key_rot,
    value_cast,
    grad_k,
    grad_v,
    logit_grad,
    probs_ref,
    query_blocks,
    context_blocks,
    last_grad,
    resid_grad,
    context_own,
    context_full,
    late_own,
    late_full,
    early_src,
    early_dst,
    resid_src,
    resid_dst,
    list_src,
    list_dst,
    partial,
    from_core,
    paired,
    from_pb,
    summed,
    from_line,
    early_sems,
    resid_sems,
    list_sems,
    core_send,
    core_recv,
    pb_send,
    pb_recv,
    line_send,
    line_recv,
    any_sem,
    load_sems,
    *gather_sem_refs,
):
    pairs, seq, groups, share = sizes
    bf16, f32 = jnp.bfloat16, jnp.float32
    at = Place()
    at.count = at.pb_count * at.neg_count
    at.me = at.slot(at.pb, at.line, at.core)
    neg = lax.axis_index("neg")
    pb_all = [at.pb] + [at.pb_peer(k) for k in range(1, at.pb_count)]
    neg_all = [neg] + [lax.rem(neg + k, at.neg_count) for k in range(1, at.neg_count)]
    at.others = [
        (pb, peer)
        for i, pb in enumerate(pb_all)
        for j, peer in enumerate(neg_all)
        if i + j > 0
    ]
    model = x.shape[1]
    rows_all = pairs * seq
    per_group = own_q.shape[1] // own_k.shape[1]
    slots = per_group * pairs
    stacked = groups * slots
    kv_width = groups * HEAD_WIDTH

    barrier = pltpu.get_barrier_semaphore()

    for target in at.others:
        pl.semaphore_signal(barrier, inc=1, device_id=target, device_id_type=MESH_ID)
    loads = []
    moves = (
        (own_k_in, own_k),
        (own_v_in, own_v),
        (own_q_in, own_q),
        (own_o_in, own_o),
        (norm_gain_in, norm_gain),
        (final_gain_in, final_gain),
        (score_vector_in, score_vector),
        (cos_table_in, cos_table),
        (sin_table_in, sin_table),
    )
    small_loads = []
    for place_of, (source, target) in enumerate(moves):
        load = pltpu.make_async_copy(source, target, load_sems.at[pairs + place_of])
        load.start()
        small_loads.append(load)
    for pair in range(pairs):
        rows = pl.ds(pair * seq, seq)
        load = pltpu.make_async_copy(hidden.at[rows], x.at[rows], load_sems.at[pair])
        load.start()
        loads.append(load)

    half_width = own_q.shape[1] // 2
    low, high = pl.ds(0, half_width), pl.ds(half_width, half_width)
    parts = (
        (own_k, full_k, True),
        (own_v, full_v, True),
        (own_q.at[:, low], full_q.at[:, low], True),
        (own_q.at[:, high], full_q.at[:, high], True),
        (own_o.at[:, low], full_o.at[:, low], True),
        (own_o.at[:, high], full_o.at[:, high], False),
        (context_own, context_full, False),
        (late_own, late_full, False),
    )
    each = len(gather_sem_refs) // len(parts)
    gathers = [
        Gather(at, own, full, gather_sem_refs[i * each : (i + 1) * each], halve, i >= 6)
        for i, (own, full, halve) in enumerate(parts)
    ]
    gather_k, gather_v, gather_q0, gather_q1, gather_o0, gather_o1 = gathers[:6]
    gather_context, gather_late = gathers[6:]

    for load in small_loads:
        load.wait()
    pl.semaphore_wait(barrier, at.count - 1)
    for gather in gathers[:4]:
        gather.start()

    def norm_pair(pair, carry):
        rows = pl.ds(pl.multiple_of(pair * seq, seq), seq)
        wide = x[rows, :].astype(f32)
        inv = lax.rsqrt(lane_mean(wide * wide) + EPSILON)
        inv_wide[rows, :] = jnp.broadcast_to(inv, (seq, HEAD_WIDTH))
        scaled = wide * inv * norm_gain[...]
        normed[rows, :] = scaled.astype(bf16)
        normed_t[:, rows] = scaled.T.astype(bf16)
        return carry

    for pair in range(pairs):
        loads[pair].wait()
        norm_pair(pair, 0)

    row8 = lax.broadcasted_iota(jnp.int32, (slots, 1), 0)
    pair8 = lax.rem(row8, pairs)
    upper8 = row8 < pairs
    last8 = jnp.zeros((slots, 1), jnp.int32)
    teacher8 = jnp.zeros((slots, 1), f32)
    for pair in range(pairs):
        last8 = jnp.where(pair8 == pair, lengths[0, pair] - 1, last8)
        teacher8 = jnp.where(pair8 == pair, teacher[0, pair], teacher8)
    place8 = pair8 * seq + last8
    column8 = lax.broadcasted_iota(jnp.int32, (slots, rows_all), 1)
    onehot8 = (column8 == place8).astype(f32).astype(bf16)
    visible8 = (column8 >= pair8 * seq) & (column8 <= place8)
    visible = jnp.concatenate([visible8.astype(f32)] * groups, axis=0) > 0.5
    position8 = (lax.broadcasted_iota(jnp.int32, (slots, seq), 1) == last8).astype(f32)

    x_last = mm(onehot8, x[...])
    normed_last = mm(onehot8, normed[...]).astype(bf16)
    cos8 = mm(position8, cos_table[...], precision=lax.Precision.HIGHEST)
    sin8 = mm(position8, sin_table[...], precision=lax.Precision.HIGHEST)
    cos_rows = jnp.concatenate([cos8] * groups, axis=0)
    sin_rows = jnp.concatenate([sin8] * groups, axis=0)

    def key_pair(pair, carry):
        rows = pl.ds(pl.multiple_of(pair * seq, seq), seq)
        proj = mm(normed[rows, :], full_k[...])
        for group in range(groups):
            lanes = slice(group * HEAD_WIDTH, (group + 1) * HEAD_WIDTH)
            part = proj[:, lanes]
            scale = lax.rsqrt(lane_mean(part * part) + EPSILON)
            unit = part * scale
            key_unit[rows, lanes] = unit
            key_scale[rows, lanes] = jnp.broadcast_to(scale, (seq, HEAD_WIDTH))
            turned = unit * cos_table[...] + pltpu.roll(unit, HEAD_WIDTH // 2, 1) * sin_table[...]
            key_rot[rows, lanes] = turned.astype(bf16)
        return carry

    def value_pair(pair, carry):
        rows = pl.ds(pl.multiple_of(pair * seq, seq), seq)
        value_cast[rows, :] = mm(normed[rows, :], full_v[...]).astype(bf16)
        return carry

    gather_k.middle()
    gather_o0.start()
    gather_o1.start()
    gather_v.middle()
    gather_q0.middle()
    gather_k.relay()
    gather_q1.middle()
    gather_v.relay()
    gather_k.hand()
    gather_o0.middle()
    gather_o1.middle()
    gather_q0.relay()
    gather_v.hand()
    gather_q1.relay()
    gather_q0.hand()
    gather_k.tail()
    gather_o0.relay()
    gather_q1.hand()
    gather_v.tail()
    gather_o1.relay()
    gather_o0.hand()
    gather_q0.tail()
    gather_k.finish()
    for pair in range(pairs):
        key_pair(pair, 0)
    gather_q1.tail()
    gather_v.finish()
    for pair in range(pairs):
        value_pair(pair, 0)
    gather_o0.tail()
    gather_q0.finish()
    gather_q1.finish()

    def stack_heads(wide):
        return jnp.concatenate(
            [
                jnp.where(upper8, tile(wide, per_group * group), tile(wide, per_group * group + 1))
                for group in range(groups)
            ],
            axis=0,
        )

    def spread_heads(stack):
        parts = []
        for group in range(groups):
            part = stack[group * slots : (group + 1) * slots]
            parts += [jnp.where(upper8, part, 0.0), jnp.where(upper8, 0.0, part)]
        return jnp.concatenate(parts, axis=1).astype(bf16)

    def diagonal_of(wide):
        return jnp.concatenate(
            [
                wide[group * slots : (group + 1) * slots, group * HEAD_WIDTH : (group + 1) * HEAD_WIDTH]
                for group in range(groups)
            ],
            axis=0,
        )

    def blocks_of(stack):
        rows = []
        for group in range(groups):
            part = stack[group * slots : (group + 1) * slots]
            rows.append(
                jnp.concatenate(
                    [part if other == group else jnp.zeros_like(part) for other in range(groups)],
                    axis=1,
                )
            )
        return jnp.concatenate(rows, axis=0).astype(bf16)

    query_proj = stack_heads(mm(normed_last, full_q[...]))
    query_scale = lax.rsqrt(lane_mean(query_proj * query_proj) + EPSILON)
    query_unit = query_proj * query_scale
    query_rot = query_unit * cos_rows + pltpu.roll(query_unit, HEAD_WIDTH // 2, 1) * sin_rows
    query_wide = blocks_of(query_rot)
    query_blocks[...] = query_wide
    logits = mm(query_wide, key_rot[...], 1, 1) * HEAD_WIDTH ** (-0.5)
    expos = jnp.where(visible, jnp.exp(logits), 0.0)
    attention_weights = expos / jnp.sum(expos, axis=-1, keepdims=True)
    probs = attention_weights.astype(bf16)
    probs_ref[...] = attention_weights.T.astype(bf16)
    context = diagonal_of(mm(probs, value_cast[...]))
    context_own[...] = context.astype(bf16)
    context_wide = spread_heads(context)
    gather_context.start()
    gather_o1.tail()

    lane_block = lax.rem(
        lax.broadcasted_iota(jnp.int32, (slots, model), 1) // share, HEAD_WIDTH // share
    )

    def pack(parts, turn):
        total = jnp.zeros((slots, model), f32)
        for block, part in enumerate(parts):
            shift = ((block - turn) * share) % model
            moved = part if shift == 0 else pltpu.roll(part, shift, 1)
            total = jnp.where(lane_block == block, moved, total)
        return total

    def by_head(wide):
        return [jnp.where(upper8, wide, 0.0), jnp.where(upper8, 0.0, wide)]

    turns = HEAD_WIDTH // share
    pulled = mm(probs, normed[...])
    pulled_parts = [pulled[group * slots : (group + 1) * slots] for group in range(groups)]
    last_parts = by_head(normed_last.astype(f32))
    for turn in range(turns):
        both = jnp.concatenate([pack(pulled_parts, turn), pack(last_parts, turn)], axis=0)
        both = both.astype(bf16)
        for index in range(model // HEAD_WIDTH):
            early_src[index * turns + turn] = tile(both, index)

    early = Exchange(at, early_src, early_dst, early_sems.at[0], early_sems.at[1])
    early.start()

    gather_o0.finish()
    gather_o1.finish()
    attended = mm(context_wide, full_o[...], 1, 1)
    attended = attended + pltpu.roll(attended, pairs, 0)
    residual = x_last + attended
    out_scale = lax.rsqrt(lane_mean(residual * residual) + EPSILON)
    out_unit = residual * out_scale
    gain = final_gain[...] * score_vector[...]
    score8 = jnp.sum(out_unit * gain, axis=-1, keepdims=True)

    lane8 = lax.broadcasted_iota(jnp.int32, (slots, HEAD_WIDTH), 1)
    row_lane = lax.broadcasted_iota(jnp.int32, (slots, HEAD_WIDTH), 0)

    def as_row(column):
        return jnp.sum(jnp.where(row_lane == lane8, column, 0.0), axis=0, keepdims=True)

    score_row = as_row(score8)
    lane1 = lax.broadcasted_iota(jnp.int32, (1, HEAD_WIDTH), 1)
    listing = jnp.where(lane1 < pairs, score_row, as_row(teacher8))
    list_src[...] = listing
    me_row = list_dst.at[at.me]
    list_here, list_there, list_sent = list_sems.at[0], list_sems.at[1], list_sems.at[2]
    for place_of, target in enumerate(at.others):
        arrived = list_here if place_of < at.neg_count - 1 else list_there
        remote(list_src, me_row, list_sent, arrived, target).start()
    list_dst[at.me] = listing
    scores_out[...] = score_row[:, :pairs]
    gather_context.middle()

    near_block = list_dst.at[pl.ds(0, at.neg_count - 1)]
    remote(near_block, near_block, list_sent, list_here, at.to_partner()).wait_recv()

    def total(array):
        return jnp.sum(jnp.sum(array, axis=1, keepdims=True), axis=0, keepdims=True)

    def query_terms(first):
        block = list_dst[pl.ds(first, at.neg_count)].reshape(at.neg_count, HEAD_WIDTH)
        real = lax.broadcasted_iota(jnp.int32, block.shape, 1) < pairs
        score = jnp.where(real, block, 0.0)
        scaled = pltpu.roll(block, HEAD_WIDTH - pairs, 1)
        scaled = jnp.where(real, scaled, 0.0) / TEACHER_TEMP
        expo_t = jnp.where(real, jnp.exp(scaled), 0.0)
        total_s = total(jnp.where(real, jnp.exp(score), 0.0))
        return score, scaled, expo_t, total_s, total(expo_t)

    _, _, _, total_s, total_t = query_terms(pl.multiple_of(at.pb * at.neg_count, at.neg_count))
    grad_score = GRAD_SCALE * (
        jnp.exp(score8) / total_s - jnp.exp(teacher8 / TEACHER_TEMP) / total_t
    )
    grad_unit = grad_score * gain
    grad_resid = out_scale * (grad_unit - out_unit * lane_mean(grad_unit * out_unit))
    resid_grad[...] = grad_resid
    resid_cast = grad_resid.astype(bf16)
    grad_context = stack_heads(mm(resid_cast, full_o[...])).astype(bf16)
    context_blocks[...] = blocks_of(grad_context.astype(f32))
    late_own[0:stacked, :] = grad_context

    grad_probs = mm(context_blocks[...], value_cast[...], 1, 1)
    spread = jnp.sum(attention_weights * grad_probs, axis=-1, keepdims=True)
    logit_gradient = (attention_weights * (grad_probs - spread)).astype(bf16)
    logit_grad[...] = (attention_weights * (grad_probs - spread)).T.astype(bf16)

    turned_q = diagonal_of(mm(logit_gradient, key_rot[...])) * HEAD_WIDTH ** (-0.5)
    back_q = turned_q * cos_rows - pltpu.roll(turned_q, HEAD_WIDTH // 2, 1) * sin_rows
    back_q = query_scale * (back_q - query_unit * lane_mean(back_q * query_unit))
    grad_q_cast = back_q.astype(bf16)
    late_own[stacked : 2 * stacked, :] = grad_q_cast
    gather_late.start()
    gather_context.relay()

    cuts = 1
    cut_width = kv_width // cuts
    block_rows = model // at.pb_count

    def key_back(cut):
        columns = slice(cut * cut_width, (cut + 1) * cut_width)

        def one(pair, carry):
            rows = pl.ds(pl.multiple_of(pair * seq, seq), seq)
            turned = mm(logit_grad[rows, :], query_blocks[:, columns]) * HEAD_WIDTH ** (-0.5)
            for group in range(groups // cuts):
                start = cut * cut_width + group * HEAD_WIDTH
                lanes = slice(start, start + HEAD_WIDTH)
                part = tile(turned, group)
                unit = key_unit[rows, lanes]
                back = part * cos_table[...] - pltpu.roll(part, HEAD_WIDTH // 2, 1) * sin_table[...]
                back = key_scale[rows, lanes] * (back - unit * lane_mean(back * unit))
                grad_k[rows, lanes] = back.astype(bf16)
            return carry

        lax.fori_loop(0, pairs, one, 0)

    def send(src, dst, send_sem, recv_sem, target):
        remote(src, dst, send_sem, recv_sem, target).start()

    def arrive(block, recv_sem):
        remote(block, block, any_sem, recv_sem, at.to_partner()).wait_recv()

    def key_products(cut):
        columns = slice(cut * cut_width, (cut + 1) * cut_width)
        for k in range(1, at.pb_count + 1):
            pb = at.pb_peer(k % at.pb_count)
            chosen = pl.ds(pl.multiple_of(pb * block_rows, block_rows), block_rows)
            product = mm(normed_t[chosen, :], grad_k[:, columns])
            partial[cut, pb] = product.astype(bf16).reshape(at.line_count, 2, share, cut_width)
            send(
                partial.at[cut, pb, :, at.partner],
                from_core.at[cut, pb],
                core_send,
                core_recv.at[cut, pb],
                at.to_partner(),
            )

    def key_pairs(cut):
        def add_pair(pb):
            arrive(from_core.at[cut, pb], core_recv.at[cut, pb])
            both = partial[cut, pb, :, at.core].astype(f32) + from_core[cut, pb].astype(f32)
            paired[pb, :, cut] = both.astype(bf16)

        for k in range(1, at.pb_count):
            add_pair(at.pb_peer(k))
        for step in range(1, at.line_count + 1):
            line = at.line_peer(step % at.line_count)
            for k in range(1, at.pb_count):
                pb = at.pb_peer(k)
                send(
                    paired.at[pb, line, cut],
                    from_pb.at[at.pb, line, cut],
                    pb_send,
                    pb_recv.at[line],
                    at.to_pb(pb),
                )
        add_pair(at.pb)

    key_back(0)
    key_products(0)
    gather_late.middle()
    key_pairs(0)

    resid_parts = by_head(resid_cast.astype(f32))
    for turn in range(turns):
        packed = pack(resid_parts, turn).astype(bf16)
        for index in range(model // HEAD_WIDTH):
            resid_src[index * turns + turn] = tile(packed, index)
    resid = Exchange(at, resid_src, resid_dst, resid_sems.at[0], resid_sems.at[1])
    resid.start()

    back_last = mm(spread_heads(grad_q_cast.astype(f32)), full_q[...], 1, 1)
    last_grad[...] = back_last + pltpu.roll(back_last, pairs, 0)

    def value_back(pair, carry):
        start = pl.multiple_of(pair * seq, seq)
        rows = pl.ds(start, seq)
        grad_v[rows, :] = mm(probs_ref[rows, :], context_blocks[...]).astype(bf16)
        return carry

    lax.fori_loop(0, pairs, value_back, 0)

    seq_row = lax.broadcasted_iota(jnp.int32, (seq, 1), 0)

    def hidden_back(pair, carry):
        rows = pl.ds(pl.multiple_of(pair * seq, seq), seq)
        total = mm(grad_k[rows, :], full_k[...], 1, 1) + mm(grad_v[rows, :], full_v[...], 1, 1)
        hit = seq_row == lengths[0, pair] - 1
        total = total + jnp.where(hit, last_grad[pl.ds(pair, 1), :], 0.0)
        scaled = total * norm_gain[...]
        wide = x[rows, :].astype(f32)
        inv = inv_wide[rows, 0:1]
        mean = lane_mean(scaled * wide)
        result = inv * scaled - wide * (inv * inv * inv * mean)
        result = result + jnp.where(hit, resid_grad[pl.ds(pair, 1), :], 0.0)
        grad_hidden[rows, :] = result.astype(bf16)
        return carry

    def add_line(step):
        line = at.line_peer(step % at.line_count)
        total = paired[at.pb, line].astype(f32)
        arrive(from_pb.at[pl.ds(0, at.pb_count - 1), line], pb_recv.at[line])
        for k in range(1, at.pb_count):
            pb = at.pb_peer(k)
            total = total + from_pb[pb, line].astype(f32)
        if step < at.line_count:
            summed[line] = total.astype(bf16)
            send(
                summed.at[line],
                from_line.at[at.line],
                line_send,
                line_recv,
                at.to_line(line),
            )
        return total

    hidden_back(0, 0)
    hidden_back(1, 0)
    add_line(1)
    gather_late.relay()

    far_block = list_dst.at[pl.ds(0, at.count - at.neg_count)]
    remote(far_block, far_block, list_sent, list_there, at.to_partner()).wait_recv()
    loss = jnp.zeros((1, 1), f32)
    for pb in range(at.pb_count):
        score, scaled, expo_t, sum_s, sum_t = query_terms(pb * at.neg_count)
        loss = loss + total(expo_t / sum_t * (scaled - jnp.log(sum_t) - (score - jnp.log(sum_s))))
    loss_out[...] = loss

    add_line(2)
    gather_context.tail()
    hidden_back(2, 0)
    for step in range(3, at.line_count + 1):
        own_sum = add_line(step)
    gather_late.tail()
    for pair in range(3, pairs):
        hidden_back(pair, 0)

    gather_context.finish()
    gather_late.finish()
    early.wait("wait_recv")
    resid.wait("wait_recv")

    def rows_of(full, start, group):
        wide = full[...].astype(f32).reshape(at.count, -1, slots, HEAD_WIDTH)
        return wide[:, start + group].reshape(at.count * slots, HEAD_WIDTH).astype(bf16)

    pulled_rows = rows_of(early_dst, 0, 0)
    last_rows = rows_of(early_dst, 1, 0)
    resid_rows = rows_of(resid_dst, 0, 0)
    for group in range(groups):
        found = mm(pulled_rows, rows_of(late_full, 0, group), 0, 0)
        lanes = slice(group * HEAD_WIDTH, (group + 1) * HEAD_WIDTH)
        grad_value[:, lanes] = found[group * share : (group + 1) * share]
        found = mm(last_rows, rows_of(late_full, groups, group), 0, 0)
        for part in range(per_group):
            head = per_group * group + part
            grad_query[:, head * HEAD_WIDTH : (head + 1) * HEAD_WIDTH] = found[
                part * share : (part + 1) * share
            ]
        found = mm(resid_rows, rows_of(context_full, 0, group), 0, 0)
        for part in range(per_group):
            head = per_group * group + part
            grad_out[:, head * HEAD_WIDTH : (head + 1) * HEAD_WIDTH] = found[
                part * share : (part + 1) * share
            ]

    final = own_sum
    arrive(from_line.at[pl.ds(0, at.line_count - 1)], line_recv)
    for step in range(1, at.line_count):
        line = at.line_peer(step)
        final = final + from_line[line].astype(f32)
    for cut in range(cuts):
        grad_key[:, cut * cut_width : (cut + 1) * cut_width] = final[cut]

    for gather in gathers:
        gather.drain()
    pieces = from_line.at[pl.ds(0, at.line_count - 1)]
    for block, sem in (
        (from_core, core_send),
        (from_pb.at[pl.ds(0, at.pb_count - 1)], pb_send),
        (pieces, line_send),
    ):
        remote(block, block, sem, any_sem, at.to_partner()).wait_send()
    early.wait("wait_send")
    resid.wait("wait_send")
    sent_block = list_dst.at[pl.ds(0, at.count - 1)]
    remote(sent_block, sent_block, list_sent, list_here, at.to_partner()).wait_send()


def write_kernel(count, *refs):
    sources, targets, sems = refs[:count], refs[count : 2 * count], refs[2 * count]
    copies = [
        pltpu.make_async_copy(sources[i], targets[i], sems.at[i]) for i in range(2, count)
    ]
    for copy in copies:
        copy.start()
    for i in range(2):
        targets[i][...] = sources[i][...]
    for copy in copies:
        copy.wait()


def write_outputs(arrays):
    count = len(arrays)
    return pl.pallas_call(
        functools.partial(write_kernel, count),
        out_shape=tuple(jax.ShapeDtypeStruct(a.shape, a.dtype) for a in arrays),
        in_specs=[VMEM_SPEC] * count,
        out_specs=(VMEM_SPEC,) * 2 + (pl.BlockSpec(memory_space=pl.ANY),) * (count - 2),
        scratch_shapes=[pltpu.SemaphoreType.DMA((count,))],
        compiler_params=pltpu.CompilerParams(vmem_limit_bytes=4 * 2**20),
    )(*arrays)


def run_step(operands, sizes, pb_count, neg_count):
    pairs, seq, groups, share = sizes
    x, own_q, own_k = operands[0], operands[8], operands[9]
    model, width, kv_width = x.shape[1], own_q.shape[1], own_k.shape[1]
    rows = pairs * seq
    count = pb_count * neg_count
    line_count = neg_count // 2
    slots = width // kv_width * pairs
    stacked = groups * slots
    bf16, f32 = jnp.bfloat16, jnp.float32
    block = (pb_count, line_count, 1, share, kv_width)
    dma = pltpu.SemaphoreType.DMA
    vmem = pltpu.VMEM
    smem_spec = pl.BlockSpec(memory_space=pltpu.SMEM)
    hbm_spec = pl.BlockSpec(memory_space=pltpu.HBM)
    return pl.pallas_call(
        functools.partial(step_kernel, sizes),
        out_shape=(
            vmem((1, pairs), f32),
            vmem((1, 1), f32),
            vmem((rows, model), bf16),
            vmem((share, width), f32),
            vmem((share, kv_width), f32),
            vmem((share, kv_width), f32),
            vmem((share, width), f32),
        ),
        in_specs=[hbm_spec, smem_spec, smem_spec] + [hbm_spec] * 9,
        out_specs=(VMEM_SPEC,) * 7,
        scratch_shapes=[
            vmem((rows, model), bf16),
        ]
        + [vmem(a.shape, a.dtype) for a in operands[3:]]
        + [
            vmem((model, width), bf16),
            vmem((model, kv_width), bf16),
            vmem((model, kv_width), bf16),
            vmem((model, width), bf16),
            vmem((rows, model), bf16),
            vmem((model, rows), bf16),
            vmem((rows, HEAD_WIDTH), f32),
            vmem((rows, kv_width), f32),
            vmem((rows, kv_width), f32),
            vmem((rows, kv_width), bf16),
            vmem((rows, kv_width), bf16),
            vmem((rows, kv_width), bf16),
            vmem((rows, kv_width), bf16),
            vmem((rows, stacked), bf16),
            vmem((rows, stacked), bf16),
            vmem((stacked, kv_width), bf16),
            vmem((stacked, kv_width), bf16),
            vmem((slots, model), f32),
            vmem((slots, model), f32),
            vmem((stacked, HEAD_WIDTH), bf16),
            vmem((stacked * count, HEAD_WIDTH), bf16),
            vmem((2 * stacked, HEAD_WIDTH), bf16),
            vmem((2 * stacked * count, HEAD_WIDTH), bf16),
            vmem((count, 2 * slots, HEAD_WIDTH), bf16),
            vmem((count, 2 * slots, HEAD_WIDTH), bf16),
            vmem((count, slots, HEAD_WIDTH), bf16),
            vmem((count, slots, HEAD_WIDTH), bf16),
            vmem((1, HEAD_WIDTH), f32),
            vmem((count, 1, HEAD_WIDTH), f32),
            vmem((1, pb_count, line_count, 2, share, kv_width), bf16),
            vmem((1, pb_count, line_count, share, kv_width), bf16),
            vmem(block, bf16),
            vmem(block, bf16),
            vmem(block[1:], bf16),
            vmem(block[1:], bf16),
            dma((2,)),
            dma((2,)),
            dma((3,)),
            dma,
            dma((1, pb_count)),
            dma,
            dma((line_count,)),
            dma,
            dma,
            dma,
            dma((pairs + 9,)),
        ]
        + gather_sems(neg_count, True) * 6
        + gather_sems(neg_count, False) * 2,
        compiler_params=pltpu.CompilerParams(
            collective_id=0, has_side_effects=True, vmem_limit_bytes=62 * 2**20
        ),
    )(*operands)


def shards(
    hidden,
    lengths,
    teacher,
    norm_gain,
    final_gain,
    score_vector,
    query_weight,
    key_matrix,
    value_matrix,
    out_weight,
):
    both = ("pb", "neg")
    width = query_weight.shape[1]
    kv_width = key_matrix.shape[1]
    share, out_share = query_weight.shape[0], out_weight.shape[1]
    pb_count, neg_count = lax.axis_size("pb"), lax.axis_size("neg")
    pair_count, seq_len, model_width = hidden.shape[1:]
    group_count = kv_width // HEAD_WIDTH
    own_kernels = (
        pb_count == 4
        and neg_count == 8
        and share == out_share
        and share % 32 == 0
        and model_width == share * pb_count * neg_count
        and width == 2 * kv_width
        and pair_count * 2 == 8
        and seq_len == HEAD_WIDTH
        and share * group_count == HEAD_WIDTH
    )
    if own_kernels:
        cos_table, sin_table = signed_tables(seq_len, HEAD_WIDTH)
        results = run_step(
            (
                hidden.reshape(pair_count * seq_len, model_width),
                lengths,
                teacher,
                norm_gain[None],
                final_gain[None],
                score_vector[None],
                cos_table,
                sin_table,
                query_weight,
                key_matrix,
                value_matrix,
                out_weight.T,
            ),
            (pair_count, seq_len, group_count, share),
            pb_count,
            neg_count,
        )
        scores, loss, grad_rows, grad_query, grad_key, grad_value, grad_out = write_outputs(results)
        return (
            scores,
            loss.reshape(()),
            grad_rows.reshape(hidden.shape),
            grad_query,
            grad_key,
            grad_value,
            grad_out.T,
        )
    packed = jnp.concatenate([query_weight, key_matrix, value_matrix, out_weight.T], axis=1)
    everything = lax.all_gather(packed, both, axis=0, tiled=True)
    full_query = everything[:, :width]
    full_key = everything[:, width : width + kv_width]
    full_value = everything[:, width + kv_width : width + 2 * kv_width]
    full_out_t = everything[:, width + 2 * kv_width :]
    weights = (full_query, full_key, full_value, full_out_t.T)
    scores_here, stored = forward_pairs(
        hidden[0], lengths[0], norm_gain, final_gain, score_vector, *weights
    )
    listing = jnp.concatenate([scores_here, teacher[0]])[None]
    listed = lax.all_gather(listing, "neg", axis=0, tiled=True)
    all_scores = listed[:, :pair_count]
    all_scaled = listed[:, pair_count:] / TEACHER_TEMP
    my_total_s = jnp.sum(jnp.exp(all_scores))
    expo_t = jnp.exp(all_scaled)
    my_total_t = jnp.sum(expo_t)
    loss_here = jnp.sum(
        expo_t
        / my_total_t
        * (all_scaled - jnp.log(my_total_t) - (all_scores - jnp.log(my_total_s)))
    )
    prob_s = jnp.exp(scores_here) / my_total_s
    prob_t = jnp.exp(teacher[0] / TEACHER_TEMP) / my_total_t
    grad_score = GRAD_SCALE * (prob_s - prob_t)
    grad_input, last_rows, grad_kv = backward_pairs(
        stored, grad_score, norm_gain, final_gain, score_vector, *weights
    )
    grad_kv = grad_kv.astype(jnp.bfloat16)
    reduced = lax.psum_scatter(grad_kv, both, scatter_dimension=0, tiled=True)
    reduced = reduced.astype(jnp.float32)
    rows = lax.all_gather(last_rows, both, axis=0, tiled=True)
    loss_value = lax.psum(loss_here, "pb")
    index = lax.axis_index("pb") * neg_count + lax.axis_index("neg")
    normed_cols = lax.dynamic_slice_in_dim(rows, index * share, share, axis=1)
    resid_cols = lax.dynamic_slice_in_dim(rows, model_width + index * out_share, out_share, axis=1)
    rest = 2 * model_width
    all_q = rows[:, rest : rest + width]
    all_context = rows[:, rest + width :]
    grad_query = jnp.dot(normed_cols.T, all_q, preferred_element_type=jnp.float32)
    grad_out = jnp.dot(all_context.T, resid_cols, preferred_element_type=jnp.float32)
    return (
        scores_here[None],
        loss_value,
        grad_input[None],
        grad_query,
        reduced[:, :kv_width],
        reduced[:, kv_width:],
        grad_out,
    )


def solution(mesh):
    placed = (
        P("pb", "neg", None, None),
        P("pb", "neg"),
        P("pb", "neg"),
        P(),
        P(),
        P(),
        P(("pb", "neg"), None),
        P(("pb", "neg"), None),
        P(("pb", "neg"), None),
        P(None, ("pb", "neg")),
    )
    return jax.shard_map(
        shards,
        mesh=mesh,
        in_specs=placed,
        out_specs=(
            P("pb", "neg"),
            P(),
            P("pb", "neg", None, None),
            P(("pb", "neg"), None),
            P(("pb", "neg"), None),
            P(("pb", "neg"), None),
            P(None, ("pb", "neg")),
        ),
        check_vma=False,
    )
```

```python
import functools

import jax
import jax.numpy as jnp
import numpy as np
from jax import lax
from jax.experimental import pallas as pl
from jax.experimental.pallas import tpu as pltpu
from jax.sharding import PartitionSpec as P

HEAD_WIDTH = 128
MESH_ID = pl.DeviceIdType.MESH

EPSILON = 1e-06
ROPE_BASE = 1000000.0
TEACHER_TEMP = 2.0
GRAD_SCALE = 512.0


def rope_tables(seq_len, head_size):
    half = head_size // 2
    freqs = ROPE_BASE ** (-(jnp.arange(half, dtype=jnp.float32) * 2.0) / head_size)
    angles = jnp.arange(seq_len, dtype=jnp.float32)[:, None] * freqs[None, :]
    angles = jnp.concatenate([angles, angles], axis=1)
    return (jnp.cos(angles), jnp.sin(angles))


def signed_tables(seq_len, head_size):
    half = head_size // 2
    freqs = ROPE_BASE ** (-(np.arange(half) * 2.0) / head_size)
    angles = np.arange(seq_len)[:, None] * freqs[None, :]
    cos = np.concatenate([np.cos(angles)] * 2, axis=1)
    sin = np.concatenate([-np.sin(angles), np.sin(angles)], axis=1)
    return (jnp.asarray(cos, jnp.float32), jnp.asarray(sin, jnp.float32))


def rotate_half(vector):
    half = vector.shape[-1] // 2
    return jnp.concatenate([-vector[..., half:], vector[..., :half]], axis=-1)


def unrotate_half(vector):
    half = vector.shape[-1] // 2
    return jnp.concatenate([vector[..., half:], -vector[..., :half]], axis=-1)


def forward_pairs(
    tokens_in,
    lengths_here,
    norm_gain,
    final_gain,
    score_vector,
    query_weight,
    key_matrix,
    value_matrix,
    out_weight,
):
    pair_count, seq_len, model_width = tokens_in.shape
    head_count = query_weight.shape[1] // HEAD_WIDTH
    group_count = key_matrix.shape[1] // HEAD_WIDTH
    group_size = head_count // group_count
    inputs_wide = tokens_in.astype(jnp.float32)
    inv_rms = lax.rsqrt(jnp.mean(inputs_wide * inputs_wide, axis=-1, keepdims=True) + EPSILON)
    normed = (inputs_wide * inv_rms * norm_gain).astype(jnp.bfloat16)
    flat_rows = normed.reshape(pair_count * seq_len, model_width)
    key_proj = jnp.dot(flat_rows, key_matrix, preferred_element_type=jnp.float32).reshape(
        pair_count, seq_len, group_count, HEAD_WIDTH
    )
    value_proj = jnp.dot(flat_rows, value_matrix, preferred_element_type=jnp.float32).reshape(
        pair_count, seq_len, group_count, HEAD_WIDTH
    )
    positions = jnp.arange(seq_len, dtype=jnp.int32)
    last_index = lengths_here - 1
    onehot = (positions[None, :] == last_index[:, None]).astype(jnp.float32)
    normed_last = jnp.take_along_axis(normed, last_index[:, None, None], axis=1)[:, 0]
    query_proj = jnp.dot(normed_last, query_weight, preferred_element_type=jnp.float32).reshape(
        pair_count, head_count, HEAD_WIDTH
    )
    query_scale = lax.rsqrt(jnp.mean(query_proj * query_proj, axis=-1, keepdims=True) + EPSILON)
    query_unit = query_proj * query_scale
    key_scale = lax.rsqrt(jnp.mean(key_proj * key_proj, axis=-1, keepdims=True) + EPSILON)
    key_unit = key_proj * key_scale
    cos_table, sin_table = rope_tables(seq_len, HEAD_WIDTH)
    cos_query = jnp.dot(onehot, cos_table, precision=lax.Precision.HIGHEST)
    sin_query = jnp.dot(onehot, sin_table, precision=lax.Precision.HIGHEST)
    query_rot = (
        query_unit * cos_query[:, None, :] + rotate_half(query_unit) * sin_query[:, None, :]
    ).astype(jnp.bfloat16)
    key_rot = (
        key_unit * cos_table[None, :, None, :] + rotate_half(key_unit) * sin_table[None, :, None, :]
    ).astype(jnp.bfloat16)
    value_cast = value_proj.astype(jnp.bfloat16)
    grouped = query_rot.reshape(pair_count, group_count, group_size, HEAD_WIDTH)
    logits = jnp.einsum(
        "pkgd,pskd->pkgs", grouped, key_rot, preferred_element_type=jnp.float32
    ) * HEAD_WIDTH ** (-0.5)
    visible = (positions[None, :] <= last_index[:, None])[:, None, None, :]
    expos = jnp.where(visible, jnp.exp(logits), 0.0)
    attention_weights = expos / jnp.sum(expos, axis=-1, keepdims=True)
    probs_cast = attention_weights.astype(jnp.bfloat16)
    context = jnp.einsum(
        "pkgs,pskd->pkgd", probs_cast, value_cast, preferred_element_type=jnp.float32
    )
    context = context.astype(jnp.bfloat16).reshape(pair_count, head_count * HEAD_WIDTH)
    attended = jnp.dot(context, out_weight, preferred_element_type=jnp.float32)
    residual = jnp.take_along_axis(inputs_wide, last_index[:, None, None], axis=1)[:, 0] + attended
    out_scale = lax.rsqrt(jnp.mean(residual * residual, axis=-1, keepdims=True) + EPSILON)
    out_unit = residual * out_scale
    scores_here = jnp.sum(out_unit * final_gain * score_vector, axis=-1)
    stored = (
        tokens_in,
        onehot,
        inv_rms,
        normed,
        normed_last,
        query_unit,
        query_scale,
        key_unit,
        key_scale,
        cos_query,
        sin_query,
        cos_table,
        sin_table,
        query_rot,
        key_rot,
        value_cast,
        attention_weights,
        probs_cast,
        context,
        out_unit,
        out_scale,
    )
    return (scores_here, stored)


def backward_pairs(
    stored,
    grad_score,
    norm_gain,
    final_gain,
    score_vector,
    query_weight,
    key_matrix,
    value_matrix,
    out_weight,
):
    (
        tokens_in,
        onehot,
        inv_rms,
        normed,
        normed_last,
        query_unit,
        query_scale,
        key_unit,
        key_scale,
        cos_query,
        sin_query,
        cos_table,
        sin_table,
        query_rot,
        key_rot,
        value_cast,
        attention_weights,
        probs_cast,
        context,
        out_unit,
        out_scale,
    ) = stored
    pair_count, seq_len, model_width = tokens_in.shape
    head_count = query_weight.shape[1] // HEAD_WIDTH
    group_count = key_matrix.shape[1] // HEAD_WIDTH
    group_size = head_count // group_count
    grad_unit = grad_score[:, None] * score_vector * final_gain
    grad_resid = out_scale * (
        grad_unit - out_unit * jnp.mean(grad_unit * out_unit, axis=-1, keepdims=True)
    )
    grad_resid_cast = grad_resid.astype(jnp.bfloat16)
    grad_context = jnp.dot(
        grad_resid_cast, out_weight.T, preferred_element_type=jnp.float32
    ).astype(jnp.bfloat16)
    grad_context = grad_context.reshape(pair_count, group_count, group_size, HEAD_WIDTH)
    grad_probs = jnp.einsum(
        "pkgd,pskd->pkgs", grad_context, value_cast, preferred_element_type=jnp.float32
    )
    grad_vals = jnp.einsum(
        "pkgs,pkgd->pskd", probs_cast, grad_context, preferred_element_type=jnp.float32
    )
    spread = jnp.sum(attention_weights * grad_probs, axis=-1, keepdims=True)
    logit_gradient = (attention_weights * (grad_probs - spread)).astype(jnp.bfloat16)
    grouped = query_rot.reshape(pair_count, group_count, group_size, HEAD_WIDTH)
    rotated_query_gradient = jnp.einsum(
        "pkgs,pskd->pkgd", logit_gradient, key_rot, preferred_element_type=jnp.float32
    ) * HEAD_WIDTH ** (-0.5)
    rotated_query_gradient = rotated_query_gradient.reshape(pair_count, head_count, HEAD_WIDTH)
    grad_krot = jnp.einsum(
        "pkgs,pkgd->pskd", logit_gradient, grouped, preferred_element_type=jnp.float32
    ) * HEAD_WIDTH ** (-0.5)
    grad_qunit = rotated_query_gradient * cos_query[:, None, :] + unrotate_half(
        rotated_query_gradient * sin_query[:, None, :]
    )
    grad_kunit = grad_krot * cos_table[None, :, None, :] + unrotate_half(
        grad_krot * sin_table[None, :, None, :]
    )
    grad_qproj = query_scale * (
        grad_qunit - query_unit * jnp.mean(grad_qunit * query_unit, axis=-1, keepdims=True)
    )
    grad_kproj = key_scale * (
        grad_kunit - key_unit * jnp.mean(grad_kunit * key_unit, axis=-1, keepdims=True)
    )
    grad_q_cast = grad_qproj.reshape(pair_count, head_count * HEAD_WIDTH).astype(jnp.bfloat16)
    grad_k_cast = grad_kproj.reshape(pair_count * seq_len, group_count * HEAD_WIDTH).astype(
        jnp.bfloat16
    )
    grad_v_cast = grad_vals.reshape(pair_count * seq_len, group_count * HEAD_WIDTH).astype(
        jnp.bfloat16
    )
    flat_rows = normed.reshape(pair_count * seq_len, model_width)
    last_rows = jnp.concatenate([normed_last, grad_resid_cast, grad_q_cast, context], axis=1)
    grad_kv = jnp.dot(
        flat_rows.T,
        jnp.concatenate([grad_k_cast, grad_v_cast], axis=1),
        preferred_element_type=jnp.float32,
    )
    grad_normed = jnp.dot(grad_k_cast, key_matrix.T, preferred_element_type=jnp.float32)
    grad_normed = grad_normed + jnp.dot(
        grad_v_cast, value_matrix.T, preferred_element_type=jnp.float32
    )
    grad_normed = grad_normed.reshape(pair_count, seq_len, model_width)
    grad_last = jnp.dot(grad_q_cast, query_weight.T, preferred_element_type=jnp.float32)
    grad_normed = grad_normed + onehot[:, :, None] * grad_last[:, None, :]
    inputs_wide = tokens_in.astype(jnp.float32)
    grad_scaled = grad_normed * norm_gain
    grad_input = inv_rms * grad_scaled - inputs_wide * inv_rms * inv_rms * inv_rms * jnp.mean(
        grad_scaled * inputs_wide, axis=-1, keepdims=True
    )
    grad_input = grad_input + onehot[:, :, None] * grad_resid[:, None, :]
    return (grad_input.astype(jnp.bfloat16), last_rows, grad_kv)


class Place:
    def __init__(self):
        self.pb_count = lax.axis_size("pb")
        self.neg_count = lax.axis_size("neg")
        self.line_count = self.neg_count // 2
        self.pb = lax.axis_index("pb")
        neg = lax.axis_index("neg")
        self.line = neg // 2
        self.core = neg % 2
        self.partner = 1 - self.core

    def slot(self, pb, line, core):
        return pb * self.neg_count + line * 2 + core

    def line_peer(self, step):
        return lax.rem(self.line + step, self.line_count)

    def pb_peer(self, step):
        return lax.rem(self.pb + step, self.pb_count)

    def to_line(self, line):
        return (self.pb, line * 2 + self.core)

    def to_pb(self, pb):
        return (pb, self.line * 2 + self.core)

    def to_partner(self):
        return (self.pb, self.line * 2 + self.partner)

    def greet(self):
        barrier = pltpu.get_barrier_semaphore()
        targets = [self.to_line(self.line_peer(k)) for k in range(1, self.line_count)]
        targets += [self.to_pb(self.pb_peer(k)) for k in range(1, self.pb_count)]
        targets += [self.to_partner()]
        for target in targets:
            pl.semaphore_signal(barrier, inc=1, device_id=target, device_id_type=MESH_ID)
        pl.semaphore_wait(barrier, len(targets))


def remote(src, dst, send_sem, recv_sem, target):
    return pltpu.make_async_remote_copy(
        src_ref=src,
        dst_ref=dst,
        send_sem=send_sem,
        recv_sem=recv_sem,
        device_id=target,
        device_id_type=MESH_ID,
    )


def gather_sems(neg_count, large):
    line_count = neg_count // 2
    dma = pltpu.SemaphoreType.DMA
    if large:
        return [dma((line_count,)), dma((line_count,)), dma((line_count,)), dma((2,))]
    return [dma((1,)), dma((1,)), dma((1,)), dma((2,))]


class Gather:
    def __init__(self, place, own, full, sems, halve_corner, direct):
        self.place, self.own, self.full = place, own, full
        self.line_recv, self.pb_recv, self.corner_recv, ends = sems
        self.send_sem, self.core_recv = ends.at[0], ends.at[1]
        self.halve_corner, self.direct = halve_corner, direct
        across = place.pb + 1 - 2 * (place.pb % 2)
        along = place.pb + 2 - 4 * (place.pb // 2)
        self.near = (across, along)
        self.corner = 3 - place.pb
        half = place.line // 2
        self.is_inner = (place.line == 1) | (place.line == 2)
        self.mate = place.line + 1 - 2 * (place.line % 2)
        self.far_inner = 2 - half
        self.far_outer = 3 - 3 * half
        self.size = own.shape[0]
        if halve_corner:
            self.own_lines = (place.line, lax.rem(place.line + 2, 4))
            self.mate_lines = (self.mate, lax.rem(self.mate + 2, 4))
        else:
            self.own_lines = (place.line, self.mate, self.far_inner, self.far_outer)
            self.mate_lines = ()

    def rows(self, pb, line, core):
        start = self.place.slot(pb, line, core) * self.size
        return self.full.at[pl.ds(pl.multiple_of(start, self.size), self.size)]

    def blocks(self, count):
        return self.full.at[pl.ds(0, count * self.size)]

    def send(self, src, dst, recv_sem, target):
        remote(src, dst, self.send_sem, recv_sem, target).start()

    def of(self, sems, line):
        return sems.at[0] if self.direct else sems.at[line]

    def spread(self, src, line):
        at = self.place
        dst = self.rows(at.pb, line, at.core)
        for side in range(2):
            self.send(src, dst, self.of(self.pb_recv, line), at.to_pb(self.near[side]))
        self.pass_on(src, at.pb, line)

    def pass_on(self, src, pb, line):
        at = self.place
        self.send(src, self.rows(pb, line, at.core), self.core_recv, at.to_partner())

    def arrive(self, block, recv_sem):
        remote(block, block, self.send_sem, recv_sem, self.place.to_partner()).wait_recv()

    def start(self):
        at = self.place
        mine = self.rows(at.pb, at.line, at.core)
        peers = (self.mate, self.far_inner) + ((self.far_outer,) if self.direct else ())
        for line in peers:
            self.send(self.own, mine, self.of(self.line_recv, at.line), at.to_line(line))
        self.spread(self.own, at.line)
        mine[...] = self.own[...]

    def middle(self):
        at = self.place
        if self.direct:
            self.arrive(self.blocks(at.line_count - 1), self.line_recv.at[0])
        for line in (self.mate, self.far_inner, self.far_outer):
            block = self.rows(at.pb, line, at.core)
            if not self.direct:
                self.arrive(block, self.line_recv.at[line])
                if line is not self.mate:

                    @pl.when(self.is_inner)
                    def _():
                        self.send(block, block, self.line_recv.at[line], at.to_line(self.mate))

            self.spread(block, line)

    def half(self, block, side):
        size = block.shape[0] // 2
        return block.at[pl.ds(side * size, size)]

    def relay(self):
        at = self.place
        if self.direct:
            self.arrive(self.blocks(2 * at.line_count), self.pb_recv.at[0])
        for line in self.own_lines + self.mate_lines:
            if not self.direct:
                self.arrive(self.blocks(2), self.pb_recv.at[line])
            for side in range(2):
                block = self.rows(self.near[side], line, at.core)
                if not any(line is other for other in self.mate_lines):
                    part = self.half(block, side)
                    target = at.to_pb(self.near[1 - side])
                    self.send(part, part, self.of(self.corner_recv, line), target)
                self.pass_on(block, self.near[side], line)

    def corner_in(self, lines, hand_over):
        at = self.place
        if self.direct:
            self.arrive(self.blocks(at.line_count), self.corner_recv.at[0])
        for line in lines:
            block = self.rows(self.corner, line, at.core)
            if not self.direct:
                self.arrive(block, self.corner_recv.at[line])
            if hand_over:
                self.send(block, block, self.corner_recv.at[line], at.to_line(self.mate))
            self.pass_on(block, self.corner, line)

    def hand(self):
        if self.halve_corner:
            self.corner_in(self.own_lines, True)

    def tail(self):
        self.corner_in(self.mate_lines if self.halve_corner else self.own_lines, False)

    def finish(self):
        self.arrive(self.blocks(self.place.count // 2), self.core_recv)

    def drain(self):
        at = self.place
        block = self.blocks(at.count - (1 if self.direct else 2))
        remote(block, block, self.send_sem, self.core_recv, at.to_partner()).wait_send()
        if not self.direct:

            @pl.when(self.is_inner)
            def _():
                block = self.blocks(2)
                remote(block, block, self.send_sem, self.core_recv, at.to_partner()).wait_send()


VMEM_SPEC = pl.BlockSpec(memory_space=pltpu.VMEM)


def mm(left, right, left_dim=1, right_dim=0, precision=None):
    return lax.dot_general(
        left,
        right,
        (((left_dim,), (right_dim,)), ((), ())),
        preferred_element_type=jnp.float32,
        precision=precision,
    )


def lane_mean(array):
    return jnp.mean(array, axis=-1, keepdims=True)


def tile(array, index):
    return array[:, index * HEAD_WIDTH : (index + 1) * HEAD_WIDTH]


class Exchange:
    def __init__(self, at, src, dst, send_sem, recv_sem):
        self.at, self.src, self.dst = at, src, dst
        self.send_sem, self.recv_sem = send_sem, recv_sem

    def start(self):
        at = self.at
        for pb, neg in at.others:
            peer = pb * at.neg_count + neg
            remote(
                self.src.at[peer], self.dst.at[at.me], self.send_sem, self.recv_sem, (pb, neg)
            ).start()
        self.dst[at.me] = self.src[at.me]

    def wait(self, sem_of):
        block = self.dst.at[pl.ds(0, self.at.count - 1)]
        copy = remote(block, block, self.send_sem, self.recv_sem, self.at.to_partner())
        getattr(copy, sem_of)()


def step_kernel(
    sizes,
    hidden,
    lengths,
    teacher,
    norm_gain_in,
    final_gain_in,
    score_vector_in,
    cos_table_in,
    sin_table_in,
    own_q_in,
    own_k_in,
    own_v_in,
    own_o_in,
    scores_out,
    loss_out,
    grad_hidden,
    grad_query,
    grad_key,
    grad_value,
    grad_out,
    x,
    norm_gain,
    final_gain,
    score_vector,
    cos_table,
    sin_table,
    own_q,
    own_k,
    own_v,
    own_o,
    full_q,
    full_k,
    full_v,
    full_o,
    normed,
    normed_t,
    inv_wide,
    key_unit,
    key_scale,
    key_rot,
    value_cast,
    grad_k,
    grad_v,
    logit_grad,
    probs_ref,
    query_blocks,
    context_blocks,
    last_grad,
    resid_grad,
    context_own,
    context_full,
    late_own,
    late_full,
    early_src,
    early_dst,
    resid_src,
    resid_dst,
    list_src,
    list_dst,
    partial,
    from_core,
    paired,
    from_pb,
    summed,
    from_line,
    early_sems,
    resid_sems,
    list_sems,
    core_send,
    core_recv,
    pb_send,
    pb_recv,
    line_send,
    line_recv,
    any_sem,
    load_sems,
    *gather_sem_refs,
):
    pairs, seq, groups, share = sizes
    bf16, f32 = jnp.bfloat16, jnp.float32
    at = Place()
    at.count = at.pb_count * at.neg_count
    at.me = at.slot(at.pb, at.line, at.core)
    neg = lax.axis_index("neg")
    pb_all = [at.pb] + [at.pb_peer(k) for k in range(1, at.pb_count)]
    neg_all = [neg] + [lax.rem(neg + k, at.neg_count) for k in range(1, at.neg_count)]
    at.others = [
        (pb, peer)
        for i, pb in enumerate(pb_all)
        for j, peer in enumerate(neg_all)
        if i + j > 0
    ]
    model = x.shape[1]
    rows_all = pairs * seq
    per_group = own_q.shape[1] // own_k.shape[1]
    slots = per_group * pairs
    stacked = groups * slots
    kv_width = groups * HEAD_WIDTH

    barrier = pltpu.get_barrier_semaphore()

    for target in at.others:
        pl.semaphore_signal(barrier, inc=1, device_id=target, device_id_type=MESH_ID)
    loads = []
    moves = (
        (own_k_in, own_k),
        (own_v_in, own_v),
        (own_q_in, own_q),
        (own_o_in, own_o),
        (norm_gain_in, norm_gain),
        (final_gain_in, final_gain),
        (score_vector_in, score_vector),
        (cos_table_in, cos_table),
        (sin_table_in, sin_table),
    )
    small_loads = []
    for place_of, (source, target) in enumerate(moves):
        load = pltpu.make_async_copy(source, target, load_sems.at[pairs + place_of])
        load.start()
        small_loads.append(load)
    for pair in range(pairs):
        rows = pl.ds(pair * seq, seq)
        load = pltpu.make_async_copy(hidden.at[rows], x.at[rows], load_sems.at[pair])
        load.start()
        loads.append(load)

    half_width = own_q.shape[1] // 2
    low, high = pl.ds(0, half_width), pl.ds(half_width, half_width)
    parts = (
        (own_k, full_k, True),
        (own_v, full_v, True),
        (own_q.at[:, low], full_q.at[:, low], True),
        (own_q.at[:, high], full_q.at[:, high], True),
        (own_o.at[:, low], full_o.at[:, low], True),
        (own_o.at[:, high], full_o.at[:, high], False),
        (context_own, context_full, False),
        (late_own, late_full, False),
    )
    each = len(gather_sem_refs) // len(parts)
    gathers = [
        Gather(at, own, full, gather_sem_refs[i * each : (i + 1) * each], halve, i >= 6)
        for i, (own, full, halve) in enumerate(parts)
    ]
    gather_k, gather_v, gather_q0, gather_q1, gather_o0, gather_o1 = gathers[:6]
    gather_context, gather_late = gathers[6:]

    for load in small_loads:
        load.wait()
    pl.semaphore_wait(barrier, at.count - 1)
    for gather in gathers[:4]:
        gather.start()

    def norm_pair(pair, carry):
        rows = pl.ds(pl.multiple_of(pair * seq, seq), seq)
        wide = x[rows, :].astype(f32)
        inv = lax.rsqrt(lane_mean(wide * wide) + EPSILON)
        inv_wide[rows, :] = jnp.broadcast_to(inv, (seq, HEAD_WIDTH))
        scaled = wide * inv * norm_gain[...]
        normed[rows, :] = scaled.astype(bf16)
        normed_t[:, rows] = scaled.T.astype(bf16)
        return carry

    for pair in range(pairs):
        loads[pair].wait()
        norm_pair(pair, 0)

    row8 = lax.broadcasted_iota(jnp.int32, (slots, 1), 0)
    pair8 = lax.rem(row8, pairs)
    upper8 = row8 < pairs
    last8 = jnp.zeros((slots, 1), jnp.int32)
    teacher8 = jnp.zeros((slots, 1), f32)
    for pair in range(pairs):
        last8 = jnp.where(pair8 == pair, lengths[0, pair] - 1, last8)
        teacher8 = jnp.where(pair8 == pair, teacher[0, pair], teacher8)
    place8 = pair8 * seq + last8
    column8 = lax.broadcasted_iota(jnp.int32, (slots, rows_all), 1)
    onehot8 = (column8 == place8).astype(f32).astype(bf16)
    visible8 = (column8 >= pair8 * seq) & (column8 <= place8)
    visible = jnp.concatenate([visible8.astype(f32)] * groups, axis=0) > 0.5
    position8 = (lax.broadcasted_iota(jnp.int32, (slots, seq), 1) == last8).astype(f32)

    x_last = mm(onehot8, x[...])
    normed_last = mm(onehot8, normed[...]).astype(bf16)
    cos8 = mm(position8, cos_table[...], precision=lax.Precision.HIGHEST)
    sin8 = mm(position8, sin_table[...], precision=lax.Precision.HIGHEST)
    cos_rows = jnp.concatenate([cos8] * groups, axis=0)
    sin_rows = jnp.concatenate([sin8] * groups, axis=0)

    def key_pair(pair, carry):
        rows = pl.ds(pl.multiple_of(pair * seq, seq), seq)
        proj = mm(normed[rows, :], full_k[...])
        for group in range(groups):
            lanes = slice(group * HEAD_WIDTH, (group + 1) * HEAD_WIDTH)
            part = proj[:, lanes]
            scale = lax.rsqrt(lane_mean(part * part) + EPSILON)
            unit = part * scale
            key_unit[rows, lanes] = unit
            key_scale[rows, lanes] = jnp.broadcast_to(scale, (seq, HEAD_WIDTH))
            turned = unit * cos_table[...] + pltpu.roll(unit, HEAD_WIDTH // 2, 1) * sin_table[...]
            key_rot[rows, lanes] = turned.astype(bf16)
        return carry

    def value_pair(pair, carry):
        rows = pl.ds(pl.multiple_of(pair * seq, seq), seq)
        value_cast[rows, :] = mm(normed[rows, :], full_v[...]).astype(bf16)
        return carry

    gather_k.middle()
    gather_o0.start()
    gather_o1.start()
    gather_v.middle()
    gather_q0.middle()
    gather_k.relay()
    gather_q1.middle()
    gather_v.relay()
    gather_k.hand()
    gather_o0.middle()
    gather_o1.middle()
    gather_q0.relay()
    gather_v.hand()
    gather_q1.relay()
    gather_q0.hand()
    gather_k.tail()
    gather_o0.relay()
    gather_q1.hand()
    gather_v.tail()
    gather_o1.relay()
    gather_o0.hand()
    gather_q0.tail()
    gather_q1.tail()
    gather_k.finish()
    for pair in range(pairs):
        key_pair(pair, 0)
    gather_v.finish()
    for pair in range(pairs):
        value_pair(pair, 0)
    gather_o0.tail()
    gather_q0.finish()
    gather_q1.finish()
    gather_o1.tail()

    def stack_heads(wide):
        return jnp.concatenate(
            [
                jnp.where(upper8, tile(wide, per_group * group), tile(wide, per_group * group + 1))
                for group in range(groups)
            ],
            axis=0,
        )

    def spread_heads(stack):
        parts = []
        for group in range(groups):
            part = stack[group * slots : (group + 1) * slots]
            parts += [jnp.where(upper8, part, 0.0), jnp.where(upper8, 0.0, part)]
        return jnp.concatenate(parts, axis=1).astype(bf16)

    def diagonal_of(wide):
        return jnp.concatenate(
            [
                wide[group * slots : (group + 1) * slots, group * HEAD_WIDTH : (group + 1) * HEAD_WIDTH]
                for group in range(groups)
            ],
            axis=0,
        )

    def blocks_of(stack):
        rows = []
        for group in range(groups):
            part = stack[group * slots : (group + 1) * slots]
            rows.append(
                jnp.concatenate(
                    [part if other == group else jnp.zeros_like(part) for other in range(groups)],
                    axis=1,
                )
            )
        return jnp.concatenate(rows, axis=0).astype(bf16)

    query_proj = stack_heads(mm(normed_last, full_q[...]))
    query_scale = lax.rsqrt(lane_mean(query_proj * query_proj) + EPSILON)
    query_unit = query_proj * query_scale
    query_rot = query_unit * cos_rows + pltpu.roll(query_unit, HEAD_WIDTH // 2, 1) * sin_rows
    query_wide = blocks_of(query_rot)
    query_blocks[...] = query_wide
    logits = mm(query_wide, key_rot[...], 1, 1) * HEAD_WIDTH ** (-0.5)
    expos = jnp.where(visible, jnp.exp(logits), 0.0)
    attention_weights = expos / jnp.sum(expos, axis=-1, keepdims=True)
    probs = attention_weights.astype(bf16)
    probs_ref[...] = attention_weights.T.astype(bf16)
    context = diagonal_of(mm(probs, value_cast[...]))
    context_own[...] = context.astype(bf16)
    context_wide = spread_heads(context)
    gather_context.start()

    lane_block = lax.rem(
        lax.broadcasted_iota(jnp.int32, (slots, model), 1) // share, HEAD_WIDTH // share
    )

    def pack(parts, turn):
        total = jnp.zeros((slots, model), f32)
        for block, part in enumerate(parts):
            shift = ((block - turn) * share) % model
            moved = part if shift == 0 else pltpu.roll(part, shift, 1)
            total = jnp.where(lane_block == block, moved, total)
        return total

    def by_head(wide):
        return [jnp.where(upper8, wide, 0.0), jnp.where(upper8, 0.0, wide)]

    turns = HEAD_WIDTH // share
    gather_o0.finish()
    attended = mm(context_wide[:, :half_width], full_o[:, :half_width], 1, 1)
    gather_o1.finish()
    attended = attended + mm(context_wide[:, half_width:], full_o[:, half_width:], 1, 1)
    attended = attended + pltpu.roll(attended, pairs, 0)
    residual = x_last + attended
    out_scale = lax.rsqrt(lane_mean(residual * residual) + EPSILON)
    out_unit = residual * out_scale
    gain = final_gain[...] * score_vector[...]
    score8 = jnp.sum(out_unit * gain, axis=-1, keepdims=True)

    lane8 = lax.broadcasted_iota(jnp.int32, (slots, HEAD_WIDTH), 1)
    row_lane = lax.broadcasted_iota(jnp.int32, (slots, HEAD_WIDTH), 0)

    def as_row(column):
        return jnp.sum(jnp.where(row_lane == lane8, column, 0.0), axis=0, keepdims=True)

    score_row = as_row(score8)
    lane1 = lax.broadcasted_iota(jnp.int32, (1, HEAD_WIDTH), 1)
    listing = jnp.where(lane1 < pairs, score_row, as_row(teacher8))
    list_src[...] = listing
    me_row = list_dst.at[at.me]
    list_here, list_there, list_sent = list_sems.at[0], list_sems.at[1], list_sems.at[2]
    for place_of, target in enumerate(at.others):
        arrived = list_here if place_of < at.neg_count - 1 else list_there
        remote(list_src, me_row, list_sent, arrived, target).start()
    list_dst[at.me] = listing
    scores_out[...] = score_row[:, :pairs]

    pulled = mm(probs, normed[...])
    pulled_parts = [pulled[group * slots : (group + 1) * slots] for group in range(groups)]
    last_parts = by_head(normed_last.astype(f32))
    for turn in range(turns):
        both = jnp.concatenate([pack(pulled_parts, turn), pack(last_parts, turn)], axis=0)
        both = both.astype(bf16)
        for index in range(model // HEAD_WIDTH):
            early_src[index * turns + turn] = tile(both, index)

    early = Exchange(at, early_src, early_dst, early_sems.at[0], early_sems.at[1])
    early.start()
    gather_context.middle()

    near_block = list_dst.at[pl.ds(0, at.neg_count - 1)]
    remote(near_block, near_block, list_sent, list_here, at.to_partner()).wait_recv()

    def total(array):
        return jnp.sum(jnp.sum(array, axis=1, keepdims=True), axis=0, keepdims=True)

    def query_terms(first):
        block = list_dst[pl.ds(first, at.neg_count)].reshape(at.neg_count, HEAD_WIDTH)
        real = lax.broadcasted_iota(jnp.int32, block.shape, 1) < pairs
        score = jnp.where(real, block, 0.0)
        scaled = pltpu.roll(block, HEAD_WIDTH - pairs, 1)
        scaled = jnp.where(real, scaled, 0.0) / TEACHER_TEMP
        expo_t = jnp.where(real, jnp.exp(scaled), 0.0)
        total_s = total(jnp.where(real, jnp.exp(score), 0.0))
        return score, scaled, expo_t, total_s, total(expo_t)

    _, _, _, total_s, total_t = query_terms(pl.multiple_of(at.pb * at.neg_count, at.neg_count))
    grad_score = GRAD_SCALE * (
        jnp.exp(score8) / total_s - jnp.exp(teacher8 / TEACHER_TEMP) / total_t
    )
    grad_unit = grad_score * gain
    grad_resid = out_scale * (grad_unit - out_unit * lane_mean(grad_unit * out_unit))
    resid_grad[...] = grad_resid
    resid_cast = grad_resid.astype(bf16)
    grad_context = stack_heads(mm(resid_cast, full_o[...])).astype(bf16)
    context_blocks[...] = blocks_of(grad_context.astype(f32))
    late_own[0:stacked, :] = grad_context

    grad_probs = mm(context_blocks[...], value_cast[...], 1, 1)
    spread = jnp.sum(attention_weights * grad_probs, axis=-1, keepdims=True)
    logit_gradient = (attention_weights * (grad_probs - spread)).astype(bf16)
    logit_grad[...] = (attention_weights * (grad_probs - spread)).T.astype(bf16)

    turned_q = diagonal_of(mm(logit_gradient, key_rot[...])) * HEAD_WIDTH ** (-0.5)
    back_q = turned_q * cos_rows - pltpu.roll(turned_q, HEAD_WIDTH // 2, 1) * sin_rows
    back_q = query_scale * (back_q - query_unit * lane_mean(back_q * query_unit))
    grad_q_cast = back_q.astype(bf16)
    late_own[stacked : 2 * stacked, :] = grad_q_cast
    gather_late.start()
    gather_context.relay()

    cuts = 1
    cut_width = kv_width // cuts
    block_rows = model // at.pb_count

    def key_back(cut):
        columns = slice(cut * cut_width, (cut + 1) * cut_width)

        def one(pair, carry):
            rows = pl.ds(pl.multiple_of(pair * seq, seq), seq)
            turned = mm(logit_grad[rows, :], query_blocks[:, columns]) * HEAD_WIDTH ** (-0.5)
            for group in range(groups // cuts):
                start = cut * cut_width + group * HEAD_WIDTH
                lanes = slice(start, start + HEAD_WIDTH)
                part = tile(turned, group)
                unit = key_unit[rows, lanes]
                back = part * cos_table[...] - pltpu.roll(part, HEAD_WIDTH // 2, 1) * sin_table[...]
                back = key_scale[rows, lanes] * (back - unit * lane_mean(back * unit))
                grad_k[rows, lanes] = back.astype(bf16)
            return carry

        lax.fori_loop(0, pairs, one, 0)

    def send(src, dst, send_sem, recv_sem, target):
        remote(src, dst, send_sem, recv_sem, target).start()

    def arrive(block, recv_sem):
        remote(block, block, any_sem, recv_sem, at.to_partner()).wait_recv()

    def key_products(cut):
        columns = slice(cut * cut_width, (cut + 1) * cut_width)
        for k in range(1, at.pb_count + 1):
            pb = at.pb_peer(k % at.pb_count)
            chosen = pl.ds(pl.multiple_of(pb * block_rows, block_rows), block_rows)
            product = mm(normed_t[chosen, :], grad_k[:, columns])
            partial[cut, pb] = product.astype(bf16).reshape(at.line_count, 2, share, cut_width)
            send(
                partial.at[cut, pb, :, at.partner],
                from_core.at[cut, pb],
                core_send,
                core_recv.at[cut, pb],
                at.to_partner(),
            )

    def key_pairs(cut):
        def add_pair(pb):
            arrive(from_core.at[cut, pb], core_recv.at[cut, pb])
            both = partial[cut, pb, :, at.core].astype(f32) + from_core[cut, pb].astype(f32)
            paired[pb, :, cut] = both.astype(bf16)

        for k in range(1, at.pb_count):
            add_pair(at.pb_peer(k))
        for step in range(1, at.line_count + 1):
            line = at.line_peer(step % at.line_count)
            for k in range(1, at.pb_count):
                pb = at.pb_peer(k)
                send(
                    paired.at[pb, line, cut],
                    from_pb.at[at.pb, line, cut],
                    pb_send,
                    pb_recv.at[line],
                    at.to_pb(pb),
                )
        add_pair(at.pb)

    key_back(0)
    key_products(0)
    gather_late.middle()
    key_pairs(0)

    resid_parts = by_head(resid_cast.astype(f32))
    for turn in range(turns):
        packed = pack(resid_parts, turn).astype(bf16)
        for index in range(model // HEAD_WIDTH):
            resid_src[index * turns + turn] = tile(packed, index)
    resid = Exchange(at, resid_src, resid_dst, resid_sems.at[0], resid_sems.at[1])
    resid.start()

    back_last = mm(spread_heads(grad_q_cast.astype(f32)), full_q[...], 1, 1)
    last_grad[...] = back_last + pltpu.roll(back_last, pairs, 0)

    def value_back(pair, carry):
        start = pl.multiple_of(pair * seq, seq)
        rows = pl.ds(start, seq)
        grad_v[rows, :] = mm(probs_ref[rows, :], context_blocks[...]).astype(bf16)
        return carry

    lax.fori_loop(0, pairs, value_back, 0)

    seq_row = lax.broadcasted_iota(jnp.int32, (seq, 1), 0)

    def hidden_back(pair, carry):
        rows = pl.ds(pl.multiple_of(pair * seq, seq), seq)
        total = mm(grad_k[rows, :], full_k[...], 1, 1) + mm(grad_v[rows, :], full_v[...], 1, 1)
        hit = seq_row == lengths[0, pair] - 1
        total = total + jnp.where(hit, last_grad[pl.ds(pair, 1), :], 0.0)
        scaled = total * norm_gain[...]
        wide = x[rows, :].astype(f32)
        inv = inv_wide[rows, 0:1]
        mean = lane_mean(scaled * wide)
        result = inv * scaled - wide * (inv * inv * inv * mean)
        result = result + jnp.where(hit, resid_grad[pl.ds(pair, 1), :], 0.0)
        grad_hidden[rows, :] = result.astype(bf16)
        return carry

    def add_line(step):
        line = at.line_peer(step % at.line_count)
        total = paired[at.pb, line].astype(f32)
        arrive(from_pb.at[pl.ds(0, at.pb_count - 1), line], pb_recv.at[line])
        for k in range(1, at.pb_count):
            pb = at.pb_peer(k)
            total = total + from_pb[pb, line].astype(f32)
        if step < at.line_count:
            summed[line] = total.astype(bf16)
            send(
                summed.at[line],
                from_line.at[at.line],
                line_send,
                line_recv,
                at.to_line(line),
            )
        return total

    hidden_back(0, 0)
    hidden_back(1, 0)
    hidden_back(2, 0)
    add_line(1)
    gather_late.relay()

    far_block = list_dst.at[pl.ds(0, at.count - at.neg_count)]
    remote(far_block, far_block, list_sent, list_there, at.to_partner()).wait_recv()
    loss = jnp.zeros((1, 1), f32)
    for pb in range(at.pb_count):
        score, scaled, expo_t, sum_s, sum_t = query_terms(pb * at.neg_count)
        loss = loss + total(expo_t / sum_t * (scaled - jnp.log(sum_t) - (score - jnp.log(sum_s))))
    loss_out[...] = loss

    add_line(2)
    gather_context.tail()
    for step in range(3, at.line_count + 1):
        own_sum = add_line(step)
    gather_late.tail()
    for pair in range(3, pairs):
        hidden_back(pair, 0)

    gather_context.finish()
    gather_late.finish()
    early.wait("wait_recv")
    resid.wait("wait_recv")

    def rows_of(full, start, group):
        wide = full[...].astype(f32).reshape(at.count, -1, slots, HEAD_WIDTH)
        return wide[:, start + group].reshape(at.count * slots, HEAD_WIDTH).astype(bf16)

    pulled_rows = rows_of(early_dst, 0, 0)
    last_rows = rows_of(early_dst, 1, 0)
    resid_rows = rows_of(resid_dst, 0, 0)
    for group in range(groups):
        found = mm(pulled_rows, rows_of(late_full, 0, group), 0, 0)
        lanes = slice(group * HEAD_WIDTH, (group + 1) * HEAD_WIDTH)
        grad_value[:, lanes] = found[group * share : (group + 1) * share]
        found = mm(last_rows, rows_of(late_full, groups, group), 0, 0)
        for part in range(per_group):
            head = per_group * group + part
            grad_query[:, head * HEAD_WIDTH : (head + 1) * HEAD_WIDTH] = found[
                part * share : (part + 1) * share
            ]
        found = mm(resid_rows, rows_of(context_full, 0, group), 0, 0)
        for part in range(per_group):
            head = per_group * group + part
            grad_out[:, head * HEAD_WIDTH : (head + 1) * HEAD_WIDTH] = found[
                part * share : (part + 1) * share
            ]

    final = own_sum
    arrive(from_line.at[pl.ds(0, at.line_count - 1)], line_recv)
    for step in range(1, at.line_count):
        line = at.line_peer(step)
        final = final + from_line[line].astype(f32)
    for cut in range(cuts):
        grad_key[:, cut * cut_width : (cut + 1) * cut_width] = final[cut]

    for gather in gathers:
        gather.drain()
    pieces = from_line.at[pl.ds(0, at.line_count - 1)]
    for block, sem in (
        (from_core, core_send),
        (from_pb.at[pl.ds(0, at.pb_count - 1)], pb_send),
        (pieces, line_send),
    ):
        remote(block, block, sem, any_sem, at.to_partner()).wait_send()
    early.wait("wait_send")
    resid.wait("wait_send")
    sent_block = list_dst.at[pl.ds(0, at.count - 1)]
    remote(sent_block, sent_block, list_sent, list_here, at.to_partner()).wait_send()


def write_kernel(count, *refs):
    sources, targets, sems = refs[:count], refs[count : 2 * count], refs[2 * count]
    copies = [
        pltpu.make_async_copy(sources[i], targets[i], sems.at[i]) for i in range(2, count)
    ]
    for copy in copies:
        copy.start()
    for i in range(2):
        targets[i][...] = sources[i][...]
    for copy in copies:
        copy.wait()


def write_outputs(arrays):
    count = len(arrays)
    return pl.pallas_call(
        functools.partial(write_kernel, count),
        out_shape=tuple(jax.ShapeDtypeStruct(a.shape, a.dtype) for a in arrays),
        in_specs=[VMEM_SPEC] * count,
        out_specs=(VMEM_SPEC,) * 2 + (pl.BlockSpec(memory_space=pl.ANY),) * (count - 2),
        scratch_shapes=[pltpu.SemaphoreType.DMA((count,))],
        compiler_params=pltpu.CompilerParams(vmem_limit_bytes=4 * 2**20),
    )(*arrays)


def run_step(operands, sizes, pb_count, neg_count):
    pairs, seq, groups, share = sizes
    x, own_q, own_k = operands[0], operands[8], operands[9]
    model, width, kv_width = x.shape[1], own_q.shape[1], own_k.shape[1]
    rows = pairs * seq
    count = pb_count * neg_count
    line_count = neg_count // 2
    slots = width // kv_width * pairs
    stacked = groups * slots
    bf16, f32 = jnp.bfloat16, jnp.float32
    block = (pb_count, line_count, 1, share, kv_width)
    dma = pltpu.SemaphoreType.DMA
    vmem = pltpu.VMEM
    smem_spec = pl.BlockSpec(memory_space=pltpu.SMEM)
    hbm_spec = pl.BlockSpec(memory_space=pltpu.HBM)
    return pl.pallas_call(
        functools.partial(step_kernel, sizes),
        out_shape=(
            vmem((1, pairs), f32),
            vmem((1, 1), f32),
            vmem((rows, model), bf16),
            vmem((share, width), f32),
            vmem((share, kv_width), f32),
            vmem((share, kv_width), f32),
            vmem((share, width), f32),
        ),
        in_specs=[hbm_spec, smem_spec, smem_spec] + [hbm_spec] * 9,
        out_specs=(VMEM_SPEC,) * 7,
        scratch_shapes=[
            vmem((rows, model), bf16),
        ]
        + [vmem(a.shape, a.dtype) for a in operands[3:]]
        + [
            vmem((model, width), bf16),
            vmem((model, kv_width), bf16),
            vmem((model, kv_width), bf16),
            vmem((model, width), bf16),
            vmem((rows, model), bf16),
            vmem((model, rows), bf16),
            vmem((rows, HEAD_WIDTH), f32),
            vmem((rows, kv_width), f32),
            vmem((rows, kv_width), f32),
            vmem((rows, kv_width), bf16),
            vmem((rows, kv_width), bf16),
            vmem((rows, kv_width), bf16),
            vmem((rows, kv_width), bf16),
            vmem((rows, stacked), bf16),
            vmem((rows, stacked), bf16),
            vmem((stacked, kv_width), bf16),
            vmem((stacked, kv_width), bf16),
            vmem((slots, model), f32),
            vmem((slots, model), f32),
            vmem((stacked, HEAD_WIDTH), bf16),
            vmem((stacked * count, HEAD_WIDTH), bf16),
            vmem((2 * stacked, HEAD_WIDTH), bf16),
            vmem((2 * stacked * count, HEAD_WIDTH), bf16),
            vmem((count, 2 * slots, HEAD_WIDTH), bf16),
            vmem((count, 2 * slots, HEAD_WIDTH), bf16),
            vmem((count, slots, HEAD_WIDTH), bf16),
            vmem((count, slots, HEAD_WIDTH), bf16),
            vmem((1, HEAD_WIDTH), f32),
            vmem((count, 1, HEAD_WIDTH), f32),
            vmem((1, pb_count, line_count, 2, share, kv_width), bf16),
            vmem((1, pb_count, line_count, share, kv_width), bf16),
            vmem(block, bf16),
            vmem(block, bf16),
            vmem(block[1:], bf16),
            vmem(block[1:], bf16),
            dma((2,)),
            dma((2,)),
            dma((3,)),
            dma,
            dma((1, pb_count)),
            dma,
            dma((line_count,)),
            dma,
            dma,
            dma,
            dma((pairs + 9,)),
        ]
        + gather_sems(neg_count, True) * 6
        + gather_sems(neg_count, False) * 2,
        compiler_params=pltpu.CompilerParams(
            collective_id=0, has_side_effects=True, vmem_limit_bytes=62 * 2**20
        ),
    )(*operands)


def shards(
    hidden,
    lengths,
    teacher,
    norm_gain,
    final_gain,
    score_vector,
    query_weight,
    key_matrix,
    value_matrix,
    out_weight,
):
    both = ("pb", "neg")
    width = query_weight.shape[1]
    kv_width = key_matrix.shape[1]
    share, out_share = query_weight.shape[0], out_weight.shape[1]
    pb_count, neg_count = lax.axis_size("pb"), lax.axis_size("neg")
    pair_count, seq_len, model_width = hidden.shape[1:]
    group_count = kv_width // HEAD_WIDTH
    own_kernels = (
        pb_count == 4
        and neg_count == 8
        and share == out_share
        and share % 32 == 0
        and model_width == share * pb_count * neg_count
        and width == 2 * kv_width
        and pair_count * 2 == 8
        and seq_len == HEAD_WIDTH
        and share * group_count == HEAD_WIDTH
    )
    if own_kernels:
        cos_table, sin_table = signed_tables(seq_len, HEAD_WIDTH)
        results = run_step(
            (
                hidden.reshape(pair_count * seq_len, model_width),
                lengths,
                teacher,
                norm_gain[None],
                final_gain[None],
                score_vector[None],
                cos_table,
                sin_table,
                query_weight,
                key_matrix,
                value_matrix,
                out_weight.T,
            ),
            (pair_count, seq_len, group_count, share),
            pb_count,
            neg_count,
        )
        scores, loss, grad_rows, grad_query, grad_key, grad_value, grad_out = write_outputs(results)
        return (
            scores,
            loss.reshape(()),
            grad_rows.reshape(hidden.shape),
            grad_query,
            grad_key,
            grad_value,
            grad_out.T,
        )
    packed = jnp.concatenate([query_weight, key_matrix, value_matrix, out_weight.T], axis=1)
    everything = lax.all_gather(packed, both, axis=0, tiled=True)
    full_query = everything[:, :width]
    full_key = everything[:, width : width + kv_width]
    full_value = everything[:, width + kv_width : width + 2 * kv_width]
    full_out_t = everything[:, width + 2 * kv_width :]
    weights = (full_query, full_key, full_value, full_out_t.T)
    scores_here, stored = forward_pairs(
        hidden[0], lengths[0], norm_gain, final_gain, score_vector, *weights
    )
    listing = jnp.concatenate([scores_here, teacher[0]])[None]
    listed = lax.all_gather(listing, "neg", axis=0, tiled=True)
    all_scores = listed[:, :pair_count]
    all_scaled = listed[:, pair_count:] / TEACHER_TEMP
    my_total_s = jnp.sum(jnp.exp(all_scores))
    expo_t = jnp.exp(all_scaled)
    my_total_t = jnp.sum(expo_t)
    loss_here = jnp.sum(
        expo_t
        / my_total_t
        * (all_scaled - jnp.log(my_total_t) - (all_scores - jnp.log(my_total_s)))
    )
    prob_s = jnp.exp(scores_here) / my_total_s
    prob_t = jnp.exp(teacher[0] / TEACHER_TEMP) / my_total_t
    grad_score = GRAD_SCALE * (prob_s - prob_t)
    grad_input, last_rows, grad_kv = backward_pairs(
        stored, grad_score, norm_gain, final_gain, score_vector, *weights
    )
    grad_kv = grad_kv.astype(jnp.bfloat16)
    reduced = lax.psum_scatter(grad_kv, both, scatter_dimension=0, tiled=True)
    reduced = reduced.astype(jnp.float32)
    rows = lax.all_gather(last_rows, both, axis=0, tiled=True)
    loss_value = lax.psum(loss_here, "pb")
    index = lax.axis_index("pb") * neg_count + lax.axis_index("neg")
    normed_cols = lax.dynamic_slice_in_dim(rows, index * share, share, axis=1)
    resid_cols = lax.dynamic_slice_in_dim(rows, model_width + index * out_share, out_share, axis=1)
    rest = 2 * model_width
    all_q = rows[:, rest : rest + width]
    all_context = rows[:, rest + width :]
    grad_query = jnp.dot(normed_cols.T, all_q, preferred_element_type=jnp.float32)
    grad_out = jnp.dot(all_context.T, resid_cols, preferred_element_type=jnp.float32)
    return (
        scores_here[None],
        loss_value,
        grad_input[None],
        grad_query,
        reduced[:, :kv_width],
        reduced[:, kv_width:],
        grad_out,
    )


def solution(mesh):
    placed = (
        P("pb", "neg", None, None),
        P("pb", "neg"),
        P("pb", "neg"),
        P(),
        P(),
        P(),
        P(("pb", "neg"), None),
        P(("pb", "neg"), None),
        P(("pb", "neg"), None),
        P(None, ("pb", "neg")),
    )
    return jax.shard_map(
        shards,
        mesh=mesh,
        in_specs=placed,
        out_specs=(
            P("pb", "neg"),
            P(),
            P("pb", "neg", None, None),
            P(("pb", "neg"), None),
            P(("pb", "neg"), None),
            P(("pb", "neg"), None),
            P(None, ("pb", "neg")),
        ),
        check_vma=False,
    )
```

```python
import functools

import jax
import jax.numpy as jnp
import numpy as np
from jax import lax
from jax.experimental import pallas as pl
from jax.experimental.pallas import tpu as pltpu
from jax.sharding import PartitionSpec as P

HEAD_WIDTH = 128
MESH_ID = pl.DeviceIdType.MESH

EPSILON = 1e-06
ROPE_BASE = 1000000.0
TEACHER_TEMP = 2.0
GRAD_SCALE = 512.0


def rope_tables(seq_len, head_size):
    half = head_size // 2
    freqs = ROPE_BASE ** (-(jnp.arange(half, dtype=jnp.float32) * 2.0) / head_size)
    angles = jnp.arange(seq_len, dtype=jnp.float32)[:, None] * freqs[None, :]
    angles = jnp.concatenate([angles, angles], axis=1)
    return (jnp.cos(angles), jnp.sin(angles))


def signed_tables(seq_len, head_size):
    half = head_size // 2
    freqs = ROPE_BASE ** (-(np.arange(half) * 2.0) / head_size)
    angles = np.arange(seq_len)[:, None] * freqs[None, :]
    cos = np.concatenate([np.cos(angles)] * 2, axis=1)
    sin = np.concatenate([-np.sin(angles), np.sin(angles)], axis=1)
    return (jnp.asarray(cos, jnp.float32), jnp.asarray(sin, jnp.float32))


def rotate_half(vector):
    half = vector.shape[-1] // 2
    return jnp.concatenate([-vector[..., half:], vector[..., :half]], axis=-1)


def unrotate_half(vector):
    half = vector.shape[-1] // 2
    return jnp.concatenate([vector[..., half:], -vector[..., :half]], axis=-1)


def forward_pairs(
    tokens_in,
    lengths_here,
    norm_gain,
    final_gain,
    score_vector,
    query_weight,
    key_matrix,
    value_matrix,
    out_weight,
):
    pair_count, seq_len, model_width = tokens_in.shape
    head_count = query_weight.shape[1] // HEAD_WIDTH
    group_count = key_matrix.shape[1] // HEAD_WIDTH
    group_size = head_count // group_count
    inputs_wide = tokens_in.astype(jnp.float32)
    inv_rms = lax.rsqrt(jnp.mean(inputs_wide * inputs_wide, axis=-1, keepdims=True) + EPSILON)
    normed = (inputs_wide * inv_rms * norm_gain).astype(jnp.bfloat16)
    flat_rows = normed.reshape(pair_count * seq_len, model_width)
    key_proj = jnp.dot(flat_rows, key_matrix, preferred_element_type=jnp.float32).reshape(
        pair_count, seq_len, group_count, HEAD_WIDTH
    )
    value_proj = jnp.dot(flat_rows, value_matrix, preferred_element_type=jnp.float32).reshape(
        pair_count, seq_len, group_count, HEAD_WIDTH
    )
    positions = jnp.arange(seq_len, dtype=jnp.int32)
    last_index = lengths_here - 1
    onehot = (positions[None, :] == last_index[:, None]).astype(jnp.float32)
    normed_last = jnp.take_along_axis(normed, last_index[:, None, None], axis=1)[:, 0]
    query_proj = jnp.dot(normed_last, query_weight, preferred_element_type=jnp.float32).reshape(
        pair_count, head_count, HEAD_WIDTH
    )
    query_scale = lax.rsqrt(jnp.mean(query_proj * query_proj, axis=-1, keepdims=True) + EPSILON)
    query_unit = query_proj * query_scale
    key_scale = lax.rsqrt(jnp.mean(key_proj * key_proj, axis=-1, keepdims=True) + EPSILON)
    key_unit = key_proj * key_scale
    cos_table, sin_table = rope_tables(seq_len, HEAD_WIDTH)
    cos_query = jnp.dot(onehot, cos_table, precision=lax.Precision.HIGHEST)
    sin_query = jnp.dot(onehot, sin_table, precision=lax.Precision.HIGHEST)
    query_rot = (
        query_unit * cos_query[:, None, :] + rotate_half(query_unit) * sin_query[:, None, :]
    ).astype(jnp.bfloat16)
    key_rot = (
        key_unit * cos_table[None, :, None, :] + rotate_half(key_unit) * sin_table[None, :, None, :]
    ).astype(jnp.bfloat16)
    value_cast = value_proj.astype(jnp.bfloat16)
    grouped = query_rot.reshape(pair_count, group_count, group_size, HEAD_WIDTH)
    logits = jnp.einsum(
        "pkgd,pskd->pkgs", grouped, key_rot, preferred_element_type=jnp.float32
    ) * HEAD_WIDTH ** (-0.5)
    visible = (positions[None, :] <= last_index[:, None])[:, None, None, :]
    expos = jnp.where(visible, jnp.exp(logits), 0.0)
    attention_weights = expos / jnp.sum(expos, axis=-1, keepdims=True)
    probs_cast = attention_weights.astype(jnp.bfloat16)
    context = jnp.einsum(
        "pkgs,pskd->pkgd", probs_cast, value_cast, preferred_element_type=jnp.float32
    )
    context = context.astype(jnp.bfloat16).reshape(pair_count, head_count * HEAD_WIDTH)
    attended = jnp.dot(context, out_weight, preferred_element_type=jnp.float32)
    residual = jnp.take_along_axis(inputs_wide, last_index[:, None, None], axis=1)[:, 0] + attended
    out_scale = lax.rsqrt(jnp.mean(residual * residual, axis=-1, keepdims=True) + EPSILON)
    out_unit = residual * out_scale
    scores_here = jnp.sum(out_unit * final_gain * score_vector, axis=-1)
    stored = (
        tokens_in,
        onehot,
        inv_rms,
        normed,
        normed_last,
        query_unit,
        query_scale,
        key_unit,
        key_scale,
        cos_query,
        sin_query,
        cos_table,
        sin_table,
        query_rot,
        key_rot,
        value_cast,
        attention_weights,
        probs_cast,
        context,
        out_unit,
        out_scale,
    )
    return (scores_here, stored)


def backward_pairs(
    stored,
    grad_score,
    norm_gain,
    final_gain,
    score_vector,
    query_weight,
    key_matrix,
    value_matrix,
    out_weight,
):
    (
        tokens_in,
        onehot,
        inv_rms,
        normed,
        normed_last,
        query_unit,
        query_scale,
        key_unit,
        key_scale,
        cos_query,
        sin_query,
        cos_table,
        sin_table,
        query_rot,
        key_rot,
        value_cast,
        attention_weights,
        probs_cast,
        context,
        out_unit,
        out_scale,
    ) = stored
    pair_count, seq_len, model_width = tokens_in.shape
    head_count = query_weight.shape[1] // HEAD_WIDTH
    group_count = key_matrix.shape[1] // HEAD_WIDTH
    group_size = head_count // group_count
    grad_unit = grad_score[:, None] * score_vector * final_gain
    grad_resid = out_scale * (
        grad_unit - out_unit * jnp.mean(grad_unit * out_unit, axis=-1, keepdims=True)
    )
    grad_resid_cast = grad_resid.astype(jnp.bfloat16)
    grad_context = jnp.dot(
        grad_resid_cast, out_weight.T, preferred_element_type=jnp.float32
    ).astype(jnp.bfloat16)
    grad_context = grad_context.reshape(pair_count, group_count, group_size, HEAD_WIDTH)
    grad_probs = jnp.einsum(
        "pkgd,pskd->pkgs", grad_context, value_cast, preferred_element_type=jnp.float32
    )
    grad_vals = jnp.einsum(
        "pkgs,pkgd->pskd", probs_cast, grad_context, preferred_element_type=jnp.float32
    )
    spread = jnp.sum(attention_weights * grad_probs, axis=-1, keepdims=True)
    logit_gradient = (attention_weights * (grad_probs - spread)).astype(jnp.bfloat16)
    grouped = query_rot.reshape(pair_count, group_count, group_size, HEAD_WIDTH)
    rotated_query_gradient = jnp.einsum(
        "pkgs,pskd->pkgd", logit_gradient, key_rot, preferred_element_type=jnp.float32
    ) * HEAD_WIDTH ** (-0.5)
    rotated_query_gradient = rotated_query_gradient.reshape(pair_count, head_count, HEAD_WIDTH)
    grad_krot = jnp.einsum(
        "pkgs,pkgd->pskd", logit_gradient, grouped, preferred_element_type=jnp.float32
    ) * HEAD_WIDTH ** (-0.5)
    grad_qunit = rotated_query_gradient * cos_query[:, None, :] + unrotate_half(
        rotated_query_gradient * sin_query[:, None, :]
    )
    grad_kunit = grad_krot * cos_table[None, :, None, :] + unrotate_half(
        grad_krot * sin_table[None, :, None, :]
    )
    grad_qproj = query_scale * (
        grad_qunit - query_unit * jnp.mean(grad_qunit * query_unit, axis=-1, keepdims=True)
    )
    grad_kproj = key_scale * (
        grad_kunit - key_unit * jnp.mean(grad_kunit * key_unit, axis=-1, keepdims=True)
    )
    grad_q_cast = grad_qproj.reshape(pair_count, head_count * HEAD_WIDTH).astype(jnp.bfloat16)
    grad_k_cast = grad_kproj.reshape(pair_count * seq_len, group_count * HEAD_WIDTH).astype(
        jnp.bfloat16
    )
    grad_v_cast = grad_vals.reshape(pair_count * seq_len, group_count * HEAD_WIDTH).astype(
        jnp.bfloat16
    )
    flat_rows = normed.reshape(pair_count * seq_len, model_width)
    last_rows = jnp.concatenate([normed_last, grad_resid_cast, grad_q_cast, context], axis=1)
    grad_kv = jnp.dot(
        flat_rows.T,
        jnp.concatenate([grad_k_cast, grad_v_cast], axis=1),
        preferred_element_type=jnp.float32,
    )
    grad_normed = jnp.dot(grad_k_cast, key_matrix.T, preferred_element_type=jnp.float32)
    grad_normed = grad_normed + jnp.dot(
        grad_v_cast, value_matrix.T, preferred_element_type=jnp.float32
    )
    grad_normed = grad_normed.reshape(pair_count, seq_len, model_width)
    grad_last = jnp.dot(grad_q_cast, query_weight.T, preferred_element_type=jnp.float32)
    grad_normed = grad_normed + onehot[:, :, None] * grad_last[:, None, :]
    inputs_wide = tokens_in.astype(jnp.float32)
    grad_scaled = grad_normed * norm_gain
    grad_input = inv_rms * grad_scaled - inputs_wide * inv_rms * inv_rms * inv_rms * jnp.mean(
        grad_scaled * inputs_wide, axis=-1, keepdims=True
    )
    grad_input = grad_input + onehot[:, :, None] * grad_resid[:, None, :]
    return (grad_input.astype(jnp.bfloat16), last_rows, grad_kv)


class Place:
    def __init__(self):
        self.pb_count = lax.axis_size("pb")
        self.neg_count = lax.axis_size("neg")
        self.line_count = self.neg_count // 2
        self.pb = lax.axis_index("pb")
        neg = lax.axis_index("neg")
        self.line = neg // 2
        self.core = neg % 2
        self.partner = 1 - self.core

    def slot(self, pb, line, core):
        return pb * self.neg_count + line * 2 + core

    def line_peer(self, step):
        return lax.rem(self.line + step, self.line_count)

    def pb_peer(self, step):
        return lax.rem(self.pb + step, self.pb_count)

    def to_line(self, line):
        return (self.pb, line * 2 + self.core)

    def to_pb(self, pb):
        return (pb, self.line * 2 + self.core)

    def to_partner(self):
        return (self.pb, self.line * 2 + self.partner)

    def greet(self):
        barrier = pltpu.get_barrier_semaphore()
        targets = [self.to_line(self.line_peer(k)) for k in range(1, self.line_count)]
        targets += [self.to_pb(self.pb_peer(k)) for k in range(1, self.pb_count)]
        targets += [self.to_partner()]
        for target in targets:
            pl.semaphore_signal(barrier, inc=1, device_id=target, device_id_type=MESH_ID)
        pl.semaphore_wait(barrier, len(targets))


def remote(src, dst, send_sem, recv_sem, target):
    return pltpu.make_async_remote_copy(
        src_ref=src,
        dst_ref=dst,
        send_sem=send_sem,
        recv_sem=recv_sem,
        device_id=target,
        device_id_type=MESH_ID,
    )


def gather_sems(neg_count, large):
    line_count = neg_count // 2
    dma = pltpu.SemaphoreType.DMA
    if large:
        return [dma((line_count,)), dma((line_count,)), dma((line_count,)), dma((2,))]
    return [dma((1,)), dma((1,)), dma((1,)), dma((2,))]


class Gather:
    def __init__(self, place, own, full, sems, halve_corner, direct):
        self.place, self.own, self.full = place, own, full
        self.line_recv, self.pb_recv, self.corner_recv, ends = sems
        self.send_sem, self.core_recv = ends.at[0], ends.at[1]
        self.halve_corner, self.direct = halve_corner, direct
        across = place.pb + 1 - 2 * (place.pb % 2)
        along = place.pb + 2 - 4 * (place.pb // 2)
        self.near = (across, along)
        self.corner = 3 - place.pb
        half = place.line // 2
        self.is_inner = (place.line == 1) | (place.line == 2)
        self.mate = place.line + 1 - 2 * (place.line % 2)
        self.far_inner = 2 - half
        self.far_outer = 3 - 3 * half
        self.size = own.shape[0]
        if halve_corner:
            self.own_lines = (place.line, lax.rem(place.line + 2, 4))
            self.mate_lines = (self.mate, lax.rem(self.mate + 2, 4))
        else:
            self.own_lines = (place.line, self.mate, self.far_inner, self.far_outer)
            self.mate_lines = ()

    def rows(self, pb, line, core):
        start = self.place.slot(pb, line, core) * self.size
        return self.full.at[pl.ds(pl.multiple_of(start, self.size), self.size)]

    def blocks(self, count):
        return self.full.at[pl.ds(0, count * self.size)]

    def send(self, src, dst, recv_sem, target):
        remote(src, dst, self.send_sem, recv_sem, target).start()

    def of(self, sems, line):
        return sems.at[0] if self.direct else sems.at[line]

    def spread(self, src, line):
        at = self.place
        dst = self.rows(at.pb, line, at.core)
        for side in range(2):
            self.send(src, dst, self.of(self.pb_recv, line), at.to_pb(self.near[side]))
        self.pass_on(src, at.pb, line)

    def pass_on(self, src, pb, line):
        at = self.place
        self.send(src, self.rows(pb, line, at.core), self.core_recv, at.to_partner())

    def arrive(self, block, recv_sem):
        remote(block, block, self.send_sem, recv_sem, self.place.to_partner()).wait_recv()

    def start(self):
        at = self.place
        mine = self.rows(at.pb, at.line, at.core)
        peers = (self.mate, self.far_inner) + ((self.far_outer,) if self.direct else ())
        for line in peers:
            self.send(self.own, mine, self.of(self.line_recv, at.line), at.to_line(line))
        self.spread(self.own, at.line)
        mine[...] = self.own[...]

    def middle(self):
        at = self.place
        if self.direct:
            self.arrive(self.blocks(at.line_count - 1), self.line_recv.at[0])
        for line in (self.mate, self.far_inner, self.far_outer):
            block = self.rows(at.pb, line, at.core)
            if not self.direct:
                self.arrive(block, self.line_recv.at[line])
                if line is not self.mate:

                    @pl.when(self.is_inner)
                    def _():
                        self.send(block, block, self.line_recv.at[line], at.to_line(self.mate))

            self.spread(block, line)

    def half(self, block, side):
        size = block.shape[0] // 2
        return block.at[pl.ds(side * size, size)]

    def relay(self):
        at = self.place
        if self.direct:
            self.arrive(self.blocks(2 * at.line_count), self.pb_recv.at[0])
        for line in self.own_lines + self.mate_lines:
            if not self.direct:
                self.arrive(self.blocks(2), self.pb_recv.at[line])
            for side in range(2):
                block = self.rows(self.near[side], line, at.core)
                if not any(line is other for other in self.mate_lines):
                    part = self.half(block, side)
                    target = at.to_pb(self.near[1 - side])
                    self.send(part, part, self.of(self.corner_recv, line), target)
                self.pass_on(block, self.near[side], line)

    def corner_in(self, lines, hand_over):
        at = self.place
        if self.direct:
            self.arrive(self.blocks(at.line_count), self.corner_recv.at[0])
        for line in lines:
            block = self.rows(self.corner, line, at.core)
            if not self.direct:
                self.arrive(block, self.corner_recv.at[line])
            if hand_over:
                self.send(block, block, self.corner_recv.at[line], at.to_line(self.mate))
            self.pass_on(block, self.corner, line)

    def hand(self):
        if self.halve_corner:
            self.corner_in(self.own_lines, True)

    def tail(self):
        self.corner_in(self.mate_lines if self.halve_corner else self.own_lines, False)

    def finish(self):
        self.arrive(self.blocks(self.place.count // 2), self.core_recv)

    def drain(self):
        at = self.place
        block = self.blocks(at.count - (1 if self.direct else 2))
        remote(block, block, self.send_sem, self.core_recv, at.to_partner()).wait_send()
        if not self.direct:

            @pl.when(self.is_inner)
            def _():
                block = self.blocks(2)
                remote(block, block, self.send_sem, self.core_recv, at.to_partner()).wait_send()


VMEM_SPEC = pl.BlockSpec(memory_space=pltpu.VMEM)


def mm(left, right, left_dim=1, right_dim=0, precision=None):
    return lax.dot_general(
        left,
        right,
        (((left_dim,), (right_dim,)), ((), ())),
        preferred_element_type=jnp.float32,
        precision=precision,
    )


def lane_mean(array):
    return jnp.mean(array, axis=-1, keepdims=True)


def tile(array, index):
    return array[:, index * HEAD_WIDTH : (index + 1) * HEAD_WIDTH]


class Exchange:
    def __init__(self, at, src, dst, send_sem, recv_sem):
        self.at, self.src, self.dst = at, src, dst
        self.send_sem, self.recv_sem = send_sem, recv_sem

    def start(self):
        at = self.at
        for pb, neg in at.others:
            peer = pb * at.neg_count + neg
            remote(
                self.src.at[peer], self.dst.at[at.me], self.send_sem, self.recv_sem, (pb, neg)
            ).start()
        self.dst[at.me] = self.src[at.me]

    def wait(self, sem_of):
        block = self.dst.at[pl.ds(0, self.at.count - 1)]
        copy = remote(block, block, self.send_sem, self.recv_sem, self.at.to_partner())
        getattr(copy, sem_of)()


def step_kernel(
    sizes,
    hidden,
    lengths,
    teacher,
    norm_gain_in,
    final_gain_in,
    score_vector_in,
    cos_table_in,
    sin_table_in,
    own_q_in,
    own_k_in,
    own_v_in,
    own_o_in,
    scores_out,
    loss_out,
    grad_hidden,
    grad_query,
    grad_key,
    grad_value,
    grad_out,
    x,
    norm_gain,
    final_gain,
    score_vector,
    cos_table,
    sin_table,
    own_q,
    own_k,
    own_v,
    own_o,
    full_q,
    full_k,
    full_v,
    full_o,
    normed,
    normed_t,
    inv_wide,
    key_unit,
    key_scale,
    key_rot,
    value_cast,
    grad_k,
    grad_v,
    logit_grad,
    probs_ref,
    query_blocks,
    context_blocks,
    last_grad,
    resid_grad,
    context_own,
    context_full,
    late_own,
    late_full,
    early_src,
    early_dst,
    resid_src,
    resid_dst,
    list_src,
    list_dst,
    partial,
    from_core,
    paired,
    from_pb,
    summed,
    from_line,
    early_sems,
    resid_sems,
    list_sems,
    core_send,
    core_recv,
    pb_send,
    pb_recv,
    line_send,
    line_recv,
    any_sem,
    load_sems,
    *gather_sem_refs,
):
    pairs, seq, groups, share = sizes
    bf16, f32 = jnp.bfloat16, jnp.float32
    at = Place()
    at.count = at.pb_count * at.neg_count
    at.me = at.slot(at.pb, at.line, at.core)
    neg = lax.axis_index("neg")
    pb_all = [at.pb] + [at.pb_peer(k) for k in range(1, at.pb_count)]
    neg_all = [neg] + [lax.rem(neg + k, at.neg_count) for k in range(1, at.neg_count)]
    at.others = [
        (pb, peer)
        for i, pb in enumerate(pb_all)
        for j, peer in enumerate(neg_all)
        if i + j > 0
    ]
    model = x.shape[1]
    rows_all = pairs * seq
    per_group = own_q.shape[1] // own_k.shape[1]
    slots = per_group * pairs
    stacked = groups * slots
    kv_width = groups * HEAD_WIDTH

    barrier = pltpu.get_barrier_semaphore()

    for target in at.others:
        pl.semaphore_signal(barrier, inc=1, device_id=target, device_id_type=MESH_ID)
    loads = []
    moves = (
        (own_k_in, own_k),
        (own_v_in, own_v),
        (own_q_in, own_q),
        (own_o_in, own_o),
        (norm_gain_in, norm_gain),
        (final_gain_in, final_gain),
        (score_vector_in, score_vector),
        (cos_table_in, cos_table),
        (sin_table_in, sin_table),
    )
    small_loads = []
    for place_of, (source, target) in enumerate(moves):
        load = pltpu.make_async_copy(source, target, load_sems.at[pairs + place_of])
        load.start()
        small_loads.append(load)
    for pair in range(pairs):
        rows = pl.ds(pair * seq, seq)
        load = pltpu.make_async_copy(hidden.at[rows], x.at[rows], load_sems.at[pair])
        load.start()
        loads.append(load)

    half_width = own_q.shape[1] // 2
    low, high = pl.ds(0, half_width), pl.ds(half_width, half_width)
    parts = (
        (own_k, full_k, True),
        (own_v, full_v, True),
        (own_q.at[:, low], full_q.at[:, low], True),
        (own_q.at[:, high], full_q.at[:, high], True),
        (own_o.at[:, low], full_o.at[:, low], True),
        (own_o.at[:, high], full_o.at[:, high], False),
        (context_own, context_full, False),
        (late_own, late_full, False),
    )
    each = len(gather_sem_refs) // len(parts)
    gathers = [
        Gather(at, own, full, gather_sem_refs[i * each : (i + 1) * each], halve, i >= 6)
        for i, (own, full, halve) in enumerate(parts)
    ]
    gather_k, gather_v, gather_q0, gather_q1, gather_o0, gather_o1 = gathers[:6]
    gather_context, gather_late = gathers[6:]

    for load in small_loads:
        load.wait()
    pl.semaphore_wait(barrier, at.count - 1)
    for gather in gathers[:4]:
        gather.start()

    def norm_pair(pair, carry):
        rows = pl.ds(pl.multiple_of(pair * seq, seq), seq)
        wide = x[rows, :].astype(f32)
        inv = lax.rsqrt(lane_mean(wide * wide) + EPSILON)
        inv_wide[rows, :] = jnp.broadcast_to(inv, (seq, HEAD_WIDTH))
        scaled = wide * inv * norm_gain[...]
        normed[rows, :] = scaled.astype(bf16)
        normed_t[:, rows] = scaled.T.astype(bf16)
        return carry

    for pair in range(pairs):
        loads[pair].wait()
        norm_pair(pair, 0)

    row8 = lax.broadcasted_iota(jnp.int32, (slots, 1), 0)
    pair8 = lax.rem(row8, pairs)
    upper8 = row8 < pairs
    last8 = jnp.zeros((slots, 1), jnp.int32)
    teacher8 = jnp.zeros((slots, 1), f32)
    for pair in range(pairs):
        last8 = jnp.where(pair8 == pair, lengths[0, pair] - 1, last8)
        teacher8 = jnp.where(pair8 == pair, teacher[0, pair], teacher8)
    place8 = pair8 * seq + last8
    column8 = lax.broadcasted_iota(jnp.int32, (slots, rows_all), 1)
    onehot8 = (column8 == place8).astype(f32).astype(bf16)
    visible8 = (column8 >= pair8 * seq) & (column8 <= place8)
    visible = jnp.concatenate([visible8.astype(f32)] * groups, axis=0) > 0.5
    position8 = (lax.broadcasted_iota(jnp.int32, (slots, seq), 1) == last8).astype(f32)

    x_last = mm(onehot8, x[...])
    normed_last = mm(onehot8, normed[...]).astype(bf16)
    cos8 = mm(position8, cos_table[...], precision=lax.Precision.HIGHEST)
    sin8 = mm(position8, sin_table[...], precision=lax.Precision.HIGHEST)
    cos_rows = jnp.concatenate([cos8] * groups, axis=0)
    sin_rows = jnp.concatenate([sin8] * groups, axis=0)

    def key_pair(pair, carry):
        rows = pl.ds(pl.multiple_of(pair * seq, seq), seq)
        proj = mm(normed[rows, :], full_k[...])
        for group in range(groups):
            lanes = slice(group * HEAD_WIDTH, (group + 1) * HEAD_WIDTH)
            part = proj[:, lanes]
            scale = lax.rsqrt(lane_mean(part * part) + EPSILON)
            unit = part * scale
            key_unit[rows, lanes] = unit
            key_scale[rows, lanes] = jnp.broadcast_to(scale, (seq, HEAD_WIDTH))
            turned = unit * cos_table[...] + pltpu.roll(unit, HEAD_WIDTH // 2, 1) * sin_table[...]
            key_rot[rows, lanes] = turned.astype(bf16)
        return carry

    def value_pair(pair, carry):
        rows = pl.ds(pl.multiple_of(pair * seq, seq), seq)
        value_cast[rows, :] = mm(normed[rows, :], full_v[...]).astype(bf16)
        return carry

    gather_k.middle()
    gather_o0.start()
    gather_o1.start()
    gather_v.middle()
    gather_q0.middle()
    gather_k.relay()
    gather_q1.middle()
    gather_v.relay()
    gather_k.hand()
    gather_o0.middle()
    gather_o1.middle()
    gather_q0.relay()
    gather_v.hand()
    gather_q1.relay()
    gather_q0.hand()
    gather_k.tail()
    gather_o0.relay()
    gather_q1.hand()
    gather_v.tail()
    gather_o1.relay()
    gather_o0.hand()
    gather_q0.tail()
    gather_q1.tail()
    gather_k.finish()
    for pair in range(pairs):
        key_pair(pair, 0)
    gather_v.finish()
    for pair in range(pairs):
        value_pair(pair, 0)
    gather_o0.tail()
    gather_q0.finish()
    gather_q1.finish()
    gather_o1.tail()

    def stack_heads(wide):
        return jnp.concatenate(
            [
                jnp.where(upper8, tile(wide, per_group * group), tile(wide, per_group * group + 1))
                for group in range(groups)
            ],
            axis=0,
        )

    def spread_heads(stack):
        parts = []
        for group in range(groups):
            part = stack[group * slots : (group + 1) * slots]
            parts += [jnp.where(upper8, part, 0.0), jnp.where(upper8, 0.0, part)]
        return jnp.concatenate(parts, axis=1).astype(bf16)

    def diagonal_of(wide):
        return jnp.concatenate(
            [
                wide[group * slots : (group + 1) * slots, group * HEAD_WIDTH : (group + 1) * HEAD_WIDTH]
                for group in range(groups)
            ],
            axis=0,
        )

    def blocks_of(stack):
        rows = []
        for group in range(groups):
            part = stack[group * slots : (group + 1) * slots]
            rows.append(
                jnp.concatenate(
                    [part if other == group else jnp.zeros_like(part) for other in range(groups)],
                    axis=1,
                )
            )
        return jnp.concatenate(rows, axis=0).astype(bf16)

    query_proj = stack_heads(mm(normed_last, full_q[...]))
    query_scale = lax.rsqrt(lane_mean(query_proj * query_proj) + EPSILON)
    query_unit = query_proj * query_scale
    query_rot = query_unit * cos_rows + pltpu.roll(query_unit, HEAD_WIDTH // 2, 1) * sin_rows
    query_wide = blocks_of(query_rot)
    query_blocks[...] = query_wide
    logits = mm(query_wide, key_rot[...], 1, 1) * HEAD_WIDTH ** (-0.5)
    expos = jnp.where(visible, jnp.exp(logits), 0.0)
    attention_weights = expos / jnp.sum(expos, axis=-1, keepdims=True)
    probs = attention_weights.astype(bf16)
    probs_ref[...] = attention_weights.T.astype(bf16)
    context = diagonal_of(mm(probs, value_cast[...]))
    context_own[...] = context.astype(bf16)
    context_wide = spread_heads(context)
    gather_context.start()

    lane_block = lax.rem(
        lax.broadcasted_iota(jnp.int32, (slots, model), 1) // share, HEAD_WIDTH // share
    )

    def pack(parts, turn):
        total = jnp.zeros((slots, model), f32)
        for block, part in enumerate(parts):
            shift = ((block - turn) * share) % model
            moved = part if shift == 0 else pltpu.roll(part, shift, 1)
            total = jnp.where(lane_block == block, moved, total)
        return total

    def by_head(wide):
        return [jnp.where(upper8, wide, 0.0), jnp.where(upper8, 0.0, wide)]

    turns = HEAD_WIDTH // share
    gather_o0.finish()
    attended = mm(context_wide[:, :half_width], full_o[:, :half_width], 1, 1)
    gather_o1.finish()
    attended = attended + mm(context_wide[:, half_width:], full_o[:, half_width:], 1, 1)
    attended = attended + pltpu.roll(attended, pairs, 0)
    residual = x_last + attended
    out_scale = lax.rsqrt(lane_mean(residual * residual) + EPSILON)
    out_unit = residual * out_scale
    gain = final_gain[...] * score_vector[...]
    score8 = jnp.sum(out_unit * gain, axis=-1, keepdims=True)

    lane8 = lax.broadcasted_iota(jnp.int32, (slots, HEAD_WIDTH), 1)
    row_lane = lax.broadcasted_iota(jnp.int32, (slots, HEAD_WIDTH), 0)

    def as_row(column):
        return jnp.sum(jnp.where(row_lane == lane8, column, 0.0), axis=0, keepdims=True)

    score_row = as_row(score8)
    lane1 = lax.broadcasted_iota(jnp.int32, (1, HEAD_WIDTH), 1)
    listing = jnp.where(lane1 < pairs, score_row, as_row(teacher8))
    list_src[...] = listing
    me_row = list_dst.at[at.me]
    list_here, list_there, list_sent = list_sems.at[0], list_sems.at[1], list_sems.at[2]
    for place_of, target in enumerate(at.others):
        arrived = list_here if place_of < at.neg_count - 1 else list_there
        remote(list_src, me_row, list_sent, arrived, target).start()
    list_dst[at.me] = listing
    scores_out[...] = score_row[:, :pairs]

    pulled = mm(probs, normed[...])
    pulled_parts = [pulled[group * slots : (group + 1) * slots] for group in range(groups)]
    last_parts = by_head(normed_last.astype(f32))
    for turn in range(turns):
        both = jnp.concatenate([pack(pulled_parts, turn), pack(last_parts, turn)], axis=0)
        both = both.astype(bf16)
        for index in range(model // HEAD_WIDTH):
            early_src[index * turns + turn] = tile(both, index)

    early = Exchange(at, early_src, early_dst, early_sems.at[0], early_sems.at[1])
    early.start()
    gather_context.middle()

    near_block = list_dst.at[pl.ds(0, at.neg_count - 1)]
    remote(near_block, near_block, list_sent, list_here, at.to_partner()).wait_recv()

    def total(array):
        return jnp.sum(jnp.sum(array, axis=1, keepdims=True), axis=0, keepdims=True)

    def query_terms(first):
        block = list_dst[pl.ds(first, at.neg_count)].reshape(at.neg_count, HEAD_WIDTH)
        real = lax.broadcasted_iota(jnp.int32, block.shape, 1) < pairs
        score = jnp.where(real, block, 0.0)
        scaled = pltpu.roll(block, HEAD_WIDTH - pairs, 1)
        scaled = jnp.where(real, scaled, 0.0) / TEACHER_TEMP
        expo_t = jnp.where(real, jnp.exp(scaled), 0.0)
        total_s = total(jnp.where(real, jnp.exp(score), 0.0))
        return score, scaled, expo_t, total_s, total(expo_t)

    _, _, _, total_s, total_t = query_terms(pl.multiple_of(at.pb * at.neg_count, at.neg_count))
    grad_score = GRAD_SCALE * (
        jnp.exp(score8) / total_s - jnp.exp(teacher8 / TEACHER_TEMP) / total_t
    )
    grad_unit = grad_score * gain
    grad_resid = out_scale * (grad_unit - out_unit * lane_mean(grad_unit * out_unit))
    resid_grad[...] = grad_resid
    resid_cast = grad_resid.astype(bf16)
    grad_context = stack_heads(mm(resid_cast, full_o[...])).astype(bf16)
    context_blocks[...] = blocks_of(grad_context.astype(f32))
    late_own[0:stacked, :] = grad_context

    grad_probs = mm(context_blocks[...], value_cast[...], 1, 1)
    spread = jnp.sum(attention_weights * grad_probs, axis=-1, keepdims=True)
    logit_gradient = (attention_weights * (grad_probs - spread)).astype(bf16)
    logit_grad[...] = (attention_weights * (grad_probs - spread)).T.astype(bf16)

    turned_q = diagonal_of(mm(logit_gradient, key_rot[...])) * HEAD_WIDTH ** (-0.5)
    back_q = turned_q * cos_rows - pltpu.roll(turned_q, HEAD_WIDTH // 2, 1) * sin_rows
    back_q = query_scale * (back_q - query_unit * lane_mean(back_q * query_unit))
    grad_q_cast = back_q.astype(bf16)
    late_own[stacked : 2 * stacked, :] = grad_q_cast
    gather_late.start()
    gather_context.relay()

    cuts = 1
    cut_width = kv_width // cuts
    block_rows = model // at.pb_count

    def key_back(cut):
        columns = slice(cut * cut_width, (cut + 1) * cut_width)

        def one(pair, carry):
            rows = pl.ds(pl.multiple_of(pair * seq, seq), seq)
            turned = mm(logit_grad[rows, :], query_blocks[:, columns]) * HEAD_WIDTH ** (-0.5)
            for group in range(groups // cuts):
                start = cut * cut_width + group * HEAD_WIDTH
                lanes = slice(start, start + HEAD_WIDTH)
                part = tile(turned, group)
                unit = key_unit[rows, lanes]
                back = part * cos_table[...] - pltpu.roll(part, HEAD_WIDTH // 2, 1) * sin_table[...]
                back = key_scale[rows, lanes] * (back - unit * lane_mean(back * unit))
                grad_k[rows, lanes] = back.astype(bf16)
            return carry

        lax.fori_loop(0, pairs, one, 0)

    def send(src, dst, send_sem, recv_sem, target):
        remote(src, dst, send_sem, recv_sem, target).start()

    def arrive(block, recv_sem):
        remote(block, block, any_sem, recv_sem, at.to_partner()).wait_recv()

    def key_products(cut):
        columns = slice(cut * cut_width, (cut + 1) * cut_width)
        for k in range(1, at.pb_count + 1):
            pb = at.pb_peer(k % at.pb_count)
            chosen = pl.ds(pl.multiple_of(pb * block_rows, block_rows), block_rows)
            product = mm(normed_t[chosen, :], grad_k[:, columns])
            partial[cut, pb] = product.astype(bf16).reshape(at.line_count, 2, share, cut_width)
            send(
                partial.at[cut, pb, :, at.partner],
                from_core.at[cut, pb],
                core_send,
                core_recv.at[cut, pb],
                at.to_partner(),
            )

    def key_pairs(cut):
        def add_pair(pb):
            arrive(from_core.at[cut, pb], core_recv.at[cut, pb])
            both = partial[cut, pb, :, at.core].astype(f32) + from_core[cut, pb].astype(f32)
            paired[pb, :, cut] = both.astype(bf16)

        for k in range(1, at.pb_count):
            add_pair(at.pb_peer(k))
        for step in range(1, at.line_count + 1):
            line = at.line_peer(step % at.line_count)
            for k in range(1, at.pb_count):
                pb = at.pb_peer(k)
                send(
                    paired.at[pb, line, cut],
                    from_pb.at[at.pb, line, cut],
                    pb_send,
                    pb_recv.at[line],
                    at.to_pb(pb),
                )
        add_pair(at.pb)

    key_back(0)
    key_products(0)
    gather_late.middle()
    key_pairs(0)

    resid_parts = by_head(resid_cast.astype(f32))
    for turn in range(turns):
        packed = pack(resid_parts, turn).astype(bf16)
        for index in range(model // HEAD_WIDTH):
            resid_src[index * turns + turn] = tile(packed, index)
    resid = Exchange(at, resid_src, resid_dst, resid_sems.at[0], resid_sems.at[1])
    resid.start()

    back_last = mm(spread_heads(grad_q_cast.astype(f32)), full_q[...], 1, 1)
    last_grad[...] = back_last + pltpu.roll(back_last, pairs, 0)

    def value_back(pair, carry):
        start = pl.multiple_of(pair * seq, seq)
        rows = pl.ds(start, seq)
        grad_v[rows, :] = mm(probs_ref[rows, :], context_blocks[...]).astype(bf16)
        return carry

    lax.fori_loop(0, pairs, value_back, 0)

    seq_row = lax.broadcasted_iota(jnp.int32, (seq, 1), 0)

    def hidden_back(pair, carry):
        rows = pl.ds(pl.multiple_of(pair * seq, seq), seq)
        total = mm(grad_k[rows, :], full_k[...], 1, 1) + mm(grad_v[rows, :], full_v[...], 1, 1)
        hit = seq_row == lengths[0, pair] - 1
        total = total + jnp.where(hit, last_grad[pl.ds(pair, 1), :], 0.0)
        scaled = total * norm_gain[...]
        wide = x[rows, :].astype(f32)
        inv = inv_wide[rows, 0:1]
        mean = lane_mean(scaled * wide)
        result = inv * scaled - wide * (inv * inv * inv * mean)
        result = result + jnp.where(hit, resid_grad[pl.ds(pair, 1), :], 0.0)
        grad_hidden[rows, :] = result.astype(bf16)
        return carry

    def add_line(step):
        line = at.line_peer(step % at.line_count)
        total = paired[at.pb, line].astype(f32)
        arrive(from_pb.at[pl.ds(0, at.pb_count - 1), line], pb_recv.at[line])
        for k in range(1, at.pb_count):
            pb = at.pb_peer(k)
            total = total + from_pb[pb, line].astype(f32)
        if step < at.line_count:
            summed[line] = total.astype(bf16)
            send(
                summed.at[line],
                from_line.at[at.line],
                line_send,
                line_recv,
                at.to_line(line),
            )
        return total

    hidden_back(0, 0)
    hidden_back(1, 0)
    hidden_back(2, 0)
    add_line(1)
    gather_late.relay()

    far_block = list_dst.at[pl.ds(0, at.count - at.neg_count)]
    remote(far_block, far_block, list_sent, list_there, at.to_partner()).wait_recv()
    loss = jnp.zeros((1, 1), f32)
    for pb in range(at.pb_count):
        score, scaled, expo_t, sum_s, sum_t = query_terms(pb * at.neg_count)
        loss = loss + total(expo_t / sum_t * (scaled - jnp.log(sum_t) - (score - jnp.log(sum_s))))
    loss_out[...] = loss

    add_line(2)
    gather_context.tail()
    for pair in range(3, pairs):
        hidden_back(pair, 0)
    gather_late.tail()
    for step in range(3, at.line_count + 1):
        own_sum = add_line(step)

    gather_context.finish()
    gather_late.finish()
    early.wait("wait_recv")
    resid.wait("wait_recv")

    def rows_of(full, start, group):
        wide = full[...].astype(f32).reshape(at.count, -1, slots, HEAD_WIDTH)
        return wide[:, start + group].reshape(at.count * slots, HEAD_WIDTH).astype(bf16)

    pulled_rows = rows_of(early_dst, 0, 0)
    last_rows = rows_of(early_dst, 1, 0)
    resid_rows = rows_of(resid_dst, 0, 0)
    for group in range(groups):
        found = mm(pulled_rows, rows_of(late_full, 0, group), 0, 0)
        lanes = slice(group * HEAD_WIDTH, (group + 1) * HEAD_WIDTH)
        grad_value[:, lanes] = found[group * share : (group + 1) * share]
        found = mm(last_rows, rows_of(late_full, groups, group), 0, 0)
        for part in range(per_group):
            head = per_group * group + part
            grad_query[:, head * HEAD_WIDTH : (head + 1) * HEAD_WIDTH] = found[
                part * share : (part + 1) * share
            ]
        found = mm(resid_rows, rows_of(context_full, 0, group), 0, 0)
        for part in range(per_group):
            head = per_group * group + part
            grad_out[:, head * HEAD_WIDTH : (head + 1) * HEAD_WIDTH] = found[
                part * share : (part + 1) * share
            ]

    final = own_sum
    arrive(from_line.at[pl.ds(0, at.line_count - 1)], line_recv)
    for step in range(1, at.line_count):
        line = at.line_peer(step)
        final = final + from_line[line].astype(f32)
    for cut in range(cuts):
        grad_key[:, cut * cut_width : (cut + 1) * cut_width] = final[cut]

    for gather in gathers:
        gather.drain()
    pieces = from_line.at[pl.ds(0, at.line_count - 1)]
    for block, sem in (
        (from_core, core_send),
        (from_pb.at[pl.ds(0, at.pb_count - 1)], pb_send),
        (pieces, line_send),
    ):
        remote(block, block, sem, any_sem, at.to_partner()).wait_send()
    early.wait("wait_send")
    resid.wait("wait_send")
    sent_block = list_dst.at[pl.ds(0, at.count - 1)]
    remote(sent_block, sent_block, list_sent, list_here, at.to_partner()).wait_send()


def write_kernel(count, *refs):
    sources, targets, sems = refs[:count], refs[count : 2 * count], refs[2 * count]
    copies = [
        pltpu.make_async_copy(sources[i], targets[i], sems.at[i]) for i in range(2, count)
    ]
    for copy in copies:
        copy.start()
    for i in range(2):
        targets[i][...] = sources[i][...]
    for copy in copies:
        copy.wait()


def write_outputs(arrays):
    count = len(arrays)
    return pl.pallas_call(
        functools.partial(write_kernel, count),
        out_shape=tuple(jax.ShapeDtypeStruct(a.shape, a.dtype) for a in arrays),
        in_specs=[VMEM_SPEC] * count,
        out_specs=(VMEM_SPEC,) * 2 + (pl.BlockSpec(memory_space=pl.ANY),) * (count - 2),
        scratch_shapes=[pltpu.SemaphoreType.DMA((count,))],
        compiler_params=pltpu.CompilerParams(vmem_limit_bytes=4 * 2**20),
    )(*arrays)


def run_step(operands, sizes, pb_count, neg_count):
    pairs, seq, groups, share = sizes
    x, own_q, own_k = operands[0], operands[8], operands[9]
    model, width, kv_width = x.shape[1], own_q.shape[1], own_k.shape[1]
    rows = pairs * seq
    count = pb_count * neg_count
    line_count = neg_count // 2
    slots = width // kv_width * pairs
    stacked = groups * slots
    bf16, f32 = jnp.bfloat16, jnp.float32
    block = (pb_count, line_count, 1, share, kv_width)
    dma = pltpu.SemaphoreType.DMA
    vmem = pltpu.VMEM
    smem_spec = pl.BlockSpec(memory_space=pltpu.SMEM)
    hbm_spec = pl.BlockSpec(memory_space=pltpu.HBM)
    return pl.pallas_call(
        functools.partial(step_kernel, sizes),
        out_shape=(
            vmem((1, pairs), f32),
            vmem((1, 1), f32),
            vmem((rows, model), bf16),
            vmem((share, width), f32),
            vmem((share, kv_width), f32),
            vmem((share, kv_width), f32),
            vmem((share, width), f32),
        ),
        in_specs=[hbm_spec, smem_spec, smem_spec] + [hbm_spec] * 9,
        out_specs=(VMEM_SPEC,) * 7,
        scratch_shapes=[
            vmem((rows, model), bf16),
        ]
        + [vmem(a.shape, a.dtype) for a in operands[3:]]
        + [
            vmem((model, width), bf16),
            vmem((model, kv_width), bf16),
            vmem((model, kv_width), bf16),
            vmem((model, width), bf16),
            vmem((rows, model), bf16),
            vmem((model, rows), bf16),
            vmem((rows, HEAD_WIDTH), f32),
            vmem((rows, kv_width), f32),
            vmem((rows, kv_width), f32),
            vmem((rows, kv_width), bf16),
            vmem((rows, kv_width), bf16),
            vmem((rows, kv_width), bf16),
            vmem((rows, kv_width), bf16),
            vmem((rows, stacked), bf16),
            vmem((rows, stacked), bf16),
            vmem((stacked, kv_width), bf16),
            vmem((stacked, kv_width), bf16),
            vmem((slots, model), f32),
            vmem((slots, model), f32),
            vmem((stacked, HEAD_WIDTH), bf16),
            vmem((stacked * count, HEAD_WIDTH), bf16),
            vmem((2 * stacked, HEAD_WIDTH), bf16),
            vmem((2 * stacked * count, HEAD_WIDTH), bf16),
            vmem((count, 2 * slots, HEAD_WIDTH), bf16),
            vmem((count, 2 * slots, HEAD_WIDTH), bf16),
            vmem((count, slots, HEAD_WIDTH), bf16),
            vmem((count, slots, HEAD_WIDTH), bf16),
            vmem((1, HEAD_WIDTH), f32),
            vmem((count, 1, HEAD_WIDTH), f32),
            vmem((1, pb_count, line_count, 2, share, kv_width), bf16),
            vmem((1, pb_count, line_count, share, kv_width), bf16),
            vmem(block, bf16),
            vmem(block, bf16),
            vmem(block[1:], bf16),
            vmem(block[1:], bf16),
            dma((2,)),
            dma((2,)),
            dma((3,)),
            dma,
            dma((1, pb_count)),
            dma,
            dma((line_count,)),
            dma,
            dma,
            dma,
            dma((pairs + 9,)),
        ]
        + gather_sems(neg_count, True) * 6
        + gather_sems(neg_count, False) * 2,
        compiler_params=pltpu.CompilerParams(
            collective_id=0, has_side_effects=True, vmem_limit_bytes=62 * 2**20
        ),
    )(*operands)


def shards(
    hidden,
    lengths,
    teacher,
    norm_gain,
    final_gain,
    score_vector,
    query_weight,
    key_matrix,
    value_matrix,
    out_weight,
):
    both = ("pb", "neg")
    width = query_weight.shape[1]
    kv_width = key_matrix.shape[1]
    share, out_share = query_weight.shape[0], out_weight.shape[1]
    pb_count, neg_count = lax.axis_size("pb"), lax.axis_size("neg")
    pair_count, seq_len, model_width = hidden.shape[1:]
    group_count = kv_width // HEAD_WIDTH
    own_kernels = (
        pb_count == 4
        and neg_count == 8
        and share == out_share
        and share % 32 == 0
        and model_width == share * pb_count * neg_count
        and width == 2 * kv_width
        and pair_count * 2 == 8
        and seq_len == HEAD_WIDTH
        and share * group_count == HEAD_WIDTH
    )
    if own_kernels:
        cos_table, sin_table = signed_tables(seq_len, HEAD_WIDTH)
        results = run_step(
            (
                hidden.reshape(pair_count * seq_len, model_width),
                lengths,
                teacher,
                norm_gain[None],
                final_gain[None],
                score_vector[None],
                cos_table,
                sin_table,
                query_weight,
                key_matrix,
                value_matrix,
                out_weight.T,
            ),
            (pair_count, seq_len, group_count, share),
            pb_count,
            neg_count,
        )
        scores, loss, grad_rows, grad_query, grad_key, grad_value, grad_out = write_outputs(results)
        return (
            scores,
            loss.reshape(()),
            grad_rows.reshape(hidden.shape),
            grad_query,
            grad_key,
            grad_value,
            grad_out.T,
        )
    packed = jnp.concatenate([query_weight, key_matrix, value_matrix, out_weight.T], axis=1)
    everything = lax.all_gather(packed, both, axis=0, tiled=True)
    full_query = everything[:, :width]
    full_key = everything[:, width : width + kv_width]
    full_value = everything[:, width + kv_width : width + 2 * kv_width]
    full_out_t = everything[:, width + 2 * kv_width :]
    weights = (full_query, full_key, full_value, full_out_t.T)
    scores_here, stored = forward_pairs(
        hidden[0], lengths[0], norm_gain, final_gain, score_vector, *weights
    )
    listing = jnp.concatenate([scores_here, teacher[0]])[None]
    listed = lax.all_gather(listing, "neg", axis=0, tiled=True)
    all_scores = listed[:, :pair_count]
    all_scaled = listed[:, pair_count:] / TEACHER_TEMP
    my_total_s = jnp.sum(jnp.exp(all_scores))
    expo_t = jnp.exp(all_scaled)
    my_total_t = jnp.sum(expo_t)
    loss_here = jnp.sum(
        expo_t
        / my_total_t
        * (all_scaled - jnp.log(my_total_t) - (all_scores - jnp.log(my_total_s)))
    )
    prob_s = jnp.exp(scores_here) / my_total_s
    prob_t = jnp.exp(teacher[0] / TEACHER_TEMP) / my_total_t
    grad_score = GRAD_SCALE * (prob_s - prob_t)
    grad_input, last_rows, grad_kv = backward_pairs(
        stored, grad_score, norm_gain, final_gain, score_vector, *weights
    )
    grad_kv = grad_kv.astype(jnp.bfloat16)
    reduced = lax.psum_scatter(grad_kv, both, scatter_dimension=0, tiled=True)
    reduced = reduced.astype(jnp.float32)
    rows = lax.all_gather(last_rows, both, axis=0, tiled=True)
    loss_value = lax.psum(loss_here, "pb")
    index = lax.axis_index("pb") * neg_count + lax.axis_index("neg")
    normed_cols = lax.dynamic_slice_in_dim(rows, index * share, share, axis=1)
    resid_cols = lax.dynamic_slice_in_dim(rows, model_width + index * out_share, out_share, axis=1)
    rest = 2 * model_width
    all_q = rows[:, rest : rest + width]
    all_context = rows[:, rest + width :]
    grad_query = jnp.dot(normed_cols.T, all_q, preferred_element_type=jnp.float32)
    grad_out = jnp.dot(all_context.T, resid_cols, preferred_element_type=jnp.float32)
    return (
        scores_here[None],
        loss_value,
        grad_input[None],
        grad_query,
        reduced[:, :kv_width],
        reduced[:, kv_width:],
        grad_out,
    )


def solution(mesh):
    placed = (
        P("pb", "neg", None, None),
        P("pb", "neg"),
        P("pb", "neg"),
        P(),
        P(),
        P(),
        P(("pb", "neg"), None),
        P(("pb", "neg"), None),
        P(("pb", "neg"), None),
        P(None, ("pb", "neg")),
    )
    return jax.shard_map(
        shards,
        mesh=mesh,
        in_specs=placed,
        out_specs=(
            P("pb", "neg"),
            P(),
            P("pb", "neg", None, None),
            P(("pb", "neg"), None),
            P(("pb", "neg"), None),
            P(("pb", "neg"), None),
            P(None, ("pb", "neg")),
        ),
        check_vma=False,
    )
```
